32 devices in a mesh: seq: 8 (over z, core), fsdp: 4 (over y, x).
Axes of the slice: x: 2, y: 2, z: 4, core: 2. Of those that a mesh axis runs over, the one named last changes fastest.
Arguments:
- inputs: bfloat16 [4, 1024, 2048], P('fsdp', 'seq'), may hold values from -6 to 6
- query_weight: bfloat16 [2048, 2048], P(('seq', 'fsdp')), may hold values from -0.125 to 0.125
- key_weight: bfloat16 [2048, 2048], P(('seq', 'fsdp')), may hold values from -0.125 to 0.125
- value_weight: bfloat16 [2048, 2048], P(('seq', 'fsdp')), may hold values from -0.125 to 0.125
- output_weight: bfloat16 [2048, 2048], P(('seq', 'fsdp')), may hold values from -0.125 to 0.125
- query_gain: bfloat16 [2048], P(('seq', 'fsdp')), may hold values from 0.5 to 7
- key_gain: bfloat16 [2048], P(('seq', 'fsdp')), may hold values from 0.5 to 7
- attention_gain: bfloat16 [2048], P(('seq', 'fsdp')), may hold values from 0.25 to 1.75
- gate_weight: bfloat16 [2048, 8192], P(('seq', 'fsdp')), may hold values from -0.125 to 0.125
- up_weight: bfloat16 [2048, 8192], P(('seq', 'fsdp')), may hold values from -0.125 to 0.125
- down_weight: bfloat16 [2048, 8192], P(('seq', 'fsdp')), may hold values from -0.0625 to 0.0625
- feedforward_gain: bfloat16 [2048], P(('seq', 'fsdp')), may hold values from 0.25 to 1.75
- segments: int32 [4, 1024], P('fsdp'), may hold values from 0 to 2, never falling along the last dimension, each value on 1 to 682 neighbouring positions
- cotangent: bfloat16 [4, 1024, 2048], P('fsdp', 'seq'), may hold values from -6 to 6
Outputs:
- result: bfloat16 [4, 1024, 2048], P('fsdp', 'seq')
- input_grad: float32 [4, 1024, 2048], P('fsdp', 'seq')
- query_weight_grad: float32 [2048, 2048], P(('seq', 'fsdp'))
- key_weight_grad: float32 [2048, 2048], P(('seq', 'fsdp'))
- value_weight_grad: float32 [2048, 2048], P(('seq', 'fsdp'))
- output_weight_grad: float32 [2048, 2048], P(('seq', 'fsdp'))
- query_gain_grad: float32 [2048], P(('seq', 'fsdp'))
- key_gain_grad: float32 [2048], P(('seq', 'fsdp'))
- attention_gain_grad: float32 [2048], P(('seq', 'fsdp'))
- gate_weight_grad: float32 [2048, 8192], P(('seq', 'fsdp'))
- up_weight_grad: float32 [2048, 8192], P(('seq', 'fsdp'))
- down_weight_grad: float32 [2048, 8192], P(('seq', 'fsdp'))
- feedforward_gain_grad: float32 [2048], P(('seq', 'fsdp'))
The draws below stay inside these ranges and needn't reach their ends.
Inputs may be any that keep to these rules, and one draw needn't show every extreme that they name: `segments`: segment numbers never fall along a pack; each document holds at most 682 tokens and one holds exactly that many.
All inputs are finite; a program needn't handle non-finite values.
Results may differ from the reference program's by a relative error of at most 0.025.
The reference program's roundings to bfloat16 on the way count: a program that leaves them out, or rounds other values in their place, can miss the bound.
Values may be sent and summed in bfloat16 or wider, within the bound.
A program may use at most 320 MiB of HBM per device.

```python
import math
import jax
import jax.numpy as jnp
import numpy as np
from jax import lax

D = 2048
HEADS = 16
DH = 128
FF = 8192
SEQLEN = 1024
PACKS = 4
QBLK = 512


def gain_values(key):
    return jax.random.uniform(key, (D,), jnp.float32, 0.5, 1.5)


def draw_query_gain(key, part):
    return gain_values(jax.random.fold_in(key, 101)).astype(jnp.bfloat16)


def draw_key_gain(key, part):
    return gain_values(jax.random.fold_in(key, 202)).astype(jnp.bfloat16)


def steps_of(own_key, shape, shards, smallest, top_value):
    factor_of = 1.0
    for position, parts in shards:
        heights = jax.random.uniform(jax.random.fold_in(jax.random.fold_in(own_key, 6), position), (parts,), jnp.float32, smallest / len(shards), top_value / len(shards))
        factor_of = factor_of * jnp.repeat(jnp.exp(heights), shape[position] // parts).reshape((-1,) + (1,) * (len(shape) - 1 - position))
    return factor_of


def profile(amount, total, bound, skew):
    weights = [(1 << 20) // math.isqrt(grade ** skew) + 1 for grade in range(2, amount + 1)]
    spare, counts = total - bound - (amount - 1), [1] * (amount - 1)
    while spare > 0:
        movable = [i for i in range(amount - 1) if counts[i] < bound]
        whole, budget = sum([weights[i] for i in movable]), spare
        for i in movable:
            extra = min(bound - counts[i], max(1, budget * weights[i] // whole), spare)
            counts[i] = counts[i] + extra
            spare = spare - extra
    return np.array([bound] + counts)


def uneven_parts(own_key, amount, total, reach, skew):
    if amount == 2:
        one = jax.random.randint(own_key, (), max(1, total - reach), min(reach, total - 1) + 1)
        return jnp.stack([one, total - one])
    lengths = jnp.asarray(profile(amount, total, reach, skew), jnp.int32)
    pairs = (amount - 1) // 2
    giver, receiver = lengths[1:1 + 2 * pairs:2], lengths[2:2 + 2 * pairs:2]
    slack = jnp.minimum(giver - 1, reach - receiver)
    passed = jax.random.randint(jax.random.fold_in(own_key, 1), (pairs,), 0, 1 << 20) % (slack + 1)
    lengths = lengths.at[1:1 + 2 * pairs:2].set(giver - passed).at[2:2 + 2 * pairs:2].set(receiver + passed)
    return lengths[jax.random.permutation(jax.random.fold_in(own_key, 2), amount)]


def gaussian(stream_key, shape, spread, bound, split=(), kind=jnp.bfloat16):
    level = steps_of(stream_key, shape, split, -0.22, 0.18) if split else 1.0
    values = jax.random.normal(stream_key, shape, jnp.float32) * spread * level
    return jnp.minimum(jnp.maximum(values, -bound), bound).astype(kind)


def setup_inputs(seed: int = 0) -> dict:
    key_of = jax.random.split(jax.random.key(seed), 15)
    inputs = gaussian(key_of[0], (PACKS, SEQLEN, D), 1.0, 6.0, ((0, 4), (1, 8)))
    query_weight = gaussian(key_of[1], (D, D), D ** -0.5, 0.125, ((0, 32),))
    key_weight = gaussian(key_of[2], (D, D), D ** -0.5, 0.125, ((0, 32),))
    value_weight = gaussian(key_of[3], (D, D), D ** -0.5, 0.125, ((0, 32),))
    output_weight = gaussian(key_of[4], (D, D), D ** -0.5, 0.125, ((0, 32),))
    query_gain = draw_query_gain(jax.random.fold_in(key_of[14], 71), 0)
    key_gain = draw_key_gain(jax.random.fold_in(key_of[14], 71), 0)
    attention_gain = jnp.clip(1.0 + 0.15 * jax.random.normal(key_of[7], (D,), jnp.float32), 0.25, 1.75).astype(jnp.bfloat16)
    gate_weight = gaussian(key_of[8], (D, FF), D ** -0.5, 0.125, ((0, 32),))
    up_weight = gaussian(key_of[9], (D, FF), D ** -0.5, 0.125, ((0, 32),))
    down_weight = gaussian(key_of[10], (D, FF), FF ** -0.5, 0.0625, ((0, 32),))
    feedforward_gain = jnp.clip(1.0 + 0.15 * jax.random.normal(key_of[11], (D,), jnp.float32), 0.25, 1.75).astype(jnp.bfloat16)
    segments = jax.vmap(lambda own: jnp.searchsorted(jnp.cumsum(uneven_parts(own, 3, SEQLEN, SEQLEN * 2 // 3, 1)), jnp.arange(SEQLEN), side="right"))(jax.random.split(key_of[12], PACKS)).reshape((PACKS, SEQLEN)).astype(jnp.int32)
    cotangent = gaussian(key_of[13], (PACKS, SEQLEN, D), 1.0, 6.0, ((0, 4), (1, 8)))
    return {"inputs": inputs, "query_weight": query_weight, "key_weight": key_weight, "value_weight": value_weight, "output_weight": output_weight, "query_gain": query_gain, "key_gain": key_gain, "attention_gain": attention_gain, "gate_weight": gate_weight, "up_weight": up_weight, "down_weight": down_weight, "feedforward_gain": feedforward_gain, "segments": segments, "cotangent": cotangent}


@jax.custom_vjp
def low(v):
    return lax.optimization_barrier(v.astype(jnp.bfloat16)).astype(jnp.float32)

@jax.custom_vjp
def low_back(v):
    return v

def low_keep(v):
    return (low(v), None)

def low_pass(kept, grad):
    return (grad,)

def back_keep(v):
    return (v, None)

def back_low(kept, grad):
    return (low(grad),)
low.defvjp(low_keep, low_pass)
low_back.defvjp(back_keep, back_low)
eps_norm = 1e-06
rope_base = 500000.0
neg_fill = -1e+30

def round_both(tensor):
    return low_back(low(tensor))

def matmul(left, right):
    return jnp.dot(left, right, precision=lax.Precision.HIGHEST)

def rms_scale(tensor, gain):
    return tensor * lax.rsqrt(lax.optimization_barrier(jnp.mean(tensor * tensor, axis=-1, keepdims=True)) + eps_norm) * gain

def rotary(tensor, positions):
    row_count = tensor.shape[0]
    grouped = tensor.reshape(row_count, HEADS, DH)
    half_width = DH // 2
    frequency = rope_base ** (-jnp.arange(half_width, dtype=jnp.float32) * 2.0 / DH)
    angles = positions.astype(jnp.float32)[:, None] * frequency[None, :]
    cosine = jnp.cos(angles)[:, None, :]
    sine_table = jnp.sin(angles)[:, None, :]
    first_half = grouped[..., :half_width]
    second_half = grouped[..., half_width:]
    turned = jnp.concatenate([first_half * cosine - second_half * sine_table, second_half * cosine + first_half * sine_table], axis=-1)
    return turned.reshape(tensor.shape)

def attention(queries, keys, values, segment_row):
    score_scale = DH ** (-0.5)
    query_heads = queries.reshape(SEQLEN, HEADS, DH)
    key_heads = keys.reshape(SEQLEN, HEADS, DH)
    value_heads = values.reshape(SEQLEN, HEADS, DH)
    key_pos = jnp.arange(SEQLEN, dtype=jnp.int32)

    def attend_block(block_index):
        first_row = (block_index * QBLK).astype(jnp.int32)
        query_block = lax.dynamic_slice_in_dim(query_heads, first_row, QBLK, 0)
        query_seg = lax.dynamic_slice_in_dim(segment_row, first_row, QBLK, 0)
        query_pos = first_row + jnp.arange(QBLK, dtype=jnp.int32)
        scores = jnp.einsum('qhd,khd->hqk', query_block, key_heads, precision=lax.Precision.HIGHEST) * score_scale
        scores = low_back(scores)
        allowed = (key_pos[None, :] <= query_pos[:, None]) & (segment_row[None, :] == query_seg[:, None])
        scores = jnp.where(allowed[None], scores, neg_fill)
        probabilities = jax.nn.softmax(scores, axis=-1)
        return jnp.einsum('hqk,khd->qhd', low(probabilities), value_heads, precision=lax.Precision.HIGHEST)
    blocks = lax.map(jax.checkpoint(attend_block), jnp.arange(SEQLEN // QBLK, dtype=jnp.int32))
    return blocks.reshape(SEQLEN, D)

def block_forward(inputs, query_weight, key_weight, value_weight, output_weight, query_gain, key_gain, attention_gain, gate_weight, up_weight, down_weight, feedforward_gain, segment_row):
    positions = jnp.arange(SEQLEN, dtype=jnp.int32)
    query_pre = low_back(matmul(inputs, query_weight))
    key_pre = low_back(matmul(inputs, key_weight))
    values = round_both(matmul(inputs, value_weight))
    queries = round_both(rotary(rms_scale(query_pre, query_gain), positions))
    keys = round_both(rotary(rms_scale(key_pre, key_gain), positions))
    attended = round_both(attention(queries, keys, values, segment_row))
    projected = low_back(matmul(attended, output_weight))
    hidden = inputs + rms_scale(projected, attention_gain)
    hidden_low = low(hidden)
    gate_linear = low_back(matmul(hidden_low, gate_weight))
    up_linear = low_back(matmul(hidden_low, up_weight))
    activated = low(jax.nn.silu(gate_linear) * up_linear)
    mixed_pre = low_back(matmul(activated, down_weight.T))
    return hidden + rms_scale(mixed_pre, feedforward_gain)

def reference(inputs, query_weight, key_weight, value_weight, output_weight, query_gain, key_gain, attention_gain, gate_weight, up_weight, down_weight, feedforward_gain, segments, cotangent):
    weight_set = tuple((item.astype(jnp.float32) for item in (query_weight, key_weight, value_weight, output_weight, query_gain, key_gain, attention_gain, gate_weight, up_weight, down_weight, feedforward_gain)))

    def one_pack(totals, pack_data):
        pack_in, segment_row, pack_grad = pack_data

        def forward_pass(tensor, *weight_args):
            return block_forward(tensor, *weight_args, segment_row)
        pack_out, pullback = jax.vjp(forward_pass, pack_in.astype(jnp.float32), *weight_set)
        gradients = pullback(pack_grad.astype(jnp.float32))
        totals = tuple((total + grad_item for total, grad_item in zip(totals, gradients[1:])))
        return (totals, (pack_out.astype(jnp.bfloat16), gradients[0]))
    zero_totals = tuple((jnp.zeros_like(item) for item in weight_set))
    totals, (outputs, input_grad) = lax.scan(one_pack, zero_totals, (inputs, segments, cotangent))
    return (outputs, input_grad, totals[0], totals[1], totals[2], totals[3], totals[4], totals[5], totals[6], totals[7], totals[8], totals[9], totals[10])
```

```python
import jax
import jax.numpy as jnp
from jax import lax
from jax.sharding import PartitionSpec as P

HEADS = 16
DH = 128


eps_norm = 1e-06
rope_base = 500000.0
neg_fill = -1e30


def rms_scale(tensor, gain):
    return tensor * lax.rsqrt(jnp.mean(tensor * tensor, axis=-1, keepdims=True) + eps_norm) * gain


def rotary(tensor, positions):
    row_count = tensor.shape[0]
    grouped = tensor.reshape(row_count, HEADS, DH)
    half_width = DH // 2
    frequency = rope_base ** (-jnp.arange(half_width, dtype=jnp.float32) * 2.0 / DH)
    angles = positions.astype(jnp.float32)[:, None] * frequency[None, :]
    cosine = jnp.cos(angles)[:, None, :]
    sine_table = jnp.sin(angles)[:, None, :]
    first_half = grouped[..., :half_width]
    second_half = grouped[..., half_width:]
    turned = jnp.concatenate(
        [
            first_half * cosine - second_half * sine_table,
            second_half * cosine + first_half * sine_table,
        ],
        axis=-1,
    )
    return turned.reshape(tensor.shape)


def norm_rotary(tensor, gain, positions):
    return rotary(rms_scale(tensor, gain), positions)


def swiglu_act(gate_linear, up_linear):
    return jax.nn.silu(gate_linear) * up_linear


def contract_rows(left, right):
    return lax.dot_general(
        left, right, (((0,), (0,)), ((), ())), preferred_element_type=jnp.float32
    )


def contract_cols(left, right):
    return lax.dot_general(
        left, right, (((1,), (1,)), ((), ())), preferred_element_type=jnp.float32
    )


def swap_blocks(tensor, outer, inner):
    block_rows = tensor.shape[0] // (outer * inner)
    return (
        tensor.reshape(outer, inner, block_rows, tensor.shape[1])
        .transpose(1, 0, 2, 3)
        .reshape(tensor.shape)
    )


def masked_scores(query_block, key_heads, first_row, segment_row, score_scale):
    block_rows = query_block.shape[0]
    sequence_rows = key_heads.shape[0]
    scores = (
        jnp.einsum("qhd,khd->hqk", query_block, key_heads, preferred_element_type=jnp.float32)
        * score_scale
    )
    query_pos = first_row + jnp.arange(block_rows, dtype=jnp.int32)
    key_pos = jnp.arange(sequence_rows, dtype=jnp.int32)
    query_seg = lax.dynamic_slice_in_dim(segment_row, first_row, block_rows, 0)
    allowed = (key_pos[None, :] <= query_pos[:, None]) & (
        segment_row[None, :] == query_seg[:, None]
    )
    return jnp.where(allowed[None], scores, neg_fill)


def gather_seq(tensor):
    return lax.all_gather(tensor, "seq", axis=0, tiled=True)


def scatter_seq(tensor):
    return lax.psum_scatter(tensor, "seq", scatter_dimension=0, tiled=True)


def columns_in(weight):
    seq_count = lax.axis_size("seq")
    fsdp_count = lax.axis_size("fsdp")
    part = lax.all_to_all(weight, "seq", split_axis=1, concat_axis=0, tiled=True)
    whole = lax.all_gather(part, "fsdp", axis=0, tiled=True)
    return swap_blocks(whole, fsdp_count, seq_count)


def columns_out(term):
    seq_count = lax.axis_size("seq")
    fsdp_count = lax.axis_size("fsdp")
    swapped = swap_blocks(term, seq_count, fsdp_count).astype(jnp.bfloat16)
    summed = lax.psum_scatter(swapped, "fsdp", scatter_dimension=0, tiled=True)
    return lax.all_to_all(summed, "seq", split_axis=0, concat_axis=1, tiled=True).astype(
        jnp.float32
    )


def rope_tables(row_count):
    half_width = DH // 2
    frequency = rope_base ** (-jnp.arange(half_width, dtype=jnp.float32) * 2.0 / DH)
    angles = jnp.arange(row_count, dtype=jnp.int32).astype(jnp.float32)[:, None] * frequency[None, :]
    return jnp.cos(angles), jnp.sin(angles)


def rotate(tensor, cosine, sine_table):
    row_count = tensor.shape[0]
    half_width = DH // 2
    grouped = tensor.reshape(row_count, -1, DH)
    first_half = grouped[..., :half_width]
    second_half = grouped[..., half_width:]
    cosine = cosine[:, None, :]
    sine_table = sine_table[:, None, :]
    turned = jnp.concatenate(
        [
            first_half * cosine - second_half * sine_table,
            second_half * cosine + first_half * sine_table,
        ],
        axis=-1,
    )
    return turned.reshape(tensor.shape)


def per_device(
    inputs,
    query_weight,
    key_weight,
    value_weight,
    output_weight,
    query_gain,
    key_gain,
    attention_gain,
    gate_weight,
    up_weight,
    down_weight,
    feedforward_gain,
    segments,
    cotangent,
):
    token_count = inputs.shape[1]
    width_all = inputs.shape[2]
    local_in = inputs.reshape(token_count, width_all)
    segment_row = segments[0]
    score_scale = DH ** (-0.5)
    seq_index = lax.axis_index("seq")
    inputs_all = gather_seq(local_in)
    sequence_rows = inputs_all.shape[0]
    query_cols = columns_in(query_weight)
    key_cols = columns_in(key_weight)
    value_cols = columns_in(value_weight)
    head_width = query_cols.shape[1]
    local_heads = head_width // DH
    output_rows = lax.all_gather(output_weight, "fsdp", axis=0, tiled=True)
    gains = lax.all_gather(
        jnp.stack([query_gain, key_gain, attention_gain, feedforward_gain]),
        ("seq", "fsdp"),
        axis=1,
        tiled=True,
    ).astype(jnp.float32)
    query_scale = lax.dynamic_slice_in_dim(gains[0], seq_index * head_width, head_width, 0)
    key_scale = lax.dynamic_slice_in_dim(gains[1], seq_index * head_width, head_width, 0)
    attention_scale = gains[2]
    feedforward_scale = gains[3]
    query_pre = jnp.dot(inputs_all, query_cols, preferred_element_type=jnp.float32)
    key_pre = jnp.dot(inputs_all, key_cols, preferred_element_type=jnp.float32)
    values_low = jnp.dot(inputs_all, value_cols, preferred_element_type=jnp.float32).astype(
        jnp.bfloat16
    )
    squares = lax.psum(
        jnp.stack([jnp.sum(query_pre * query_pre, axis=-1), jnp.sum(key_pre * key_pre, axis=-1)]),
        "seq",
    )
    inverse = lax.rsqrt(squares / width_all + eps_norm)
    query_unit = query_pre * inverse[0][:, None]
    key_unit = key_pre * inverse[1][:, None]
    cosine, sine_table = rope_tables(sequence_rows)
    queries_low = rotate(query_unit * query_scale, cosine, sine_table).astype(jnp.bfloat16)
    keys_low = rotate(key_unit * key_scale, cosine, sine_table).astype(jnp.bfloat16)
    query_heads = queries_low.reshape(sequence_rows, local_heads, DH)
    key_heads = keys_low.reshape(sequence_rows, local_heads, DH)
    value_heads = values_low.reshape(sequence_rows, local_heads, DH)
    block_rows = min(512, sequence_rows)
    block_count = sequence_rows // block_rows
    block_ids = jnp.arange(block_count, dtype=jnp.int32)

    def attend_block(loop_state, block_index):
        first_row = block_index * block_rows
        query_block = lax.dynamic_slice_in_dim(query_heads, first_row, block_rows, 0)
        scores = masked_scores(query_block, key_heads, first_row, segment_row, score_scale)
        row_max = jnp.max(scores, axis=-1, keepdims=True)
        expanded = jnp.exp(scores - row_max)
        row_total = jnp.sum(expanded, axis=-1, keepdims=True)
        softmax_low = (expanded / row_total).astype(jnp.bfloat16)
        block_out = jnp.einsum(
            "hqk,khd->qhd", softmax_low, value_heads, preferred_element_type=jnp.float32
        )
        log_total = (row_max + jnp.log(row_total))[..., 0]
        return (loop_state, (block_out.astype(jnp.bfloat16), log_total))

    _, (out_blocks, log_totals) = lax.scan(attend_block, jnp.zeros((), jnp.int32), block_ids)
    attended_heads = out_blocks.reshape(sequence_rows, head_width)
    projected = scatter_seq(
        jnp.dot(attended_heads, output_rows, preferred_element_type=jnp.float32).astype(
            jnp.bfloat16
        )
    ).astype(jnp.float32)
    hidden = local_in.astype(jnp.float32) + rms_scale(projected, attention_scale)
    hidden_low = hidden.astype(jnp.bfloat16)
    gate_cols = columns_in(gate_weight)
    up_cols = columns_in(up_weight)
    down_cols = columns_in(down_weight)
    hidden_all = gather_seq(hidden_low)
    gate_linear = jnp.dot(hidden_all, gate_cols, preferred_element_type=jnp.float32)
    up_linear = jnp.dot(hidden_all, up_cols, preferred_element_type=jnp.float32)
    activated = swiglu_act(gate_linear, up_linear).astype(jnp.bfloat16)
    mixed_pre = scatter_seq(contract_cols(activated, down_cols).astype(jnp.bfloat16)).astype(
        jnp.float32
    )
    result = (
        (hidden + rms_scale(mixed_pre, feedforward_scale))
        .astype(jnp.bfloat16)
        .reshape(1, token_count, width_all)
    )
    grad_result = cotangent.reshape(token_count, width_all).astype(jnp.float32)
    _, mixed_pull = jax.vjp(rms_scale, mixed_pre, feedforward_scale)
    grad_mixed, grad_feedforward_gain = mixed_pull(grad_result)
    grad_mixed_low = grad_mixed.astype(jnp.bfloat16)
    grad_all = gather_seq(grad_mixed_low)
    grad_activated = jnp.dot(grad_all, down_cols, preferred_element_type=jnp.float32)
    _, swiglu_pull = jax.vjp(swiglu_act, gate_linear, up_linear)
    grad_gate, grad_upward = swiglu_pull(grad_activated)
    grad_gate_low = grad_gate.astype(jnp.bfloat16)
    grad_upward_low = grad_upward.astype(jnp.bfloat16)
    grad_hidden = grad_result + scatter_seq(
        (contract_cols(grad_gate_low, gate_cols) + contract_cols(grad_upward_low, up_cols)).astype(
            jnp.bfloat16
        )
    ).astype(jnp.float32)
    gate_weight_grad = columns_out(contract_rows(hidden_all, grad_gate_low))
    up_weight_grad = columns_out(contract_rows(hidden_all, grad_upward_low))
    down_weight_grad = columns_out(contract_rows(grad_all, activated))
    _, branch_pull = jax.vjp(rms_scale, projected, attention_scale)
    grad_projected, grad_attention_gain = branch_pull(grad_hidden)
    grad_projected_all = gather_seq(grad_projected.astype(jnp.bfloat16))
    output_weight_grad = lax.psum_scatter(
        contract_rows(attended_heads, grad_projected_all).astype(jnp.bfloat16),
        "fsdp",
        scatter_dimension=0,
        tiled=True,
    ).astype(jnp.float32)
    grad_attended = contract_cols(grad_projected_all, output_rows).astype(jnp.bfloat16)
    grad_out_heads = grad_attended.reshape(sequence_rows, local_heads, DH)

    def attend_back(loop_state, block_index):
        key_total, value_total = loop_state
        first_row = block_index * block_rows
        query_block = lax.dynamic_slice_in_dim(query_heads, first_row, block_rows, 0)
        grad_block = lax.dynamic_slice_in_dim(grad_out_heads, first_row, block_rows, 0)
        log_block = lax.dynamic_index_in_dim(log_totals, block_index, 0, keepdims=False)
        scores = masked_scores(query_block, key_heads, first_row, segment_row, score_scale)
        probabilities = jnp.exp(scores - log_block[..., None])
        softmax_low = probabilities.astype(jnp.bfloat16)
        value_total = value_total + jnp.einsum(
            "hqk,qhd->khd", softmax_low, grad_block, preferred_element_type=jnp.float32
        )
        grad_softmax = jnp.einsum(
            "qhd,khd->hqk", grad_block, value_heads, preferred_element_type=jnp.float32
        )
        row_dot = jnp.sum(probabilities * grad_softmax, axis=-1, keepdims=True)
        grad_scores = (probabilities * (grad_softmax - row_dot)).astype(jnp.bfloat16)
        grad_query_block = (
            jnp.einsum("hqk,khd->qhd", grad_scores, key_heads, preferred_element_type=jnp.float32)
            * score_scale
        )
        key_total = (
            key_total
            + jnp.einsum(
                "hqk,qhd->khd", grad_scores, query_block, preferred_element_type=jnp.float32
            )
            * score_scale
        )
        return ((key_total, value_total), grad_query_block.astype(jnp.bfloat16))

    zero_heads = jnp.zeros((sequence_rows, local_heads, DH), jnp.float32)
    (key_total, value_total), grad_query_blocks = lax.scan(
        attend_back, (zero_heads, zero_heads), block_ids
    )
    grad_queries = grad_query_blocks.reshape(sequence_rows, head_width).astype(jnp.float32)
    grad_keys = (
        key_total.astype(jnp.bfloat16).reshape(sequence_rows, head_width).astype(jnp.float32)
    )
    grad_values = value_total.astype(jnp.bfloat16).reshape(sequence_rows, head_width)
    query_error = rotate(grad_queries, cosine, -sine_table)
    key_error = rotate(grad_keys, cosine, -sine_table)
    grad_query_gain = jnp.sum(query_error * query_unit, axis=0)
    grad_key_gain = jnp.sum(key_error * key_unit, axis=0)
    query_error = query_error * query_scale
    key_error = key_error * key_scale
    means = (
        lax.psum(
            jnp.stack(
                [
                    jnp.sum(query_error * query_unit, axis=-1),
                    jnp.sum(key_error * key_unit, axis=-1),
                ]
            ),
            "seq",
        )
        / width_all
    )
    grad_query_low = (
        inverse[0][:, None] * (query_error - query_unit * means[0][:, None])
    ).astype(jnp.bfloat16)
    grad_key_low = (inverse[1][:, None] * (key_error - key_unit * means[1][:, None])).astype(
        jnp.bfloat16
    )
    grad_input = grad_hidden + scatter_seq(
        (
            contract_cols(grad_query_low, query_cols)
            + contract_cols(grad_key_low, key_cols)
            + contract_cols(grad_values, value_cols)
        ).astype(jnp.bfloat16)
    ).astype(jnp.float32)
    query_weight_grad = columns_out(contract_rows(inputs_all, grad_query_low))
    key_weight_grad = columns_out(contract_rows(inputs_all, grad_key_low))
    value_weight_grad = columns_out(contract_rows(inputs_all, grad_values))
    head_gains = lax.psum_scatter(
        jnp.stack([grad_query_gain, grad_key_gain]), "fsdp", scatter_dimension=1, tiled=True
    )
    token_gains = lax.psum_scatter(
        jnp.stack([grad_attention_gain, grad_feedforward_gain]),
        ("seq", "fsdp"),
        scatter_dimension=1,
        tiled=True,
    )
    return (
        result,
        grad_input.reshape(1, token_count, width_all),
        query_weight_grad,
        key_weight_grad,
        value_weight_grad,
        output_weight_grad,
        head_gains[0],
        head_gains[1],
        token_gains[0],
        gate_weight_grad,
        up_weight_grad,
        down_weight_grad,
        token_gains[1],
    )


def solution(mesh):
    in_specs = (
        P("fsdp", "seq", None),
        P(("seq", "fsdp"), None),
        P(("seq", "fsdp"), None),
        P(("seq", "fsdp"), None),
        P(("seq", "fsdp"), None),
        P(("seq", "fsdp")),
        P(("seq", "fsdp")),
        P(("seq", "fsdp")),
        P(("seq", "fsdp"), None),
        P(("seq", "fsdp"), None),
        P(("seq", "fsdp"), None),
        P(("seq", "fsdp")),
        P("fsdp", None),
        P("fsdp", "seq", None),
    )
    out_specs = (
        P("fsdp", "seq", None),
        P("fsdp", "seq", None),
        P(("seq", "fsdp"), None),
        P(("seq", "fsdp"), None),
        P(("seq", "fsdp"), None),
        P(("seq", "fsdp"), None),
        P(("seq", "fsdp")),
        P(("seq", "fsdp")),
        P(("seq", "fsdp")),
        P(("seq", "fsdp"), None),
        P(("seq", "fsdp"), None),
        P(("seq", "fsdp"), None),
        P(("seq", "fsdp")),
    )
    return jax.shard_map(
        per_device, mesh=mesh, in_specs=in_specs, out_specs=out_specs, check_vma=False
    )
```

```python
import functools

import jax
import jax.numpy as jnp
from jax import lax
from jax.experimental import pallas as pl
from jax.experimental.pallas import tpu as pltpu
from jax.sharding import PartitionSpec as P

HEADS = 16
DH = 128


eps_norm = 1e-06
rope_base = 500000.0
neg_fill = -1e30


def rms_scale(tensor, gain):
    return tensor * lax.rsqrt(jnp.mean(tensor * tensor, axis=-1, keepdims=True) + eps_norm) * gain


def rotary(tensor, positions):
    row_count = tensor.shape[0]
    grouped = tensor.reshape(row_count, HEADS, DH)
    half_width = DH // 2
    frequency = rope_base ** (-jnp.arange(half_width, dtype=jnp.float32) * 2.0 / DH)
    angles = positions.astype(jnp.float32)[:, None] * frequency[None, :]
    cosine = jnp.cos(angles)[:, None, :]
    sine_table = jnp.sin(angles)[:, None, :]
    first_half = grouped[..., :half_width]
    second_half = grouped[..., half_width:]
    turned = jnp.concatenate(
        [
            first_half * cosine - second_half * sine_table,
            second_half * cosine + first_half * sine_table,
        ],
        axis=-1,
    )
    return turned.reshape(tensor.shape)


def norm_rotary(tensor, gain, positions):
    return rotary(rms_scale(tensor, gain), positions)


def swiglu_act(gate_linear, up_linear):
    return jax.nn.silu(gate_linear) * up_linear


def contract_rows(left, right):
    return lax.dot_general(
        left, right, (((0,), (0,)), ((), ())), preferred_element_type=jnp.float32
    )


def contract_cols(left, right):
    return lax.dot_general(
        left, right, (((1,), (1,)), ((), ())), preferred_element_type=jnp.float32
    )


def swap_blocks(tensor, outer, inner):
    block_rows = tensor.shape[0] // (outer * inner)
    return (
        tensor.reshape(outer, inner, block_rows, tensor.shape[1])
        .transpose(1, 0, 2, 3)
        .reshape(tensor.shape)
    )


def masked_scores(query_block, key_heads, first_row, segment_row, score_scale):
    block_rows = query_block.shape[0]
    sequence_rows = key_heads.shape[0]
    scores = (
        jnp.einsum("qhd,khd->hqk", query_block, key_heads, preferred_element_type=jnp.float32)
        * score_scale
    )
    query_pos = first_row + jnp.arange(block_rows, dtype=jnp.int32)
    key_pos = jnp.arange(sequence_rows, dtype=jnp.int32)
    query_seg = lax.dynamic_slice_in_dim(segment_row, first_row, block_rows, 0)
    allowed = (key_pos[None, :] <= query_pos[:, None]) & (
        segment_row[None, :] == query_seg[:, None]
    )
    return jnp.where(allowed[None], scores, neg_fill)

MESH = pl.DeviceIdType.MESH
RS_PARTS = 4


class Line:
    def __init__(self, chips):
        index = lax.axis_index("seq")
        self.chips = chips
        self.fsdp = lax.axis_index("fsdp")
        self.place = index // 2
        self.core = index % 2

    def device(self, place, core):
        return (place * 2 + core, self.fsdp)

    @property
    def partner(self):
        return self.device(self.place, 1 - self.core)

    @property
    def above(self):
        return self.device(jnp.minimum(self.place + 1, self.chips - 1), self.core)

    @property
    def below(self):
        return self.device(jnp.maximum(self.place - 1, 0), self.core)

    @property
    def has_above(self):
        return self.place < self.chips - 1

    @property
    def has_below(self):
        return self.place > 0

    def greet(self):
        barrier = pltpu.get_barrier_semaphore()
        pl.semaphore_signal(barrier, inc=1, device_id=self.partner, device_id_type=MESH)

        @pl.when(self.has_above)
        def _():
            pl.semaphore_signal(barrier, inc=1, device_id=self.above, device_id_type=MESH)

        @pl.when(self.has_below)
        def _():
            pl.semaphore_signal(barrier, inc=1, device_id=self.below, device_id_type=MESH)

        peers = (
            1 + jnp.minimum(self.place, 1) + jnp.minimum(self.chips - 1 - self.place, 1)
        )
        pl.semaphore_wait(barrier, peers)

    def order(self, step):
        place, last = self.place, self.chips - 1
        near = jnp.minimum(place, last - place)
        both = jnp.where(step % 2 == 1, place - (step + 1) // 2, place + step // 2)
        rest = jnp.where(place <= last - place, step, last - step)
        return jnp.where(step <= 2 * near, both, rest)

    def paired(self, step):
        near = jnp.minimum(self.place, self.chips - 1 - self.place)
        return (step % 2 == 1) & (step <= 2 * near)

    def second_of_pair(self, step):
        near = jnp.minimum(self.place, self.chips - 1 - self.place)
        return (step % 2 == 0) & (step > 0) & (step <= 2 * near)


class Gather:
    def __init__(self, line, blocks, arrive, up_sem, down_sem, side_sem):
        self.line, self.blocks, self.arrive = line, blocks, arrive
        self.up_sem, self.down_sem, self.side_sem = up_sem, down_sem, side_sem

    @staticmethod
    def scratch(chips, rows, width):
        return [
            pltpu.VMEM((2 * chips, rows, width), jnp.bfloat16),
            pltpu.SemaphoreType.DMA((2 * chips,)),
            pltpu.SemaphoreType.DMA((chips,)),
            pltpu.SemaphoreType.DMA((chips,)),
            pltpu.SemaphoreType.DMA((chips,)),
        ]

    def copy(self, chip, sem, target):
        slot = chip * 2 + self.line.core
        return pltpu.make_async_remote_copy(
            src_ref=self.blocks.at[slot],
            dst_ref=self.blocks.at[slot],
            send_sem=sem.at[chip],
            recv_sem=self.arrive.at[slot],
            device_id=target,
            device_id_type=MESH,
        )

    def wait_slot(self, slot):
        pltpu.make_async_remote_copy(
            src_ref=self.blocks.at[slot],
            dst_ref=self.blocks.at[slot],
            send_sem=self.side_sem.at[0],
            recv_sem=self.arrive.at[slot],
            device_id=self.line.partner,
            device_id_type=MESH,
        ).wait_recv()

    def send(self, chip):
        line = self.line

        @pl.when((chip <= line.place) & line.has_above)
        def _():
            self.copy(chip, self.up_sem, line.above).start()

        @pl.when((chip >= line.place) & line.has_below)
        def _():
            self.copy(chip, self.down_sem, line.below).start()

        self.copy(chip, self.side_sem, line.partner).start()

    def take(self, chip):
        self.wait_slot(chip * 2 + self.line.core)
        self.send(chip)

    def step(self, step):
        line = self.line
        chip = line.order(step)

        @pl.when((step > 0) & jnp.logical_not(line.second_of_pair(step)))
        def _():
            self.take(chip)

        @pl.when(line.paired(step))
        def _():
            self.take(line.order(step + 1))

        self.wait_slot(chip * 2 + 1 - line.core)
        return chip

    def finish(self):
        line = self.line

        @pl.loop(0, line.chips)
        def _(chip):
            @pl.when((chip <= line.place) & line.has_above)
            def _():
                self.copy(chip, self.up_sem, line.above).wait_send()

            @pl.when((chip >= line.place) & line.has_below)
            def _():
                self.copy(chip, self.down_sem, line.below).wait_send()

            self.copy(chip, self.side_sem, line.partner).wait_send()


class Scatter:
    def __init__(self, line, fresh, terms, side_out, side_in, out, inward, side_send, side_recv, send_sem, recv_sem):
        self.line, self.fresh, self.terms = line, fresh, terms
        self.side_out, self.side_in = side_out, side_in
        self.out, self.inward = out, inward
        self.side_send, self.side_recv = side_send, side_recv
        self.send_sem, self.recv_sem = send_sem, recv_sem
        self.rows = terms.shape[1] // RS_PARTS

    @staticmethod
    def scratch(chips, rows, width):
        return [
            pltpu.VMEM((2, rows, width), jnp.float32),
            pltpu.VMEM((chips, rows, width), jnp.float32),
            pltpu.VMEM((chips, rows, width), jnp.bfloat16),
            pltpu.VMEM((chips, rows, width), jnp.bfloat16),
            pltpu.VMEM((chips, rows, width), jnp.bfloat16),
            pltpu.VMEM((2, chips, rows, width), jnp.bfloat16),
            pltpu.SemaphoreType.DMA((chips,)),
            pltpu.SemaphoreType.DMA((chips,)),
            pltpu.SemaphoreType.DMA((chips, RS_PARTS)),
            pltpu.SemaphoreType.DMA((2, chips, RS_PARTS)),
        ]

    def side(self, chip):
        return pltpu.make_async_remote_copy(
            src_ref=self.side_out.at[chip],
            dst_ref=self.side_in.at[chip],
            send_sem=self.side_send.at[chip],
            recv_sem=self.side_recv.at[chip],
            device_id=self.line.partner,
            device_id_type=MESH,
        )

    def part(self, chip, part, upward, target):
        rows = pl.ds(part * self.rows, self.rows)
        return pltpu.make_async_remote_copy(
            src_ref=self.out.at[chip, rows],
            dst_ref=self.inward.at[upward, chip, rows],
            send_sem=self.send_sem.at[chip, part],
            recv_sem=self.recv_sem.at[upward, chip, part],
            device_id=target,
            device_id_type=MESH,
        )

    def share(self, chip):
        self.side_out[chip] = self.fresh[1 - self.line.core].astype(jnp.bfloat16)
        self.side(chip).start()
        self.terms[chip] = self.fresh[self.line.core]

    def total(self, chip, part, ways):
        rows = pl.ds(part * self.rows, self.rows)
        total = self.terms[chip, rows] + self.side_in[chip, rows].astype(jnp.float32)
        for way in ways:
            total = total + self.inward[way, chip, rows].astype(jnp.float32)
        return rows, total

    def pass_on(self, chip, upward, first):
        target = self.line.above if upward else self.line.below
        self.side(chip).wait_recv()

        @pl.loop(0, RS_PARTS)
        def _(part):
            if not first:
                self.part(chip, part, upward, target).wait_recv()
            rows, total = self.total(chip, part, () if first else (upward,))
            self.out[chip, rows] = total.astype(jnp.bfloat16)
            self.part(chip, part, upward, target).start()

    def after_term(self, chip):
        line = self.line
        self.share(chip)

        @pl.when((chip < line.place) & jnp.logical_not(line.has_above))
        def _():
            self.pass_on(chip, 0, True)

        @pl.when((chip > line.place) & jnp.logical_not(line.has_below))
        def _():
            self.pass_on(chip, 1, True)

    def finish(self, result):
        line = self.line
        lower = line.place * 2 < line.chips

        @pl.loop(0, line.chips)
        def _(step):
            up_chip, down_chip = step, line.chips - 1 - step
            go_up = (up_chip > line.place) & line.has_below
            go_down = (down_chip < line.place) & line.has_above

            @pl.when(go_up & lower)
            def _():
                self.pass_on(up_chip, 1, False)

            @pl.when(go_down)
            def _():
                self.pass_on(down_chip, 0, False)

            @pl.when(go_up & jnp.logical_not(lower))
            def _():
                self.pass_on(up_chip, 1, False)

        place = line.place
        self.side(place).wait_recv()

        @pl.loop(0, RS_PARTS)
        def _(part):
            @pl.when(line.has_above)
            def _():
                self.part(place, part, 0, line.below).wait_recv()

            @pl.when(line.has_below)
            def _():
                self.part(place, part, 1, line.above).wait_recv()

            @pl.when(line.has_above & line.has_below)
            def _():
                rows, total = self.total(place, part, (0, 1))
                result[rows] = total

            @pl.when(line.has_above & jnp.logical_not(line.has_below))
            def _():
                rows, total = self.total(place, part, (0,))
                result[rows] = total

            @pl.when(line.has_below & jnp.logical_not(line.has_above))
            def _():
                rows, total = self.total(place, part, (1,))
                result[rows] = total

        @pl.loop(0, line.chips)
        def _(chip):
            self.side(chip).wait_send()

            @pl.when(chip != place)
            def _():
                @pl.loop(0, RS_PARTS)
                def _(part):
                    self.part(chip, part, 0, line.below).wait_send()


def tile_of(extent):
    return min(256, extent)


def dot_cols(left, right):
    return lax.dot_general(
        left, right, (((1,), (1,)), ((), ())), preferred_element_type=jnp.float32
    )


def load(pairs):
    copies = [pltpu.make_async_copy(src, dst, sem) for src, dst, sem in pairs]
    for copy in copies:
        copy.start()
    return copies


def feed_forward_kernel(
    chips,
    hidden_ref,
    gate_hbm,
    up_hbm,
    down_hbm,
    mixed_ref,
    gate_out,
    up_out,
    act_out,
    all_out,
    gate_w,
    up_w,
    down_w,
    gate_keep,
    up_keep,
    act_keep,
    load_sem,
    store_sem,
    *comm,
):
    line = Line(chips)
    gather = Gather(line, *comm[:5])
    scatter = Scatter(line, *comm[5:])
    blocks, fresh = gather.blocks, scatter.fresh
    _, rows, width = blocks.shape
    units = gate_w.shape[1]
    copies = load(
        [
            (gate_hbm, gate_w, load_sem.at[0]),
            (up_hbm, up_w, load_sem.at[1]),
            (down_hbm, down_w, load_sem.at[2]),
        ]
    )
    line.greet()
    blocks[line.place * 2 + line.core] = hidden_ref[...]
    gather.send(line.place)

    def stores(chip):
        pair = pl.ds(chip * 2, 2)
        return [
            pltpu.make_async_copy(gate_keep.at[pair], gate_out.at[pair], store_sem.at[0, chip]),
            pltpu.make_async_copy(up_keep.at[pair], up_out.at[pair], store_sem.at[1, chip]),
            pltpu.make_async_copy(act_keep.at[pair], act_out.at[pair], store_sem.at[2, chip]),
            pltpu.make_async_copy(blocks.at[pair], all_out.at[pair], store_sem.at[3, chip]),
        ]

    for copy in copies:
        copy.wait()

    @pl.loop(0, chips)
    def _(step):
        chip = gather.step(step)
        pair = pl.ds(chip * 2, 2)

        @pl.loop(0, units // tile_of(units))
        def _(tile):
            columns = pl.ds(pl.multiple_of(tile * tile_of(units), 128), tile_of(units))
            tokens = blocks[pair].reshape(2 * rows, width)
            gate = jnp.dot(tokens, gate_w[:, columns], preferred_element_type=jnp.float32)
            up = jnp.dot(tokens, up_w[:, columns], preferred_element_type=jnp.float32)
            gate_keep[pair, :, columns] = gate.reshape(2, rows, -1)
            up_keep[pair, :, columns] = up.reshape(2, rows, -1)
            act_keep[pair, :, columns] = (
                (gate / (1.0 + jnp.exp(-gate)) * up).astype(jnp.bfloat16).reshape(2, rows, -1)
            )

        @pl.loop(0, width // tile_of(width))
        def _(tile):
            columns = pl.ds(pl.multiple_of(tile * tile_of(width), 128), tile_of(width))
            act = act_keep[pair].reshape(2 * rows, units)
            fresh[:, :, columns] = dot_cols(act, down_w[columns, :]).reshape(2, rows, -1)

        for copy in stores(chip):
            copy.start()
        scatter.after_term(chip)

    scatter.finish(mixed_ref)
    gather.finish()

    @pl.loop(0, chips)
    def _(chip):
        for copy in stores(chip):
            copy.wait()


def feed_forward_back_kernel(
    chips,
    grad_ref,
    gate_hbm,
    up_hbm,
    down_hbm,
    gate_lin_hbm,
    up_lin_hbm,
    hidden_grad_ref,
    gate_out,
    up_out,
    all_out,
    gate_w,
    up_w,
    down_w,
    gate_lin,
    up_lin,
    gate_keep,
    up_keep,
    load_sem,
    store_sem,
    *comm,
):
    line = Line(chips)
    gather = Gather(line, *comm[:5])
    scatter = Scatter(line, *comm[5:])
    blocks, fresh = gather.blocks, scatter.fresh
    _, rows, width = blocks.shape
    units = gate_w.shape[1]
    copies = load(
        [
            (down_hbm, down_w, load_sem.at[0]),
            (gate_lin_hbm, gate_lin, load_sem.at[1]),
            (up_lin_hbm, up_lin, load_sem.at[2]),
            (gate_hbm, gate_w, load_sem.at[3]),
            (up_hbm, up_w, load_sem.at[4]),
        ]
    )
    line.greet()
    blocks[line.place * 2 + line.core] = grad_ref[...]
    gather.send(line.place)

    def stores(chip):
        pair = pl.ds(chip * 2, 2)
        return [
            pltpu.make_async_copy(gate_keep.at[pair], gate_out.at[pair], store_sem.at[0, chip]),
            pltpu.make_async_copy(up_keep.at[pair], up_out.at[pair], store_sem.at[1, chip]),
            pltpu.make_async_copy(blocks.at[pair], all_out.at[pair], store_sem.at[2, chip]),
        ]

    for copy in copies:
        copy.wait()

    @pl.loop(0, chips)
    def _(step):
        chip = gather.step(step)
        pair = pl.ds(chip * 2, 2)

        @pl.loop(0, units // tile_of(units))
        def _(tile):
            columns = pl.ds(pl.multiple_of(tile * tile_of(units), 128), tile_of(units))
            tokens = blocks[pair].reshape(2 * rows, width)
            grad = jnp.dot(tokens, down_w[:, columns], preferred_element_type=jnp.float32)
            gate = gate_lin[pair, :, columns].reshape(2 * rows, -1)
            up = up_lin[pair, :, columns].reshape(2 * rows, -1)
            sig = 1.0 / (1.0 + jnp.exp(-gate))
            gate_keep[pair, :, columns] = (
                (grad * up * sig * (1.0 + gate * (1.0 - sig)))
                .astype(jnp.bfloat16)
                .reshape(2, rows, -1)
            )
            up_keep[pair, :, columns] = (
                (grad * (gate * sig)).astype(jnp.bfloat16).reshape(2, rows, -1)
            )

        @pl.loop(0, width // tile_of(width))
        def _(tile):
            columns = pl.ds(pl.multiple_of(tile * tile_of(width), 128), tile_of(width))
            gate = gate_keep[pair].reshape(2 * rows, units)
            up = up_keep[pair].reshape(2 * rows, units)
            fresh[:, :, columns] = (
                dot_cols(gate, gate_w[columns, :]) + dot_cols(up, up_w[columns, :])
            ).reshape(2, rows, -1)

        for copy in stores(chip):
            copy.start()
        scatter.after_term(chip)

    scatter.finish(hidden_grad_ref)
    gather.finish()

    @pl.loop(0, chips)
    def _(chip):
        for copy in stores(chip):
            copy.wait()


def whole_spec():
    return pl.BlockSpec(memory_space=pltpu.VMEM)


def far_spec():
    return pl.BlockSpec(memory_space=pl.ANY)


def line_params(collective_id):
    return pltpu.CompilerParams(
        collective_id=collective_id, has_side_effects=True, vmem_limit_bytes=60 * 2**20
    )


def feed_forward(hidden_low, gate_cols, up_cols, down_cols):
    rows, width = hidden_low.shape
    units = gate_cols.shape[1]
    slots = lax.axis_size("seq")
    chips = slots // 2
    weights = [pltpu.VMEM((width, units), jnp.bfloat16)] * 3
    mixed, gate, up, act, every = pl.pallas_call(
        functools.partial(feed_forward_kernel, chips),
        out_shape=(
            jax.ShapeDtypeStruct((rows, width), jnp.float32),
            jax.ShapeDtypeStruct((slots, rows, units), jnp.float32),
            jax.ShapeDtypeStruct((slots, rows, units), jnp.float32),
            jax.ShapeDtypeStruct((slots, rows, units), jnp.bfloat16),
            jax.ShapeDtypeStruct((slots, rows, width), jnp.bfloat16),
        ),
        in_specs=[whole_spec()] + [far_spec()] * 3,
        out_specs=(whole_spec(),) + (far_spec(),) * 4,
        scratch_shapes=weights
        + [
            pltpu.VMEM((slots, rows, units), jnp.float32),
            pltpu.VMEM((slots, rows, units), jnp.float32),
            pltpu.VMEM((slots, rows, units), jnp.bfloat16),
            pltpu.SemaphoreType.DMA((3,)),
            pltpu.SemaphoreType.DMA((4, chips)),
        ]
        + Gather.scratch(chips, rows, width)
        + Scatter.scratch(chips, rows, width),
        compiler_params=line_params(1),
        name="feed_forward",
    )(hidden_low, gate_cols, up_cols, down_cols)
    return mixed, gate, up, act.reshape(-1, units), every.reshape(-1, width)


def feed_forward_back(grad_low, gate_cols, up_cols, down_cols, gate, up):
    rows, width = grad_low.shape
    units = gate_cols.shape[1]
    slots = lax.axis_size("seq")
    chips = slots // 2
    weights = [pltpu.VMEM((width, units), jnp.bfloat16)] * 3
    hidden_grad, gate_grad, up_grad, every = pl.pallas_call(
        functools.partial(feed_forward_back_kernel, chips),
        out_shape=(
            jax.ShapeDtypeStruct((rows, width), jnp.float32),
            jax.ShapeDtypeStruct((slots, rows, units), jnp.bfloat16),
            jax.ShapeDtypeStruct((slots, rows, units), jnp.bfloat16),
            jax.ShapeDtypeStruct((slots, rows, width), jnp.bfloat16),
        ),
        in_specs=[whole_spec()] + [far_spec()] * 5,
        out_specs=(whole_spec(),) + (far_spec(),) * 3,
        scratch_shapes=weights
        + [
            pltpu.VMEM((slots, rows, units), jnp.float32),
            pltpu.VMEM((slots, rows, units), jnp.float32),
            pltpu.VMEM((slots, rows, units), jnp.bfloat16),
            pltpu.VMEM((slots, rows, units), jnp.bfloat16),
            pltpu.SemaphoreType.DMA((5,)),
            pltpu.SemaphoreType.DMA((3, chips)),
        ]
        + Gather.scratch(chips, rows, width)
        + Scatter.scratch(chips, rows, width),
        compiler_params=line_params(2),
        name="feed_forward_back",
    )(grad_low, gate_cols, up_cols, down_cols, gate, up)
    return (
        hidden_grad,
        gate_grad.reshape(-1, units),
        up_grad.reshape(-1, units),
        every.reshape(-1, width),
    )


def gather_seq(tensor):
    return lax.all_gather(tensor, "seq", axis=0, tiled=True)


def scatter_seq(tensor):
    return lax.psum_scatter(tensor, "seq", scatter_dimension=0, tiled=True)


def columns_in(weight):
    seq_count = lax.axis_size("seq")
    fsdp_count = lax.axis_size("fsdp")
    part = lax.all_to_all(weight, "seq", split_axis=1, concat_axis=0, tiled=True)
    whole = lax.all_gather(part, "fsdp", axis=0, tiled=True)
    return swap_blocks(whole, fsdp_count, seq_count)


def columns_out(term):
    seq_count = lax.axis_size("seq")
    fsdp_count = lax.axis_size("fsdp")
    swapped = swap_blocks(term, seq_count, fsdp_count).astype(jnp.bfloat16)
    summed = lax.psum_scatter(swapped, "fsdp", scatter_dimension=0, tiled=True)
    return lax.all_to_all(summed, "seq", split_axis=0, concat_axis=1, tiled=True).astype(
        jnp.float32
    )


def rope_tables(row_count):
    half_width = DH // 2
    frequency = rope_base ** (-jnp.arange(half_width, dtype=jnp.float32) * 2.0 / DH)
    angles = jnp.arange(row_count, dtype=jnp.int32).astype(jnp.float32)[:, None] * frequency[None, :]
    return jnp.cos(angles), jnp.sin(angles)


def rotate(tensor, cosine, sine_table):
    row_count = tensor.shape[0]
    half_width = DH // 2
    grouped = tensor.reshape(row_count, -1, DH)
    first_half = grouped[..., :half_width]
    second_half = grouped[..., half_width:]
    cosine = cosine[:, None, :]
    sine_table = sine_table[:, None, :]
    turned = jnp.concatenate(
        [
            first_half * cosine - second_half * sine_table,
            second_half * cosine + first_half * sine_table,
        ],
        axis=-1,
    )
    return turned.reshape(tensor.shape)


def per_device(
    inputs,
    query_weight,
    key_weight,
    value_weight,
    output_weight,
    query_gain,
    key_gain,
    attention_gain,
    gate_weight,
    up_weight,
    down_weight,
    feedforward_gain,
    segments,
    cotangent,
):
    token_count = inputs.shape[1]
    width_all = inputs.shape[2]
    local_in = inputs.reshape(token_count, width_all)
    segment_row = segments[0]
    score_scale = DH ** (-0.5)
    seq_index = lax.axis_index("seq")
    inputs_all = gather_seq(local_in)
    sequence_rows = inputs_all.shape[0]
    query_cols = columns_in(query_weight)
    key_cols = columns_in(key_weight)
    value_cols = columns_in(value_weight)
    head_width = query_cols.shape[1]
    local_heads = head_width // DH
    output_rows = lax.all_gather(output_weight, "fsdp", axis=0, tiled=True)
    gains = lax.all_gather(
        jnp.stack([query_gain, key_gain, attention_gain, feedforward_gain]),
        ("seq", "fsdp"),
        axis=1,
        tiled=True,
    ).astype(jnp.float32)
    query_scale = lax.dynamic_slice_in_dim(gains[0], seq_index * head_width, head_width, 0)
    key_scale = lax.dynamic_slice_in_dim(gains[1], seq_index * head_width, head_width, 0)
    attention_scale = gains[2]
    feedforward_scale = gains[3]
    query_pre = jnp.dot(inputs_all, query_cols, preferred_element_type=jnp.float32)
    key_pre = jnp.dot(inputs_all, key_cols, preferred_element_type=jnp.float32)
    values_low = jnp.dot(inputs_all, value_cols, preferred_element_type=jnp.float32).astype(
        jnp.bfloat16
    )
    squares = lax.psum(
        jnp.stack([jnp.sum(query_pre * query_pre, axis=-1), jnp.sum(key_pre * key_pre, axis=-1)]),
        "seq",
    )
    inverse = lax.rsqrt(squares / width_all + eps_norm)
    query_unit = query_pre * inverse[0][:, None]
    key_unit = key_pre * inverse[1][:, None]
    cosine, sine_table = rope_tables(sequence_rows)
    queries_low = rotate(query_unit * query_scale, cosine, sine_table).astype(jnp.bfloat16)
    keys_low = rotate(key_unit * key_scale, cosine, sine_table).astype(jnp.bfloat16)
    query_heads = queries_low.reshape(sequence_rows, local_heads, DH)
    key_heads = keys_low.reshape(sequence_rows, local_heads, DH)
    value_heads = values_low.reshape(sequence_rows, local_heads, DH)
    block_rows = min(512, sequence_rows)
    block_count = sequence_rows // block_rows
    block_ids = jnp.arange(block_count, dtype=jnp.int32)

    def attend_block(loop_state, block_index):
        first_row = block_index * block_rows
        query_block = lax.dynamic_slice_in_dim(query_heads, first_row, block_rows, 0)
        scores = masked_scores(query_block, key_heads, first_row, segment_row, score_scale)
        row_max = jnp.max(scores, axis=-1, keepdims=True)
        expanded = jnp.exp(scores - row_max)
        row_total = jnp.sum(expanded, axis=-1, keepdims=True)
        softmax_low = (expanded / row_total).astype(jnp.bfloat16)
        block_out = jnp.einsum(
            "hqk,khd->qhd", softmax_low, value_heads, preferred_element_type=jnp.float32
        )
        log_total = (row_max + jnp.log(row_total))[..., 0]
        return (loop_state, (block_out.astype(jnp.bfloat16), log_total))

    _, (out_blocks, log_totals) = lax.scan(attend_block, jnp.zeros((), jnp.int32), block_ids)
    attended_heads = out_blocks.reshape(sequence_rows, head_width)
    projected = scatter_seq(
        jnp.dot(attended_heads, output_rows, preferred_element_type=jnp.float32).astype(
            jnp.bfloat16
        )
    ).astype(jnp.float32)
    hidden = local_in.astype(jnp.float32) + rms_scale(projected, attention_scale)
    hidden_low = hidden.astype(jnp.bfloat16)
    gate_cols = columns_in(gate_weight)
    up_cols = columns_in(up_weight)
    down_cols = columns_in(down_weight)
    mixed_pre, gate_linear, up_linear, activated, hidden_all = feed_forward(
        hidden_low, gate_cols, up_cols, down_cols
    )
    result = (
        (hidden + rms_scale(mixed_pre, feedforward_scale))
        .astype(jnp.bfloat16)
        .reshape(1, token_count, width_all)
    )
    grad_result = cotangent.reshape(token_count, width_all).astype(jnp.float32)
    _, mixed_pull = jax.vjp(rms_scale, mixed_pre, feedforward_scale)
    grad_mixed, grad_feedforward_gain = mixed_pull(grad_result)
    grad_mixed_low = grad_mixed.astype(jnp.bfloat16)
    hidden_term, grad_gate_low, grad_upward_low, grad_all = feed_forward_back(
        grad_mixed_low, gate_cols, up_cols, down_cols, gate_linear, up_linear
    )
    grad_hidden = grad_result + hidden_term
    gate_weight_grad = columns_out(contract_rows(hidden_all, grad_gate_low))
    up_weight_grad = columns_out(contract_rows(hidden_all, grad_upward_low))
    down_weight_grad = columns_out(contract_rows(grad_all, activated))
    _, branch_pull = jax.vjp(rms_scale, projected, attention_scale)
    grad_projected, grad_attention_gain = branch_pull(grad_hidden)
    grad_projected_all = gather_seq(grad_projected.astype(jnp.bfloat16))
    output_weight_grad = lax.psum_scatter(
        contract_rows(attended_heads, grad_projected_all).astype(jnp.bfloat16),
        "fsdp",
        scatter_dimension=0,
        tiled=True,
    ).astype(jnp.float32)
    grad_attended = contract_cols(grad_projected_all, output_rows).astype(jnp.bfloat16)
    grad_out_heads = grad_attended.reshape(sequence_rows, local_heads, DH)

    def attend_back(loop_state, block_index):
        key_total, value_total = loop_state
        first_row = block_index * block_rows
        query_block = lax.dynamic_slice_in_dim(query_heads, first_row, block_rows, 0)
        grad_block = lax.dynamic_slice_in_dim(grad_out_heads, first_row, block_rows, 0)
        log_block = lax.dynamic_index_in_dim(log_totals, block_index, 0, keepdims=False)
        scores = masked_scores(query_block, key_heads, first_row, segment_row, score_scale)
        probabilities = jnp.exp(scores - log_block[..., None])
        softmax_low = probabilities.astype(jnp.bfloat16)
        value_total = value_total + jnp.einsum(
            "hqk,qhd->khd", softmax_low, grad_block, preferred_element_type=jnp.float32
        )
        grad_softmax = jnp.einsum(
            "qhd,khd->hqk", grad_block, value_heads, preferred_element_type=jnp.float32
        )
        row_dot = jnp.sum(probabilities * grad_softmax, axis=-1, keepdims=True)
        grad_scores = (probabilities * (grad_softmax - row_dot)).astype(jnp.bfloat16)
        grad_query_block = (
            jnp.einsum("hqk,khd->qhd", grad_scores, key_heads, preferred_element_type=jnp.float32)
            * score_scale
        )
        key_total = (
            key_total
            + jnp.einsum(
                "hqk,qhd->khd", grad_scores, query_block, preferred_element_type=jnp.float32
            )
            * score_scale
        )
        return ((key_total, value_total), grad_query_block.astype(jnp.bfloat16))

    zero_heads = jnp.zeros((sequence_rows, local_heads, DH), jnp.float32)
    (key_total, value_total), grad_query_blocks = lax.scan(
        attend_back, (zero_heads, zero_heads), block_ids
    )
    grad_queries = grad_query_blocks.reshape(sequence_rows, head_width).astype(jnp.float32)
    grad_keys = (
        key_total.astype(jnp.bfloat16).reshape(sequence_rows, head_width).astype(jnp.float32)
    )
    grad_values = value_total.astype(jnp.bfloat16).reshape(sequence_rows, head_width)
    query_error = rotate(grad_queries, cosine, -sine_table)
    key_error = rotate(grad_keys, cosine, -sine_table)
    grad_query_gain = jnp.sum(query_error * query_unit, axis=0)
    grad_key_gain = jnp.sum(key_error * key_unit, axis=0)
    query_error = query_error * query_scale
    key_error = key_error * key_scale
    means = (
        lax.psum(
            jnp.stack(
                [
                    jnp.sum(query_error * query_unit, axis=-1),
                    jnp.sum(key_error * key_unit, axis=-1),
                ]
            ),
            "seq",
        )
        / width_all
    )
    grad_query_low = (
        inverse[0][:, None] * (query_error - query_unit * means[0][:, None])
    ).astype(jnp.bfloat16)
    grad_key_low = (inverse[1][:, None] * (key_error - key_unit * means[1][:, None])).astype(
        jnp.bfloat16
    )
    grad_input = grad_hidden + scatter_seq(
        (
            contract_cols(grad_query_low, query_cols)
            + contract_cols(grad_key_low, key_cols)
            + contract_cols(grad_values, value_cols)
        ).astype(jnp.bfloat16)
    ).astype(jnp.float32)
    query_weight_grad = columns_out(contract_rows(inputs_all, grad_query_low))
    key_weight_grad = columns_out(contract_rows(inputs_all, grad_key_low))
    value_weight_grad = columns_out(contract_rows(inputs_all, grad_values))
    head_gains = lax.psum_scatter(
        jnp.stack([grad_query_gain, grad_key_gain]), "fsdp", scatter_dimension=1, tiled=True
    )
    token_gains = lax.psum_scatter(
        jnp.stack([grad_attention_gain, grad_feedforward_gain]),
        ("seq", "fsdp"),
        scatter_dimension=1,
        tiled=True,
    )
    return (
        result,
        grad_input.reshape(1, token_count, width_all),
        query_weight_grad,
        key_weight_grad,
        value_weight_grad,
        output_weight_grad,
        head_gains[0],
        head_gains[1],
        token_gains[0],
        gate_weight_grad,
        up_weight_grad,
        down_weight_grad,
        token_gains[1],
    )


def solution(mesh):
    in_specs = (
        P("fsdp", "seq", None),
        P(("seq", "fsdp"), None),
        P(("seq", "fsdp"), None),
        P(("seq", "fsdp"), None),
        P(("seq", "fsdp"), None),
        P(("seq", "fsdp")),
        P(("seq", "fsdp")),
        P(("seq", "fsdp")),
        P(("seq", "fsdp"), None),
        P(("seq", "fsdp"), None),
        P(("seq", "fsdp"), None),
        P(("seq", "fsdp")),
        P("fsdp", None),
        P("fsdp", "seq", None),
    )
    out_specs = (
        P("fsdp", "seq", None),
        P("fsdp", "seq", None),
        P(("seq", "fsdp"), None),
        P(("seq", "fsdp"), None),
        P(("seq", "fsdp"), None),
        P(("seq", "fsdp"), None),
        P(("seq", "fsdp")),
        P(("seq", "fsdp")),
        P(("seq", "fsdp")),
        P(("seq", "fsdp"), None),
        P(("seq", "fsdp"), None),
        P(("seq", "fsdp"), None),
        P(("seq", "fsdp")),
    )
    return jax.shard_map(
        per_device, mesh=mesh, in_specs=in_specs, out_specs=out_specs, check_vma=False
    )
```

```python
import functools

import jax
import jax.numpy as jnp
from jax import lax
from jax.experimental import pallas as pl
from jax.experimental.pallas import tpu as pltpu
from jax.sharding import PartitionSpec as P

HEADS = 16
DH = 128


eps_norm = 1e-06
rope_base = 500000.0
neg_fill = -1e30


def rms_scale(tensor, gain):
    return tensor * lax.rsqrt(jnp.mean(tensor * tensor, axis=-1, keepdims=True) + eps_norm) * gain


def rotary(tensor, positions):
    row_count = tensor.shape[0]
    grouped = tensor.reshape(row_count, HEADS, DH)
    half_width = DH // 2
    frequency = rope_base ** (-jnp.arange(half_width, dtype=jnp.float32) * 2.0 / DH)
    angles = positions.astype(jnp.float32)[:, None] * frequency[None, :]
    cosine = jnp.cos(angles)[:, None, :]
    sine_table = jnp.sin(angles)[:, None, :]
    first_half = grouped[..., :half_width]
    second_half = grouped[..., half_width:]
    turned = jnp.concatenate(
        [
            first_half * cosine - second_half * sine_table,
            second_half * cosine + first_half * sine_table,
        ],
        axis=-1,
    )
    return turned.reshape(tensor.shape)


def norm_rotary(tensor, gain, positions):
    return rotary(rms_scale(tensor, gain), positions)


def swiglu_act(gate_linear, up_linear):
    return jax.nn.silu(gate_linear) * up_linear


def contract_rows(left, right):
    return lax.dot_general(
        left, right, (((0,), (0,)), ((), ())), preferred_element_type=jnp.float32
    )


def contract_cols(left, right):
    return lax.dot_general(
        left, right, (((1,), (1,)), ((), ())), preferred_element_type=jnp.float32
    )


def swap_blocks(tensor, outer, inner):
    block_rows = tensor.shape[0] // (outer * inner)
    return (
        tensor.reshape(outer, inner, block_rows, tensor.shape[1])
        .transpose(1, 0, 2, 3)
        .reshape(tensor.shape)
    )


def masked_scores(query_block, key_heads, first_row, segment_row, score_scale):
    block_rows = query_block.shape[0]
    sequence_rows = key_heads.shape[0]
    scores = (
        jnp.einsum("qhd,khd->hqk", query_block, key_heads, preferred_element_type=jnp.float32)
        * score_scale
    )
    query_pos = first_row + jnp.arange(block_rows, dtype=jnp.int32)
    key_pos = jnp.arange(sequence_rows, dtype=jnp.int32)
    query_seg = lax.dynamic_slice_in_dim(segment_row, first_row, block_rows, 0)
    allowed = (key_pos[None, :] <= query_pos[:, None]) & (
        segment_row[None, :] == query_seg[:, None]
    )
    return jnp.where(allowed[None], scores, neg_fill)

MESH = pl.DeviceIdType.MESH
RS_PARTS = 4


class Line:
    def __init__(self, chips):
        index = lax.axis_index("seq")
        self.chips = chips
        self.fsdp = lax.axis_index("fsdp")
        self.place = index // 2
        self.core = index % 2

    def device(self, place, core):
        return (place * 2 + core, self.fsdp)

    @property
    def partner(self):
        return self.device(self.place, 1 - self.core)

    @property
    def above(self):
        return self.device(jnp.minimum(self.place + 1, self.chips - 1), self.core)

    @property
    def below(self):
        return self.device(jnp.maximum(self.place - 1, 0), self.core)

    @property
    def has_above(self):
        return self.place < self.chips - 1

    @property
    def has_below(self):
        return self.place > 0

    def greet(self):
        barrier = pltpu.get_barrier_semaphore()
        pl.semaphore_signal(barrier, inc=1, device_id=self.partner, device_id_type=MESH)

        @pl.when(self.has_above)
        def _():
            pl.semaphore_signal(barrier, inc=1, device_id=self.above, device_id_type=MESH)

        @pl.when(self.has_below)
        def _():
            pl.semaphore_signal(barrier, inc=1, device_id=self.below, device_id_type=MESH)

        peers = (
            1 + jnp.minimum(self.place, 1) + jnp.minimum(self.chips - 1 - self.place, 1)
        )
        pl.semaphore_wait(barrier, peers)

    def order(self, step):
        place, last = self.place, self.chips - 1
        near = jnp.minimum(place, last - place)
        both = jnp.where(step % 2 == 1, place - (step + 1) // 2, place + step // 2)
        rest = jnp.where(place <= last - place, step, last - step)
        return jnp.where(step <= 2 * near, both, rest)

    def paired(self, step):
        near = jnp.minimum(self.place, self.chips - 1 - self.place)
        return (step % 2 == 1) & (step <= 2 * near)

    def second_of_pair(self, step):
        near = jnp.minimum(self.place, self.chips - 1 - self.place)
        return (step % 2 == 0) & (step > 0) & (step <= 2 * near)


class Gather:
    def __init__(self, line, blocks, arrive, up_sem, down_sem, side_sem):
        self.line, self.blocks, self.arrive = line, blocks, arrive
        self.up_sem, self.down_sem, self.side_sem = up_sem, down_sem, side_sem

    @staticmethod
    def scratch(chips, rows, width):
        return [
            pltpu.VMEM((2 * chips, rows, width), jnp.bfloat16),
            pltpu.SemaphoreType.DMA((2 * chips,)),
            pltpu.SemaphoreType.DMA((chips,)),
            pltpu.SemaphoreType.DMA((chips,)),
            pltpu.SemaphoreType.DMA((chips,)),
        ]

    def copy(self, chip, sem, target):
        slot = chip * 2 + self.line.core
        return pltpu.make_async_remote_copy(
            src_ref=self.blocks.at[slot],
            dst_ref=self.blocks.at[slot],
            send_sem=sem.at[chip],
            recv_sem=self.arrive.at[slot],
            device_id=target,
            device_id_type=MESH,
        )

    def wait_slot(self, slot):
        pltpu.make_async_remote_copy(
            src_ref=self.blocks.at[slot],
            dst_ref=self.blocks.at[slot],
            send_sem=self.side_sem.at[0],
            recv_sem=self.arrive.at[slot],
            device_id=self.line.partner,
            device_id_type=MESH,
        ).wait_recv()

    def send(self, chip):
        line = self.line

        @pl.when((chip <= line.place) & line.has_above)
        def _():
            self.copy(chip, self.up_sem, line.above).start()

        @pl.when((chip >= line.place) & line.has_below)
        def _():
            self.copy(chip, self.down_sem, line.below).start()

        self.copy(chip, self.side_sem, line.partner).start()

    def take(self, chip):
        self.wait_slot(chip * 2 + self.line.core)
        self.send(chip)

    def step(self, step):
        line = self.line
        chip = line.order(step)

        @pl.when((step > 0) & jnp.logical_not(line.second_of_pair(step)))
        def _():
            self.take(chip)

        @pl.when(line.paired(step))
        def _():
            self.take(line.order(step + 1))

        self.wait_slot(chip * 2 + 1 - line.core)
        return chip

    def finish(self):
        line = self.line

        @pl.loop(0, line.chips)
        def _(chip):
            @pl.when((chip <= line.place) & line.has_above)
            def _():
                self.copy(chip, self.up_sem, line.above).wait_send()

            @pl.when((chip >= line.place) & line.has_below)
            def _():
                self.copy(chip, self.down_sem, line.below).wait_send()

            self.copy(chip, self.side_sem, line.partner).wait_send()


class Scatter:
    def __init__(self, line, fresh, terms, side_out, side_in, out, inward, side_send, side_recv, send_sem, recv_sem):
        self.line, self.fresh, self.terms = line, fresh, terms
        self.side_out, self.side_in = side_out, side_in
        self.out, self.inward = out, inward
        self.side_send, self.side_recv = side_send, side_recv
        self.send_sem, self.recv_sem = send_sem, recv_sem
        self.rows = terms.shape[1] // RS_PARTS

    @staticmethod
    def scratch(chips, rows, width):
        return [
            pltpu.VMEM((2, rows, width), jnp.float32),
            pltpu.VMEM((chips, rows, width), jnp.float32),
            pltpu.VMEM((chips, rows, width), jnp.bfloat16),
            pltpu.VMEM((chips, rows, width), jnp.bfloat16),
            pltpu.VMEM((chips, rows, width), jnp.bfloat16),
            pltpu.VMEM((2, chips, rows, width), jnp.bfloat16),
            pltpu.SemaphoreType.DMA((chips,)),
            pltpu.SemaphoreType.DMA((chips,)),
            pltpu.SemaphoreType.DMA((chips, RS_PARTS)),
            pltpu.SemaphoreType.DMA((2, chips, RS_PARTS)),
        ]

    def side(self, chip):
        return pltpu.make_async_remote_copy(
            src_ref=self.side_out.at[chip],
            dst_ref=self.side_in.at[chip],
            send_sem=self.side_send.at[chip],
            recv_sem=self.side_recv.at[chip],
            device_id=self.line.partner,
            device_id_type=MESH,
        )

    def part(self, chip, part, upward, target):
        rows = pl.ds(part * self.rows, self.rows)
        return pltpu.make_async_remote_copy(
            src_ref=self.out.at[chip, rows],
            dst_ref=self.inward.at[upward, chip, rows],
            send_sem=self.send_sem.at[chip, part],
            recv_sem=self.recv_sem.at[upward, chip, part],
            device_id=target,
            device_id_type=MESH,
        )

    def share(self, chip):
        self.side_out[chip] = self.fresh[1 - self.line.core].astype(jnp.bfloat16)
        self.side(chip).start()
        self.terms[chip] = self.fresh[self.line.core]

    def total(self, chip, part, ways):
        rows = pl.ds(part * self.rows, self.rows)
        total = self.terms[chip, rows] + self.side_in[chip, rows].astype(jnp.float32)
        for way in ways:
            total = total + self.inward[way, chip, rows].astype(jnp.float32)
        return rows, total

    def pass_on(self, chip, upward, first):
        target = self.line.above if upward else self.line.below
        self.side(chip).wait_recv()

        @pl.loop(0, RS_PARTS)
        def _(part):
            if not first:
                self.part(chip, part, upward, target).wait_recv()
            rows, total = self.total(chip, part, () if first else (upward,))
            self.out[chip, rows] = total.astype(jnp.bfloat16)
            self.part(chip, part, upward, target).start()

    def after_term(self, chip):
        line = self.line
        self.share(chip)

        @pl.when((chip < line.place) & jnp.logical_not(line.has_above))
        def _():
            self.pass_on(chip, 0, True)

        @pl.when((chip > line.place) & jnp.logical_not(line.has_below))
        def _():
            self.pass_on(chip, 1, True)

    def finish(self, result):
        line = self.line
        lower = line.place * 2 < line.chips

        @pl.loop(0, line.chips)
        def _(step):
            up_chip, down_chip = step, line.chips - 1 - step
            go_up = (up_chip > line.place) & line.has_below
            go_down = (down_chip < line.place) & line.has_above

            @pl.when(go_up & lower)
            def _():
                self.pass_on(up_chip, 1, False)

            @pl.when(go_down)
            def _():
                self.pass_on(down_chip, 0, False)

            @pl.when(go_up & jnp.logical_not(lower))
            def _():
                self.pass_on(up_chip, 1, False)

        place = line.place
        self.side(place).wait_recv()

        @pl.loop(0, RS_PARTS)
        def _(part):
            @pl.when(line.has_above)
            def _():
                self.part(place, part, 0, line.below).wait_recv()

            @pl.when(line.has_below)
            def _():
                self.part(place, part, 1, line.above).wait_recv()

            @pl.when(line.has_above & line.has_below)
            def _():
                rows, total = self.total(place, part, (0, 1))
                result[rows] = total

            @pl.when(line.has_above & jnp.logical_not(line.has_below))
            def _():
                rows, total = self.total(place, part, (0,))
                result[rows] = total

            @pl.when(line.has_below & jnp.logical_not(line.has_above))
            def _():
                rows, total = self.total(place, part, (1,))
                result[rows] = total

        @pl.loop(0, line.chips)
        def _(chip):
            self.side(chip).wait_send()

            @pl.when(chip != place)
            def _():
                @pl.loop(0, RS_PARTS)
                def _(part):
                    self.part(chip, part, 0, line.below).wait_send()


def tile_of(extent):
    return min(256, extent)


def dot_cols(left, right):
    return lax.dot_general(
        left, right, (((1,), (1,)), ((), ())), preferred_element_type=jnp.float32
    )


def load(pairs):
    copies = [pltpu.make_async_copy(src, dst, sem) for src, dst, sem in pairs]
    for copy in copies:
        copy.start()
    return copies


def feed_forward_kernel(
    chips,
    hidden_ref,
    gate_hbm,
    up_hbm,
    down_hbm,
    mixed_ref,
    gate_out,
    up_out,
    act_out,
    all_out,
    gate_w,
    up_w,
    down_w,
    gate_keep,
    up_keep,
    act_keep,
    load_sem,
    store_sem,
    *comm,
):
    line = Line(chips)
    gather = Gather(line, *comm[:5])
    scatter = Scatter(line, *comm[5:])
    blocks, fresh = gather.blocks, scatter.fresh
    _, rows, width = blocks.shape
    units = gate_w.shape[1]
    copies = load(
        [
            (gate_hbm, gate_w, load_sem.at[0]),
            (up_hbm, up_w, load_sem.at[1]),
            (down_hbm, down_w, load_sem.at[2]),
        ]
    )
    line.greet()
    blocks[line.place * 2 + line.core] = hidden_ref[...]
    gather.send(line.place)

    def stores(chip):
        pair = pl.ds(chip * 2, 2)
        return [
            pltpu.make_async_copy(gate_keep.at[pair], gate_out.at[pair], store_sem.at[0, chip]),
            pltpu.make_async_copy(up_keep.at[pair], up_out.at[pair], store_sem.at[1, chip]),
            pltpu.make_async_copy(act_keep.at[pair], act_out.at[pair], store_sem.at[2, chip]),
            pltpu.make_async_copy(blocks.at[pair], all_out.at[pair], store_sem.at[3, chip]),
        ]

    for copy in copies:
        copy.wait()

    @pl.loop(0, chips)
    def _(step):
        chip = gather.step(step)
        pair = pl.ds(chip * 2, 2)

        @pl.loop(0, units // tile_of(units))
        def _(tile):
            columns = pl.ds(pl.multiple_of(tile * tile_of(units), 128), tile_of(units))
            tokens = blocks[pair].reshape(2 * rows, width)
            gate = jnp.dot(tokens, gate_w[:, columns], preferred_element_type=jnp.float32)
            up = jnp.dot(tokens, up_w[:, columns], preferred_element_type=jnp.float32)
            gate_keep[pair, :, columns] = gate.reshape(2, rows, -1)
            up_keep[pair, :, columns] = up.reshape(2, rows, -1)
            act_keep[pair, :, columns] = (
                (gate / (1.0 + jnp.exp(-gate)) * up).astype(jnp.bfloat16).reshape(2, rows, -1)
            )

        @pl.loop(0, width // tile_of(width))
        def _(tile):
            columns = pl.ds(pl.multiple_of(tile * tile_of(width), 128), tile_of(width))
            act = act_keep[pair].reshape(2 * rows, units)
            fresh[:, :, columns] = dot_cols(act, down_w[columns, :]).reshape(2, rows, -1)

        for copy in stores(chip):
            copy.start()
        scatter.after_term(chip)

    scatter.finish(mixed_ref)
    gather.finish()

    @pl.loop(0, chips)
    def _(chip):
        for copy in stores(chip):
            copy.wait()


def feed_forward_back_kernel(
    chips,
    grad_ref,
    gate_hbm,
    up_hbm,
    down_hbm,
    gate_lin_hbm,
    up_lin_hbm,
    hidden_grad_ref,
    gate_out,
    up_out,
    all_out,
    gate_w,
    up_w,
    down_w,
    gate_lin,
    up_lin,
    gate_keep,
    up_keep,
    load_sem,
    store_sem,
    *comm,
):
    line = Line(chips)
    gather = Gather(line, *comm[:5])
    scatter = Scatter(line, *comm[5:])
    blocks, fresh = gather.blocks, scatter.fresh
    _, rows, width = blocks.shape
    units = gate_w.shape[1]
    copies = load(
        [
            (down_hbm, down_w, load_sem.at[0]),
            (gate_lin_hbm, gate_lin, load_sem.at[1]),
            (up_lin_hbm, up_lin, load_sem.at[2]),
            (gate_hbm, gate_w, load_sem.at[3]),
            (up_hbm, up_w, load_sem.at[4]),
        ]
    )
    line.greet()
    blocks[line.place * 2 + line.core] = grad_ref[...]
    gather.send(line.place)

    def stores(chip):
        pair = pl.ds(chip * 2, 2)
        return [
            pltpu.make_async_copy(gate_keep.at[pair], gate_out.at[pair], store_sem.at[0, chip]),
            pltpu.make_async_copy(up_keep.at[pair], up_out.at[pair], store_sem.at[1, chip]),
            pltpu.make_async_copy(blocks.at[pair], all_out.at[pair], store_sem.at[2, chip]),
        ]

    for copy in copies:
        copy.wait()

    @pl.loop(0, chips)
    def _(step):
        chip = gather.step(step)
        pair = pl.ds(chip * 2, 2)

        @pl.loop(0, units // tile_of(units))
        def _(tile):
            columns = pl.ds(pl.multiple_of(tile * tile_of(units), 128), tile_of(units))
            tokens = blocks[pair].reshape(2 * rows, width)
            grad = jnp.dot(tokens, down_w[:, columns], preferred_element_type=jnp.float32)
            gate = gate_lin[pair, :, columns].reshape(2 * rows, -1)
            up = up_lin[pair, :, columns].reshape(2 * rows, -1)
            sig = 1.0 / (1.0 + jnp.exp(-gate))
            gate_keep[pair, :, columns] = (
                (grad * up * sig * (1.0 + gate * (1.0 - sig)))
                .astype(jnp.bfloat16)
                .reshape(2, rows, -1)
            )
            up_keep[pair, :, columns] = (
                (grad * (gate * sig)).astype(jnp.bfloat16).reshape(2, rows, -1)
            )

        @pl.loop(0, width // tile_of(width))
        def _(tile):
            columns = pl.ds(pl.multiple_of(tile * tile_of(width), 128), tile_of(width))
            gate = gate_keep[pair].reshape(2 * rows, units)
            up = up_keep[pair].reshape(2 * rows, units)
            fresh[:, :, columns] = (
                dot_cols(gate, gate_w[columns, :]) + dot_cols(up, up_w[columns, :])
            ).reshape(2, rows, -1)

        for copy in stores(chip):
            copy.start()
        scatter.after_term(chip)

    scatter.finish(hidden_grad_ref)
    gather.finish()

    @pl.loop(0, chips)
    def _(chip):
        for copy in stores(chip):
            copy.wait()


def whole_spec():
    return pl.BlockSpec(memory_space=pltpu.VMEM)


def far_spec():
    return pl.BlockSpec(memory_space=pl.ANY)


def line_params(collective_id):
    return pltpu.CompilerParams(
        collective_id=collective_id, has_side_effects=True, vmem_limit_bytes=60 * 2**20
    )


def feed_forward(hidden_low, gate_cols, up_cols, down_cols):
    rows, width = hidden_low.shape
    units = gate_cols.shape[1]
    slots = lax.axis_size("seq")
    chips = slots // 2
    weights = [pltpu.VMEM((width, units), jnp.bfloat16)] * 3
    mixed, gate, up, act, every = pl.pallas_call(
        functools.partial(feed_forward_kernel, chips),
        out_shape=(
            jax.ShapeDtypeStruct((rows, width), jnp.float32),
            jax.ShapeDtypeStruct((slots, rows, units), jnp.float32),
            jax.ShapeDtypeStruct((slots, rows, units), jnp.float32),
            jax.ShapeDtypeStruct((slots, rows, units), jnp.bfloat16),
            jax.ShapeDtypeStruct((slots, rows, width), jnp.bfloat16),
        ),
        in_specs=[whole_spec()] + [far_spec()] * 3,
        out_specs=(whole_spec(),) + (far_spec(),) * 4,
        scratch_shapes=weights
        + [
            pltpu.VMEM((slots, rows, units), jnp.float32),
            pltpu.VMEM((slots, rows, units), jnp.float32),
            pltpu.VMEM((slots, rows, units), jnp.bfloat16),
            pltpu.SemaphoreType.DMA((3,)),
            pltpu.SemaphoreType.DMA((4, chips)),
        ]
        + Gather.scratch(chips, rows, width)
        + Scatter.scratch(chips, rows, width),
        compiler_params=line_params(1),
        name="feed_forward",
    )(hidden_low, gate_cols, up_cols, down_cols)
    return mixed, gate, up, act.reshape(-1, units), every.reshape(-1, width)


def feed_forward_back(grad_low, gate_cols, up_cols, down_cols, gate, up):
    rows, width = grad_low.shape
    units = gate_cols.shape[1]
    slots = lax.axis_size("seq")
    chips = slots // 2
    weights = [pltpu.VMEM((width, units), jnp.bfloat16)] * 3
    hidden_grad, gate_grad, up_grad, every = pl.pallas_call(
        functools.partial(feed_forward_back_kernel, chips),
        out_shape=(
            jax.ShapeDtypeStruct((rows, width), jnp.float32),
            jax.ShapeDtypeStruct((slots, rows, units), jnp.bfloat16),
            jax.ShapeDtypeStruct((slots, rows, units), jnp.bfloat16),
            jax.ShapeDtypeStruct((slots, rows, width), jnp.bfloat16),
        ),
        in_specs=[whole_spec()] + [far_spec()] * 5,
        out_specs=(whole_spec(),) + (far_spec(),) * 3,
        scratch_shapes=weights
        + [
            pltpu.VMEM((slots, rows, units), jnp.float32),
            pltpu.VMEM((slots, rows, units), jnp.float32),
            pltpu.VMEM((slots, rows, units), jnp.bfloat16),
            pltpu.VMEM((slots, rows, units), jnp.bfloat16),
            pltpu.SemaphoreType.DMA((5,)),
            pltpu.SemaphoreType.DMA((3, chips)),
        ]
        + Gather.scratch(chips, rows, width)
        + Scatter.scratch(chips, rows, width),
        compiler_params=line_params(2),
        name="feed_forward_back",
    )(grad_low, gate_cols, up_cols, down_cols, gate, up)
    return (
        hidden_grad,
        gate_grad.reshape(-1, units),
        up_grad.reshape(-1, units),
        every.reshape(-1, width),
    )


def peers_of(axis, size):
    me = lax.axis_index(axis)
    return me, lambda step: (me + step) % size


def greet_cross(seq_count, fsdp_count):
    seq, seq_peer = peers_of("seq", seq_count)
    fsdp, fsdp_peer = peers_of("fsdp", fsdp_count)
    barrier = pltpu.get_barrier_semaphore()
    for step in range(1, seq_count):
        pl.semaphore_signal(
            barrier, inc=1, device_id=(seq_peer(step), fsdp), device_id_type=MESH
        )
    for step in range(1, fsdp_count):
        pl.semaphore_signal(
            barrier, inc=1, device_id=(seq, fsdp_peer(step)), device_id_type=MESH
        )
    pl.semaphore_wait(barrier, seq_count + fsdp_count - 2)


def bring_in_kernel(
    chips,
    fsdp_count,
    inputs_ref,
    query_ref,
    key_ref,
    value_ref,
    output_ref,
    gains_ref,
    inputs_out,
    weights_out,
    output_out,
    gains_out,
    weights,
    outputs,
    gains,
    row_send,
    row_recv,
    column_send,
    column_recv,
    gain_row_send,
    gain_row_recv,
    gain_column_send,
    gain_column_recv,
    output_send,
    output_recv,
    store_sem,
    *comm,
):
    line = Line(chips)
    gather = Gather(line, *comm)
    seq_count = 2 * chips
    seq, seq_peer = peers_of("seq", seq_count)
    fsdp, fsdp_peer = peers_of("fsdp", fsdp_count)
    columns = weights.shape[-1]
    sources = (query_ref, key_ref, value_ref)

    def block(owner):
        return pl.ds(pl.multiple_of(owner * columns, 128), columns)

    def row_copy(which, step):
        peer = seq_peer(step)
        return pltpu.make_async_remote_copy(
            src_ref=sources[which].at[:, block(peer)],
            dst_ref=weights.at[which, seq, fsdp],
            send_sem=row_send.at[which, step],
            recv_sem=row_recv.at[which, step],
            device_id=(peer, fsdp),
            device_id_type=MESH,
        )

    def column_copy(owner, step):
        return pltpu.make_async_remote_copy(
            src_ref=weights.at[:, owner, fsdp],
            dst_ref=weights.at[:, owner, fsdp],
            send_sem=column_send.at[owner, step],
            recv_sem=column_recv.at[owner, step],
            device_id=(seq, fsdp_peer(step)),
            device_id_type=MESH,
        )

    def gain_row_copy(step):
        return pltpu.make_async_remote_copy(
            src_ref=gains_ref,
            dst_ref=gains.at[seq, fsdp],
            send_sem=gain_row_send.at[step],
            recv_sem=gain_row_recv.at[step],
            device_id=(seq_peer(step), fsdp),
            device_id_type=MESH,
        )

    def gain_column_copy(owner, step):
        return pltpu.make_async_remote_copy(
            src_ref=gains.at[owner, fsdp],
            dst_ref=gains.at[owner, fsdp],
            send_sem=gain_column_send.at[owner, step],
            recv_sem=gain_column_recv.at[owner, step],
            device_id=(seq, fsdp_peer(step)),
            device_id_type=MESH,
        )

    def output_copy(step):
        return pltpu.make_async_remote_copy(
            src_ref=output_ref,
            dst_ref=outputs.at[fsdp],
            send_sem=output_send.at[step],
            recv_sem=output_recv.at[step],
            device_id=(seq, fsdp_peer(step)),
            device_id_type=MESH,
        )

    greet_cross(seq_count, fsdp_count)
    for step in range(1, seq_count):
        for which in range(3):
            row_copy(which, step).start()
        gain_row_copy(step).start()
    gather.blocks[line.place * 2 + line.core] = inputs_ref[...]
    gather.send(line.place)
    for which in range(3):
        weights[which, seq, fsdp] = sources[which][:, block(seq)]
    gains[seq, fsdp] = gains_ref[...]
    outputs[fsdp] = output_ref[...]

    def forward(owner):
        for step in range(1, fsdp_count):
            column_copy(owner, step).start()
            gain_column_copy(owner, step).start()

    forward(seq)

    @pl.loop(1, seq_count)
    def _(step):
        for which in range(3):
            row_copy(which, step).wait_recv()
        gain_row_copy(step).wait_recv()
        forward((seq - step + seq_count) % seq_count)

    for step in range(1, fsdp_count):
        output_copy(step).start()

    @pl.loop(0, chips)
    def _(step):
        gather.step(step)

    inputs_store = pltpu.make_async_copy(gather.blocks, inputs_out, store_sem.at[0])
    inputs_store.start()

    @pl.loop(0, seq_count)
    def _(owner):
        for step in range(1, fsdp_count):
            column_copy(owner, step).wait_recv()
            gain_column_copy(owner, step).wait_recv()

    weights_store = pltpu.make_async_copy(weights, weights_out, store_sem.at[1])
    weights_store.start()
    for step in range(1, fsdp_count):
        output_copy(step).wait_recv()
    output_store = pltpu.make_async_copy(outputs, output_out, store_sem.at[2])
    output_store.start()
    gains_out[...] = gains[...]

    gather.finish()

    @pl.loop(1, seq_count)
    def _(step):
        for which in range(3):
            row_copy(which, step).wait_send()
        gain_row_copy(step).wait_send()

    @pl.loop(0, seq_count)
    def _(owner):
        for step in range(1, fsdp_count):
            column_copy(owner, step).wait_send()
            gain_column_copy(owner, step).wait_send()

    for step in range(1, fsdp_count):
        output_copy(step).wait_send()
    inputs_store.wait()
    weights_store.wait()
    output_store.wait()


def bring_in(local_in, query_weight, key_weight, value_weight, output_weight, gains):
    rows, width = local_in.shape
    slots = lax.axis_size("seq")
    fsdp_count = lax.axis_size("fsdp")
    chips = slots // 2
    own_rows, columns = query_weight.shape[0], query_weight.shape[1] // slots
    bf16, dma = jnp.bfloat16, pltpu.SemaphoreType.DMA
    lanes = pl.cdiv(gains.shape[1], 128) * 128
    padded = jnp.pad(gains, ((0, 16 - gains.shape[0]), (0, lanes - gains.shape[1])))
    weight_shape = (3, slots, fsdp_count, own_rows, columns)
    inputs_all, weights, outputs, gains_all = pl.pallas_call(
        functools.partial(bring_in_kernel, chips, fsdp_count),
        out_shape=(
            jax.ShapeDtypeStruct((slots, rows, width), bf16),
            jax.ShapeDtypeStruct(weight_shape, bf16),
            jax.ShapeDtypeStruct((fsdp_count, own_rows, width), bf16),
            jax.ShapeDtypeStruct((slots, fsdp_count, 16, lanes), bf16),
        ),
        in_specs=[whole_spec()] * 6,
        out_specs=(far_spec(),) * 3 + (whole_spec(),),
        scratch_shapes=[
            pltpu.VMEM(weight_shape, bf16),
            pltpu.VMEM((fsdp_count, own_rows, width), bf16),
            pltpu.VMEM((slots, fsdp_count, 16, lanes), bf16),
            dma((3, slots)),
            dma((3, slots)),
            dma((slots, fsdp_count)),
            dma((slots, fsdp_count)),
            dma((slots,)),
            dma((slots,)),
            dma((slots, fsdp_count)),
            dma((slots, fsdp_count)),
            dma((fsdp_count,)),
            dma((fsdp_count,)),
            dma((3,)),
        ]
        + Gather.scratch(chips, rows, width),
        compiler_params=line_params(3),
        name="bring_in",
    )(local_in, query_weight, key_weight, value_weight, output_weight, padded)
    gains_all = gains_all[:, :, : gains.shape[0], : gains.shape[1]]
    return (
        inputs_all.reshape(-1, width),
        weights.reshape(3, -1, columns),
        outputs.reshape(-1, width),
        gains_all.transpose(2, 0, 1, 3).reshape(gains.shape[0], -1),
    )


def take_out_kernel(
    chips,
    fsdp_count,
    terms_ref,
    output_ref,
    gains_ref,
    query_ref,
    key_ref,
    value_ref,
    output_out,
    gains_out,
    column_in,
    row_out,
    row_in,
    output_in,
    gain_in,
    gain_out,
    gain_row,
    column_send,
    column_recv,
    row_send,
    row_recv,
    output_send,
    output_recv,
    gain_send,
    gain_recv,
    gain_row_send,
    gain_row_recv,
):
    seq_count = 2 * chips
    seq, seq_peer = peers_of("seq", seq_count)
    fsdp, fsdp_peer = peers_of("fsdp", fsdp_count)
    columns = terms_ref.shape[-1]
    f32 = jnp.float32

    def column_copy(owner, step):
        peer = fsdp_peer(step)
        return pltpu.make_async_remote_copy(
            src_ref=terms_ref.at[:, owner, peer],
            dst_ref=column_in.at[owner, step],
            send_sem=column_send.at[owner, step],
            recv_sem=column_recv.at[owner, step],
            device_id=(seq, peer),
            device_id_type=MESH,
        )

    def row_copy(step):
        peer = seq_peer(step)
        return pltpu.make_async_remote_copy(
            src_ref=row_out.at[step],
            dst_ref=row_in.at[step],
            send_sem=row_send.at[step],
            recv_sem=row_recv.at[step],
            device_id=(peer, fsdp),
            device_id_type=MESH,
        )

    def output_copy(step):
        peer = fsdp_peer(step)
        return pltpu.make_async_remote_copy(
            src_ref=output_ref.at[peer],
            dst_ref=output_in.at[step],
            send_sem=output_send.at[step],
            recv_sem=output_recv.at[step],
            device_id=(seq, peer),
            device_id_type=MESH,
        )

    def gain_copy(step):
        peer = fsdp_peer(step)
        return pltpu.make_async_remote_copy(
            src_ref=gains_ref.at[peer],
            dst_ref=gain_in.at[step],
            send_sem=gain_send.at[step],
            recv_sem=gain_recv.at[step],
            device_id=(seq, peer),
            device_id_type=MESH,
        )

    def gain_row_copy(step):
        peer = seq_peer(step)
        return pltpu.make_async_remote_copy(
            src_ref=gain_out.at[peer],
            dst_ref=gain_row.at[step],
            send_sem=gain_row_send.at[step],
            recv_sem=gain_row_recv.at[step],
            device_id=(peer, fsdp),
            device_id_type=MESH,
        )

    greet_cross(seq_count, fsdp_count)
    for step in range(1, fsdp_count):
        gain_copy(step).start()

    @pl.loop(1, seq_count + 1)
    def _(turn):
        owner = (seq + turn) % seq_count
        for step in range(1, fsdp_count):
            column_copy(owner, step).start()

    for step in range(1, fsdp_count):
        output_copy(step).start()
    total = gains_ref[fsdp]
    for step in range(1, fsdp_count):
        gain_copy(step).wait_recv()
        total = total + gain_in[step]
    gain_out[...] = total
    for step in range(1, seq_count):
        gain_row_copy(step).start()

    def summed(owner):
        for step in range(1, fsdp_count):
            column_copy(owner, step).wait_recv()
        total = terms_ref[:, owner, fsdp].astype(f32)
        for step in range(1, fsdp_count):
            total = total + column_in[owner, step].astype(f32)
        return total

    @pl.loop(1, seq_count)
    def _(turn):
        row_out[turn] = summed((seq + turn) % seq_count).astype(jnp.bfloat16)
        row_copy(turn).start()

    def put(owner, value):
        block = pl.ds(pl.multiple_of(owner * columns, 128), columns)
        query_ref[:, block] = value[0]
        key_ref[:, block] = value[1]
        value_ref[:, block] = value[2]

    put(seq, summed(seq))
    total = output_ref[fsdp].astype(f32)
    for step in range(1, fsdp_count):
        output_copy(step).wait_recv()
        total = total + output_in[step].astype(f32)
    output_out[...] = total
    total = gain_out[seq]
    for step in range(1, seq_count):
        gain_row_copy(step).wait_recv()
        total = total + gain_row[step]
    gains_out[...] = total

    @pl.loop(1, seq_count)
    def _(step):
        row_copy(step).wait_recv()
        put((seq - step + seq_count) % seq_count, row_in[step].astype(f32))

    @pl.loop(0, seq_count)
    def _(owner):
        for step in range(1, fsdp_count):
            column_copy(owner, step).wait_send()

    @pl.loop(1, seq_count)
    def _(step):
        row_copy(step).wait_send()
        gain_row_copy(step).wait_send()

    for step in range(1, fsdp_count):
        output_copy(step).wait_send()
        gain_copy(step).wait_send()


def take_out(terms, output_term, gain_terms):
    slots = lax.axis_size("seq")
    fsdp_count = lax.axis_size("fsdp")
    chips = slots // 2
    _, width, columns = terms.shape
    own = width // (slots * fsdp_count)
    kinds = gain_terms.shape[0]
    bf16, f32, dma = jnp.bfloat16, jnp.float32, pltpu.SemaphoreType.DMA
    gains = gain_terms.reshape(kinds, slots, fsdp_count, own).transpose(2, 1, 0, 3)
    lanes = pl.cdiv(own, 128) * 128
    gains = jnp.pad(gains, ((0, 0), (0, 0), (0, 8 - kinds), (0, lanes - own)))
    block = (3, own, columns)
    query, key, value, output, gains = pl.pallas_call(
        functools.partial(take_out_kernel, chips, fsdp_count),
        out_shape=(jax.ShapeDtypeStruct((own, width), f32),) * 4
        + (jax.ShapeDtypeStruct((8, lanes), f32),),
        in_specs=[whole_spec()] * 3,
        out_specs=(whole_spec(),) * 5,
        scratch_shapes=[
            pltpu.VMEM((slots, fsdp_count) + block, bf16),
            pltpu.VMEM((slots,) + block, bf16),
            pltpu.VMEM((slots,) + block, bf16),
            pltpu.VMEM((fsdp_count, own, width), bf16),
            pltpu.VMEM((fsdp_count, slots, 8, lanes), f32),
            pltpu.VMEM((slots, 8, lanes), f32),
            pltpu.VMEM((slots, 8, lanes), f32),
            dma((slots, fsdp_count)),
            dma((slots, fsdp_count)),
            dma((slots,)),
            dma((slots,)),
            dma((fsdp_count,)),
            dma((fsdp_count,)),
            dma((fsdp_count,)),
            dma((fsdp_count,)),
            dma((slots,)),
            dma((slots,)),
        ],
        compiler_params=line_params(4),
        name="take_out",
    )(
        terms.reshape(3, slots, fsdp_count, own, columns),
        output_term.reshape(fsdp_count, own, width),
        gains,
    )
    return query, key, value, output, gains[:kinds, :own]


def scatter_product_kernel(chips, count, *refs):
    lefts, rights = refs[:count], refs[count : 2 * count]
    result, comm = refs[2 * count], refs[2 * count + 1 :]
    line = Line(chips)
    scatter = Scatter(line, *comm)
    _, rows, width = scatter.fresh.shape
    line.greet()

    @pl.loop(0, chips)
    def _(step):
        chip = line.order(chips - 1 - step)
        pair = pl.ds(chip * 2, 2)

        @pl.loop(0, width // tile_of(width))
        def _(tile):
            columns = pl.ds(pl.multiple_of(tile * tile_of(width), 128), tile_of(width))
            total = None
            for left, right in zip(lefts, rights):
                term = dot_cols(left[pair].reshape(2 * rows, -1), right[columns, :])
                total = term if total is None else total + term
            scatter.fresh[:, :, columns] = total.reshape(2, rows, -1)

        scatter.after_term(chip)

    scatter.finish(result)


def scatter_product(collective_id, name, pairs):
    slots = lax.axis_size("seq")
    chips = slots // 2
    rows = pairs[0][0].shape[0] // slots
    width = pairs[0][1].shape[0]
    return pl.pallas_call(
        functools.partial(scatter_product_kernel, chips, len(pairs)),
        out_shape=jax.ShapeDtypeStruct((rows, width), jnp.float32),
        in_specs=[whole_spec()] * (2 * len(pairs)),
        out_specs=whole_spec(),
        scratch_shapes=Scatter.scratch(chips, rows, width),
        compiler_params=line_params(collective_id),
        name=name,
    )(*[left.reshape(slots, rows, -1) for left, _ in pairs], *[right for _, right in pairs])


def gather_kernel(chips, local_ref, out, store_sem, *comm):
    line = Line(chips)
    gather = Gather(line, *comm)
    line.greet()
    gather.blocks[line.place * 2 + line.core] = local_ref[...]
    gather.send(line.place)

    def store(chip):
        pair = pl.ds(chip * 2, 2)
        return pltpu.make_async_copy(gather.blocks.at[pair], out.at[pair], store_sem.at[chip])

    @pl.loop(0, chips)
    def _(step):
        store(gather.step(step)).start()

    gather.finish()

    @pl.loop(0, chips)
    def _(chip):
        store(chip).wait()


def gather_line(collective_id, name, local):
    rows, width = local.shape
    slots = lax.axis_size("seq")
    chips = slots // 2
    return pl.pallas_call(
        functools.partial(gather_kernel, chips),
        out_shape=jax.ShapeDtypeStruct((slots, rows, width), jnp.bfloat16),
        in_specs=[whole_spec()],
        out_specs=far_spec(),
        scratch_shapes=[pltpu.SemaphoreType.DMA((chips,))] + Gather.scratch(chips, rows, width),
        compiler_params=line_params(collective_id),
        name=name,
    )(local).reshape(-1, width)


def row_exchange(weight):
    return lax.all_to_all(weight, "seq", split_axis=1, concat_axis=0, tiled=True)


def columns_in(part):
    whole = lax.all_gather(part, "fsdp", axis=0, tiled=True)
    return swap_blocks(whole, lax.axis_size("fsdp"), lax.axis_size("seq"))


def columns_out(term):
    seq_count = lax.axis_size("seq")
    fsdp_count = lax.axis_size("fsdp")
    swapped = swap_blocks(term, seq_count, fsdp_count).astype(jnp.bfloat16)
    summed = lax.psum_scatter(swapped, "fsdp", scatter_dimension=0, tiled=True)
    return lax.all_to_all(summed, "seq", split_axis=0, concat_axis=1, tiled=True).astype(
        jnp.float32
    )


def rope_tables(row_count):
    half_width = DH // 2
    frequency = rope_base ** (-jnp.arange(half_width, dtype=jnp.float32) * 2.0 / DH)
    angles = jnp.arange(row_count, dtype=jnp.int32).astype(jnp.float32)[:, None] * frequency[None, :]
    return jnp.cos(angles), jnp.sin(angles)


def rotate(tensor, cosine, sine_table):
    row_count = tensor.shape[0]
    half_width = DH // 2
    grouped = tensor.reshape(row_count, -1, DH)
    first_half = grouped[..., :half_width]
    second_half = grouped[..., half_width:]
    cosine = cosine[:, None, :]
    sine_table = sine_table[:, None, :]
    turned = jnp.concatenate(
        [
            first_half * cosine - second_half * sine_table,
            second_half * cosine + first_half * sine_table,
        ],
        axis=-1,
    )
    return turned.reshape(tensor.shape)


def per_device(
    inputs,
    query_weight,
    key_weight,
    value_weight,
    output_weight,
    query_gain,
    key_gain,
    attention_gain,
    gate_weight,
    up_weight,
    down_weight,
    feedforward_gain,
    segments,
    cotangent,
):
    token_count = inputs.shape[1]
    width_all = inputs.shape[2]
    local_in = inputs.reshape(token_count, width_all)
    segment_row = segments[0]
    score_scale = DH ** (-0.5)
    seq_index = lax.axis_index("seq")
    gate_part, up_part, down_part, local_in, output_own = lax.optimization_barrier(
        (
            row_exchange(gate_weight),
            row_exchange(up_weight),
            row_exchange(down_weight),
            local_in,
            output_weight,
        )
    )
    inputs_all, attention_cols, output_rows, gains = bring_in(
        local_in,
        query_weight,
        key_weight,
        value_weight,
        output_own,
        jnp.stack([query_gain, key_gain, attention_gain, feedforward_gain]),
    )
    query_cols, key_cols, value_cols = attention_cols[0], attention_cols[1], attention_cols[2]
    gains = gains.astype(jnp.float32)
    sequence_rows = inputs_all.shape[0]
    head_width = query_cols.shape[1]
    local_heads = head_width // DH
    query_scale = lax.dynamic_slice_in_dim(gains[0], seq_index * head_width, head_width, 0)
    key_scale = lax.dynamic_slice_in_dim(gains[1], seq_index * head_width, head_width, 0)
    attention_scale = gains[2]
    feedforward_scale = gains[3]
    query_pre = jnp.dot(inputs_all, query_cols, preferred_element_type=jnp.float32)
    key_pre = jnp.dot(inputs_all, key_cols, preferred_element_type=jnp.float32)
    values_low = jnp.dot(inputs_all, value_cols, preferred_element_type=jnp.float32).astype(
        jnp.bfloat16
    )
    squares = lax.psum(
        jnp.stack([jnp.sum(query_pre * query_pre, axis=-1), jnp.sum(key_pre * key_pre, axis=-1)]),
        "seq",
    )
    inverse = lax.rsqrt(squares / width_all + eps_norm)
    query_unit = query_pre * inverse[0][:, None]
    key_unit = key_pre * inverse[1][:, None]
    cosine, sine_table = rope_tables(sequence_rows)
    queries_low = rotate(query_unit * query_scale, cosine, sine_table).astype(jnp.bfloat16)
    keys_low = rotate(key_unit * key_scale, cosine, sine_table).astype(jnp.bfloat16)
    query_heads = queries_low.reshape(sequence_rows, local_heads, DH)
    key_heads = keys_low.reshape(sequence_rows, local_heads, DH)
    value_heads = values_low.reshape(sequence_rows, local_heads, DH)
    block_rows = min(512, sequence_rows)
    block_count = sequence_rows // block_rows
    block_ids = jnp.arange(block_count, dtype=jnp.int32)

    def attend_block(loop_state, block_index):
        first_row = block_index * block_rows
        query_block = lax.dynamic_slice_in_dim(query_heads, first_row, block_rows, 0)
        scores = masked_scores(query_block, key_heads, first_row, segment_row, score_scale)
        row_max = jnp.max(scores, axis=-1, keepdims=True)
        expanded = jnp.exp(scores - row_max)
        row_total = jnp.sum(expanded, axis=-1, keepdims=True)
        softmax_low = (expanded / row_total).astype(jnp.bfloat16)
        block_out = jnp.einsum(
            "hqk,khd->qhd", softmax_low, value_heads, preferred_element_type=jnp.float32
        )
        log_total = (row_max + jnp.log(row_total))[..., 0]
        return (loop_state, (block_out.astype(jnp.bfloat16), log_total))

    _, (out_blocks, log_totals) = lax.scan(attend_block, jnp.zeros((), jnp.int32), block_ids)
    attended_heads = out_blocks.reshape(sequence_rows, head_width)
    projected = scatter_product(5, "project", [(attended_heads, output_rows.T)])
    hidden = local_in.astype(jnp.float32) + rms_scale(projected, attention_scale)
    hidden_low = hidden.astype(jnp.bfloat16)
    gate_cols = columns_in(gate_part)
    up_cols = columns_in(up_part)
    down_cols = columns_in(down_part)
    mixed_pre, gate_linear, up_linear, activated, hidden_all = feed_forward(
        hidden_low, gate_cols, up_cols, down_cols
    )
    result = (
        (hidden + rms_scale(mixed_pre, feedforward_scale))
        .astype(jnp.bfloat16)
        .reshape(1, token_count, width_all)
    )
    grad_result = cotangent.reshape(token_count, width_all).astype(jnp.float32)
    _, mixed_pull = jax.vjp(rms_scale, mixed_pre, feedforward_scale)
    grad_mixed, grad_feedforward_gain = mixed_pull(grad_result)
    grad_mixed_low = grad_mixed.astype(jnp.bfloat16)
    hidden_term, grad_gate_low, grad_upward_low, grad_all = feed_forward_back(
        grad_mixed_low, gate_cols, up_cols, down_cols, gate_linear, up_linear
    )
    grad_hidden = grad_result + hidden_term
    gate_weight_grad = columns_out(contract_rows(hidden_all, grad_gate_low))
    up_weight_grad = columns_out(contract_rows(hidden_all, grad_upward_low))
    down_weight_grad = columns_out(contract_rows(grad_all, activated))
    _, branch_pull = jax.vjp(rms_scale, projected, attention_scale)
    grad_projected, grad_attention_gain = branch_pull(grad_hidden)
    grad_projected_all = gather_line(6, "gather_projected", grad_projected.astype(jnp.bfloat16))
    output_term = contract_rows(attended_heads, grad_projected_all).astype(jnp.bfloat16)
    grad_attended = contract_cols(grad_projected_all, output_rows).astype(jnp.bfloat16)
    grad_out_heads = grad_attended.reshape(sequence_rows, local_heads, DH)

    def attend_back(loop_state, block_index):
        key_total, value_total = loop_state
        first_row = block_index * block_rows
        query_block = lax.dynamic_slice_in_dim(query_heads, first_row, block_rows, 0)
        grad_block = lax.dynamic_slice_in_dim(grad_out_heads, first_row, block_rows, 0)
        log_block = lax.dynamic_index_in_dim(log_totals, block_index, 0, keepdims=False)
        scores = masked_scores(query_block, key_heads, first_row, segment_row, score_scale)
        probabilities = jnp.exp(scores - log_block[..., None])
        softmax_low = probabilities.astype(jnp.bfloat16)
        value_total = value_total + jnp.einsum(
            "hqk,qhd->khd", softmax_low, grad_block, preferred_element_type=jnp.float32
        )
        grad_softmax = jnp.einsum(
            "qhd,khd->hqk", grad_block, value_heads, preferred_element_type=jnp.float32
        )
        row_dot = jnp.sum(probabilities * grad_softmax, axis=-1, keepdims=True)
        grad_scores = (probabilities * (grad_softmax - row_dot)).astype(jnp.bfloat16)
        grad_query_block = (
            jnp.einsum("hqk,khd->qhd", grad_scores, key_heads, preferred_element_type=jnp.float32)
            * score_scale
        )
        key_total = (
            key_total
            + jnp.einsum(
                "hqk,qhd->khd", grad_scores, query_block, preferred_element_type=jnp.float32
            )
            * score_scale
        )
        return ((key_total, value_total), grad_query_block.astype(jnp.bfloat16))

    zero_heads = jnp.zeros((sequence_rows, local_heads, DH), jnp.float32)
    (key_total, value_total), grad_query_blocks = lax.scan(
        attend_back, (zero_heads, zero_heads), block_ids
    )
    grad_queries = grad_query_blocks.reshape(sequence_rows, head_width).astype(jnp.float32)
    grad_keys = (
        key_total.astype(jnp.bfloat16).reshape(sequence_rows, head_width).astype(jnp.float32)
    )
    grad_values = value_total.astype(jnp.bfloat16).reshape(sequence_rows, head_width)
    query_error = rotate(grad_queries, cosine, -sine_table)
    key_error = rotate(grad_keys, cosine, -sine_table)
    grad_query_gain = jnp.sum(query_error * query_unit, axis=0)
    grad_key_gain = jnp.sum(key_error * key_unit, axis=0)
    query_error = query_error * query_scale
    key_error = key_error * key_scale
    means = (
        lax.psum(
            jnp.stack(
                [
                    jnp.sum(query_error * query_unit, axis=-1),
                    jnp.sum(key_error * key_unit, axis=-1),
                ]
            ),
            "seq",
        )
        / width_all
    )
    grad_query_low = (
        inverse[0][:, None] * (query_error - query_unit * means[0][:, None])
    ).astype(jnp.bfloat16)
    grad_key_low = (inverse[1][:, None] * (key_error - key_unit * means[1][:, None])).astype(
        jnp.bfloat16
    )
    grad_input = grad_hidden + scatter_product(
        7,
        "input_back",
        [(grad_query_low, query_cols), (grad_key_low, key_cols), (grad_values, value_cols)],
    )
    attention_terms = jnp.stack(
        [
            contract_rows(inputs_all, grad_query_low).astype(jnp.bfloat16),
            contract_rows(inputs_all, grad_key_low).astype(jnp.bfloat16),
            contract_rows(inputs_all, grad_values).astype(jnp.bfloat16),
        ]
    )
    head_gains = lax.dynamic_update_slice_in_dim(
        jnp.zeros((2, width_all), jnp.float32),
        jnp.stack([grad_query_gain, grad_key_gain]),
        seq_index * head_width,
        1,
    )
    gain_terms = jnp.concatenate(
        [head_gains, jnp.stack([grad_attention_gain, grad_feedforward_gain])], axis=0
    )
    query_weight_grad, key_weight_grad, value_weight_grad, output_weight_grad, gain_grads = (
        take_out(attention_terms, output_term, gain_terms)
    )
    return (
        result,
        grad_input.reshape(1, token_count, width_all),
        query_weight_grad,
        key_weight_grad,
        value_weight_grad,
        output_weight_grad,
        gain_grads[0],
        gain_grads[1],
        gain_grads[2],
        gate_weight_grad,
        up_weight_grad,
        down_weight_grad,
        gain_grads[3],
    )


def solution(mesh):
    in_specs = (
        P("fsdp", "seq", None),
        P(("seq", "fsdp"), None),
        P(("seq", "fsdp"), None),
        P(("seq", "fsdp"), None),
        P(("seq", "fsdp"), None),
        P(("seq", "fsdp")),
        P(("seq", "fsdp")),
        P(("seq", "fsdp")),
        P(("seq", "fsdp"), None),
        P(("seq", "fsdp"), None),
        P(("seq", "fsdp"), None),
        P(("seq", "fsdp")),
        P("fsdp", None),
        P("fsdp", "seq", None),
    )
    out_specs = (
        P("fsdp", "seq", None),
        P("fsdp", "seq", None),
        P(("seq", "fsdp"), None),
        P(("seq", "fsdp"), None),
        P(("seq", "fsdp"), None),
        P(("seq", "fsdp"), None),
        P(("seq", "fsdp")),
        P(("seq", "fsdp")),
        P(("seq", "fsdp")),
        P(("seq", "fsdp"), None),
        P(("seq", "fsdp"), None),
        P(("seq", "fsdp"), None),
        P(("seq", "fsdp")),
    )
    return jax.shard_map(
        per_device, mesh=mesh, in_specs=in_specs, out_specs=out_specs, check_vma=False
    )
```

```python
import functools

import jax
import jax.numpy as jnp
from jax import lax
from jax.experimental import pallas as pl
from jax.experimental.pallas import tpu as pltpu
from jax.sharding import PartitionSpec as P

HEADS = 16
DH = 128


eps_norm = 1e-06
rope_base = 500000.0
neg_fill = -1e30


def rms_scale(tensor, gain):
    return tensor * lax.rsqrt(jnp.mean(tensor * tensor, axis=-1, keepdims=True) + eps_norm) * gain


def rotary(tensor, positions):
    row_count = tensor.shape[0]
    grouped = tensor.reshape(row_count, HEADS, DH)
    half_width = DH // 2
    frequency = rope_base ** (-jnp.arange(half_width, dtype=jnp.float32) * 2.0 / DH)
    angles = positions.astype(jnp.float32)[:, None] * frequency[None, :]
    cosine = jnp.cos(angles)[:, None, :]
    sine_table = jnp.sin(angles)[:, None, :]
    first_half = grouped[..., :half_width]
    second_half = grouped[..., half_width:]
    turned = jnp.concatenate(
        [
            first_half * cosine - second_half * sine_table,
            second_half * cosine + first_half * sine_table,
        ],
        axis=-1,
    )
    return turned.reshape(tensor.shape)


def norm_rotary(tensor, gain, positions):
    return rotary(rms_scale(tensor, gain), positions)


def swiglu_act(gate_linear, up_linear):
    return jax.nn.silu(gate_linear) * up_linear


def contract_rows(left, right):
    return lax.dot_general(
        left, right, (((0,), (0,)), ((), ())), preferred_element_type=jnp.float32
    )


def contract_cols(left, right):
    return lax.dot_general(
        left, right, (((1,), (1,)), ((), ())), preferred_element_type=jnp.float32
    )


def masked_scores(query_block, key_heads, first_row, segment_row, score_scale):
    block_rows = query_block.shape[0]
    sequence_rows = key_heads.shape[0]
    scores = (
        jnp.einsum("qhd,khd->hqk", query_block, key_heads, preferred_element_type=jnp.float32)
        * score_scale
    )
    query_pos = first_row + jnp.arange(block_rows, dtype=jnp.int32)
    key_pos = jnp.arange(sequence_rows, dtype=jnp.int32)
    query_seg = lax.dynamic_slice_in_dim(segment_row, first_row, block_rows, 0)
    allowed = (key_pos[None, :] <= query_pos[:, None]) & (
        segment_row[None, :] == query_seg[:, None]
    )
    return jnp.where(allowed[None], scores, neg_fill)


MESH = pl.DeviceIdType.MESH
RS_PARTS = 4


class Line:
    def __init__(self, chips):
        index = lax.axis_index("seq")
        self.chips = chips
        self.fsdp = lax.axis_index("fsdp")
        self.place = index // 2
        self.core = index % 2

    def device(self, place, core):
        return (place * 2 + core, self.fsdp)

    @property
    def partner(self):
        return self.device(self.place, 1 - self.core)

    @property
    def above(self):
        return self.device(jnp.minimum(self.place + 1, self.chips - 1), self.core)

    @property
    def below(self):
        return self.device(jnp.maximum(self.place - 1, 0), self.core)

    @property
    def has_above(self):
        return self.place < self.chips - 1

    @property
    def has_below(self):
        return self.place > 0

    def greet(self):
        barrier = pltpu.get_barrier_semaphore()
        pl.semaphore_signal(barrier, inc=1, device_id=self.partner, device_id_type=MESH)

        @pl.when(self.has_above)
        def _():
            pl.semaphore_signal(barrier, inc=1, device_id=self.above, device_id_type=MESH)

        @pl.when(self.has_below)
        def _():
            pl.semaphore_signal(barrier, inc=1, device_id=self.below, device_id_type=MESH)

        peers = (
            1 + jnp.minimum(self.place, 1) + jnp.minimum(self.chips - 1 - self.place, 1)
        )
        pl.semaphore_wait(barrier, peers)

    def order(self, step):
        place, last = self.place, self.chips - 1
        near = jnp.minimum(place, last - place)
        both = jnp.where(step % 2 == 1, place - (step + 1) // 2, place + step // 2)
        rest = jnp.where(place <= last - place, step, last - step)
        return jnp.where(step <= 2 * near, both, rest)

    def paired(self, step):
        near = jnp.minimum(self.place, self.chips - 1 - self.place)
        return (step % 2 == 1) & (step <= 2 * near)

    def second_of_pair(self, step):
        near = jnp.minimum(self.place, self.chips - 1 - self.place)
        return (step % 2 == 0) & (step > 0) & (step <= 2 * near)


class Gather:
    def __init__(self, line, blocks, arrive, up_sem, down_sem, side_sem):
        self.line, self.blocks, self.arrive = line, blocks, arrive
        self.up_sem, self.down_sem, self.side_sem = up_sem, down_sem, side_sem

    @staticmethod
    def scratch(chips, rows, width):
        return [
            pltpu.VMEM((2 * chips, rows, width), jnp.bfloat16),
            pltpu.SemaphoreType.DMA((2 * chips,)),
            pltpu.SemaphoreType.DMA((chips,)),
            pltpu.SemaphoreType.DMA((chips,)),
            pltpu.SemaphoreType.DMA((chips,)),
        ]

    def copy(self, chip, sem, target):
        slot = chip * 2 + self.line.core
        return pltpu.make_async_remote_copy(
            src_ref=self.blocks.at[slot],
            dst_ref=self.blocks.at[slot],
            send_sem=sem.at[chip],
            recv_sem=self.arrive.at[slot],
            device_id=target,
            device_id_type=MESH,
        )

    def wait_slot(self, slot):
        pltpu.make_async_remote_copy(
            src_ref=self.blocks.at[slot],
            dst_ref=self.blocks.at[slot],
            send_sem=self.side_sem.at[0],
            recv_sem=self.arrive.at[slot],
            device_id=self.line.partner,
            device_id_type=MESH,
        ).wait_recv()

    def send(self, chip):
        line = self.line

        @pl.when((chip <= line.place) & line.has_above)
        def _():
            self.copy(chip, self.up_sem, line.above).start()

        @pl.when((chip >= line.place) & line.has_below)
        def _():
            self.copy(chip, self.down_sem, line.below).start()

        self.copy(chip, self.side_sem, line.partner).start()

    def take(self, chip):
        self.wait_slot(chip * 2 + self.line.core)
        self.send(chip)

    def step(self, step):
        line = self.line
        chip = line.order(step)

        @pl.when((step > 0) & jnp.logical_not(line.second_of_pair(step)))
        def _():
            self.take(chip)

        @pl.when(line.paired(step))
        def _():
            self.take(line.order(step + 1))

        self.wait_slot(chip * 2 + 1 - line.core)
        return chip

    def finish(self):
        line = self.line

        @pl.loop(0, line.chips)
        def _(chip):
            @pl.when((chip <= line.place) & line.has_above)
            def _():
                self.copy(chip, self.up_sem, line.above).wait_send()

            @pl.when((chip >= line.place) & line.has_below)
            def _():
                self.copy(chip, self.down_sem, line.below).wait_send()

            self.copy(chip, self.side_sem, line.partner).wait_send()


class Scatter:
    def __init__(self, line, fresh, terms, side_out, side_in, out, inward, side_send, side_recv, send_sem, recv_sem):
        self.line, self.fresh, self.terms = line, fresh, terms
        self.side_out, self.side_in = side_out, side_in
        self.out, self.inward = out, inward
        self.side_send, self.side_recv = side_send, side_recv
        self.send_sem, self.recv_sem = send_sem, recv_sem
        self.rows = terms.shape[1] // RS_PARTS

    @staticmethod
    def scratch(chips, rows, width):
        return [
            pltpu.VMEM((2, rows, width), jnp.float32),
            pltpu.VMEM((chips, rows, width), jnp.float32),
            pltpu.VMEM((chips, rows, width), jnp.bfloat16),
            pltpu.VMEM((chips, rows, width), jnp.bfloat16),
            pltpu.VMEM((chips, rows, width), jnp.bfloat16),
            pltpu.VMEM((2, chips, rows, width), jnp.bfloat16),
            pltpu.SemaphoreType.DMA((chips,)),
            pltpu.SemaphoreType.DMA((chips,)),
            pltpu.SemaphoreType.DMA((chips, RS_PARTS)),
            pltpu.SemaphoreType.DMA((2, chips, RS_PARTS)),
        ]

    def side(self, chip):
        return pltpu.make_async_remote_copy(
            src_ref=self.side_out.at[chip],
            dst_ref=self.side_in.at[chip],
            send_sem=self.side_send.at[chip],
            recv_sem=self.side_recv.at[chip],
            device_id=self.line.partner,
            device_id_type=MESH,
        )

    def part(self, chip, part, upward, target):
        rows = pl.ds(part * self.rows, self.rows)
        return pltpu.make_async_remote_copy(
            src_ref=self.out.at[chip, rows],
            dst_ref=self.inward.at[upward, chip, rows],
            send_sem=self.send_sem.at[chip, part],
            recv_sem=self.recv_sem.at[upward, chip, part],
            device_id=target,
            device_id_type=MESH,
        )

    def share(self, chip):
        self.side_out[chip] = self.fresh[1 - self.line.core].astype(jnp.bfloat16)
        self.side(chip).start()
        self.terms[chip] = self.fresh[self.line.core]

    def total(self, chip, part, ways):
        rows = pl.ds(part * self.rows, self.rows)
        total = self.terms[chip, rows] + self.side_in[chip, rows].astype(jnp.float32)
        for way in ways:
            total = total + self.inward[way, chip, rows].astype(jnp.float32)
        return rows, total

    def pass_on(self, chip, upward, first):
        target = self.line.above if upward else self.line.below
        self.side(chip).wait_recv()

        @pl.loop(0, RS_PARTS)
        def _(part):
            if not first:
                self.part(chip, part, upward, target).wait_recv()
            rows, total = self.total(chip, part, () if first else (upward,))
            self.out[chip, rows] = total.astype(jnp.bfloat16)
            self.part(chip, part, upward, target).start()

    def after_term(self, chip):
        line = self.line
        self.share(chip)

        @pl.when((chip < line.place) & jnp.logical_not(line.has_above))
        def _():
            self.pass_on(chip, 0, True)

        @pl.when((chip > line.place) & jnp.logical_not(line.has_below))
        def _():
            self.pass_on(chip, 1, True)

    def hop(self, step):
        line = self.line
        lower = line.place * 2 < line.chips
        up_chip, down_chip = step, line.chips - 1 - step
        go_up = (up_chip > line.place) & line.has_below
        go_down = (down_chip < line.place) & line.has_above

        @pl.when(go_up & lower)
        def _():
            self.pass_on(up_chip, 1, False)

        @pl.when(go_down)
        def _():
            self.pass_on(down_chip, 0, False)

        @pl.when(go_up & jnp.logical_not(lower))
        def _():
            self.pass_on(up_chip, 1, False)

    def settle(self, result):
        line = self.line
        place = line.place
        self.side(place).wait_recv()

        @pl.loop(0, RS_PARTS)
        def _(part):
            @pl.when(line.has_above)
            def _():
                self.part(place, part, 0, line.below).wait_recv()

            @pl.when(line.has_below)
            def _():
                self.part(place, part, 1, line.above).wait_recv()

            @pl.when(line.has_above & line.has_below)
            def _():
                rows, total = self.total(place, part, (0, 1))
                result[rows] = total

            @pl.when(line.has_above & jnp.logical_not(line.has_below))
            def _():
                rows, total = self.total(place, part, (0,))
                result[rows] = total

            @pl.when(line.has_below & jnp.logical_not(line.has_above))
            def _():
                rows, total = self.total(place, part, (1,))
                result[rows] = total

    def hops(self):
        @pl.loop(0, self.line.chips)
        def _(step):
            self.hop(step)

    def finish(self):
        line = self.line

        @pl.loop(0, line.chips)
        def _(chip):
            self.side(chip).wait_send()

            @pl.when(chip != line.place)
            def _():
                @pl.loop(0, RS_PARTS)
                def _(part):
                    self.part(chip, part, 0, line.below).wait_send()


def tile_of(extent):
    return min(256, extent)


def dot_cols(left, right):
    return lax.dot_general(
        left, right, (((1,), (1,)), ((), ())), preferred_element_type=jnp.float32
    )


def load(pairs):
    copies = [pltpu.make_async_copy(src, dst, sem) for src, dst, sem in pairs]
    for copy in copies:
        copy.start()
    return copies


def feed_forward_kernel(
    chips,
    hidden_ref,
    gate_hbm,
    up_hbm,
    down_hbm,
    mixed_ref,
    gate_out,
    up_out,
    act_out,
    all_out,
    gate_w,
    up_w,
    down_w,
    gate_keep,
    up_keep,
    act_keep,
    load_sem,
    store_sem,
    *comm,
):
    line = Line(chips)
    gather = Gather(line, *comm[:5])
    scatter = Scatter(line, *comm[5:])
    blocks, fresh = gather.blocks, scatter.fresh
    _, rows, width = blocks.shape
    units = gate_w.shape[1]
    copies = load(
        [
            (gate_hbm, gate_w, load_sem.at[0]),
            (up_hbm, up_w, load_sem.at[1]),
            (down_hbm, down_w, load_sem.at[2]),
        ]
    )
    line.greet()
    blocks[line.place * 2 + line.core] = hidden_ref[...]
    gather.send(line.place)

    def stores(chip):
        pair = pl.ds(chip * 2, 2)
        return [
            pltpu.make_async_copy(gate_keep.at[pair], gate_out.at[pair], store_sem.at[0, chip]),
            pltpu.make_async_copy(up_keep.at[pair], up_out.at[pair], store_sem.at[1, chip]),
            pltpu.make_async_copy(act_keep.at[pair], act_out.at[pair], store_sem.at[2, chip]),
            pltpu.make_async_copy(blocks.at[pair], all_out.at[pair], store_sem.at[3, chip]),
        ]

    for copy in copies:
        copy.wait()

    @pl.loop(0, chips)
    def _(step):
        chip = gather.step(step)
        pair = pl.ds(chip * 2, 2)

        @pl.loop(0, units // tile_of(units))
        def _(tile):
            columns = pl.ds(pl.multiple_of(tile * tile_of(units), 128), tile_of(units))
            tokens = blocks[pair].reshape(2 * rows, width)
            gate = jnp.dot(tokens, gate_w[:, columns], preferred_element_type=jnp.float32)
            up = jnp.dot(tokens, up_w[:, columns], preferred_element_type=jnp.float32)
            gate_keep[pair, :, columns] = gate.reshape(2, rows, -1)
            up_keep[pair, :, columns] = up.reshape(2, rows, -1)
            act_keep[pair, :, columns] = (
                (gate / (1.0 + jnp.exp(-gate)) * up).astype(jnp.bfloat16).reshape(2, rows, -1)
            )

        @pl.loop(0, width // tile_of(width))
        def _(tile):
            columns = pl.ds(pl.multiple_of(tile * tile_of(width), 128), tile_of(width))
            act = act_keep[pair].reshape(2 * rows, units)
            fresh[:, :, columns] = dot_cols(act, down_w[columns, :]).reshape(2, rows, -1)

        for copy in stores(chip):
            copy.start()
        scatter.after_term(chip)

    scatter.hops()
    scatter.settle(mixed_ref)
    scatter.finish()
    gather.finish()

    @pl.loop(0, chips)
    def _(chip):
        for copy in stores(chip):
            copy.wait()


def feed_forward_back_kernel(
    chips,
    grad_ref,
    gate_hbm,
    up_hbm,
    down_hbm,
    gate_lin_hbm,
    up_lin_hbm,
    hidden_grad_ref,
    gate_out,
    up_out,
    all_out,
    gate_w,
    up_w,
    down_w,
    gate_lin,
    up_lin,
    gate_keep,
    up_keep,
    load_sem,
    store_sem,
    *comm,
):
    line = Line(chips)
    gather = Gather(line, *comm[:5])
    scatter = Scatter(line, *comm[5:])
    blocks, fresh = gather.blocks, scatter.fresh
    _, rows, width = blocks.shape
    units = gate_w.shape[1]
    copies = load(
        [
            (down_hbm, down_w, load_sem.at[0]),
            (gate_lin_hbm, gate_lin, load_sem.at[1]),
            (up_lin_hbm, up_lin, load_sem.at[2]),
            (gate_hbm, gate_w, load_sem.at[3]),
            (up_hbm, up_w, load_sem.at[4]),
        ]
    )
    line.greet()
    blocks[line.place * 2 + line.core] = grad_ref[...]
    gather.send(line.place)

    def stores(chip):
        pair = pl.ds(chip * 2, 2)
        return [
            pltpu.make_async_copy(gate_keep.at[pair], gate_out.at[pair], store_sem.at[0, chip]),
            pltpu.make_async_copy(up_keep.at[pair], up_out.at[pair], store_sem.at[1, chip]),
            pltpu.make_async_copy(blocks.at[pair], all_out.at[pair], store_sem.at[2, chip]),
        ]

    for copy in copies:
        copy.wait()

    @pl.loop(0, chips)
    def _(step):
        chip = gather.step(step)
        pair = pl.ds(chip * 2, 2)

        @pl.loop(0, units // tile_of(units))
        def _(tile):
            columns = pl.ds(pl.multiple_of(tile * tile_of(units), 128), tile_of(units))
            tokens = blocks[pair].reshape(2 * rows, width)
            grad = jnp.dot(tokens, down_w[:, columns], preferred_element_type=jnp.float32)
            gate = gate_lin[pair, :, columns].reshape(2 * rows, -1)
            up = up_lin[pair, :, columns].reshape(2 * rows, -1)
            sig = 1.0 / (1.0 + jnp.exp(-gate))
            gate_keep[pair, :, columns] = (
                (grad * up * sig * (1.0 + gate * (1.0 - sig)))
                .astype(jnp.bfloat16)
                .reshape(2, rows, -1)
            )
            up_keep[pair, :, columns] = (
                (grad * (gate * sig)).astype(jnp.bfloat16).reshape(2, rows, -1)
            )

        @pl.loop(0, width // tile_of(width))
        def _(tile):
            columns = pl.ds(pl.multiple_of(tile * tile_of(width), 128), tile_of(width))
            gate = gate_keep[pair].reshape(2 * rows, units)
            up = up_keep[pair].reshape(2 * rows, units)
            fresh[:, :, columns] = (
                dot_cols(gate, gate_w[columns, :]) + dot_cols(up, up_w[columns, :])
            ).reshape(2, rows, -1)

        for copy in stores(chip):
            copy.start()
        scatter.after_term(chip)

    scatter.hops()
    scatter.settle(hidden_grad_ref)
    scatter.finish()
    gather.finish()

    @pl.loop(0, chips)
    def _(chip):
        for copy in stores(chip):
            copy.wait()


def whole_spec():
    return pl.BlockSpec(memory_space=pltpu.VMEM)


def far_spec():
    return pl.BlockSpec(memory_space=pl.ANY)


def line_params(collective_id):
    return pltpu.CompilerParams(
        collective_id=collective_id, has_side_effects=True, vmem_limit_bytes=60 * 2**20
    )


def feed_forward(hidden_low, gate_cols, up_cols, down_cols):
    rows, width = hidden_low.shape
    units = gate_cols.shape[1]
    slots = lax.axis_size("seq")
    chips = slots // 2
    weights = [pltpu.VMEM((width, units), jnp.bfloat16)] * 3
    mixed, gate, up, act, every = pl.pallas_call(
        functools.partial(feed_forward_kernel, chips),
        out_shape=(
            jax.ShapeDtypeStruct((rows, width), jnp.float32),
            jax.ShapeDtypeStruct((slots, rows, units), jnp.float32),
            jax.ShapeDtypeStruct((slots, rows, units), jnp.float32),
            jax.ShapeDtypeStruct((slots, rows, units), jnp.bfloat16),
            jax.ShapeDtypeStruct((slots, rows, width), jnp.bfloat16),
        ),
        in_specs=[whole_spec()] + [far_spec()] * 3,
        out_specs=(whole_spec(),) + (far_spec(),) * 4,
        scratch_shapes=weights
        + [
            pltpu.VMEM((slots, rows, units), jnp.float32),
            pltpu.VMEM((slots, rows, units), jnp.float32),
            pltpu.VMEM((slots, rows, units), jnp.bfloat16),
            pltpu.SemaphoreType.DMA((3,)),
            pltpu.SemaphoreType.DMA((4, chips)),
        ]
        + Gather.scratch(chips, rows, width)
        + Scatter.scratch(chips, rows, width),
        compiler_params=line_params(1),
        name="feed_forward",
    )(hidden_low, gate_cols, up_cols, down_cols)
    return mixed, gate, up, act.reshape(-1, units), every.reshape(-1, width)


def feed_forward_back(grad_low, gate_cols, up_cols, down_cols, gate, up):
    rows, width = grad_low.shape
    units = gate_cols.shape[1]
    slots = lax.axis_size("seq")
    chips = slots // 2
    weights = [pltpu.VMEM((width, units), jnp.bfloat16)] * 3
    hidden_grad, gate_grad, up_grad, every = pl.pallas_call(
        functools.partial(feed_forward_back_kernel, chips),
        out_shape=(
            jax.ShapeDtypeStruct((rows, width), jnp.float32),
            jax.ShapeDtypeStruct((slots, rows, units), jnp.bfloat16),
            jax.ShapeDtypeStruct((slots, rows, units), jnp.bfloat16),
            jax.ShapeDtypeStruct((slots, rows, width), jnp.bfloat16),
        ),
        in_specs=[whole_spec()] + [far_spec()] * 5,
        out_specs=(whole_spec(),) + (far_spec(),) * 3,
        scratch_shapes=weights
        + [
            pltpu.VMEM((slots, rows, units), jnp.float32),
            pltpu.VMEM((slots, rows, units), jnp.float32),
            pltpu.VMEM((slots, rows, units), jnp.bfloat16),
            pltpu.VMEM((slots, rows, units), jnp.bfloat16),
            pltpu.SemaphoreType.DMA((5,)),
            pltpu.SemaphoreType.DMA((3, chips)),
        ]
        + Gather.scratch(chips, rows, width)
        + Scatter.scratch(chips, rows, width),
        compiler_params=line_params(2),
        name="feed_forward_back",
    )(grad_low, gate_cols, up_cols, down_cols, gate, up)
    return (
        hidden_grad,
        gate_grad.reshape(-1, units),
        up_grad.reshape(-1, units),
        every.reshape(-1, width),
    )


def peers_of(axis, size):
    me = lax.axis_index(axis)
    return me, lambda step: (me + step) % size


def greet_cross(seq_count, fsdp_count):
    seq, seq_peer = peers_of("seq", seq_count)
    fsdp, fsdp_peer = peers_of("fsdp", fsdp_count)
    barrier = pltpu.get_barrier_semaphore()
    for step in range(1, seq_count):
        pl.semaphore_signal(
            barrier, inc=1, device_id=(seq_peer(step), fsdp), device_id_type=MESH
        )
    for step in range(1, fsdp_count):
        pl.semaphore_signal(
            barrier, inc=1, device_id=(seq, fsdp_peer(step)), device_id_type=MESH
        )
    pl.semaphore_wait(barrier, seq_count + fsdp_count - 2)


class Cross:
    def __init__(self, seq_count, fsdp_count):
        self.seq_count, self.fsdp_count = seq_count, fsdp_count
        self.seq, self.seq_peer = peers_of("seq", seq_count)
        self.fsdp, self.fsdp_peer = peers_of("fsdp", fsdp_count)
        self.square = fsdp_count == 4
        if self.square:
            row, place = self.fsdp // 2, self.fsdp % 2
            self.sides = (row * 2 + 1 - place, (1 - row) * 2 + place)
            self.corner = (1 - row) * 2 + 1 - place
        else:
            self.sides = tuple(self.fsdp_peer(step) for step in range(1, fsdp_count))

    def remote(self, src, dst, send, recv, seq, fsdp):
        return pltpu.make_async_remote_copy(
            src_ref=src,
            dst_ref=dst,
            send_sem=send,
            recv_sem=recv,
            device_id=(seq, fsdp),
            device_id_type=MESH,
        )


class Spread:
    def __init__(self, cross, sources, weights, row_send, row_recv, side_send, side_recv, half_send, half_recv):
        self.cross, self.sources, self.weights = cross, sources, weights
        self.row_send, self.row_recv = row_send, row_recv
        self.side_send, self.side_recv = side_send, side_recv
        self.half_send, self.half_recv = half_send, half_recv
        self.kinds, self.columns = len(sources), weights.shape[-1]
        self.rows = weights.shape[-2]

    @staticmethod
    def scratch(kinds, seq_count, fsdp_count, rows, columns):
        dma = pltpu.SemaphoreType.DMA
        sides = 2 if fsdp_count == 4 else fsdp_count - 1
        return [
            pltpu.VMEM((kinds, seq_count, fsdp_count, rows, columns), jnp.bfloat16),
            dma((kinds, seq_count)),
            dma((kinds, seq_count)),
            dma((seq_count, sides)),
            dma((seq_count, sides)),
            dma((seq_count, 2)),
            dma((seq_count, 2)),
        ]

    def block(self, owner):
        return pl.ds(pl.multiple_of(owner * self.columns, 128), self.columns)

    def row(self, kind, step):
        cross = self.cross
        peer = cross.seq_peer(step)
        return cross.remote(
            self.sources[kind].at[:, self.block(peer)],
            self.weights.at[kind, cross.seq, cross.fsdp],
            self.row_send.at[kind, step],
            self.row_recv.at[kind, step],
            peer,
            cross.fsdp,
        )

    def side(self, owner, side):
        cross = self.cross
        ref = self.weights.at[:, owner, cross.fsdp]
        return cross.remote(
            ref,
            ref,
            self.side_send.at[owner, side],
            self.side_recv.at[owner, side],
            cross.seq,
            cross.sides[side],
        )

    def half(self, owner, side):
        cross = self.cross
        rows = pl.ds(side * (self.rows // 2), self.rows // 2)
        ref = self.weights.at[:, owner, cross.sides[side], rows]
        return cross.remote(
            ref,
            ref,
            self.half_send.at[owner, side],
            self.half_recv.at[owner, side],
            cross.seq,
            cross.sides[1 - side],
        )

    def start(self):
        cross = self.cross
        for step in range(1, cross.seq_count):
            for kind in range(self.kinds):
                self.row(kind, step).start()

    def own(self):
        cross = self.cross
        for kind in range(self.kinds):
            self.weights[kind, cross.seq, cross.fsdp] = self.sources[kind][:, self.block(cross.seq)]
        self.pass_on(0)

    def owner(self, step):
        return (self.cross.seq - step + self.cross.seq_count) % self.cross.seq_count

    def take(self, step):
        for kind in range(self.kinds):
            self.row(kind, step).wait_recv()
        self.pass_on(step)

    def pass_on(self, step):
        for side in range(len(self.cross.sides)):
            self.side(self.owner(step), side).start()

    def relay(self, step):
        owner = self.owner(step)
        for side in range(len(self.cross.sides)):
            self.side(owner, side).wait_recv()
            if self.cross.square:
                self.half(owner, side).start()

    def settle(self, step):
        if self.cross.square:
            for side in range(2):
                self.half(self.owner(step), side).wait_recv()

    def finish(self):
        cross = self.cross

        @pl.loop(1, cross.seq_count)
        def _(step):
            for kind in range(self.kinds):
                self.row(kind, step).wait_send()

        @pl.loop(0, cross.seq_count)
        def _(owner):
            for side in range(len(cross.sides)):
                self.side(owner, side).wait_send()
                if cross.square:
                    self.half(owner, side).wait_send()


class Collect:
    def __init__(self, cross, terms, side_in, half_out, half_in, row_out, row_in, side_send, side_recv, half_send, half_recv, row_send, row_recv):
        self.cross, self.terms = cross, terms
        self.side_in, self.half_out, self.half_in = side_in, half_out, half_in
        self.row_out, self.row_in = row_out, row_in
        self.side_send, self.side_recv = side_send, side_recv
        self.half_send, self.half_recv = half_send, half_recv
        self.row_send, self.row_recv = row_send, row_recv
        self.rows, self.columns = terms.shape[-2:]
        self.kinds = terms.shape[:-4]

    @staticmethod
    def scratch(seq_count, fsdp_count, rows, columns):
        dma = pltpu.SemaphoreType.DMA
        vmem = pltpu.VMEM
        bf16 = jnp.bfloat16
        if fsdp_count == 4:
            arrays = [
                vmem((seq_count, 2, 2, rows // 2, columns), bf16),
                vmem((seq_count, 2, rows // 2, columns), bf16),
                vmem((seq_count, 2, rows // 2, columns), bf16),
            ]
            sides = (2, 2)
        else:
            arrays = [
                vmem((seq_count, fsdp_count - 1, rows, columns), bf16),
                vmem((1, 1, 16, 128), bf16),
                vmem((1, 1, 16, 128), bf16),
            ]
            sides = (fsdp_count - 1, 1)
        return arrays + [
            vmem((seq_count, rows, columns), bf16),
            vmem((seq_count, rows, columns), bf16),
            dma((seq_count,) + sides),
            dma((seq_count,) + sides),
            dma((seq_count, 2)),
            dma((seq_count, 2)),
            dma((seq_count,)),
            dma((seq_count,)),
        ]

    def half_rows(self, side):
        return pl.ds(side * (self.rows // 2), self.rows // 2)

    def side(self, owner, side, which):
        cross = self.cross
        if not cross.square:
            return cross.remote(
                self.terms.at[owner, cross.sides[side]],
                self.side_in.at[owner, side],
                self.side_send.at[owner, side, 0],
                self.side_recv.at[owner, side, 0],
                cross.seq,
                cross.sides[side],
            )
        target = cross.sides[side] if which == 0 else cross.corner
        return cross.remote(
            self.terms.at[owner, target, self.half_rows(side)],
            self.side_in.at[owner, side, which],
            self.side_send.at[owner, side, which],
            self.side_recv.at[owner, side, which],
            cross.seq,
            cross.sides[side],
        )

    def half(self, owner, side):
        cross = self.cross
        return cross.remote(
            self.half_out.at[owner, side],
            self.half_in.at[owner, side],
            self.half_send.at[owner, side],
            self.half_recv.at[owner, side],
            cross.seq,
            cross.sides[1 - side],
        )

    def row(self, step):
        cross = self.cross
        return cross.remote(
            self.row_out.at[step],
            self.row_in.at[step],
            self.row_send.at[step],
            self.row_recv.at[step],
            cross.seq_peer(step),
            cross.fsdp,
        )

    def owner(self, turn):
        return self.cross.seq_peer(turn + 1)

    @property
    def ways(self):
        return range(2) if self.cross.square else range(1)

    def send(self, turn):
        owner = self.owner(turn)
        for which in reversed(self.ways):
            for side in range(len(self.cross.sides)):
                self.side(owner, side, which).start()

    def middle(self, turn):
        if not self.cross.square:
            return
        cross, owner = self.cross, self.owner(turn)
        for side in range(2):
            self.side(owner, side, 1).wait_recv()
            mine = self.terms[owner, cross.sides[1 - side], self.half_rows(side)]
            self.half_out[owner, side] = (
                mine.astype(jnp.float32) + self.side_in[owner, side, 1].astype(jnp.float32)
            ).astype(jnp.bfloat16)
            self.half(owner, side).start()

    def totals(self, turn):
        cross, owner = self.cross, self.owner(turn)
        found = []
        if cross.square:
            for side in range(2):
                self.side(owner, side, 0).wait_recv()
                self.half(owner, side).wait_recv()
                rows = self.half_rows(side)
                total = self.terms[owner, cross.fsdp, rows].astype(jnp.float32)
                total = total + self.side_in[owner, side, 0].astype(jnp.float32)
                total = total + self.half_in[owner, side].astype(jnp.float32)
                found.append((rows, total))
        else:
            total = self.terms[owner, cross.fsdp].astype(jnp.float32)
            for side in range(len(cross.sides)):
                self.side(owner, side, 0).wait_recv()
                total = total + self.side_in[owner, side].astype(jnp.float32)
            found.append((pl.ds(0, self.rows), total))
        return found

    def ship(self, turn):
        for rows, total in self.totals(turn):
            self.row_out[turn + 1, rows] = total.astype(jnp.bfloat16)
        self.row(turn + 1).start()

    def block(self, owner):
        return pl.ds(pl.multiple_of(owner * self.columns, 128), self.columns)

    def keep(self, result):
        cross = self.cross
        for rows, total in self.totals(cross.seq_count - 1):
            result[rows, self.block(cross.seq)] = total

    def receive(self, step, result):
        cross = self.cross
        self.row(step).wait_recv()
        owner = (cross.seq - step + cross.seq_count) % cross.seq_count
        result[:, self.block(owner)] = self.row_in[step].astype(jnp.float32)

    def finish(self):
        cross = self.cross

        @pl.loop(0, cross.seq_count)
        def _(owner):
            for side in range(len(cross.sides)):
                for which in self.ways:
                    self.side(owner, side, which).wait_send()
                if cross.square:
                    self.half(owner, side).wait_send()

        @pl.loop(1, cross.seq_count)
        def _(step):
            self.row(step).wait_send()


def bring_in_kernel(
    chips,
    fsdp_count,
    inputs_ref,
    query_ref,
    key_ref,
    value_ref,
    output_ref,
    gate_ref,
    gains_ref,
    inputs_out,
    weights_out,
    output_out,
    gate_out,
    gains_out,
    outputs,
    gains,
    gain_row_send,
    gain_row_recv,
    gain_column_send,
    gain_column_recv,
    output_send,
    output_recv,
    store_sem,
    *comm,
):
    line = Line(chips)
    cross = Cross(2 * chips, fsdp_count)
    gather = Gather(line, *comm[:5])
    attention = Spread(cross, (query_ref, key_ref, value_ref), *comm[5:12])
    gate = Spread(cross, (gate_ref,), *comm[12:])
    seq_count, seq, fsdp = cross.seq_count, cross.seq, cross.fsdp

    def gain_row(step):
        return cross.remote(
            gains_ref,
            gains.at[seq, fsdp],
            gain_row_send.at[step],
            gain_row_recv.at[step],
            cross.seq_peer(step),
            fsdp,
        )

    def gain_column(owner, step):
        ref = gains.at[owner, fsdp]
        return cross.remote(
            ref,
            ref,
            gain_column_send.at[owner, step],
            gain_column_recv.at[owner, step],
            seq,
            cross.fsdp_peer(step),
        )

    def output_copy(step):
        return cross.remote(
            output_ref,
            outputs.at[fsdp],
            output_send.at[step],
            output_recv.at[step],
            seq,
            cross.fsdp_peer(step),
        )

    greet_cross(seq_count, fsdp_count)
    for step in range(1, seq_count):
        gain_row(step).start()
    attention.start()
    gather.blocks[line.place * 2 + line.core] = inputs_ref[...]
    gather.send(line.place)
    gate.start()
    gains[seq, fsdp] = gains_ref[...]
    outputs[fsdp] = output_ref[...]
    attention.own()
    for step in range(1, fsdp_count):
        gain_column(seq, step).start()

    @pl.loop(1, seq_count)
    def _(step):
        attention.take(step)
        gain_row(step).wait_recv()
        for peer in range(1, fsdp_count):
            gain_column(attention.owner(step), peer).start()

    gate.own()
    for step in range(1, fsdp_count):
        output_copy(step).start()

    @pl.loop(0, chips)
    def _(step):
        gather.step(step)
        for late in range(2):
            attention.relay(2 * step + late)

            @pl.when(2 * step + late > 0)
            def _():
                gate.take(2 * step + late)

    inputs_store = pltpu.make_async_copy(gather.blocks, inputs_out, store_sem.at[0])
    inputs_store.start()

    @pl.loop(0, seq_count)
    def _(step):
        gate.relay(step)
        attention.settle(step)
        for peer in range(1, fsdp_count):
            gain_column(step, peer).wait_recv()

    weights_store = pltpu.make_async_copy(attention.weights, weights_out, store_sem.at[1])
    weights_store.start()
    for step in range(1, fsdp_count):
        output_copy(step).wait_recv()
    output_store = pltpu.make_async_copy(outputs, output_out, store_sem.at[2])
    output_store.start()
    gains_out[...] = gains[...]

    @pl.loop(0, seq_count)
    def _(step):
        gate.settle(step)

    gate_store = pltpu.make_async_copy(gate.weights, gate_out, store_sem.at[3])
    gate_store.start()
    gather.finish()
    attention.finish()
    gate.finish()

    @pl.loop(1, seq_count)
    def _(step):
        gain_row(step).wait_send()

    @pl.loop(0, seq_count)
    def _(owner):
        for step in range(1, fsdp_count):
            gain_column(owner, step).wait_send()

    for step in range(1, fsdp_count):
        output_copy(step).wait_send()
    inputs_store.wait()
    weights_store.wait()
    output_store.wait()
    gate_store.wait()


def bring_in(local_in, query_weight, key_weight, value_weight, output_weight, gate_weight, gains):
    rows, width = local_in.shape
    slots = lax.axis_size("seq")
    fsdp_count = lax.axis_size("fsdp")
    chips = slots // 2
    own_rows, columns = query_weight.shape[0], query_weight.shape[1] // slots
    units = gate_weight.shape[1] // slots
    bf16, dma = jnp.bfloat16, pltpu.SemaphoreType.DMA
    lanes = pl.cdiv(gains.shape[1], 128) * 128
    padded = jnp.pad(gains, ((0, 16 - gains.shape[0]), (0, lanes - gains.shape[1])))
    inputs_all, weights, outputs, gate, gains_all = pl.pallas_call(
        functools.partial(bring_in_kernel, chips, fsdp_count),
        out_shape=(
            jax.ShapeDtypeStruct((slots, rows, width), bf16),
            jax.ShapeDtypeStruct((3, slots, fsdp_count, own_rows, columns), bf16),
            jax.ShapeDtypeStruct((fsdp_count, own_rows, width), bf16),
            jax.ShapeDtypeStruct((1, slots, fsdp_count, own_rows, units), bf16),
            jax.ShapeDtypeStruct((slots, fsdp_count, 16, lanes), bf16),
        ),
        in_specs=[whole_spec()] * 7,
        out_specs=(far_spec(),) * 4 + (whole_spec(),),
        scratch_shapes=[
            pltpu.VMEM((fsdp_count, own_rows, width), bf16),
            pltpu.VMEM((slots, fsdp_count, 16, lanes), bf16),
            dma((slots,)),
            dma((slots,)),
            dma((slots, fsdp_count)),
            dma((slots, fsdp_count)),
            dma((fsdp_count,)),
            dma((fsdp_count,)),
            dma((4,)),
        ]
        + Gather.scratch(chips, rows, width)
        + Spread.scratch(3, slots, fsdp_count, own_rows, columns)
        + Spread.scratch(1, slots, fsdp_count, own_rows, units),
        compiler_params=line_params(3),
        name="bring_in",
    )(local_in, query_weight, key_weight, value_weight, output_weight, gate_weight, padded)
    gains_all = gains_all[:, :, : gains.shape[0], : gains.shape[1]]
    return (
        inputs_all.reshape(-1, width),
        weights.reshape(3, -1, columns),
        outputs.reshape(-1, width),
        gate.reshape(-1, units),
        gains_all.transpose(2, 0, 1, 3).reshape(gains.shape[0], -1),
    )


def product_terms(scatter, pairs, chip):
    _, rows, width = scatter.fresh.shape
    pair = pl.ds(chip * 2, 2)

    @pl.loop(0, width // tile_of(width))
    def _(tile):
        columns = pl.ds(pl.multiple_of(tile * tile_of(width), 128), tile_of(width))
        total = None
        for left, right, across in pairs:
            tokens = left[pair].reshape(2 * rows, -1)
            if across:
                term = dot_cols(tokens, right[columns, :])
            else:
                term = jnp.dot(tokens, right[:, columns], preferred_element_type=jnp.float32)
            total = term if total is None else total + term
        scatter.fresh[:, :, columns] = total.reshape(2, rows, -1)

    scatter.after_term(chip)


def project_kernel(
    chips,
    fsdp_count,
    attended_ref,
    output_ref,
    up_ref,
    down_ref,
    result,
    up_out,
    down_out,
    store_sem,
    *comm,
):
    line = Line(chips)
    cross = Cross(2 * chips, fsdp_count)
    count = len(Scatter.scratch(chips, 4, 128))
    scatter = Scatter(line, *comm[:count])
    up = Spread(cross, (up_ref,), *comm[count : count + 7])
    down = Spread(cross, (down_ref,), *comm[count + 7 :])
    greet_cross(cross.seq_count, fsdp_count)
    up.start()
    up.own()

    @pl.loop(0, chips)
    def _(step):
        product_terms(scatter, [(attended_ref, output_ref, False)], line.order(chips - 1 - step))

    down.start()

    @pl.loop(1, cross.seq_count)
    def _(step):
        up.take(step)
        up.relay(step - 1)

    down.own()

    @pl.loop(0, chips)
    def _(step):
        scatter.hop(step)
        for late in range(2):

            @pl.when(2 * step + late > 0)
            def _():
                down.take(2 * step + late)

    up.relay(cross.seq_count - 1)

    @pl.loop(0, cross.seq_count)
    def _(step):
        down.relay(step)
        up.settle(step)

    up_store = pltpu.make_async_copy(up.weights, up_out, store_sem.at[0])
    up_store.start()
    scatter.settle(result)

    @pl.loop(0, cross.seq_count)
    def _(step):
        down.settle(step)

    down_store = pltpu.make_async_copy(down.weights, down_out, store_sem.at[1])
    down_store.start()
    scatter.finish()
    up.finish()
    down.finish()
    up_store.wait()
    down_store.wait()


def project(attended, output_rows, up_weight, down_weight):
    slots = lax.axis_size("seq")
    fsdp_count = lax.axis_size("fsdp")
    chips = slots // 2
    rows = attended.shape[0] // slots
    width = output_rows.shape[1]
    own_rows, units = up_weight.shape[0], up_weight.shape[1] // slots
    weight = jax.ShapeDtypeStruct((1, slots, fsdp_count, own_rows, units), jnp.bfloat16)
    projected, up, down = pl.pallas_call(
        functools.partial(project_kernel, chips, fsdp_count),
        out_shape=(jax.ShapeDtypeStruct((rows, width), jnp.float32), weight, weight),
        in_specs=[whole_spec()] * 4,
        out_specs=(whole_spec(), far_spec(), far_spec()),
        scratch_shapes=[pltpu.SemaphoreType.DMA((2,))]
        + Scatter.scratch(chips, rows, width)
        + Spread.scratch(1, slots, fsdp_count, own_rows, units) * 2,
        compiler_params=line_params(5),
        name="project",
    )(attended.reshape(slots, rows, -1), output_rows, up_weight, down_weight)
    return projected, up.reshape(-1, units), down.reshape(-1, units)


def gather_back_kernel(chips, fsdp_count, count, local_ref, *refs):
    terms, refs = refs[:count], refs[count:]
    out, results, store_sem, comm = refs[0], refs[1 : 1 + count], refs[1 + count], refs[2 + count :]
    line = Line(chips)
    cross = Cross(2 * chips, fsdp_count)
    gather = Gather(line, *comm[:5])
    collects = [
        Collect(cross, terms[kind], *comm[5 + 11 * kind : 16 + 11 * kind]) for kind in range(count)
    ]
    seq_count = cross.seq_count
    greet_cross(seq_count, fsdp_count)
    gather.blocks[line.place * 2 + line.core] = local_ref[...]
    gather.send(line.place)

    def store(chip):
        pair = pl.ds(chip * 2, 2)
        return pltpu.make_async_copy(gather.blocks.at[pair], out.at[pair], store_sem.at[chip])

    for collect in collects:

        @pl.loop(0, seq_count)
        def _(turn):
            collect.send(turn)

    store(gather.step(0)).start()
    for kind, collect in enumerate(collects):
        collect.middle(0)

        @pl.loop(1, seq_count)
        def _(turn):
            collect.middle(turn)
            collect.ship(turn - 1)
            if kind == 0:

                @pl.when((turn % 2 == 1) & ((turn + 1) // 2 < chips))
                def _():
                    store(gather.step((turn + 1) // 2)).start()

        collect.keep(results[kind])

    for kind, collect in enumerate(collects):

        @pl.loop(1, seq_count)
        def _(step):
            collect.receive(step, results[kind])

        collect.finish()

    gather.finish()

    @pl.loop(0, chips)
    def _(chip):
        store(chip).wait()


def gather_back(local, terms):
    rows, width = local.shape
    slots = lax.axis_size("seq")
    fsdp_count = lax.axis_size("fsdp")
    chips = slots // 2
    own = terms[0].shape[0] // (slots * fsdp_count)
    units = terms[0].shape[1]
    found = pl.pallas_call(
        functools.partial(gather_back_kernel, chips, fsdp_count, len(terms)),
        out_shape=(jax.ShapeDtypeStruct((slots, rows, width), jnp.bfloat16),)
        + (jax.ShapeDtypeStruct((own, units * slots), jnp.float32),) * len(terms),
        in_specs=[whole_spec()] * (1 + len(terms)),
        out_specs=(far_spec(),) + (whole_spec(),) * len(terms),
        scratch_shapes=[pltpu.SemaphoreType.DMA((chips,))]
        + Gather.scratch(chips, rows, width)
        + Collect.scratch(slots, fsdp_count, own, units) * len(terms),
        compiler_params=line_params(6),
        name="gather_back",
    )(local, *[term.reshape(slots, fsdp_count, own, units) for term in terms])
    return (found[0].reshape(-1, width),) + tuple(found[1:])


def take_out_kernel(
    chips,
    fsdp_count,
    *refs,
):
    lefts, rights, refs = refs[:3], refs[3:6], refs[6:]
    terms, output_ref, gains_ref, refs = refs[0], refs[1], refs[2], refs[3:]
    result, weight_out, output_out, gains_out, refs = refs[0], refs[1], refs[2], refs[3], refs[4:]
    output_in, gain_in, gain_out, gain_rows, refs = refs[0], refs[1], refs[2], refs[3], refs[4:]
    output_send, output_recv, gain_send, gain_recv, gain_row_send, gain_row_recv = refs[:6]
    comm = refs[6:]
    line = Line(chips)
    cross = Cross(2 * chips, fsdp_count)
    scatter = Scatter(line, *comm[:-11])
    collect = Collect(cross, terms, *comm[-11:])
    seq_count, seq, fsdp = cross.seq_count, cross.seq, cross.fsdp

    def output_copy(step):
        peer = cross.fsdp_peer(step)
        return cross.remote(
            output_ref.at[peer],
            output_in.at[step],
            output_send.at[step],
            output_recv.at[step],
            seq,
            peer,
        )

    def gain_copy(step):
        peer = cross.fsdp_peer(step)
        return cross.remote(
            gains_ref.at[peer], gain_in.at[step], gain_send.at[step], gain_recv.at[step], seq, peer
        )

    def gain_row(step):
        peer = cross.seq_peer(step)
        return cross.remote(
            gain_out.at[peer],
            gain_rows.at[step],
            gain_row_send.at[step],
            gain_row_recv.at[step],
            peer,
            fsdp,
        )

    greet_cross(seq_count, fsdp_count)
    for step in range(1, fsdp_count):
        gain_copy(step).start()

    @pl.loop(0, seq_count)
    def _(turn):
        collect.send(turn)

    for step in range(1, fsdp_count):
        output_copy(step).start()

    @pl.loop(0, chips)
    def _(step):
        product_terms(
            scatter,
            [(left, right, True) for left, right in zip(lefts, rights)],
            line.order(chips - 1 - step),
        )

    total = gains_ref[fsdp]
    for step in range(1, fsdp_count):
        gain_copy(step).wait_recv()
        total = total + gain_in[step]
    gain_out[...] = total
    for step in range(1, seq_count):
        gain_row(step).start()

    collect.middle(0)

    @pl.loop(1, seq_count)
    def _(turn):
        collect.middle(turn)
        collect.ship(turn - 1)

        @pl.when(turn % 2 == 1)
        def _():
            scatter.hop(turn // 2)

    collect.keep(weight_out)
    total = output_ref[fsdp].astype(jnp.float32)
    for step in range(1, fsdp_count):
        output_copy(step).wait_recv()
        total = total + output_in[step].astype(jnp.float32)
    output_out[...] = total
    scatter.settle(result)
    total = gain_out[seq]
    for step in range(1, seq_count):
        gain_row(step).wait_recv()
        total = total + gain_rows[step]
    gains_out[...] = total

    @pl.loop(1, seq_count)
    def _(step):
        collect.receive(step, weight_out)

    scatter.finish()
    collect.finish()

    @pl.loop(1, seq_count)
    def _(step):
        gain_row(step).wait_send()

    for step in range(1, fsdp_count):
        output_copy(step).wait_send()
        gain_copy(step).wait_send()


def take_out(pairs, terms, output_term, gain_terms):
    slots = lax.axis_size("seq")
    fsdp_count = lax.axis_size("fsdp")
    chips = slots // 2
    width, columns = terms.shape
    rows = pairs[0][0].shape[0] // slots
    own = width // (slots * fsdp_count)
    kinds = gain_terms.shape[0]
    bf16, f32, dma = jnp.bfloat16, jnp.float32, pltpu.SemaphoreType.DMA
    gains = gain_terms.reshape(kinds, slots, fsdp_count, own).transpose(2, 1, 0, 3)
    lanes = pl.cdiv(own, 128) * 128
    gains = jnp.pad(gains, ((0, 0), (0, 0), (0, 8 - kinds), (0, lanes - own)))
    result, weights, output, gains = pl.pallas_call(
        functools.partial(take_out_kernel, chips, fsdp_count),
        out_shape=(
            jax.ShapeDtypeStruct((rows, width), f32),
            jax.ShapeDtypeStruct((own, columns * slots), f32),
            jax.ShapeDtypeStruct((own, width), f32),
            jax.ShapeDtypeStruct((8, lanes), f32),
        ),
        in_specs=[whole_spec()] * 9,
        out_specs=(whole_spec(),) * 4,
        scratch_shapes=[
            pltpu.VMEM((fsdp_count, own, width), bf16),
            pltpu.VMEM((fsdp_count, slots, 8, lanes), f32),
            pltpu.VMEM((slots, 8, lanes), f32),
            pltpu.VMEM((slots, 8, lanes), f32),
            dma((fsdp_count,)),
            dma((fsdp_count,)),
            dma((fsdp_count,)),
            dma((fsdp_count,)),
            dma((slots,)),
            dma((slots,)),
        ]
        + Scatter.scratch(chips, rows, width)
        + Collect.scratch(slots, fsdp_count, own, columns),
        compiler_params=line_params(4),
        name="take_out",
    )(
        *[left.reshape(slots, rows, -1) for left, _ in pairs],
        *[right for _, right in pairs],
        terms.reshape(slots, fsdp_count, own, columns),
        output_term.reshape(fsdp_count, own, width),
        gains,
    )
    weights = weights.reshape(own, slots, 3, columns // 3)
    weights = [weights[:, :, kind].reshape(own, -1) for kind in range(3)]
    return result, weights, output, gains[:kinds, :own]


def row_sum_kernel(seq_count, local_ref, result, every, send, recv):
    seq, seq_peer = peers_of("seq", seq_count)
    fsdp = lax.axis_index("fsdp")
    barrier = pltpu.get_barrier_semaphore()
    for step in range(1, seq_count):
        pl.semaphore_signal(
            barrier, inc=1, device_id=(seq_peer(step), fsdp), device_id_type=MESH
        )
    pl.semaphore_wait(barrier, seq_count - 1)
    copies = [
        pltpu.make_async_remote_copy(
            src_ref=local_ref,
            dst_ref=every.at[step],
            send_sem=send.at[step],
            recv_sem=recv.at[step],
            device_id=(seq_peer(step), fsdp),
            device_id_type=MESH,
        )
        for step in range(1, seq_count)
    ]
    for copy in copies:
        copy.start()
    total = local_ref[...]
    for step in range(1, seq_count):
        copies[step - 1].wait_recv()
        total = total + every[step]
    result[...] = total
    for copy in copies:
        copy.wait_send()


def row_sum(collective_id, name, local):
    slots = lax.axis_size("seq")
    flat = local.reshape(-1, 128)
    return pl.pallas_call(
        functools.partial(row_sum_kernel, slots),
        out_shape=jax.ShapeDtypeStruct(flat.shape, jnp.float32),
        in_specs=[whole_spec()],
        out_specs=whole_spec(),
        scratch_shapes=[
            pltpu.VMEM((slots,) + flat.shape, jnp.float32),
            pltpu.SemaphoreType.DMA((slots,)),
            pltpu.SemaphoreType.DMA((slots,)),
        ],
        compiler_params=line_params(collective_id),
        name=name,
    )(flat).reshape(local.shape)


def rope_tables(row_count):
    half_width = DH // 2
    frequency = rope_base ** (-jnp.arange(half_width, dtype=jnp.float32) * 2.0 / DH)
    angles = jnp.arange(row_count, dtype=jnp.int32).astype(jnp.float32)[:, None] * frequency[None, :]
    return jnp.cos(angles), jnp.sin(angles)


def rotate(tensor, cosine, sine_table):
    row_count = tensor.shape[0]
    half_width = DH // 2
    grouped = tensor.reshape(row_count, -1, DH)
    first_half = grouped[..., :half_width]
    second_half = grouped[..., half_width:]
    cosine = cosine[:, None, :]
    sine_table = sine_table[:, None, :]
    turned = jnp.concatenate(
        [
            first_half * cosine - second_half * sine_table,
            second_half * cosine + first_half * sine_table,
        ],
        axis=-1,
    )
    return turned.reshape(tensor.shape)


def per_device(
    inputs,
    query_weight,
    key_weight,
    value_weight,
    output_weight,
    query_gain,
    key_gain,
    attention_gain,
    gate_weight,
    up_weight,
    down_weight,
    feedforward_gain,
    segments,
    cotangent,
):
    token_count = inputs.shape[1]
    width_all = inputs.shape[2]
    local_in = inputs.reshape(token_count, width_all)
    segment_row = segments[0]
    score_scale = DH ** (-0.5)
    seq_index = lax.axis_index("seq")
    inputs_all, attention_cols, output_rows, gate_cols, gains = bring_in(
        local_in,
        query_weight,
        key_weight,
        value_weight,
        output_weight,
        gate_weight,
        jnp.stack([query_gain, key_gain, attention_gain, feedforward_gain]),
    )
    query_cols, key_cols, value_cols = attention_cols[0], attention_cols[1], attention_cols[2]
    gains = gains.astype(jnp.float32)
    sequence_rows = inputs_all.shape[0]
    head_width = query_cols.shape[1]
    local_heads = head_width // DH
    query_scale = lax.dynamic_slice_in_dim(gains[0], seq_index * head_width, head_width, 0)
    key_scale = lax.dynamic_slice_in_dim(gains[1], seq_index * head_width, head_width, 0)
    attention_scale = gains[2]
    feedforward_scale = gains[3]
    query_pre = jnp.dot(inputs_all, query_cols, preferred_element_type=jnp.float32)
    key_pre = jnp.dot(inputs_all, key_cols, preferred_element_type=jnp.float32)
    values_low = jnp.dot(inputs_all, value_cols, preferred_element_type=jnp.float32).astype(
        jnp.bfloat16
    )
    squares = row_sum(
        7,
        "square_sum",
        jnp.stack([jnp.sum(query_pre * query_pre, axis=-1), jnp.sum(key_pre * key_pre, axis=-1)]),
    )
    inverse = lax.rsqrt(squares / width_all + eps_norm)
    query_unit = query_pre * inverse[0][:, None]
    key_unit = key_pre * inverse[1][:, None]
    cosine, sine_table = rope_tables(sequence_rows)
    queries_low = rotate(query_unit * query_scale, cosine, sine_table).astype(jnp.bfloat16)
    keys_low = rotate(key_unit * key_scale, cosine, sine_table).astype(jnp.bfloat16)
    query_heads = queries_low.reshape(sequence_rows, local_heads, DH)
    key_heads = keys_low.reshape(sequence_rows, local_heads, DH)
    value_heads = values_low.reshape(sequence_rows, local_heads, DH)
    block_rows = min(512, sequence_rows)
    block_count = sequence_rows // block_rows
    block_ids = jnp.arange(block_count, dtype=jnp.int32)

    def attend_block(loop_state, block_index):
        first_row = block_index * block_rows
        query_block = lax.dynamic_slice_in_dim(query_heads, first_row, block_rows, 0)
        scores = masked_scores(query_block, key_heads, first_row, segment_row, score_scale)
        row_max = jnp.max(scores, axis=-1, keepdims=True)
        expanded = jnp.exp(scores - row_max)
        row_total = jnp.sum(expanded, axis=-1, keepdims=True)
        softmax_low = (expanded / row_total).astype(jnp.bfloat16)
        block_out = jnp.einsum(
            "hqk,khd->qhd", softmax_low, value_heads, preferred_element_type=jnp.float32
        )
        log_total = (row_max + jnp.log(row_total))[..., 0]
        return (loop_state, (block_out.astype(jnp.bfloat16), log_total))

    _, (out_blocks, log_totals) = lax.scan(attend_block, jnp.zeros((), jnp.int32), block_ids)
    attended_heads = out_blocks.reshape(sequence_rows, head_width)
    projected, up_cols, down_cols = project(attended_heads, output_rows, up_weight, down_weight)
    hidden = local_in.astype(jnp.float32) + rms_scale(projected, attention_scale)
    hidden_low = hidden.astype(jnp.bfloat16)
    mixed_pre, gate_linear, up_linear, activated, hidden_all = feed_forward(
        hidden_low, gate_cols, up_cols, down_cols
    )
    result = (
        (hidden + rms_scale(mixed_pre, feedforward_scale))
        .astype(jnp.bfloat16)
        .reshape(1, token_count, width_all)
    )
    grad_result = cotangent.reshape(token_count, width_all).astype(jnp.float32)
    _, mixed_pull = jax.vjp(rms_scale, mixed_pre, feedforward_scale)
    grad_mixed, grad_feedforward_gain = mixed_pull(grad_result)
    grad_mixed_low = grad_mixed.astype(jnp.bfloat16)
    hidden_term, grad_gate_low, grad_upward_low, grad_all = feed_forward_back(
        grad_mixed_low, gate_cols, up_cols, down_cols, gate_linear, up_linear
    )
    grad_hidden = grad_result + hidden_term
    _, branch_pull = jax.vjp(rms_scale, projected, attention_scale)
    grad_projected, grad_attention_gain = branch_pull(grad_hidden)
    grad_projected_all, gate_weight_grad, up_weight_grad, down_weight_grad = gather_back(
        grad_projected.astype(jnp.bfloat16),
        [
            contract_rows(hidden_all, grad_gate_low).astype(jnp.bfloat16),
            contract_rows(hidden_all, grad_upward_low).astype(jnp.bfloat16),
            contract_rows(grad_all, activated).astype(jnp.bfloat16),
        ],
    )
    output_term = contract_rows(attended_heads, grad_projected_all).astype(jnp.bfloat16)
    grad_attended = contract_cols(grad_projected_all, output_rows).astype(jnp.bfloat16)
    grad_out_heads = grad_attended.reshape(sequence_rows, local_heads, DH)

    def attend_back(loop_state, block_index):
        key_total, value_total = loop_state
        first_row = block_index * block_rows
        query_block = lax.dynamic_slice_in_dim(query_heads, first_row, block_rows, 0)
        grad_block = lax.dynamic_slice_in_dim(grad_out_heads, first_row, block_rows, 0)
        log_block = lax.dynamic_index_in_dim(log_totals, block_index, 0, keepdims=False)
        scores = masked_scores(query_block, key_heads, first_row, segment_row, score_scale)
        probabilities = jnp.exp(scores - log_block[..., None])
        softmax_low = probabilities.astype(jnp.bfloat16)
        value_total = value_total + jnp.einsum(
            "hqk,qhd->khd", softmax_low, grad_block, preferred_element_type=jnp.float32
        )
        grad_softmax = jnp.einsum(
            "qhd,khd->hqk", grad_block, value_heads, preferred_element_type=jnp.float32
        )
        row_dot = jnp.sum(probabilities * grad_softmax, axis=-1, keepdims=True)
        grad_scores = (probabilities * (grad_softmax - row_dot)).astype(jnp.bfloat16)
        grad_query_block = (
            jnp.einsum("hqk,khd->qhd", grad_scores, key_heads, preferred_element_type=jnp.float32)
            * score_scale
        )
        key_total = (
            key_total
            + jnp.einsum(
                "hqk,qhd->khd", grad_scores, query_block, preferred_element_type=jnp.float32
            )
            * score_scale
        )
        return ((key_total, value_total), grad_query_block.astype(jnp.bfloat16))

    zero_heads = jnp.zeros((sequence_rows, local_heads, DH), jnp.float32)
    (key_total, value_total), grad_query_blocks = lax.scan(
        attend_back, (zero_heads, zero_heads), block_ids
    )
    grad_queries = grad_query_blocks.reshape(sequence_rows, head_width).astype(jnp.float32)
    grad_keys = (
        key_total.astype(jnp.bfloat16).reshape(sequence_rows, head_width).astype(jnp.float32)
    )
    grad_values = value_total.astype(jnp.bfloat16).reshape(sequence_rows, head_width)
    query_error = rotate(grad_queries, cosine, -sine_table)
    key_error = rotate(grad_keys, cosine, -sine_table)
    grad_query_gain = jnp.sum(query_error * query_unit, axis=0)
    grad_key_gain = jnp.sum(key_error * key_unit, axis=0)
    query_error = query_error * query_scale
    key_error = key_error * key_scale
    means = (
        row_sum(
            8,
            "mean_sum",
            jnp.stack(
                [
                    jnp.sum(query_error * query_unit, axis=-1),
                    jnp.sum(key_error * key_unit, axis=-1),
                ]
            ),
        )
        / width_all
    )
    grad_query_low = (
        inverse[0][:, None] * (query_error - query_unit * means[0][:, None])
    ).astype(jnp.bfloat16)
    grad_key_low = (inverse[1][:, None] * (key_error - key_unit * means[1][:, None])).astype(
        jnp.bfloat16
    )
    grads_low = jnp.concatenate([grad_query_low, grad_key_low, grad_values], axis=1)
    attention_terms = contract_rows(inputs_all, grads_low).astype(jnp.bfloat16)
    head_gains = lax.dynamic_update_slice_in_dim(
        jnp.zeros((2, width_all), jnp.float32),
        jnp.stack([grad_query_gain, grad_key_gain]),
        seq_index * head_width,
        1,
    )
    gain_terms = jnp.concatenate(
        [head_gains, jnp.stack([grad_attention_gain, grad_feedforward_gain])], axis=0
    )
    input_term, attention_grads, output_weight_grad, gain_grads = take_out(
        [(grad_query_low, query_cols), (grad_key_low, key_cols), (grad_values, value_cols)],
        attention_terms,
        output_term,
        gain_terms,
    )
    query_weight_grad, key_weight_grad, value_weight_grad = attention_grads
    grad_input = grad_hidden + input_term
    return (
        result,
        grad_input.reshape(1, token_count, width_all),
        query_weight_grad,
        key_weight_grad,
        value_weight_grad,
        output_weight_grad,
        gain_grads[0],
        gain_grads[1],
        gain_grads[2],
        gate_weight_grad,
        up_weight_grad,
        down_weight_grad,
        gain_grads[3],
    )


def solution(mesh):
    in_specs = (
        P("fsdp", "seq", None),
        P(("seq", "fsdp"), None),
        P(("seq", "fsdp"), None),
        P(("seq", "fsdp"), None),
        P(("seq", "fsdp"), None),
        P(("seq", "fsdp")),
        P(("seq", "fsdp")),
        P(("seq", "fsdp")),
        P(("seq", "fsdp"), None),
        P(("seq", "fsdp"), None),
        P(("seq", "fsdp"), None),
        P(("seq", "fsdp")),
        P("fsdp", None),
        P("fsdp", "seq", None),
    )
    out_specs = (
        P("fsdp", "seq", None),
        P("fsdp", "seq", None),
        P(("seq", "fsdp"), None),
        P(("seq", "fsdp"), None),
        P(("seq", "fsdp"), None),
        P(("seq", "fsdp"), None),
        P(("seq", "fsdp")),
        P(("seq", "fsdp")),
        P(("seq", "fsdp")),
        P(("seq", "fsdp"), None),
        P(("seq", "fsdp"), None),
        P(("seq", "fsdp"), None),
        P(("seq", "fsdp")),
    )
    return jax.shard_map(
        per_device, mesh=mesh, in_specs=in_specs, out_specs=out_specs, check_vma=False
    )
```

```python
import functools

import jax
import jax.numpy as jnp
from jax import lax
from jax.experimental import pallas as pl
from jax.experimental.pallas import tpu as pltpu
from jax.sharding import PartitionSpec as P

HEADS = 16
DH = 128


eps_norm = 1e-06
rope_base = 500000.0
neg_fill = -1e30


def rms_scale(tensor, gain):
    return tensor * lax.rsqrt(jnp.mean(tensor * tensor, axis=-1, keepdims=True) + eps_norm) * gain


def rotary(tensor, positions):
    row_count = tensor.shape[0]
    grouped = tensor.reshape(row_count, HEADS, DH)
    half_width = DH // 2
    frequency = rope_base ** (-jnp.arange(half_width, dtype=jnp.float32) * 2.0 / DH)
    angles = positions.astype(jnp.float32)[:, None] * frequency[None, :]
    cosine = jnp.cos(angles)[:, None, :]
    sine_table = jnp.sin(angles)[:, None, :]
    first_half = grouped[..., :half_width]
    second_half = grouped[..., half_width:]
    turned = jnp.concatenate(
        [
            first_half * cosine - second_half * sine_table,
            second_half * cosine + first_half * sine_table,
        ],
        axis=-1,
    )
    return turned.reshape(tensor.shape)


def norm_rotary(tensor, gain, positions):
    return rotary(rms_scale(tensor, gain), positions)


def swiglu_act(gate_linear, up_linear):
    return jax.nn.silu(gate_linear) * up_linear


def contract_rows(left, right):
    return lax.dot_general(
        left, right, (((0,), (0,)), ((), ())), preferred_element_type=jnp.float32
    )


def contract_cols(left, right):
    return lax.dot_general(
        left, right, (((1,), (1,)), ((), ())), preferred_element_type=jnp.float32
    )


def masked_scores(query_block, key_heads, first_row, segment_row, score_scale):
    block_rows = query_block.shape[0]
    sequence_rows = key_heads.shape[0]
    scores = (
        jnp.einsum("qhd,khd->hqk", query_block, key_heads, preferred_element_type=jnp.float32)
        * score_scale
    )
    query_pos = first_row + jnp.arange(block_rows, dtype=jnp.int32)
    key_pos = jnp.arange(sequence_rows, dtype=jnp.int32)
    query_seg = lax.dynamic_slice_in_dim(segment_row, first_row, block_rows, 0)
    allowed = (key_pos[None, :] <= query_pos[:, None]) & (
        segment_row[None, :] == query_seg[:, None]
    )
    return jnp.where(allowed[None], scores, neg_fill)


MESH = pl.DeviceIdType.MESH
RS_PARTS = 4


class Line:
    def __init__(self, chips):
        index = lax.axis_index("seq")
        self.chips = chips
        self.fsdp = lax.axis_index("fsdp")
        self.place = index // 2
        self.core = index % 2

    def device(self, place, core):
        return (place * 2 + core, self.fsdp)

    @property
    def partner(self):
        return self.device(self.place, 1 - self.core)

    @property
    def above(self):
        return self.device(jnp.minimum(self.place + 1, self.chips - 1), self.core)

    @property
    def below(self):
        return self.device(jnp.maximum(self.place - 1, 0), self.core)

    @property
    def has_above(self):
        return self.place < self.chips - 1

    @property
    def has_below(self):
        return self.place > 0

    def greet(self):
        barrier = pltpu.get_barrier_semaphore()
        pl.semaphore_signal(barrier, inc=1, device_id=self.partner, device_id_type=MESH)

        @pl.when(self.has_above)
        def _():
            pl.semaphore_signal(barrier, inc=1, device_id=self.above, device_id_type=MESH)

        @pl.when(self.has_below)
        def _():
            pl.semaphore_signal(barrier, inc=1, device_id=self.below, device_id_type=MESH)

        peers = (
            1 + jnp.minimum(self.place, 1) + jnp.minimum(self.chips - 1 - self.place, 1)
        )
        pl.semaphore_wait(barrier, peers)

    def order(self, step):
        place, last = self.place, self.chips - 1
        near = jnp.minimum(place, last - place)
        both = jnp.where(step % 2 == 1, place - (step + 1) // 2, place + step // 2)
        rest = jnp.where(place <= last - place, step, last - step)
        return jnp.where(step <= 2 * near, both, rest)

    def paired(self, step):
        near = jnp.minimum(self.place, self.chips - 1 - self.place)
        return (step % 2 == 1) & (step <= 2 * near)

    def second_of_pair(self, step):
        near = jnp.minimum(self.place, self.chips - 1 - self.place)
        return (step % 2 == 0) & (step > 0) & (step <= 2 * near)


class Gather:
    def __init__(self, line, blocks, arrive, up_sem, down_sem, side_sem):
        self.line, self.blocks, self.arrive = line, blocks, arrive
        self.up_sem, self.down_sem, self.side_sem = up_sem, down_sem, side_sem

    @staticmethod
    def scratch(chips, rows, width):
        return [
            pltpu.VMEM((2 * chips, rows, width), jnp.bfloat16),
            pltpu.SemaphoreType.DMA((2 * chips,)),
            pltpu.SemaphoreType.DMA((chips,)),
            pltpu.SemaphoreType.DMA((chips,)),
            pltpu.SemaphoreType.DMA((chips,)),
        ]

    def copy(self, chip, sem, target):
        slot = chip * 2 + self.line.core
        return pltpu.make_async_remote_copy(
            src_ref=self.blocks.at[slot],
            dst_ref=self.blocks.at[slot],
            send_sem=sem.at[chip],
            recv_sem=self.arrive.at[slot],
            device_id=target,
            device_id_type=MESH,
        )

    def wait_slot(self, slot):
        pltpu.make_async_remote_copy(
            src_ref=self.blocks.at[slot],
            dst_ref=self.blocks.at[slot],
            send_sem=self.side_sem.at[0],
            recv_sem=self.arrive.at[slot],
            device_id=self.line.partner,
            device_id_type=MESH,
        ).wait_recv()

    def send(self, chip):
        line = self.line

        @pl.when((chip <= line.place) & line.has_above)
        def _():
            self.copy(chip, self.up_sem, line.above).start()

        @pl.when((chip >= line.place) & line.has_below)
        def _():
            self.copy(chip, self.down_sem, line.below).start()

        self.copy(chip, self.side_sem, line.partner).start()

    def take(self, chip):
        self.wait_slot(chip * 2 + self.line.core)
        self.send(chip)

    def step(self, step):
        line = self.line
        chip = line.order(step)

        @pl.when((step > 0) & jnp.logical_not(line.second_of_pair(step)))
        def _():
            self.take(chip)

        @pl.when(line.paired(step))
        def _():
            self.take(line.order(step + 1))

        self.wait_slot(chip * 2 + 1 - line.core)
        return chip

    def finish(self):
        line = self.line

        @pl.loop(0, line.chips)
        def _(chip):
            @pl.when((chip <= line.place) & line.has_above)
            def _():
                self.copy(chip, self.up_sem, line.above).wait_send()

            @pl.when((chip >= line.place) & line.has_below)
            def _():
                self.copy(chip, self.down_sem, line.below).wait_send()

            self.copy(chip, self.side_sem, line.partner).wait_send()


class Scatter:
    def __init__(self, line, fresh, terms, side_out, side_in, out, inward, side_send, side_recv, send_sem, recv_sem):
        self.line, self.fresh, self.terms = line, fresh, terms
        self.side_out, self.side_in = side_out, side_in
        self.out, self.inward = out, inward
        self.side_send, self.side_recv = side_send, side_recv
        self.send_sem, self.recv_sem = send_sem, recv_sem
        self.rows = terms.shape[1] // RS_PARTS

    @staticmethod
    def scratch(chips, rows, width):
        return [
            pltpu.VMEM((2, rows, width), jnp.float32),
            pltpu.VMEM((chips, rows, width), jnp.float32),
            pltpu.VMEM((chips, rows, width), jnp.bfloat16),
            pltpu.VMEM((chips, rows, width), jnp.bfloat16),
            pltpu.VMEM((chips, rows, width), jnp.bfloat16),
            pltpu.VMEM((2, chips, rows, width), jnp.bfloat16),
            pltpu.SemaphoreType.DMA((chips,)),
            pltpu.SemaphoreType.DMA((chips,)),
            pltpu.SemaphoreType.DMA((chips, RS_PARTS)),
            pltpu.SemaphoreType.DMA((2, chips, RS_PARTS)),
        ]

    def side(self, chip):
        return pltpu.make_async_remote_copy(
            src_ref=self.side_out.at[chip],
            dst_ref=self.side_in.at[chip],
            send_sem=self.side_send.at[chip],
            recv_sem=self.side_recv.at[chip],
            device_id=self.line.partner,
            device_id_type=MESH,
        )

    def part(self, chip, part, upward, target):
        rows = pl.ds(part * self.rows, self.rows)
        return pltpu.make_async_remote_copy(
            src_ref=self.out.at[chip, rows],
            dst_ref=self.inward.at[upward, chip, rows],
            send_sem=self.send_sem.at[chip, part],
            recv_sem=self.recv_sem.at[upward, chip, part],
            device_id=target,
            device_id_type=MESH,
        )

    def share(self, chip):
        self.side_out[chip] = self.fresh[1 - self.line.core].astype(jnp.bfloat16)
        self.side(chip).start()
        self.terms[chip] = self.fresh[self.line.core]

    def total(self, chip, part, ways):
        rows = pl.ds(part * self.rows, self.rows)
        total = self.terms[chip, rows] + self.side_in[chip, rows].astype(jnp.float32)
        for way in ways:
            total = total + self.inward[way, chip, rows].astype(jnp.float32)
        return rows, total

    def pass_on(self, chip, upward, first):
        target = self.line.above if upward else self.line.below
        self.side(chip).wait_recv()

        @pl.loop(0, RS_PARTS)
        def _(part):
            if not first:
                self.part(chip, part, upward, target).wait_recv()
            rows, total = self.total(chip, part, () if first else (upward,))
            self.out[chip, rows] = total.astype(jnp.bfloat16)
            self.part(chip, part, upward, target).start()

    def after_term(self, chip):
        line = self.line
        self.share(chip)

        @pl.when((chip < line.place) & jnp.logical_not(line.has_above))
        def _():
            self.pass_on(chip, 0, True)

        @pl.when((chip > line.place) & jnp.logical_not(line.has_below))
        def _():
            self.pass_on(chip, 1, True)

    def hop(self, step):
        line = self.line
        lower = line.place * 2 < line.chips
        up_chip, down_chip = step, line.chips - 1 - step
        go_up = (up_chip > line.place) & line.has_below
        go_down = (down_chip < line.place) & line.has_above

        @pl.when(go_up & lower)
        def _():
            self.pass_on(up_chip, 1, False)

        @pl.when(go_down)
        def _():
            self.pass_on(down_chip, 0, False)

        @pl.when(go_up & jnp.logical_not(lower))
        def _():
            self.pass_on(up_chip, 1, False)

    def settle(self, result):
        line = self.line
        place = line.place
        self.side(place).wait_recv()

        @pl.loop(0, RS_PARTS)
        def _(part):
            @pl.when(line.has_above)
            def _():
                self.part(place, part, 0, line.below).wait_recv()

            @pl.when(line.has_below)
            def _():
                self.part(place, part, 1, line.above).wait_recv()

            @pl.when(line.has_above & line.has_below)
            def _():
                rows, total = self.total(place, part, (0, 1))
                result[rows] = total

            @pl.when(line.has_above & jnp.logical_not(line.has_below))
            def _():
                rows, total = self.total(place, part, (0,))
                result[rows] = total

            @pl.when(line.has_below & jnp.logical_not(line.has_above))
            def _():
                rows, total = self.total(place, part, (1,))
                result[rows] = total

    def hops(self):
        @pl.loop(0, self.line.chips)
        def _(step):
            self.hop(step)

    def finish(self):
        line = self.line

        @pl.loop(0, line.chips)
        def _(chip):
            self.side(chip).wait_send()

            @pl.when(chip != line.place)
            def _():
                @pl.loop(0, RS_PARTS)
                def _(part):
                    self.part(chip, part, 0, line.below).wait_send()


def tile_of(extent):
    return min(256, extent)


def dot_cols(left, right):
    return lax.dot_general(
        left, right, (((1,), (1,)), ((), ())), preferred_element_type=jnp.float32
    )


def load(pairs):
    copies = [pltpu.make_async_copy(src, dst, sem) for src, dst, sem in pairs]
    for copy in copies:
        copy.start()
    return copies


def feed_forward_kernel(
    chips,
    hidden_ref,
    gate_hbm,
    up_hbm,
    down_hbm,
    mixed_ref,
    gate_out,
    up_out,
    act_out,
    all_out,
    gate_w,
    up_w,
    down_w,
    gate_keep,
    up_keep,
    act_keep,
    load_sem,
    store_sem,
    *comm,
):
    line = Line(chips)
    gather = Gather(line, *comm[:5])
    scatter = Scatter(line, *comm[5:])
    blocks, fresh = gather.blocks, scatter.fresh
    _, rows, width = blocks.shape
    units = gate_w.shape[1]
    copies = load(
        [
            (gate_hbm, gate_w, load_sem.at[0]),
            (up_hbm, up_w, load_sem.at[1]),
            (down_hbm, down_w, load_sem.at[2]),
        ]
    )
    line.greet()
    blocks[line.place * 2 + line.core] = hidden_ref[...]
    gather.send(line.place)

    def stores(chip):
        pair = pl.ds(chip * 2, 2)
        return [
            pltpu.make_async_copy(gate_keep.at[pair], gate_out.at[pair], store_sem.at[0, chip]),
            pltpu.make_async_copy(up_keep.at[pair], up_out.at[pair], store_sem.at[1, chip]),
            pltpu.make_async_copy(act_keep.at[pair], act_out.at[pair], store_sem.at[2, chip]),
            pltpu.make_async_copy(blocks.at[pair], all_out.at[pair], store_sem.at[3, chip]),
        ]

    for copy in copies:
        copy.wait()

    @pl.loop(0, chips)
    def _(step):
        chip = gather.step(step)
        pair = pl.ds(chip * 2, 2)

        @pl.loop(0, units // tile_of(units))
        def _(tile):
            columns = pl.ds(pl.multiple_of(tile * tile_of(units), 128), tile_of(units))
            tokens = blocks[pair].reshape(2 * rows, width)
            gate = jnp.dot(tokens, gate_w[:, columns], preferred_element_type=jnp.float32)
            up = jnp.dot(tokens, up_w[:, columns], preferred_element_type=jnp.float32)
            gate_keep[pair, :, columns] = gate.reshape(2, rows, -1)
            up_keep[pair, :, columns] = up.reshape(2, rows, -1)
            act_keep[pair, :, columns] = (
                (gate / (1.0 + jnp.exp(-gate)) * up).astype(jnp.bfloat16).reshape(2, rows, -1)
            )

        @pl.loop(0, width // tile_of(width))
        def _(tile):
            columns = pl.ds(pl.multiple_of(tile * tile_of(width), 128), tile_of(width))
            act = act_keep[pair].reshape(2 * rows, units)
            fresh[:, :, columns] = dot_cols(act, down_w[columns, :]).reshape(2, rows, -1)

        for copy in stores(chip):
            copy.start()
        scatter.after_term(chip)

    scatter.hops()
    scatter.settle(mixed_ref)
    scatter.finish()
    gather.finish()

    @pl.loop(0, chips)
    def _(chip):
        for copy in stores(chip):
            copy.wait()


def feed_forward_back_kernel(
    chips,
    grad_ref,
    gate_hbm,
    up_hbm,
    down_hbm,
    gate_lin_hbm,
    up_lin_hbm,
    hidden_grad_ref,
    gate_out,
    up_out,
    all_out,
    gate_w,
    up_w,
    down_w,
    gate_lin,
    up_lin,
    gate_keep,
    up_keep,
    load_sem,
    store_sem,
    *comm,
):
    line = Line(chips)
    gather = Gather(line, *comm[:5])
    scatter = Scatter(line, *comm[5:])
    blocks, fresh = gather.blocks, scatter.fresh
    _, rows, width = blocks.shape
    units = gate_w.shape[1]
    copies = load(
        [
            (down_hbm, down_w, load_sem.at[0]),
            (gate_lin_hbm, gate_lin, load_sem.at[1]),
            (up_lin_hbm, up_lin, load_sem.at[2]),
            (gate_hbm, gate_w, load_sem.at[3]),
            (up_hbm, up_w, load_sem.at[4]),
        ]
    )
    line.greet()
    blocks[line.place * 2 + line.core] = grad_ref[...]
    gather.send(line.place)

    def stores(chip):
        pair = pl.ds(chip * 2, 2)
        return [
            pltpu.make_async_copy(gate_keep.at[pair], gate_out.at[pair], store_sem.at[0, chip]),
            pltpu.make_async_copy(up_keep.at[pair], up_out.at[pair], store_sem.at[1, chip]),
            pltpu.make_async_copy(blocks.at[pair], all_out.at[pair], store_sem.at[2, chip]),
        ]

    for copy in copies:
        copy.wait()

    @pl.loop(0, chips)
    def _(step):
        chip = gather.step(step)
        pair = pl.ds(chip * 2, 2)

        @pl.loop(0, units // tile_of(units))
        def _(tile):
            columns = pl.ds(pl.multiple_of(tile * tile_of(units), 128), tile_of(units))
            tokens = blocks[pair].reshape(2 * rows, width)
            grad = jnp.dot(tokens, down_w[:, columns], preferred_element_type=jnp.float32)
            gate = gate_lin[pair, :, columns].reshape(2 * rows, -1)
            up = up_lin[pair, :, columns].reshape(2 * rows, -1)
            sig = 1.0 / (1.0 + jnp.exp(-gate))
            gate_keep[pair, :, columns] = (
                (grad * up * sig * (1.0 + gate * (1.0 - sig)))
                .astype(jnp.bfloat16)
                .reshape(2, rows, -1)
            )
            up_keep[pair, :, columns] = (
                (grad * (gate * sig)).astype(jnp.bfloat16).reshape(2, rows, -1)
            )

        @pl.loop(0, width // tile_of(width))
        def _(tile):
            columns = pl.ds(pl.multiple_of(tile * tile_of(width), 128), tile_of(width))
            gate = gate_keep[pair].reshape(2 * rows, units)
            up = up_keep[pair].reshape(2 * rows, units)
            fresh[:, :, columns] = (
                dot_cols(gate, gate_w[columns, :]) + dot_cols(up, up_w[columns, :])
            ).reshape(2, rows, -1)

        for copy in stores(chip):
            copy.start()
        scatter.after_term(chip)

    scatter.hops()
    scatter.settle(hidden_grad_ref)
    scatter.finish()
    gather.finish()

    @pl.loop(0, chips)
    def _(chip):
        for copy in stores(chip):
            copy.wait()


def whole_spec():
    return pl.BlockSpec(memory_space=pltpu.VMEM)


def far_spec():
    return pl.BlockSpec(memory_space=pl.ANY)


def line_params(collective_id):
    return pltpu.CompilerParams(
        collective_id=collective_id, has_side_effects=True, vmem_limit_bytes=60 * 2**20
    )


def feed_forward(hidden_low, gate_cols, up_cols, down_cols):
    rows, width = hidden_low.shape
    units = gate_cols.shape[1]
    slots = lax.axis_size("seq")
    chips = slots // 2
    weights = [pltpu.VMEM((width, units), jnp.bfloat16)] * 3
    mixed, gate, up, act, every = pl.pallas_call(
        functools.partial(feed_forward_kernel, chips),
        out_shape=(
            jax.ShapeDtypeStruct((rows, width), jnp.float32),
            jax.ShapeDtypeStruct((slots, rows, units), jnp.float32),
            jax.ShapeDtypeStruct((slots, rows, units), jnp.float32),
            jax.ShapeDtypeStruct((slots, rows, units), jnp.bfloat16),
            jax.ShapeDtypeStruct((slots, rows, width), jnp.bfloat16),
        ),
        in_specs=[whole_spec()] + [far_spec()] * 3,
        out_specs=(whole_spec(),) + (far_spec(),) * 4,
        scratch_shapes=weights
        + [
            pltpu.VMEM((slots, rows, units), jnp.float32),
            pltpu.VMEM((slots, rows, units), jnp.float32),
            pltpu.VMEM((slots, rows, units), jnp.bfloat16),
            pltpu.SemaphoreType.DMA((3,)),
            pltpu.SemaphoreType.DMA((4, chips)),
        ]
        + Gather.scratch(chips, rows, width)
        + Scatter.scratch(chips, rows, width),
        compiler_params=line_params(1),
        name="feed_forward",
    )(hidden_low, gate_cols, up_cols, down_cols)
    return mixed, gate, up, act.reshape(-1, units), every.reshape(-1, width)


def feed_forward_back(grad_low, gate_cols, up_cols, down_cols, gate, up):
    rows, width = grad_low.shape
    units = gate_cols.shape[1]
    slots = lax.axis_size("seq")
    chips = slots // 2
    weights = [pltpu.VMEM((width, units), jnp.bfloat16)] * 3
    hidden_grad, gate_grad, up_grad, every = pl.pallas_call(
        functools.partial(feed_forward_back_kernel, chips),
        out_shape=(
            jax.ShapeDtypeStruct((rows, width), jnp.float32),
            jax.ShapeDtypeStruct((slots, rows, units), jnp.bfloat16),
            jax.ShapeDtypeStruct((slots, rows, units), jnp.bfloat16),
            jax.ShapeDtypeStruct((slots, rows, width), jnp.bfloat16),
        ),
        in_specs=[whole_spec()] + [far_spec()] * 5,
        out_specs=(whole_spec(),) + (far_spec(),) * 3,
        scratch_shapes=weights
        + [
            pltpu.VMEM((slots, rows, units), jnp.float32),
            pltpu.VMEM((slots, rows, units), jnp.float32),
            pltpu.VMEM((slots, rows, units), jnp.bfloat16),
            pltpu.VMEM((slots, rows, units), jnp.bfloat16),
            pltpu.SemaphoreType.DMA((5,)),
            pltpu.SemaphoreType.DMA((3, chips)),
        ]
        + Gather.scratch(chips, rows, width)
        + Scatter.scratch(chips, rows, width),
        compiler_params=line_params(2),
        name="feed_forward_back",
    )(grad_low, gate_cols, up_cols, down_cols, gate, up)
    return (
        hidden_grad,
        gate_grad.reshape(-1, units),
        up_grad.reshape(-1, units),
        every.reshape(-1, width),
    )


def peers_of(axis, size):
    me = lax.axis_index(axis)
    return me, lambda step: (me + step) % size


def greet_cross(seq_count, fsdp_count):
    seq, seq_peer = peers_of("seq", seq_count)
    fsdp, fsdp_peer = peers_of("fsdp", fsdp_count)
    barrier = pltpu.get_barrier_semaphore()
    for step in range(1, seq_count):
        pl.semaphore_signal(
            barrier, inc=1, device_id=(seq_peer(step), fsdp), device_id_type=MESH
        )
    for step in range(1, fsdp_count):
        pl.semaphore_signal(
            barrier, inc=1, device_id=(seq, fsdp_peer(step)), device_id_type=MESH
        )
    pl.semaphore_wait(barrier, seq_count + fsdp_count - 2)


class Cross:
    def __init__(self, seq_count, fsdp_count):
        self.seq_count, self.fsdp_count = seq_count, fsdp_count
        self.seq, self.seq_peer = peers_of("seq", seq_count)
        self.fsdp, self.fsdp_peer = peers_of("fsdp", fsdp_count)
        self.square = fsdp_count == 4
        if self.square:
            row, place = self.fsdp // 2, self.fsdp % 2
            self.sides = (row * 2 + 1 - place, (1 - row) * 2 + place)
            self.corner = (1 - row) * 2 + 1 - place
        else:
            self.sides = tuple(self.fsdp_peer(step) for step in range(1, fsdp_count))

    def remote(self, src, dst, send, recv, seq, fsdp):
        return pltpu.make_async_remote_copy(
            src_ref=src,
            dst_ref=dst,
            send_sem=send,
            recv_sem=recv,
            device_id=(seq, fsdp),
            device_id_type=MESH,
        )


class Spread:
    def __init__(self, cross, sources, weights, row_send, row_recv, side_send, side_recv, half_send, half_recv):
        self.cross, self.sources, self.weights = cross, sources, weights
        self.row_send, self.row_recv = row_send, row_recv
        self.side_send, self.side_recv = side_send, side_recv
        self.half_send, self.half_recv = half_send, half_recv
        self.kinds, self.columns = len(sources), weights.shape[-1]
        self.rows = weights.shape[-2]

    @staticmethod
    def scratch(kinds, seq_count, fsdp_count, rows, columns):
        dma = pltpu.SemaphoreType.DMA
        sides = 2 if fsdp_count == 4 else fsdp_count - 1
        return [
            pltpu.VMEM((kinds, seq_count, fsdp_count, rows, columns), jnp.bfloat16),
            dma((kinds, seq_count)),
            dma((kinds, seq_count)),
            dma((seq_count, sides)),
            dma((seq_count, sides)),
            dma((seq_count, 2)),
            dma((seq_count, 2)),
        ]

    def block(self, owner):
        return pl.ds(pl.multiple_of(owner * self.columns, 128), self.columns)

    def row(self, kind, step):
        cross = self.cross
        peer = cross.seq_peer(step)
        return cross.remote(
            self.sources[kind].at[:, self.block(peer)],
            self.weights.at[kind, cross.seq, cross.fsdp],
            self.row_send.at[kind, step],
            self.row_recv.at[kind, step],
            peer,
            cross.fsdp,
        )

    def side(self, owner, side):
        cross = self.cross
        ref = self.weights.at[:, owner, cross.fsdp]
        return cross.remote(
            ref,
            ref,
            self.side_send.at[owner, side],
            self.side_recv.at[owner, side],
            cross.seq,
            cross.sides[side],
        )

    def half(self, owner, side):
        cross = self.cross
        rows = pl.ds(side * (self.rows // 2), self.rows // 2)
        ref = self.weights.at[:, owner, cross.sides[side], rows]
        return cross.remote(
            ref,
            ref,
            self.half_send.at[owner, side],
            self.half_recv.at[owner, side],
            cross.seq,
            cross.sides[1 - side],
        )

    def start(self):
        cross = self.cross
        for step in range(1, cross.seq_count):
            for kind in range(self.kinds):
                self.row(kind, step).start()

    def own(self):
        cross = self.cross
        for kind in range(self.kinds):
            self.weights[kind, cross.seq, cross.fsdp] = self.sources[kind][:, self.block(cross.seq)]
        self.pass_on(0)

    def owner(self, step):
        return (self.cross.seq - step + self.cross.seq_count) % self.cross.seq_count

    def take(self, step):
        for kind in range(self.kinds):
            self.row(kind, step).wait_recv()
        self.pass_on(step)

    def pass_on(self, step):
        for side in range(len(self.cross.sides)):
            self.side(self.owner(step), side).start()

    def relay(self, step):
        owner = self.owner(step)
        for side in range(len(self.cross.sides)):
            self.side(owner, side).wait_recv()
            if self.cross.square:
                self.half(owner, side).start()

    def settle(self, step):
        if self.cross.square:
            for side in range(2):
                self.half(self.owner(step), side).wait_recv()

    def finish(self):
        cross = self.cross

        @pl.loop(1, cross.seq_count)
        def _(step):
            for kind in range(self.kinds):
                self.row(kind, step).wait_send()

        @pl.loop(0, cross.seq_count)
        def _(owner):
            for side in range(len(cross.sides)):
                self.side(owner, side).wait_send()
                if cross.square:
                    self.half(owner, side).wait_send()


AHEAD = 2
LAG = 3


class Collect:
    def __init__(self, cross, terms, side_in, half_out, half_in, row_out, row_in, side_send, side_recv, half_send, half_recv, row_send, row_recv):
        self.cross, self.terms = cross, terms
        self.side_in, self.half_out, self.half_in = side_in, half_out, half_in
        self.row_out, self.row_in = row_out, row_in
        self.side_send, self.side_recv = side_send, side_recv
        self.half_send, self.half_recv = half_send, half_recv
        self.row_send, self.row_recv = row_send, row_recv
        self.rows, self.columns = terms.shape[-2:]
        self.items = terms.shape[0] * cross.seq_count

    @staticmethod
    def scratch(kinds, seq_count, fsdp_count, rows, columns):
        seq_count = kinds * seq_count
        dma = pltpu.SemaphoreType.DMA
        vmem = pltpu.VMEM
        bf16 = jnp.bfloat16
        if fsdp_count == 4:
            arrays = [
                vmem((seq_count, 2, 2, rows // 2, columns), bf16),
                vmem((seq_count, 2, rows // 2, columns), bf16),
                vmem((seq_count, 2, rows // 2, columns), bf16),
            ]
            sides = (2, 2)
        else:
            arrays = [
                vmem((seq_count, fsdp_count - 1, rows, columns), bf16),
                vmem((1, 1, 16, 128), bf16),
                vmem((1, 1, 16, 128), bf16),
            ]
            sides = (fsdp_count - 1, 1)
        return arrays + [
            vmem((seq_count, rows, columns), bf16),
            vmem((seq_count, rows, columns), bf16),
            dma((seq_count,) + sides),
            dma((seq_count,) + sides),
            dma((seq_count, 2)),
            dma((seq_count, 2)),
            dma((seq_count,)),
            dma((seq_count,)),
        ]

    def half_rows(self, side):
        return pl.ds(side * (self.rows // 2), self.rows // 2)

    def side(self, turn, side, which):
        cross = self.cross
        if not cross.square:
            return cross.remote(
                self.terms.at[(*self.place(turn), cross.sides[side])],
                self.side_in.at[turn, side],
                self.side_send.at[turn, side, 0],
                self.side_recv.at[turn, side, 0],
                cross.seq,
                cross.sides[side],
            )
        target = cross.sides[side] if which == 0 else cross.corner
        return cross.remote(
            self.terms.at[(*self.place(turn), target, self.half_rows(side))],
            self.side_in.at[turn, side, which],
            self.side_send.at[turn, side, which],
            self.side_recv.at[turn, side, which],
            cross.seq,
            cross.sides[side],
        )

    def half(self, turn, side):
        cross = self.cross
        return cross.remote(
            self.half_out.at[turn, side],
            self.half_in.at[turn, side],
            self.half_send.at[turn, side],
            self.half_recv.at[turn, side],
            cross.seq,
            cross.sides[1 - side],
        )

    def row(self, turn):
        cross = self.cross
        return cross.remote(
            self.row_out.at[turn],
            self.row_in.at[turn],
            self.row_send.at[turn],
            self.row_recv.at[turn],
            self.place(turn)[1],
            cross.fsdp,
        )

    def place(self, turn):
        count = self.cross.seq_count
        return turn // count, self.cross.seq_peer(turn % count + 1)

    def is_own(self, turn):
        return turn % self.cross.seq_count == self.cross.seq_count - 1

    @property
    def ways(self):
        return range(2) if self.cross.square else range(1)

    def send(self, turn):
        for which in reversed(self.ways):
            for side in range(len(self.cross.sides)):
                self.side(turn, side, which).start()

    def middle(self, turn):
        if not self.cross.square:
            return
        cross = self.cross
        kind, owner = self.place(turn)
        for side in range(2):
            self.side(turn, side, 1).wait_recv()
            mine = self.terms[kind, owner, cross.sides[1 - side], self.half_rows(side)]
            self.half_out[turn, side] = (
                mine.astype(jnp.float32) + self.side_in[turn, side, 1].astype(jnp.float32)
            ).astype(jnp.bfloat16)
            self.half(turn, side).start()

    def totals(self, turn):
        cross = self.cross
        kind, owner = self.place(turn)
        found = []
        if cross.square:
            for side in range(2):
                self.side(turn, side, 0).wait_recv()
                self.half(turn, side).wait_recv()
                rows = self.half_rows(side)
                total = self.terms[kind, owner, cross.fsdp, rows].astype(jnp.float32)
                total = total + self.side_in[turn, side, 0].astype(jnp.float32)
                total = total + self.half_in[turn, side].astype(jnp.float32)
                found.append((rows, total))
        else:
            total = self.terms[kind, owner, cross.fsdp].astype(jnp.float32)
            for side in range(len(cross.sides)):
                self.side(turn, side, 0).wait_recv()
                total = total + self.side_in[turn, side].astype(jnp.float32)
            found.append((pl.ds(0, self.rows), total))
        return found

    def ship(self, turn):
        own = self.is_own(turn)

        @pl.when(own)
        def _():
            for rows, total in self.totals(turn):
                self.row_in[turn, rows] = total.astype(jnp.bfloat16)

        @pl.when(jnp.logical_not(own))
        def _():
            for rows, total in self.totals(turn):
                self.row_out[turn, rows] = total.astype(jnp.bfloat16)
            self.row(turn).start()

    def beat(self, turn):
        ahead = turn + AHEAD

        @pl.when(ahead < self.items)
        def _():
            self.send(ahead)

        @pl.when(turn < self.items)
        def _():
            self.middle(turn)

        @pl.when(turn >= LAG)
        def _():
            self.ship(turn - LAG)

    def begin(self):
        for turn in range(min(AHEAD, self.items)):
            self.send(turn)

    @property
    def beats(self):
        return self.items + LAG

    def receive(self, turn, put):
        count = self.cross.seq_count

        @pl.when(jnp.logical_not(self.is_own(turn)))
        def _():
            self.row(turn).wait_recv()

        sender = (self.cross.seq - turn % count - 1 + count) % count
        put(turn // count, sender, self.row_in[turn].astype(jnp.float32))

    def finish(self):
        cross = self.cross

        @pl.loop(0, self.items)
        def _(turn):
            for side in range(len(cross.sides)):
                for which in self.ways:
                    self.side(turn, side, which).wait_send()
                if cross.square:
                    self.half(turn, side).wait_send()

            @pl.when(jnp.logical_not(self.is_own(turn)))
            def _():
                self.row(turn).wait_send()


def bring_in_kernel(
    chips,
    fsdp_count,
    inputs_ref,
    query_ref,
    key_ref,
    value_ref,
    output_ref,
    gate_ref,
    gains_ref,
    inputs_out,
    weights_out,
    output_out,
    gate_out,
    gains_out,
    outputs,
    gains,
    gain_row_send,
    gain_row_recv,
    gain_column_send,
    gain_column_recv,
    output_send,
    output_recv,
    store_sem,
    *comm,
):
    line = Line(chips)
    cross = Cross(2 * chips, fsdp_count)
    gather = Gather(line, *comm[:5])
    attention = Spread(cross, (query_ref, key_ref, value_ref), *comm[5:12])
    gate = Spread(cross, (gate_ref,), *comm[12:])
    seq_count, seq, fsdp = cross.seq_count, cross.seq, cross.fsdp

    def gain_row(step):
        return cross.remote(
            gains_ref,
            gains.at[seq, fsdp],
            gain_row_send.at[step],
            gain_row_recv.at[step],
            cross.seq_peer(step),
            fsdp,
        )

    def gain_column(owner, step):
        ref = gains.at[owner, fsdp]
        return cross.remote(
            ref,
            ref,
            gain_column_send.at[owner, step],
            gain_column_recv.at[owner, step],
            seq,
            cross.fsdp_peer(step),
        )

    def output_copy(step):
        return cross.remote(
            output_ref,
            outputs.at[fsdp],
            output_send.at[step],
            output_recv.at[step],
            seq,
            cross.fsdp_peer(step),
        )

    greet_cross(seq_count, fsdp_count)
    for step in range(1, seq_count):
        gain_row(step).start()
    attention.start()
    gate.start()
    gather.blocks[line.place * 2 + line.core] = inputs_ref[...]
    gather.send(line.place)
    gains[seq, fsdp] = gains_ref[...]
    outputs[fsdp] = output_ref[...]
    attention.own()
    for step in range(1, fsdp_count):
        gain_column(seq, step).start()

    @pl.loop(1, seq_count)
    def _(step):
        attention.take(step)
        gain_row(step).wait_recv()
        for peer in range(1, fsdp_count):
            gain_column(attention.owner(step), peer).start()
        attention.relay(step - 1)

    gate.own()
    attention.relay(seq_count - 1)
    gather.step(0)

    @pl.loop(1, seq_count)
    def _(step):
        gate.take(step)
        gate.relay(step - 1)

        @pl.when((step % 2 == 0) & (step > 2))
        def _():
            gather.step(step // 2 - 1)

    for step in range(1, fsdp_count):
        output_copy(step).start()
    gate.relay(seq_count - 1)
    if chips > 1:
        gather.step(chips - 1)
    inputs_store = pltpu.make_async_copy(gather.blocks, inputs_out, store_sem.at[0])
    inputs_store.start()

    @pl.loop(0, seq_count)
    def _(step):
        attention.settle(step)
        for peer in range(1, fsdp_count):
            gain_column(step, peer).wait_recv()

    weights_store = pltpu.make_async_copy(attention.weights, weights_out, store_sem.at[1])
    weights_store.start()
    for step in range(1, fsdp_count):
        output_copy(step).wait_recv()
    output_store = pltpu.make_async_copy(outputs, output_out, store_sem.at[2])
    output_store.start()
    gains_out[...] = gains[...]

    @pl.loop(0, seq_count)
    def _(step):
        gate.settle(step)

    gate_store = pltpu.make_async_copy(gate.weights, gate_out, store_sem.at[3])
    gate_store.start()
    gather.finish()
    attention.finish()
    gate.finish()

    @pl.loop(1, seq_count)
    def _(step):
        gain_row(step).wait_send()

    @pl.loop(0, seq_count)
    def _(owner):
        for step in range(1, fsdp_count):
            gain_column(owner, step).wait_send()

    for step in range(1, fsdp_count):
        output_copy(step).wait_send()
    inputs_store.wait()
    weights_store.wait()
    output_store.wait()
    gate_store.wait()


def bring_in(local_in, query_weight, key_weight, value_weight, output_weight, gate_weight, gains):
    rows, width = local_in.shape
    slots = lax.axis_size("seq")
    fsdp_count = lax.axis_size("fsdp")
    chips = slots // 2
    own_rows, columns = query_weight.shape[0], query_weight.shape[1] // slots
    units = gate_weight.shape[1] // slots
    bf16, dma = jnp.bfloat16, pltpu.SemaphoreType.DMA
    lanes = pl.cdiv(gains.shape[1], 128) * 128
    padded = jnp.pad(gains, ((0, 16 - gains.shape[0]), (0, lanes - gains.shape[1])))
    inputs_all, weights, outputs, gate, gains_all = pl.pallas_call(
        functools.partial(bring_in_kernel, chips, fsdp_count),
        out_shape=(
            jax.ShapeDtypeStruct((slots, rows, width), bf16),
            jax.ShapeDtypeStruct((3, slots, fsdp_count, own_rows, columns), bf16),
            jax.ShapeDtypeStruct((fsdp_count, own_rows, width), bf16),
            jax.ShapeDtypeStruct((1, slots, fsdp_count, own_rows, units), bf16),
            jax.ShapeDtypeStruct((slots, fsdp_count, 16, lanes), bf16),
        ),
        in_specs=[whole_spec()] * 7,
        out_specs=(far_spec(),) * 4 + (whole_spec(),),
        scratch_shapes=[
            pltpu.VMEM((fsdp_count, own_rows, width), bf16),
            pltpu.VMEM((slots, fsdp_count, 16, lanes), bf16),
            dma((slots,)),
            dma((slots,)),
            dma((slots, fsdp_count)),
            dma((slots, fsdp_count)),
            dma((fsdp_count,)),
            dma((fsdp_count,)),
            dma((4,)),
        ]
        + Gather.scratch(chips, rows, width)
        + Spread.scratch(3, slots, fsdp_count, own_rows, columns)
        + Spread.scratch(1, slots, fsdp_count, own_rows, units),
        compiler_params=line_params(3),
        name="bring_in",
    )(local_in, query_weight, key_weight, value_weight, output_weight, gate_weight, padded)
    gains_all = gains_all[:, :, : gains.shape[0], : gains.shape[1]]
    return (
        inputs_all.reshape(-1, width),
        weights.reshape(3, -1, columns),
        outputs.reshape(-1, width),
        gate.reshape(-1, units),
        gains_all.transpose(2, 0, 1, 3).reshape(gains.shape[0], -1),
    )


def product_terms(scatter, pairs, chip):
    _, rows, width = scatter.fresh.shape
    pair = pl.ds(chip * 2, 2)

    @pl.loop(0, width // tile_of(width))
    def _(tile):
        columns = pl.ds(pl.multiple_of(tile * tile_of(width), 128), tile_of(width))
        total = None
        for left, right, across in pairs:
            tokens = left[pair].reshape(2 * rows, -1)
            if across:
                term = dot_cols(tokens, right[columns, :])
            else:
                term = jnp.dot(tokens, right[:, columns], preferred_element_type=jnp.float32)
            total = term if total is None else total + term
        scatter.fresh[:, :, columns] = total.reshape(2, rows, -1)

    scatter.after_term(chip)


def project_kernel(
    chips,
    fsdp_count,
    attended_ref,
    output_ref,
    up_ref,
    down_ref,
    result,
    up_out,
    down_out,
    store_sem,
    *comm,
):
    line = Line(chips)
    cross = Cross(2 * chips, fsdp_count)
    count = len(Scatter.scratch(chips, 4, 128))
    scatter = Scatter(line, *comm[:count])
    up = Spread(cross, (up_ref,), *comm[count : count + 7])
    down = Spread(cross, (down_ref,), *comm[count + 7 :])
    greet_cross(cross.seq_count, fsdp_count)
    up.start()
    down.start()
    up.own()

    @pl.loop(0, chips)
    def _(step):
        product_terms(scatter, [(attended_ref, output_ref, False)], line.order(chips - 1 - step))

    @pl.loop(1, cross.seq_count)
    def _(step):
        up.take(step)
        up.relay(step - 1)

    down.own()
    up.relay(cross.seq_count - 1)
    scatter.hop(0)

    @pl.loop(1, cross.seq_count)
    def _(step):
        down.take(step)
        down.relay(step - 1)

        @pl.when(step % 2 == 0)
        def _():
            scatter.hop(step // 2)

    down.relay(cross.seq_count - 1)

    @pl.loop(0, cross.seq_count)
    def _(step):
        up.settle(step)

    up_store = pltpu.make_async_copy(up.weights, up_out, store_sem.at[0])
    up_store.start()
    scatter.settle(result)

    @pl.loop(0, cross.seq_count)
    def _(step):
        down.settle(step)

    down_store = pltpu.make_async_copy(down.weights, down_out, store_sem.at[1])
    down_store.start()
    scatter.finish()
    up.finish()
    down.finish()
    up_store.wait()
    down_store.wait()


def project(attended, output_rows, up_weight, down_weight):
    slots = lax.axis_size("seq")
    fsdp_count = lax.axis_size("fsdp")
    chips = slots // 2
    rows = attended.shape[0] // slots
    width = output_rows.shape[1]
    own_rows, units = up_weight.shape[0], up_weight.shape[1] // slots
    weight = jax.ShapeDtypeStruct((1, slots, fsdp_count, own_rows, units), jnp.bfloat16)
    projected, up, down = pl.pallas_call(
        functools.partial(project_kernel, chips, fsdp_count),
        out_shape=(jax.ShapeDtypeStruct((rows, width), jnp.float32), weight, weight),
        in_specs=[whole_spec()] * 4,
        out_specs=(whole_spec(), far_spec(), far_spec()),
        scratch_shapes=[pltpu.SemaphoreType.DMA((2,))]
        + Scatter.scratch(chips, rows, width)
        + Spread.scratch(1, slots, fsdp_count, own_rows, units) * 2,
        compiler_params=line_params(5),
        name="project",
    )(attended.reshape(slots, rows, -1), output_rows, up_weight, down_weight)
    return projected, up.reshape(-1, units), down.reshape(-1, units)


def gather_back_kernel(chips, fsdp_count, count, local_ref, *refs):
    sources, refs = refs[:count], refs[count:]
    out, results, refs = refs[0], refs[1 : 1 + count], refs[1 + count :]
    terms, load_sem, store_sem, comm = refs[0], refs[1], refs[2], refs[3:]
    line = Line(chips)
    cross = Cross(2 * chips, fsdp_count)
    gather = Gather(line, *comm[:5])
    collect = Collect(cross, terms, *comm[5:])
    copies = load([(sources[kind], terms.at[kind], load_sem.at[kind]) for kind in range(count)])
    greet_cross(cross.seq_count, fsdp_count)
    gather.blocks[line.place * 2 + line.core] = local_ref[...]
    gather.send(line.place)

    def store(chip):
        pair = pl.ds(chip * 2, 2)
        return pltpu.make_async_copy(gather.blocks.at[pair], out.at[pair], store_sem.at[chip])

    for copy in copies:
        copy.wait()
    collect.begin()
    store(gather.step(0)).start()

    @pl.loop(0, collect.beats)
    def _(turn):
        collect.beat(turn)

        @pl.when((turn % 3 == 2) & (turn // 3 + 1 < chips))
        def _():
            store(gather.step(turn // 3 + 1)).start()

    block = terms.shape[-1]

    @pl.loop(0, cross.seq_count)
    def _(turn):
        for kind in range(count):

            def put(_, sender, value):
                columns = pl.ds(pl.multiple_of(sender * block, 128), block)
                results[kind][:, columns] = value

            collect.receive(kind * cross.seq_count + turn, put)

    collect.finish()
    gather.finish()

    @pl.loop(0, chips)
    def _(chip):
        store(chip).wait()


def gather_back(local, terms):
    rows, width = local.shape
    slots = lax.axis_size("seq")
    fsdp_count = lax.axis_size("fsdp")
    chips = slots // 2
    count = len(terms)
    own = terms[0].shape[0] // (slots * fsdp_count)
    units = terms[0].shape[1]
    found = pl.pallas_call(
        functools.partial(gather_back_kernel, chips, fsdp_count, count),
        out_shape=(jax.ShapeDtypeStruct((slots, rows, width), jnp.bfloat16),)
        + (jax.ShapeDtypeStruct((own, units * slots), jnp.float32),) * count,
        in_specs=[whole_spec()] + [far_spec()] * count,
        out_specs=(far_spec(),) + (whole_spec(),) * count,
        scratch_shapes=[
            pltpu.VMEM((count, slots, fsdp_count, own, units), jnp.bfloat16),
            pltpu.SemaphoreType.DMA((count,)),
            pltpu.SemaphoreType.DMA((chips,)),
        ]
        + Gather.scratch(chips, rows, width)
        + Collect.scratch(count, slots, fsdp_count, own, units),
        compiler_params=line_params(6),
        name="gather_back",
    )(local, *[term.reshape(slots, fsdp_count, own, units) for term in terms])
    return (found[0].reshape(-1, width),) + tuple(found[1:])


def take_out_kernel(
    chips,
    fsdp_count,
    *refs,
):
    lefts, rights, refs = refs[:3], refs[3:6], refs[6:]
    terms, output_ref, gains_ref, refs = refs[0], refs[1], refs[2], refs[3:]
    result, weight_outs, output_out, gains_out, refs = refs[0], refs[1:4], refs[4], refs[5], refs[6:]
    output_in, gain_in, gain_out, gain_rows, refs = refs[0], refs[1], refs[2], refs[3], refs[4:]
    output_send, output_recv, gain_send, gain_recv, gain_row_send, gain_row_recv = refs[:6]
    comm = refs[6:]
    line = Line(chips)
    cross = Cross(2 * chips, fsdp_count)
    scatter = Scatter(line, *comm[:-11])
    collect = Collect(cross, terms, *comm[-11:])
    seq_count, seq, fsdp = cross.seq_count, cross.seq, cross.fsdp

    def output_copy(step):
        peer = cross.fsdp_peer(step)
        return cross.remote(
            output_ref.at[peer],
            output_in.at[step],
            output_send.at[step],
            output_recv.at[step],
            seq,
            peer,
        )

    def gain_copy(step):
        peer = cross.fsdp_peer(step)
        return cross.remote(
            gains_ref.at[peer], gain_in.at[step], gain_send.at[step], gain_recv.at[step], seq, peer
        )

    def gain_row(step):
        peer = cross.seq_peer(step)
        return cross.remote(
            gain_out.at[peer],
            gain_rows.at[step],
            gain_row_send.at[step],
            gain_row_recv.at[step],
            peer,
            fsdp,
        )

    greet_cross(seq_count, fsdp_count)
    for step in range(1, fsdp_count):
        gain_copy(step).start()

    collect.begin()

    @pl.loop(0, chips)
    def _(step):
        product_terms(
            scatter,
            [(left, right, True) for left, right in zip(lefts, rights)],
            line.order(chips - 1 - step),
        )

    total = gains_ref[fsdp]
    for step in range(1, fsdp_count):
        gain_copy(step).wait_recv()
        total = total + gain_in[step]
    gain_out[...] = total
    for step in range(1, seq_count):
        gain_row(step).start()

    @pl.loop(0, collect.beats)
    def _(turn):
        collect.beat(turn)

        @pl.when(turn == seq_count - AHEAD)
        def _():
            for step in range(1, fsdp_count):
                output_copy(step).start()

        @pl.when((turn % 2 == 0) & (turn < seq_count))
        def _():
            scatter.hop(turn // 2)

    total = output_ref[fsdp].astype(jnp.float32)
    for step in range(1, fsdp_count):
        output_copy(step).wait_recv()
        total = total + output_in[step].astype(jnp.float32)
    output_out[...] = total
    scatter.settle(result)
    total = gain_out[seq]
    for step in range(1, seq_count):
        gain_row(step).wait_recv()
        total = total + gain_rows[step]
    gains_out[...] = total

    columns = terms.shape[-1] // 3

    def put(_, sender, value):
        block = pl.ds(pl.multiple_of(sender * columns, 128), columns)
        for kind in range(3):
            weight_outs[kind][:, block] = value[:, kind * columns : (kind + 1) * columns]

    @pl.loop(0, seq_count)
    def _(turn):
        collect.receive(turn, put)

    scatter.finish()
    collect.finish()

    @pl.loop(1, seq_count)
    def _(step):
        gain_row(step).wait_send()

    for step in range(1, fsdp_count):
        output_copy(step).wait_send()
        gain_copy(step).wait_send()


def take_out(pairs, terms, output_term, gain_terms):
    slots = lax.axis_size("seq")
    fsdp_count = lax.axis_size("fsdp")
    chips = slots // 2
    width, columns = terms.shape
    rows = pairs[0][0].shape[0] // slots
    own = width // (slots * fsdp_count)
    kinds = gain_terms.shape[0]
    bf16, f32, dma = jnp.bfloat16, jnp.float32, pltpu.SemaphoreType.DMA
    gains = gain_terms.reshape(kinds, slots, fsdp_count, own).transpose(2, 1, 0, 3)
    lanes = pl.cdiv(own, 128) * 128
    gains = jnp.pad(gains, ((0, 0), (0, 0), (0, 8 - kinds), (0, lanes - own)))
    result, query, key, value, output, gains = pl.pallas_call(
        functools.partial(take_out_kernel, chips, fsdp_count),
        out_shape=(
            jax.ShapeDtypeStruct((rows, width), f32),
            jax.ShapeDtypeStruct((own, columns // 3 * slots), f32),
            jax.ShapeDtypeStruct((own, columns // 3 * slots), f32),
            jax.ShapeDtypeStruct((own, columns // 3 * slots), f32),
            jax.ShapeDtypeStruct((own, width), f32),
            jax.ShapeDtypeStruct((8, lanes), f32),
        ),
        in_specs=[whole_spec()] * 9,
        out_specs=(whole_spec(),) * 6,
        scratch_shapes=[
            pltpu.VMEM((fsdp_count, own, width), bf16),
            pltpu.VMEM((fsdp_count, slots, 8, lanes), f32),
            pltpu.VMEM((slots, 8, lanes), f32),
            pltpu.VMEM((slots, 8, lanes), f32),
            dma((fsdp_count,)),
            dma((fsdp_count,)),
            dma((fsdp_count,)),
            dma((fsdp_count,)),
            dma((slots,)),
            dma((slots,)),
        ]
        + Scatter.scratch(chips, rows, width)
        + Collect.scratch(1, slots, fsdp_count, own, columns),
        compiler_params=line_params(4),
        name="take_out",
    )(
        *[left.reshape(slots, rows, -1) for left, _ in pairs],
        *[right for _, right in pairs],
        terms.reshape(1, slots, fsdp_count, own, columns),
        output_term.reshape(fsdp_count, own, width),
        gains,
    )
    return result, (query, key, value), output, gains[:kinds, :own]


def row_sum_kernel(seq_count, local_ref, result, every, send, recv):
    seq, seq_peer = peers_of("seq", seq_count)
    fsdp = lax.axis_index("fsdp")
    barrier = pltpu.get_barrier_semaphore()
    for step in range(1, seq_count):
        pl.semaphore_signal(
            barrier, inc=1, device_id=(seq_peer(step), fsdp), device_id_type=MESH
        )
    pl.semaphore_wait(barrier, seq_count - 1)
    copies = [
        pltpu.make_async_remote_copy(
            src_ref=local_ref,
            dst_ref=every.at[step],
            send_sem=send.at[step],
            recv_sem=recv.at[step],
            device_id=(seq_peer(step), fsdp),
            device_id_type=MESH,
        )
        for step in range(1, seq_count)
    ]
    for copy in copies:
        copy.start()
    total = local_ref[...]
    for step in range(1, seq_count):
        copies[step - 1].wait_recv()
        total = total + every[step]
    result[...] = total
    for copy in copies:
        copy.wait_send()


def row_sum(collective_id, name, local):
    slots = lax.axis_size("seq")
    flat = local.reshape(-1, 128)
    return pl.pallas_call(
        functools.partial(row_sum_kernel, slots),
        out_shape=jax.ShapeDtypeStruct(flat.shape, jnp.float32),
        in_specs=[whole_spec()],
        out_specs=whole_spec(),
        scratch_shapes=[
            pltpu.VMEM((slots,) + flat.shape, jnp.float32),
            pltpu.SemaphoreType.DMA((slots,)),
            pltpu.SemaphoreType.DMA((slots,)),
        ],
        compiler_params=line_params(collective_id),
        name=name,
    )(flat).reshape(local.shape)


def rope_tables(row_count):
    half_width = DH // 2
    frequency = rope_base ** (-jnp.arange(half_width, dtype=jnp.float32) * 2.0 / DH)
    angles = jnp.arange(row_count, dtype=jnp.int32).astype(jnp.float32)[:, None] * frequency[None, :]
    return jnp.cos(angles), jnp.sin(angles)


def rotate(tensor, cosine, sine_table):
    row_count = tensor.shape[0]
    half_width = DH // 2
    grouped = tensor.reshape(row_count, -1, DH)
    first_half = grouped[..., :half_width]
    second_half = grouped[..., half_width:]
    cosine = cosine[:, None, :]
    sine_table = sine_table[:, None, :]
    turned = jnp.concatenate(
        [
            first_half * cosine - second_half * sine_table,
            second_half * cosine + first_half * sine_table,
        ],
        axis=-1,
    )
    return turned.reshape(tensor.shape)


def per_device(
    inputs,
    query_weight,
    key_weight,
    value_weight,
    output_weight,
    query_gain,
    key_gain,
    attention_gain,
    gate_weight,
    up_weight,
    down_weight,
    feedforward_gain,
    segments,
    cotangent,
):
    token_count = inputs.shape[1]
    width_all = inputs.shape[2]
    local_in = inputs.reshape(token_count, width_all)
    segment_row = segments[0]
    score_scale = DH ** (-0.5)
    seq_index = lax.axis_index("seq")
    inputs_all, attention_cols, output_rows, gate_cols, gains = bring_in(
        local_in,
        query_weight,
        key_weight,
        value_weight,
        output_weight,
        gate_weight,
        jnp.stack([query_gain, key_gain, attention_gain, feedforward_gain]),
    )
    query_cols, key_cols, value_cols = attention_cols[0], attention_cols[1], attention_cols[2]
    gains = gains.astype(jnp.float32)
    sequence_rows = inputs_all.shape[0]
    head_width = query_cols.shape[1]
    local_heads = head_width // DH
    query_scale = lax.dynamic_slice_in_dim(gains[0], seq_index * head_width, head_width, 0)
    key_scale = lax.dynamic_slice_in_dim(gains[1], seq_index * head_width, head_width, 0)
    attention_scale = gains[2]
    feedforward_scale = gains[3]
    query_pre = jnp.dot(inputs_all, query_cols, preferred_element_type=jnp.float32)
    key_pre = jnp.dot(inputs_all, key_cols, preferred_element_type=jnp.float32)
    values_low = jnp.dot(inputs_all, value_cols, preferred_element_type=jnp.float32).astype(
        jnp.bfloat16
    )
    squares = row_sum(
        7,
        "square_sum",
        jnp.stack([jnp.sum(query_pre * query_pre, axis=-1), jnp.sum(key_pre * key_pre, axis=-1)]),
    )
    inverse = lax.rsqrt(squares / width_all + eps_norm)
    query_unit = query_pre * inverse[0][:, None]
    key_unit = key_pre * inverse[1][:, None]
    cosine, sine_table = rope_tables(sequence_rows)
    queries_low = rotate(query_unit * query_scale, cosine, sine_table).astype(jnp.bfloat16)
    keys_low = rotate(key_unit * key_scale, cosine, sine_table).astype(jnp.bfloat16)
    query_heads = queries_low.reshape(sequence_rows, local_heads, DH)
    key_heads = keys_low.reshape(sequence_rows, local_heads, DH)
    value_heads = values_low.reshape(sequence_rows, local_heads, DH)
    block_rows = min(512, sequence_rows)
    block_count = sequence_rows // block_rows
    block_ids = jnp.arange(block_count, dtype=jnp.int32)

    def attend_block(loop_state, block_index):
        first_row = block_index * block_rows
        query_block = lax.dynamic_slice_in_dim(query_heads, first_row, block_rows, 0)
        scores = masked_scores(query_block, key_heads, first_row, segment_row, score_scale)
        row_max = jnp.max(scores, axis=-1, keepdims=True)
        expanded = jnp.exp(scores - row_max)
        row_total = jnp.sum(expanded, axis=-1, keepdims=True)
        softmax_low = (expanded / row_total).astype(jnp.bfloat16)
        block_out = jnp.einsum(
            "hqk,khd->qhd", softmax_low, value_heads, preferred_element_type=jnp.float32
        )
        log_total = (row_max + jnp.log(row_total))[..., 0]
        return (loop_state, (block_out.astype(jnp.bfloat16), log_total))

    _, (out_blocks, log_totals) = lax.scan(attend_block, jnp.zeros((), jnp.int32), block_ids)
    attended_heads = out_blocks.reshape(sequence_rows, head_width)
    projected, up_cols, down_cols = project(attended_heads, output_rows, up_weight, down_weight)
    hidden = local_in.astype(jnp.float32) + rms_scale(projected, attention_scale)
    hidden_low = hidden.astype(jnp.bfloat16)
    mixed_pre, gate_linear, up_linear, activated, hidden_all = feed_forward(
        hidden_low, gate_cols, up_cols, down_cols
    )
    result = (
        (hidden + rms_scale(mixed_pre, feedforward_scale))
        .astype(jnp.bfloat16)
        .reshape(1, token_count, width_all)
    )
    grad_result = cotangent.reshape(token_count, width_all).astype(jnp.float32)
    _, mixed_pull = jax.vjp(rms_scale, mixed_pre, feedforward_scale)
    grad_mixed, grad_feedforward_gain = mixed_pull(grad_result)
    grad_mixed_low = grad_mixed.astype(jnp.bfloat16)
    hidden_term, grad_gate_low, grad_upward_low, grad_all = feed_forward_back(
        grad_mixed_low, gate_cols, up_cols, down_cols, gate_linear, up_linear
    )
    grad_hidden = grad_result + hidden_term
    _, branch_pull = jax.vjp(rms_scale, projected, attention_scale)
    grad_projected, grad_attention_gain = branch_pull(grad_hidden)
    grad_projected_all, gate_weight_grad, up_weight_grad, down_weight_grad = gather_back(
        grad_projected.astype(jnp.bfloat16),
        [
            contract_rows(hidden_all, grad_gate_low).astype(jnp.bfloat16),
            contract_rows(hidden_all, grad_upward_low).astype(jnp.bfloat16),
            contract_rows(grad_all, activated).astype(jnp.bfloat16),
        ],
    )
    output_term = contract_rows(attended_heads, grad_projected_all).astype(jnp.bfloat16)
    grad_attended = contract_cols(grad_projected_all, output_rows).astype(jnp.bfloat16)
    grad_out_heads = grad_attended.reshape(sequence_rows, local_heads, DH)

    def attend_back(loop_state, block_index):
        key_total, value_total = loop_state
        first_row = block_index * block_rows
        query_block = lax.dynamic_slice_in_dim(query_heads, first_row, block_rows, 0)
        grad_block = lax.dynamic_slice_in_dim(grad_out_heads, first_row, block_rows, 0)
        log_block = lax.dynamic_index_in_dim(log_totals, block_index, 0, keepdims=False)
        scores = masked_scores(query_block, key_heads, first_row, segment_row, score_scale)
        probabilities = jnp.exp(scores - log_block[..., None])
        softmax_low = probabilities.astype(jnp.bfloat16)
        value_total = value_total + jnp.einsum(
            "hqk,qhd->khd", softmax_low, grad_block, preferred_element_type=jnp.float32
        )
        grad_softmax = jnp.einsum(
            "qhd,khd->hqk", grad_block, value_heads, preferred_element_type=jnp.float32
        )
        row_dot = jnp.sum(probabilities * grad_softmax, axis=-1, keepdims=True)
        grad_scores = (probabilities * (grad_softmax - row_dot)).astype(jnp.bfloat16)
        grad_query_block = (
            jnp.einsum("hqk,khd->qhd", grad_scores, key_heads, preferred_element_type=jnp.float32)
            * score_scale
        )
        key_total = (
            key_total
            + jnp.einsum(
                "hqk,qhd->khd", grad_scores, query_block, preferred_element_type=jnp.float32
            )
            * score_scale
        )
        return ((key_total, value_total), grad_query_block.astype(jnp.bfloat16))

    zero_heads = jnp.zeros((sequence_rows, local_heads, DH), jnp.float32)
    (key_total, value_total), grad_query_blocks = lax.scan(
        attend_back, (zero_heads, zero_heads), block_ids
    )
    grad_queries = grad_query_blocks.reshape(sequence_rows, head_width).astype(jnp.float32)
    grad_keys = (
        key_total.astype(jnp.bfloat16).reshape(sequence_rows, head_width).astype(jnp.float32)
    )
    grad_values = value_total.astype(jnp.bfloat16).reshape(sequence_rows, head_width)
    query_error = rotate(grad_queries, cosine, -sine_table)
    key_error = rotate(grad_keys, cosine, -sine_table)
    grad_query_gain = jnp.sum(query_error * query_unit, axis=0)
    grad_key_gain = jnp.sum(key_error * key_unit, axis=0)
    query_error = query_error * query_scale
    key_error = key_error * key_scale
    means = (
        row_sum(
            8,
            "mean_sum",
            jnp.stack(
                [
                    jnp.sum(query_error * query_unit, axis=-1),
                    jnp.sum(key_error * key_unit, axis=-1),
                ]
            ),
        )
        / width_all
    )
    grad_query_low = (
        inverse[0][:, None] * (query_error - query_unit * means[0][:, None])
    ).astype(jnp.bfloat16)
    grad_key_low = (inverse[1][:, None] * (key_error - key_unit * means[1][:, None])).astype(
        jnp.bfloat16
    )
    grads_low = jnp.concatenate([grad_query_low, grad_key_low, grad_values], axis=1)
    attention_terms = contract_rows(inputs_all, grads_low).astype(jnp.bfloat16)
    head_gains = lax.dynamic_update_slice_in_dim(
        jnp.zeros((2, width_all), jnp.float32),
        jnp.stack([grad_query_gain, grad_key_gain]),
        seq_index * head_width,
        1,
    )
    gain_terms = jnp.concatenate(
        [head_gains, jnp.stack([grad_attention_gain, grad_feedforward_gain])], axis=0
    )
    input_term, attention_grads, output_weight_grad, gain_grads = take_out(
        [(grad_query_low, query_cols), (grad_key_low, key_cols), (grad_values, value_cols)],
        attention_terms,
        output_term,
        gain_terms,
    )
    query_weight_grad, key_weight_grad, value_weight_grad = attention_grads
    grad_input = grad_hidden + input_term
    return (
        result,
        grad_input.reshape(1, token_count, width_all),
        query_weight_grad,
        key_weight_grad,
        value_weight_grad,
        output_weight_grad,
        gain_grads[0],
        gain_grads[1],
        gain_grads[2],
        gate_weight_grad,
        up_weight_grad,
        down_weight_grad,
        gain_grads[3],
    )


def solution(mesh):
    in_specs = (
        P("fsdp", "seq", None),
        P(("seq", "fsdp"), None),
        P(("seq", "fsdp"), None),
        P(("seq", "fsdp"), None),
        P(("seq", "fsdp"), None),
        P(("seq", "fsdp")),
        P(("seq", "fsdp")),
        P(("seq", "fsdp")),
        P(("seq", "fsdp"), None),
        P(("seq", "fsdp"), None),
        P(("seq", "fsdp"), None),
        P(("seq", "fsdp")),
        P("fsdp", None),
        P("fsdp", "seq", None),
    )
    out_specs = (
        P("fsdp", "seq", None),
        P("fsdp", "seq", None),
        P(("seq", "fsdp"), None),
        P(("seq", "fsdp"), None),
        P(("seq", "fsdp"), None),
        P(("seq", "fsdp"), None),
        P(("seq", "fsdp")),
        P(("seq", "fsdp")),
        P(("seq", "fsdp")),
        P(("seq", "fsdp"), None),
        P(("seq", "fsdp"), None),
        P(("seq", "fsdp"), None),
        P(("seq", "fsdp")),
    )
    return jax.shard_map(
        per_device, mesh=mesh, in_specs=in_specs, out_specs=out_specs, check_vma=False
    )
```

```python
import functools

import jax
import jax.numpy as jnp
from jax import lax
from jax.experimental import pallas as pl
from jax.experimental.pallas import tpu as pltpu
from jax.sharding import PartitionSpec as P

HEADS = 16
DH = 128


eps_norm = 1e-06
rope_base = 500000.0
neg_fill = -1e30


def rms_scale(tensor, gain):
    return tensor * lax.rsqrt(jnp.mean(tensor * tensor, axis=-1, keepdims=True) + eps_norm) * gain


def rotary(tensor, positions):
    row_count = tensor.shape[0]
    grouped = tensor.reshape(row_count, HEADS, DH)
    half_width = DH // 2
    frequency = rope_base ** (-jnp.arange(half_width, dtype=jnp.float32) * 2.0 / DH)
    angles = positions.astype(jnp.float32)[:, None] * frequency[None, :]
    cosine = jnp.cos(angles)[:, None, :]
    sine_table = jnp.sin(angles)[:, None, :]
    first_half = grouped[..., :half_width]
    second_half = grouped[..., half_width:]
    turned = jnp.concatenate(
        [
            first_half * cosine - second_half * sine_table,
            second_half * cosine + first_half * sine_table,
        ],
        axis=-1,
    )
    return turned.reshape(tensor.shape)


def norm_rotary(tensor, gain, positions):
    return rotary(rms_scale(tensor, gain), positions)


def swiglu_act(gate_linear, up_linear):
    return jax.nn.silu(gate_linear) * up_linear


def contract_rows(left, right):
    return lax.dot_general(
        left, right, (((0,), (0,)), ((), ())), preferred_element_type=jnp.float32
    )


def contract_cols(left, right):
    return lax.dot_general(
        left, right, (((1,), (1,)), ((), ())), preferred_element_type=jnp.float32
    )


def masked_scores(query_block, key_heads, first_row, segment_row, score_scale):
    block_rows = query_block.shape[0]
    sequence_rows = key_heads.shape[0]
    scores = (
        jnp.einsum("qhd,khd->hqk", query_block, key_heads, preferred_element_type=jnp.float32)
        * score_scale
    )
    query_pos = first_row + jnp.arange(block_rows, dtype=jnp.int32)
    key_pos = jnp.arange(sequence_rows, dtype=jnp.int32)
    query_seg = lax.dynamic_slice_in_dim(segment_row, first_row, block_rows, 0)
    allowed = (key_pos[None, :] <= query_pos[:, None]) & (
        segment_row[None, :] == query_seg[:, None]
    )
    return jnp.where(allowed[None], scores, neg_fill)


MESH = pl.DeviceIdType.MESH
RS_PARTS = 4


class Line:
    def __init__(self, chips):
        index = lax.axis_index("seq")
        self.chips = chips
        self.fsdp = lax.axis_index("fsdp")
        self.place = index // 2
        self.core = index % 2

    def device(self, place, core):
        return (place * 2 + core, self.fsdp)

    @property
    def partner(self):
        return self.device(self.place, 1 - self.core)

    @property
    def above(self):
        return self.device(jnp.minimum(self.place + 1, self.chips - 1), self.core)

    @property
    def below(self):
        return self.device(jnp.maximum(self.place - 1, 0), self.core)

    @property
    def has_above(self):
        return self.place < self.chips - 1

    @property
    def has_below(self):
        return self.place > 0

    def greet(self):
        barrier = pltpu.get_barrier_semaphore()
        pl.semaphore_signal(barrier, inc=1, device_id=self.partner, device_id_type=MESH)

        @pl.when(self.has_above)
        def _():
            pl.semaphore_signal(barrier, inc=1, device_id=self.above, device_id_type=MESH)

        @pl.when(self.has_below)
        def _():
            pl.semaphore_signal(barrier, inc=1, device_id=self.below, device_id_type=MESH)

        peers = (
            1 + jnp.minimum(self.place, 1) + jnp.minimum(self.chips - 1 - self.place, 1)
        )
        pl.semaphore_wait(barrier, peers)

    def order(self, step):
        place, last = self.place, self.chips - 1
        near = jnp.minimum(place, last - place)
        both = jnp.where(step % 2 == 1, place - (step + 1) // 2, place + step // 2)
        rest = jnp.where(place <= last - place, step, last - step)
        return jnp.where(step <= 2 * near, both, rest)

    def paired(self, step):
        near = jnp.minimum(self.place, self.chips - 1 - self.place)
        return (step % 2 == 1) & (step <= 2 * near)

    def second_of_pair(self, step):
        near = jnp.minimum(self.place, self.chips - 1 - self.place)
        return (step % 2 == 0) & (step > 0) & (step <= 2 * near)


class Gather:
    def __init__(self, line, blocks, arrive, up_sem, down_sem, side_sem):
        self.line, self.blocks, self.arrive = line, blocks, arrive
        self.up_sem, self.down_sem, self.side_sem = up_sem, down_sem, side_sem

    @staticmethod
    def scratch(chips, rows, width):
        return [
            pltpu.VMEM((2 * chips, rows, width), jnp.bfloat16),
            pltpu.SemaphoreType.DMA((2 * chips,)),
            pltpu.SemaphoreType.DMA((chips,)),
            pltpu.SemaphoreType.DMA((chips,)),
            pltpu.SemaphoreType.DMA((chips,)),
        ]

    def copy(self, chip, sem, target):
        slot = chip * 2 + self.line.core
        return pltpu.make_async_remote_copy(
            src_ref=self.blocks.at[slot],
            dst_ref=self.blocks.at[slot],
            send_sem=sem.at[chip],
            recv_sem=self.arrive.at[slot],
            device_id=target,
            device_id_type=MESH,
        )

    def wait_slot(self, slot):
        pltpu.make_async_remote_copy(
            src_ref=self.blocks.at[slot],
            dst_ref=self.blocks.at[slot],
            send_sem=self.side_sem.at[0],
            recv_sem=self.arrive.at[slot],
            device_id=self.line.partner,
            device_id_type=MESH,
        ).wait_recv()

    def send(self, chip):
        line = self.line

        @pl.when((chip <= line.place) & line.has_above)
        def _():
            self.copy(chip, self.up_sem, line.above).start()

        @pl.when((chip >= line.place) & line.has_below)
        def _():
            self.copy(chip, self.down_sem, line.below).start()

        self.copy(chip, self.side_sem, line.partner).start()

    def take(self, chip):
        self.wait_slot(chip * 2 + self.line.core)
        self.send(chip)

    def step(self, step):
        line = self.line
        chip = line.order(step)

        @pl.when((step > 0) & jnp.logical_not(line.second_of_pair(step)))
        def _():
            self.take(chip)

        @pl.when(line.paired(step))
        def _():
            self.take(line.order(step + 1))

        self.wait_slot(chip * 2 + 1 - line.core)
        return chip

    def finish(self):
        line = self.line

        @pl.loop(0, line.chips)
        def _(chip):
            @pl.when((chip <= line.place) & line.has_above)
            def _():
                self.copy(chip, self.up_sem, line.above).wait_send()

            @pl.when((chip >= line.place) & line.has_below)
            def _():
                self.copy(chip, self.down_sem, line.below).wait_send()

            self.copy(chip, self.side_sem, line.partner).wait_send()


class Scatter:
    def __init__(self, line, fresh, terms, side_out, side_in, out, inward, side_send, side_recv, send_sem, recv_sem):
        self.line, self.fresh, self.terms = line, fresh, terms
        self.side_out, self.side_in = side_out, side_in
        self.out, self.inward = out, inward
        self.side_send, self.side_recv = side_send, side_recv
        self.send_sem, self.recv_sem = send_sem, recv_sem
        self.rows = terms.shape[1] // RS_PARTS

    @staticmethod
    def scratch(chips, rows, width):
        return [
            pltpu.VMEM((2, rows, width), jnp.float32),
            pltpu.VMEM((chips, rows, width), jnp.float32),
            pltpu.VMEM((chips, rows, width), jnp.bfloat16),
            pltpu.VMEM((chips, rows, width), jnp.bfloat16),
            pltpu.VMEM((chips, rows, width), jnp.bfloat16),
            pltpu.VMEM((2, chips, rows, width), jnp.bfloat16),
            pltpu.SemaphoreType.DMA((chips,)),
            pltpu.SemaphoreType.DMA((chips,)),
            pltpu.SemaphoreType.DMA((chips, RS_PARTS)),
            pltpu.SemaphoreType.DMA((2, chips, RS_PARTS)),
        ]

    def side(self, chip):
        return pltpu.make_async_remote_copy(
            src_ref=self.side_out.at[chip],
            dst_ref=self.side_in.at[chip],
            send_sem=self.side_send.at[chip],
            recv_sem=self.side_recv.at[chip],
            device_id=self.line.partner,
            device_id_type=MESH,
        )

    def part(self, chip, part, upward, target):
        rows = pl.ds(part * self.rows, self.rows)
        return pltpu.make_async_remote_copy(
            src_ref=self.out.at[chip, rows],
            dst_ref=self.inward.at[upward, chip, rows],
            send_sem=self.send_sem.at[chip, part],
            recv_sem=self.recv_sem.at[upward, chip, part],
            device_id=target,
            device_id_type=MESH,
        )

    def share(self, chip):
        self.side_out[chip] = self.fresh[1 - self.line.core].astype(jnp.bfloat16)
        self.side(chip).start()
        self.terms[chip] = self.fresh[self.line.core]

    def total(self, chip, part, ways):
        rows = pl.ds(part * self.rows, self.rows)
        total = self.terms[chip, rows] + self.side_in[chip, rows].astype(jnp.float32)
        for way in ways:
            total = total + self.inward[way, chip, rows].astype(jnp.float32)
        return rows, total

    def pass_on(self, chip, upward, first):
        target = self.line.above if upward else self.line.below
        self.side(chip).wait_recv()

        @pl.loop(0, RS_PARTS)
        def _(part):
            if not first:
                self.part(chip, part, upward, target).wait_recv()
            rows, total = self.total(chip, part, () if first else (upward,))
            self.out[chip, rows] = total.astype(jnp.bfloat16)
            self.part(chip, part, upward, target).start()

    def after_term(self, chip):
        line = self.line
        self.share(chip)

        @pl.when((chip < line.place) & jnp.logical_not(line.has_above))
        def _():
            self.pass_on(chip, 0, True)

        @pl.when((chip > line.place) & jnp.logical_not(line.has_below))
        def _():
            self.pass_on(chip, 1, True)

    def hop(self, step):
        line = self.line
        lower = line.place * 2 < line.chips
        up_chip, down_chip = step, line.chips - 1 - step
        go_up = (up_chip > line.place) & line.has_below
        go_down = (down_chip < line.place) & line.has_above

        @pl.when(go_up & lower)
        def _():
            self.pass_on(up_chip, 1, False)

        @pl.when(go_down)
        def _():
            self.pass_on(down_chip, 0, False)

        @pl.when(go_up & jnp.logical_not(lower))
        def _():
            self.pass_on(up_chip, 1, False)

    def settle(self, result):
        line = self.line
        place = line.place
        self.side(place).wait_recv()

        @pl.loop(0, RS_PARTS)
        def _(part):
            @pl.when(line.has_above)
            def _():
                self.part(place, part, 0, line.below).wait_recv()

            @pl.when(line.has_below)
            def _():
                self.part(place, part, 1, line.above).wait_recv()

            @pl.when(line.has_above & line.has_below)
            def _():
                rows, total = self.total(place, part, (0, 1))
                result[rows] = total

            @pl.when(line.has_above & jnp.logical_not(line.has_below))
            def _():
                rows, total = self.total(place, part, (0,))
                result[rows] = total

            @pl.when(line.has_below & jnp.logical_not(line.has_above))
            def _():
                rows, total = self.total(place, part, (1,))
                result[rows] = total

    def hops(self):
        @pl.loop(0, self.line.chips)
        def _(step):
            self.hop(step)

    def finish(self):
        line = self.line

        @pl.loop(0, line.chips)
        def _(chip):
            self.side(chip).wait_send()

            @pl.when(chip != line.place)
            def _():
                @pl.loop(0, RS_PARTS)
                def _(part):
                    self.part(chip, part, 0, line.below).wait_send()


def tile_of(extent):
    return min(256, extent)


def dot_cols(left, right):
    return lax.dot_general(
        left, right, (((1,), (1,)), ((), ())), preferred_element_type=jnp.float32
    )


def load(pairs):
    copies = [pltpu.make_async_copy(src, dst, sem) for src, dst, sem in pairs]
    for copy in copies:
        copy.start()
    return copies


def feed_forward_kernel(
    chips,
    hidden_ref,
    gate_hbm,
    up_hbm,
    down_hbm,
    mixed_ref,
    gate_out,
    up_out,
    act_out,
    all_out,
    gate_w,
    up_w,
    down_w,
    gate_keep,
    up_keep,
    act_keep,
    load_sem,
    store_sem,
    *comm,
):
    line = Line(chips)
    gather = Gather(line, *comm[:5])
    scatter = Scatter(line, *comm[5:])
    blocks, fresh = gather.blocks, scatter.fresh
    _, rows, width = blocks.shape
    units = gate_w.shape[1]
    copies = load(
        [
            (gate_hbm, gate_w, load_sem.at[0]),
            (up_hbm, up_w, load_sem.at[1]),
            (down_hbm, down_w, load_sem.at[2]),
        ]
    )
    line.greet()
    blocks[line.place * 2 + line.core] = hidden_ref[...]
    gather.send(line.place)

    def stores(chip):
        pair = pl.ds(chip * 2, 2)
        return [
            pltpu.make_async_copy(gate_keep.at[pair], gate_out.at[pair], store_sem.at[0, chip]),
            pltpu.make_async_copy(up_keep.at[pair], up_out.at[pair], store_sem.at[1, chip]),
            pltpu.make_async_copy(act_keep.at[pair], act_out.at[pair], store_sem.at[2, chip]),
            pltpu.make_async_copy(blocks.at[pair], all_out.at[pair], store_sem.at[3, chip]),
        ]

    for copy in copies:
        copy.wait()

    @pl.loop(0, chips)
    def _(step):
        chip = gather.step(step)
        pair = pl.ds(chip * 2, 2)

        @pl.loop(0, units // tile_of(units))
        def _(tile):
            columns = pl.ds(pl.multiple_of(tile * tile_of(units), 128), tile_of(units))
            tokens = blocks[pair].reshape(2 * rows, width)
            gate = jnp.dot(tokens, gate_w[:, columns], preferred_element_type=jnp.float32)
            up = jnp.dot(tokens, up_w[:, columns], preferred_element_type=jnp.float32)
            gate_keep[pair, :, columns] = gate.reshape(2, rows, -1)
            up_keep[pair, :, columns] = up.reshape(2, rows, -1)
            act_keep[pair, :, columns] = (
                (gate / (1.0 + jnp.exp(-gate)) * up).astype(jnp.bfloat16).reshape(2, rows, -1)
            )

        @pl.loop(0, width // tile_of(width))
        def _(tile):
            columns = pl.ds(pl.multiple_of(tile * tile_of(width), 128), tile_of(width))
            act = act_keep[pair].reshape(2 * rows, units)
            fresh[:, :, columns] = dot_cols(act, down_w[columns, :]).reshape(2, rows, -1)

        for copy in stores(chip):
            copy.start()
        scatter.after_term(chip)

    scatter.hops()
    scatter.settle(mixed_ref)
    scatter.finish()
    gather.finish()

    @pl.loop(0, chips)
    def _(chip):
        for copy in stores(chip):
            copy.wait()


def feed_forward_back_kernel(
    chips,
    grad_ref,
    gate_hbm,
    up_hbm,
    down_hbm,
    gate_lin_hbm,
    up_lin_hbm,
    hidden_grad_ref,
    gate_out,
    up_out,
    all_out,
    gate_w,
    up_w,
    down_w,
    gate_lin,
    up_lin,
    gate_keep,
    up_keep,
    load_sem,
    store_sem,
    *comm,
):
    line = Line(chips)
    gather = Gather(line, *comm[:5])
    scatter = Scatter(line, *comm[5:])
    blocks, fresh = gather.blocks, scatter.fresh
    _, rows, width = blocks.shape
    units = gate_w.shape[1]
    copies = load(
        [
            (down_hbm, down_w, load_sem.at[0]),
            (gate_lin_hbm, gate_lin, load_sem.at[1]),
            (up_lin_hbm, up_lin, load_sem.at[2]),
            (gate_hbm, gate_w, load_sem.at[3]),
            (up_hbm, up_w, load_sem.at[4]),
        ]
    )
    line.greet()
    blocks[line.place * 2 + line.core] = grad_ref[...]
    gather.send(line.place)

    def stores(chip):
        pair = pl.ds(chip * 2, 2)
        return [
            pltpu.make_async_copy(gate_keep.at[pair], gate_out.at[pair], store_sem.at[0, chip]),
            pltpu.make_async_copy(up_keep.at[pair], up_out.at[pair], store_sem.at[1, chip]),
            pltpu.make_async_copy(blocks.at[pair], all_out.at[pair], store_sem.at[2, chip]),
        ]

    for copy in copies:
        copy.wait()

    @pl.loop(0, chips)
    def _(step):
        chip = gather.step(step)
        pair = pl.ds(chip * 2, 2)

        @pl.loop(0, units // tile_of(units))
        def _(tile):
            columns = pl.ds(pl.multiple_of(tile * tile_of(units), 128), tile_of(units))
            tokens = blocks[pair].reshape(2 * rows, width)
            grad = jnp.dot(tokens, down_w[:, columns], preferred_element_type=jnp.float32)
            gate = gate_lin[pair, :, columns].reshape(2 * rows, -1)
            up = up_lin[pair, :, columns].reshape(2 * rows, -1)
            sig = 1.0 / (1.0 + jnp.exp(-gate))
            gate_keep[pair, :, columns] = (
                (grad * up * sig * (1.0 + gate * (1.0 - sig)))
                .astype(jnp.bfloat16)
                .reshape(2, rows, -1)
            )
            up_keep[pair, :, columns] = (
                (grad * (gate * sig)).astype(jnp.bfloat16).reshape(2, rows, -1)
            )

        @pl.loop(0, width // tile_of(width))
        def _(tile):
            columns = pl.ds(pl.multiple_of(tile * tile_of(width), 128), tile_of(width))
            gate = gate_keep[pair].reshape(2 * rows, units)
            up = up_keep[pair].reshape(2 * rows, units)
            fresh[:, :, columns] = (
                dot_cols(gate, gate_w[columns, :]) + dot_cols(up, up_w[columns, :])
            ).reshape(2, rows, -1)

        for copy in stores(chip):
            copy.start()
        scatter.after_term(chip)

    scatter.hops()
    scatter.settle(hidden_grad_ref)
    scatter.finish()
    gather.finish()

    @pl.loop(0, chips)
    def _(chip):
        for copy in stores(chip):
            copy.wait()


def whole_spec():
    return pl.BlockSpec(memory_space=pltpu.VMEM)


def far_spec():
    return pl.BlockSpec(memory_space=pl.ANY)


def line_params(collective_id):
    return pltpu.CompilerParams(
        collective_id=collective_id, has_side_effects=True, vmem_limit_bytes=63 * 2**20
    )


def feed_forward(hidden_low, gate_cols, up_cols, down_cols):
    rows, width = hidden_low.shape
    units = gate_cols.shape[1]
    slots = lax.axis_size("seq")
    chips = slots // 2
    weights = [pltpu.VMEM((width, units), jnp.bfloat16)] * 3
    mixed, gate, up, act, every = pl.pallas_call(
        functools.partial(feed_forward_kernel, chips),
        out_shape=(
            jax.ShapeDtypeStruct((rows, width), jnp.float32),
            jax.ShapeDtypeStruct((slots, rows, units), jnp.float32),
            jax.ShapeDtypeStruct((slots, rows, units), jnp.float32),
            jax.ShapeDtypeStruct((slots, rows, units), jnp.bfloat16),
            jax.ShapeDtypeStruct((slots, rows, width), jnp.bfloat16),
        ),
        in_specs=[whole_spec()] + [far_spec()] * 3,
        out_specs=(whole_spec(),) + (far_spec(),) * 4,
        scratch_shapes=weights
        + [
            pltpu.VMEM((slots, rows, units), jnp.float32),
            pltpu.VMEM((slots, rows, units), jnp.float32),
            pltpu.VMEM((slots, rows, units), jnp.bfloat16),
            pltpu.SemaphoreType.DMA((3,)),
            pltpu.SemaphoreType.DMA((4, chips)),
        ]
        + Gather.scratch(chips, rows, width)
        + Scatter.scratch(chips, rows, width),
        compiler_params=line_params(1),
        name="feed_forward",
    )(hidden_low, gate_cols, up_cols, down_cols)
    return mixed, gate, up, act.reshape(-1, units), every.reshape(-1, width)


def feed_forward_back(grad_low, gate_cols, up_cols, down_cols, gate, up):
    rows, width = grad_low.shape
    units = gate_cols.shape[1]
    slots = lax.axis_size("seq")
    chips = slots // 2
    weights = [pltpu.VMEM((width, units), jnp.bfloat16)] * 3
    hidden_grad, gate_grad, up_grad, every = pl.pallas_call(
        functools.partial(feed_forward_back_kernel, chips),
        out_shape=(
            jax.ShapeDtypeStruct((rows, width), jnp.float32),
            jax.ShapeDtypeStruct((slots, rows, units), jnp.bfloat16),
            jax.ShapeDtypeStruct((slots, rows, units), jnp.bfloat16),
            jax.ShapeDtypeStruct((slots, rows, width), jnp.bfloat16),
        ),
        in_specs=[whole_spec()] + [far_spec()] * 5,
        out_specs=(whole_spec(),) + (far_spec(),) * 3,
        scratch_shapes=weights
        + [
            pltpu.VMEM((slots, rows, units), jnp.float32),
            pltpu.VMEM((slots, rows, units), jnp.float32),
            pltpu.VMEM((slots, rows, units), jnp.bfloat16),
            pltpu.VMEM((slots, rows, units), jnp.bfloat16),
            pltpu.SemaphoreType.DMA((5,)),
            pltpu.SemaphoreType.DMA((3, chips)),
        ]
        + Gather.scratch(chips, rows, width)
        + Scatter.scratch(chips, rows, width),
        compiler_params=line_params(2),
        name="feed_forward_back",
    )(grad_low, gate_cols, up_cols, down_cols, gate, up)
    return (
        hidden_grad,
        gate_grad.reshape(-1, units),
        up_grad.reshape(-1, units),
        every.reshape(-1, width),
    )


def peers_of(axis, size):
    me = lax.axis_index(axis)
    return me, lambda step: (me + step) % size


def greet_cross(seq_count, fsdp_count):
    seq, seq_peer = peers_of("seq", seq_count)
    fsdp, fsdp_peer = peers_of("fsdp", fsdp_count)
    barrier = pltpu.get_barrier_semaphore()
    for step in range(1, seq_count):
        pl.semaphore_signal(
            barrier, inc=1, device_id=(seq_peer(step), fsdp), device_id_type=MESH
        )
    for step in range(1, fsdp_count):
        pl.semaphore_signal(
            barrier, inc=1, device_id=(seq, fsdp_peer(step)), device_id_type=MESH
        )
    pl.semaphore_wait(barrier, seq_count + fsdp_count - 2)


class Cross:
    def __init__(self, seq_count, fsdp_count):
        self.seq_count, self.fsdp_count = seq_count, fsdp_count
        self.seq, self.seq_peer = peers_of("seq", seq_count)
        self.fsdp, self.fsdp_peer = peers_of("fsdp", fsdp_count)
        self.square = fsdp_count == 4
        if self.square:
            row, place = self.fsdp // 2, self.fsdp % 2
            self.sides = (row * 2 + 1 - place, (1 - row) * 2 + place)
            self.corner = (1 - row) * 2 + 1 - place
        else:
            self.sides = tuple(self.fsdp_peer(step) for step in range(1, fsdp_count))

    def remote(self, src, dst, send, recv, seq, fsdp):
        return pltpu.make_async_remote_copy(
            src_ref=src,
            dst_ref=dst,
            send_sem=send,
            recv_sem=recv,
            device_id=(seq, fsdp),
            device_id_type=MESH,
        )


class Spread:
    def __init__(self, cross, sources, weights, row_send, row_recv, side_send, side_recv, half_send, half_recv):
        self.cross, self.sources, self.weights = cross, sources, weights
        self.row_send, self.row_recv = row_send, row_recv
        self.side_send, self.side_recv = side_send, side_recv
        self.half_send, self.half_recv = half_send, half_recv
        self.kinds, self.columns = len(sources), weights.shape[-1]
        self.rows = weights.shape[-2]

    @staticmethod
    def scratch(kinds, seq_count, fsdp_count, rows, columns):
        dma = pltpu.SemaphoreType.DMA
        sides = 2 if fsdp_count == 4 else fsdp_count - 1
        return [
            pltpu.VMEM((kinds, seq_count, fsdp_count, rows, columns), jnp.bfloat16),
            dma((kinds, seq_count)),
            dma((kinds, seq_count)),
            dma((seq_count, sides)),
            dma((seq_count, sides)),
            dma((seq_count, 2)),
            dma((seq_count, 2)),
        ]

    def block(self, owner):
        return pl.ds(pl.multiple_of(owner * self.columns, 128), self.columns)

    def row(self, kind, step):
        cross = self.cross
        peer = cross.seq_peer(step)
        return cross.remote(
            self.sources[kind].at[:, self.block(peer)],
            self.weights.at[kind, cross.seq, cross.fsdp],
            self.row_send.at[kind, step],
            self.row_recv.at[kind, step],
            peer,
            cross.fsdp,
        )

    def side(self, owner, side):
        cross = self.cross
        ref = self.weights.at[:, owner, cross.fsdp]
        return cross.remote(
            ref,
            ref,
            self.side_send.at[owner, side],
            self.side_recv.at[owner, side],
            cross.seq,
            cross.sides[side],
        )

    def half(self, owner, side):
        cross = self.cross
        rows = pl.ds(side * (self.rows // 2), self.rows // 2)
        ref = self.weights.at[:, owner, cross.sides[side], rows]
        return cross.remote(
            ref,
            ref,
            self.half_send.at[owner, side],
            self.half_recv.at[owner, side],
            cross.seq,
            cross.sides[1 - side],
        )

    def start(self):
        cross = self.cross
        for step in range(1, cross.seq_count):
            for kind in range(self.kinds):
                self.row(kind, step).start()

    def own(self):
        cross = self.cross
        for kind in range(self.kinds):
            self.weights[kind, cross.seq, cross.fsdp] = self.sources[kind][:, self.block(cross.seq)]
        self.pass_on(0)

    def owner(self, step):
        return (self.cross.seq - step + self.cross.seq_count) % self.cross.seq_count

    def take(self, step):
        for kind in range(self.kinds):
            self.row(kind, step).wait_recv()
        self.pass_on(step)

    def pass_on(self, step):
        for side in range(len(self.cross.sides)):
            self.side(self.owner(step), side).start()

    def relay(self, step):
        owner = self.owner(step)
        for side in range(len(self.cross.sides)):
            self.side(owner, side).wait_recv()
            if self.cross.square:
                self.half(owner, side).start()

    def settle(self, step):
        if self.cross.square:
            for side in range(2):
                self.half(self.owner(step), side).wait_recv()

    def finish(self):
        cross = self.cross

        @pl.loop(1, cross.seq_count)
        def _(step):
            for kind in range(self.kinds):
                self.row(kind, step).wait_send()

        @pl.loop(0, cross.seq_count)
        def _(owner):
            for side in range(len(cross.sides)):
                self.side(owner, side).wait_send()
                if cross.square:
                    self.half(owner, side).wait_send()


AHEAD = 2
LAG = 3
RING = 8


class Collect:
    def __init__(self, cross, kinds, fill, terms, side_in, half_out, half_in, row_out, row_in, side_send, side_recv, half_send, half_recv, row_send, row_recv):
        self.cross, self.fill, self.terms = cross, fill, terms
        self.side_in, self.half_out, self.half_in = side_in, half_out, half_in
        self.row_out, self.row_in = row_out, row_in
        self.side_send, self.side_recv = side_send, side_recv
        self.half_send, self.half_recv = half_send, half_recv
        self.row_send, self.row_recv = row_send, row_recv
        self.rows, self.columns = terms.shape[-2:]
        self.items = kinds * cross.seq_count

    @staticmethod
    def scratch(kinds, seq_count, fsdp_count, rows, columns):
        dma = pltpu.SemaphoreType.DMA
        vmem = pltpu.VMEM
        bf16 = jnp.bfloat16
        items = kinds * seq_count
        if fsdp_count == 4:
            arrays = [
                vmem((items, 2, 2, rows // 2, columns), bf16),
                vmem((RING, 2, rows // 2, columns), bf16),
                vmem((items, 2, rows // 2, columns), bf16),
            ]
            sides = (2, 2)
        else:
            arrays = [
                vmem((items, fsdp_count - 1, rows, columns), bf16),
                vmem((1, 1, 16, 128), bf16),
                vmem((1, 1, 16, 128), bf16),
            ]
            sides = (fsdp_count - 1, 1)
        return [vmem((RING, fsdp_count, rows, columns), bf16)] + arrays + [
            vmem((RING, rows, columns), bf16),
            vmem((items, rows, columns), bf16),
            dma((items,) + sides),
            dma((items,) + sides),
            dma((items, 2)),
            dma((items, 2)),
            dma((items,)),
            dma((items,)),
        ]

    def half_rows(self, side):
        return pl.ds(side * (self.rows // 2), self.rows // 2)

    def side(self, turn, side, which):
        cross = self.cross
        if not cross.square:
            return cross.remote(
                self.terms.at[turn % RING, cross.sides[side]],
                self.side_in.at[turn, side],
                self.side_send.at[turn, side, 0],
                self.side_recv.at[turn, side, 0],
                cross.seq,
                cross.sides[side],
            )
        target = cross.sides[side] if which == 0 else cross.corner
        return cross.remote(
            self.terms.at[turn % RING, target, self.half_rows(side)],
            self.side_in.at[turn, side, which],
            self.side_send.at[turn, side, which],
            self.side_recv.at[turn, side, which],
            cross.seq,
            cross.sides[side],
        )

    def half(self, turn, side):
        cross = self.cross
        return cross.remote(
            self.half_out.at[turn % RING, side],
            self.half_in.at[turn, side],
            self.half_send.at[turn, side],
            self.half_recv.at[turn, side],
            cross.seq,
            cross.sides[1 - side],
        )

    def row(self, turn):
        cross = self.cross
        return cross.remote(
            self.row_out.at[turn % RING],
            self.row_in.at[turn],
            self.row_send.at[turn],
            self.row_recv.at[turn],
            self.place(turn)[1],
            cross.fsdp,
        )

    def place(self, turn):
        count = self.cross.seq_count
        return turn // count, self.cross.seq_peer(turn % count + 1)

    def is_own(self, turn):
        return turn % self.cross.seq_count == self.cross.seq_count - 1

    @property
    def ways(self):
        return range(2) if self.cross.square else range(1)

    def sides(self, turn):
        return [
            self.side(turn, side, which)
            for which in reversed(self.ways)
            for side in range(len(self.cross.sides))
        ]

    def send(self, turn, first):
        if not first:

            @pl.when(turn >= RING)
            def _():
                for copy in self.sides(turn - RING):
                    copy.wait_send()

        kind, owner = self.place(turn)
        self.fill(kind, owner, turn % RING)
        for copy in self.sides(turn):
            copy.start()

    def middle(self, turn):
        if not self.cross.square:
            return
        cross = self.cross

        @pl.when(turn >= RING)
        def _():
            for side in range(2):
                self.half(turn - RING, side).wait_send()

        for side in range(2):
            self.side(turn, side, 1).wait_recv()
            mine = self.terms[turn % RING, cross.sides[1 - side], self.half_rows(side)]
            self.half_out[turn % RING, side] = (
                mine.astype(jnp.float32) + self.side_in[turn, side, 1].astype(jnp.float32)
            ).astype(jnp.bfloat16)
            self.half(turn, side).start()

    def totals(self, turn):
        cross = self.cross
        found = []
        if cross.square:
            for side in range(2):
                self.side(turn, side, 0).wait_recv()
                self.half(turn, side).wait_recv()
                rows = self.half_rows(side)
                total = self.terms[turn % RING, cross.fsdp, rows].astype(jnp.float32)
                total = total + self.side_in[turn, side, 0].astype(jnp.float32)
                total = total + self.half_in[turn, side].astype(jnp.float32)
                found.append((rows, total))
        else:
            total = self.terms[turn % RING, cross.fsdp].astype(jnp.float32)
            for side in range(len(cross.sides)):
                self.side(turn, side, 0).wait_recv()
                total = total + self.side_in[turn, side].astype(jnp.float32)
            found.append((pl.ds(0, self.rows), total))
        return found

    def ship(self, turn):
        own = self.is_own(turn)
        self.free_row(turn - RING)

        @pl.when(own)
        def _():
            for rows, total in self.totals(turn):
                self.row_in[turn, rows] = total.astype(jnp.bfloat16)

        @pl.when(jnp.logical_not(own))
        def _():
            for rows, total in self.totals(turn):
                self.row_out[turn % RING, rows] = total.astype(jnp.bfloat16)
            self.row(turn).start()

    def free_row(self, turn):
        @pl.when((turn >= 0) & jnp.logical_not(self.is_own(turn)))
        def _():
            self.row(turn).wait_send()

    def beat(self, turn):
        ahead = turn + AHEAD

        @pl.when(ahead < self.items)
        def _():
            self.send(ahead, False)

        @pl.when(turn < self.items)
        def _():
            self.middle(turn)

        @pl.when(turn >= LAG)
        def _():
            self.ship(turn - LAG)

    def begin(self):
        @pl.loop(0, min(AHEAD, self.items))
        def _(turn):
            self.send(turn, True)

    @property
    def beats(self):
        return self.items + LAG

    def receive(self, turn, put):
        count = self.cross.seq_count

        @pl.when(jnp.logical_not(self.is_own(turn)))
        def _():
            self.row(turn).wait_recv()

        sender = (self.cross.seq - turn % count - 1 + count) % count
        put(turn // count, sender, self.row_in[turn].astype(jnp.float32))

    def finish(self):
        cross = self.cross
        late = max(self.items - RING, 0)

        @pl.loop(late, self.items)
        def _(turn):
            for copy in self.sides(turn):
                copy.wait_send()
            if cross.square:
                for side in range(2):
                    self.half(turn, side).wait_send()
            self.free_row(turn)


def bring_in_kernel(
    chips,
    fsdp_count,
    inputs_ref,
    query_ref,
    key_ref,
    value_ref,
    output_ref,
    gate_ref,
    gains_ref,
    inputs_out,
    weights_out,
    output_out,
    gate_out,
    gains_out,
    outputs,
    gains,
    gain_row_send,
    gain_row_recv,
    gain_column_send,
    gain_column_recv,
    output_send,
    output_recv,
    store_sem,
    *comm,
):
    line = Line(chips)
    cross = Cross(2 * chips, fsdp_count)
    gather = Gather(line, *comm[:5])
    attention = Spread(cross, (query_ref, key_ref, value_ref), *comm[5:12])
    gate = Spread(cross, (gate_ref,), *comm[12:])
    seq_count, seq, fsdp = cross.seq_count, cross.seq, cross.fsdp

    def gain_row(step):
        return cross.remote(
            gains_ref,
            gains.at[seq, fsdp],
            gain_row_send.at[step],
            gain_row_recv.at[step],
            cross.seq_peer(step),
            fsdp,
        )

    def gain_column(owner, step):
        ref = gains.at[owner, fsdp]
        return cross.remote(
            ref,
            ref,
            gain_column_send.at[owner, step],
            gain_column_recv.at[owner, step],
            seq,
            cross.fsdp_peer(step),
        )

    def output_copy(step):
        return cross.remote(
            output_ref,
            outputs.at[fsdp],
            output_send.at[step],
            output_recv.at[step],
            seq,
            cross.fsdp_peer(step),
        )

    greet_cross(seq_count, fsdp_count)
    for step in range(1, seq_count):
        gain_row(step).start()
    attention.start()
    gate.start()
    gather.blocks[line.place * 2 + line.core] = inputs_ref[...]
    gather.send(line.place)
    gains[seq, fsdp] = gains_ref[...]
    outputs[fsdp] = output_ref[...]
    attention.own()
    for step in range(1, fsdp_count):
        gain_column(seq, step).start()

    @pl.loop(1, seq_count)
    def _(step):
        attention.take(step)
        gain_row(step).wait_recv()
        for peer in range(1, fsdp_count):
            gain_column(attention.owner(step), peer).start()
        attention.relay(step - 1)

    gate.own()
    attention.relay(seq_count - 1)
    gather.step(0)

    @pl.loop(1, seq_count)
    def _(step):
        gate.take(step)
        gate.relay(step - 1)

        @pl.when((step % 2 == 0) & (step > 2))
        def _():
            gather.step(step // 2 - 1)

    for step in range(1, fsdp_count):
        output_copy(step).start()
    gate.relay(seq_count - 1)
    if chips > 1:
        gather.step(chips - 1)
    inputs_store = pltpu.make_async_copy(gather.blocks, inputs_out, store_sem.at[0])
    inputs_store.start()

    @pl.loop(0, seq_count)
    def _(step):
        attention.settle(step)
        for peer in range(1, fsdp_count):
            gain_column(step, peer).wait_recv()

    weights_store = pltpu.make_async_copy(attention.weights, weights_out, store_sem.at[1])
    weights_store.start()
    for step in range(1, fsdp_count):
        output_copy(step).wait_recv()
    output_store = pltpu.make_async_copy(outputs, output_out, store_sem.at[2])
    output_store.start()
    gains_out[...] = gains[...]

    @pl.loop(0, seq_count)
    def _(step):
        gate.settle(step)

    gate_store = pltpu.make_async_copy(gate.weights, gate_out, store_sem.at[3])
    gate_store.start()
    gather.finish()
    attention.finish()
    gate.finish()

    @pl.loop(1, seq_count)
    def _(step):
        gain_row(step).wait_send()

    @pl.loop(0, seq_count)
    def _(owner):
        for step in range(1, fsdp_count):
            gain_column(owner, step).wait_send()

    for step in range(1, fsdp_count):
        output_copy(step).wait_send()
    inputs_store.wait()
    weights_store.wait()
    output_store.wait()
    gate_store.wait()


def bring_in(local_in, query_weight, key_weight, value_weight, output_weight, gate_weight, gains):
    rows, width = local_in.shape
    slots = lax.axis_size("seq")
    fsdp_count = lax.axis_size("fsdp")
    chips = slots // 2
    own_rows, columns = query_weight.shape[0], query_weight.shape[1] // slots
    units = gate_weight.shape[1] // slots
    bf16, dma = jnp.bfloat16, pltpu.SemaphoreType.DMA
    lanes = pl.cdiv(gains.shape[1], 128) * 128
    padded = jnp.pad(gains, ((0, 16 - gains.shape[0]), (0, lanes - gains.shape[1])))
    inputs_all, weights, outputs, gate, gains_all = pl.pallas_call(
        functools.partial(bring_in_kernel, chips, fsdp_count),
        out_shape=(
            jax.ShapeDtypeStruct((slots, rows, width), bf16),
            jax.ShapeDtypeStruct((3, slots, fsdp_count, own_rows, columns), bf16),
            jax.ShapeDtypeStruct((fsdp_count, own_rows, width), bf16),
            jax.ShapeDtypeStruct((1, slots, fsdp_count, own_rows, units), bf16),
            jax.ShapeDtypeStruct((slots, fsdp_count, 16, lanes), bf16),
        ),
        in_specs=[whole_spec()] * 7,
        out_specs=(far_spec(),) * 4 + (whole_spec(),),
        scratch_shapes=[
            pltpu.VMEM((fsdp_count, own_rows, width), bf16),
            pltpu.VMEM((slots, fsdp_count, 16, lanes), bf16),
            dma((slots,)),
            dma((slots,)),
            dma((slots, fsdp_count)),
            dma((slots, fsdp_count)),
            dma((fsdp_count,)),
            dma((fsdp_count,)),
            dma((4,)),
        ]
        + Gather.scratch(chips, rows, width)
        + Spread.scratch(3, slots, fsdp_count, own_rows, columns)
        + Spread.scratch(1, slots, fsdp_count, own_rows, units),
        compiler_params=line_params(3),
        name="bring_in",
    )(local_in, query_weight, key_weight, value_weight, output_weight, gate_weight, padded)
    gains_all = gains_all[:, :, : gains.shape[0], : gains.shape[1]]
    return (
        inputs_all.reshape(-1, width),
        weights.reshape(3, -1, columns),
        outputs.reshape(-1, width),
        gate.reshape(-1, units),
        gains_all.transpose(2, 0, 1, 3).reshape(gains.shape[0], -1),
    )


def product_terms(scatter, pairs, chip):
    _, rows, width = scatter.fresh.shape
    pair = pl.ds(chip * 2, 2)

    @pl.loop(0, width // tile_of(width))
    def _(tile):
        columns = pl.ds(pl.multiple_of(tile * tile_of(width), 128), tile_of(width))
        total = None
        for left, right, across in pairs:
            tokens = left[pair].reshape(2 * rows, -1)
            if across:
                term = dot_cols(tokens, right[columns, :])
            else:
                term = jnp.dot(tokens, right[:, columns], preferred_element_type=jnp.float32)
            total = term if total is None else total + term
        scatter.fresh[:, :, columns] = total.reshape(2, rows, -1)

    scatter.after_term(chip)


def project_kernel(
    chips,
    fsdp_count,
    attended_ref,
    output_ref,
    up_ref,
    down_ref,
    result,
    up_out,
    down_out,
    store_sem,
    *comm,
):
    line = Line(chips)
    cross = Cross(2 * chips, fsdp_count)
    count = len(Scatter.scratch(chips, 4, 128))
    scatter = Scatter(line, *comm[:count])
    up = Spread(cross, (up_ref,), *comm[count : count + 7])
    down = Spread(cross, (down_ref,), *comm[count + 7 :])
    greet_cross(cross.seq_count, fsdp_count)
    up.start()
    down.start()
    up.own()

    @pl.loop(0, chips)
    def _(step):
        product_terms(scatter, [(attended_ref, output_ref, False)], line.order(chips - 1 - step))

    @pl.loop(1, cross.seq_count)
    def _(step):
        up.take(step)
        up.relay(step - 1)

    down.own()
    up.relay(cross.seq_count - 1)
    scatter.hop(0)

    @pl.loop(1, cross.seq_count)
    def _(step):
        down.take(step)
        down.relay(step - 1)

        @pl.when(step % 2 == 0)
        def _():
            scatter.hop(step // 2)

    down.relay(cross.seq_count - 1)

    @pl.loop(0, cross.seq_count)
    def _(step):
        up.settle(step)

    up_store = pltpu.make_async_copy(up.weights, up_out, store_sem.at[0])
    up_store.start()
    scatter.settle(result)

    @pl.loop(0, cross.seq_count)
    def _(step):
        down.settle(step)

    down_store = pltpu.make_async_copy(down.weights, down_out, store_sem.at[1])
    down_store.start()
    scatter.finish()
    up.finish()
    down.finish()
    up_store.wait()
    down_store.wait()


def project(attended, output_rows, up_weight, down_weight):
    slots = lax.axis_size("seq")
    fsdp_count = lax.axis_size("fsdp")
    chips = slots // 2
    rows = attended.shape[0] // slots
    width = output_rows.shape[1]
    own_rows, units = up_weight.shape[0], up_weight.shape[1] // slots
    weight = jax.ShapeDtypeStruct((1, slots, fsdp_count, own_rows, units), jnp.bfloat16)
    projected, up, down = pl.pallas_call(
        functools.partial(project_kernel, chips, fsdp_count),
        out_shape=(jax.ShapeDtypeStruct((rows, width), jnp.float32), weight, weight),
        in_specs=[whole_spec()] * 4,
        out_specs=(whole_spec(), far_spec(), far_spec()),
        scratch_shapes=[pltpu.SemaphoreType.DMA((2,))]
        + Scatter.scratch(chips, rows, width)
        + Spread.scratch(1, slots, fsdp_count, own_rows, units) * 2,
        compiler_params=line_params(5),
        name="project",
    )(attended.reshape(slots, rows, -1), output_rows, up_weight, down_weight)
    return projected, up.reshape(-1, units), down.reshape(-1, units)


def dot_rows(left, right, precision=None):
    return lax.dot_general(
        left,
        right,
        (((0,), (0,)), ((), ())),
        precision=precision,
        preferred_element_type=jnp.float32,
    )


EXACT = lax.Precision.HIGHEST


def turn_heads(tensor, cosine, sine):
    heads = [
        tensor[:, first : first + DH] * cosine
        + pltpu.roll(tensor[:, first : first + DH], DH // 2, 1) * sine
        for first in range(0, tensor.shape[1], DH)
    ]
    return jnp.concatenate(heads, axis=1) if len(heads) > 1 else heads[0]


def attention_weights(queries, keys, first_row, segment_column, segment_row):
    rows, count = queries.shape[0], keys.shape[0]
    scores = dot_cols(queries, keys) * DH ** (-0.5)
    query_place = first_row + lax.broadcasted_iota(jnp.int32, (rows, count), 0)
    key_place = lax.broadcasted_iota(jnp.int32, (rows, count), 1)
    allowed = (key_place <= query_place) & (segment_row == segment_column)
    scores = jnp.where(allowed, scores, neg_fill)
    expanded = jnp.exp(scores - jnp.max(scores, axis=-1, keepdims=True))
    return expanded / jnp.sum(expanded, axis=-1, keepdims=True)


class RowSum:
    def __init__(self, cross, local, every, send_sem, recv_sem):
        self.cross, self.local, self.every = cross, local, every
        self.send_sem, self.recv_sem = send_sem, recv_sem

    @staticmethod
    def scratch(seq_count, shape):
        dma = pltpu.SemaphoreType.DMA
        return [
            pltpu.VMEM(shape, jnp.float32),
            pltpu.VMEM((seq_count,) + shape, jnp.float32),
            dma((seq_count,)),
            dma((seq_count,)),
        ]

    def copy(self, step):
        cross = self.cross
        return cross.remote(
            self.local,
            self.every.at[step],
            self.send_sem.at[step],
            self.recv_sem.at[step],
            cross.seq_peer(step),
            cross.fsdp,
        )

    def send(self, value):
        self.local[...] = value
        for step in range(1, self.cross.seq_count):
            self.copy(step).start()

    def receive(self):
        total = self.local[...]
        for step in range(1, self.cross.seq_count):
            self.copy(step).wait_recv()
            total = total + self.every[step]
        return total

    def finish(self):
        for step in range(1, self.cross.seq_count):
            self.copy(step).wait_send()


def pick_row(row, shape):
    return jnp.where(lax.broadcasted_iota(jnp.int32, shape, 0) == row, 1.0, 0.0)


def gather_back_kernel(chips, fsdp_count, *refs):
    local_ref, output_ref, gains_ref, inverse_ref, cosine_ref, sine_ref = refs[:6]
    segment_column, segment_row = refs[6:8]
    hidden_hbm, grad_hbm, gate_hbm, up_hbm, act_hbm = refs[8:13]
    heads_hbm, pre_hbm = refs[13:15]
    refs = refs[15:]
    results, output_term, grads_out, gain_out = refs[:3], refs[3], refs[4], refs[5]
    refs = refs[6:]
    tokens, units, heads, pre, gathered, grad_query, grad_key, grad_value = refs[:8]
    load_sem, refs = refs[8], refs[9:]
    line = Line(chips)
    cross = Cross(2 * chips, fsdp_count)
    gather = Gather(line, *refs[:5])
    sums = RowSum(cross, *refs[5:9])
    all_tokens, width = tokens.shape[1:]
    block_units = units.shape[-1]
    columns = output_ref.shape[0]
    blocks = gather.blocks
    rows = blocks.shape[1]

    def fill(kind, owner, slot):
        span = width // cross.seq_count
        chosen = tokens[kind // 2, :, pl.ds(pl.multiple_of(owner * span, 128), span)]

        @pl.loop(0, block_units // tile_of(block_units))
        def _(tile):
            part = pl.ds(pl.multiple_of(tile * tile_of(block_units), 128), tile_of(block_units))
            term = dot_rows(chosen, units[kind, :, part]).astype(jnp.bfloat16)
            collect.terms[slot, :, :, part] = term.reshape(fsdp_count, -1, term.shape[1])

    collect = Collect(cross, 3, fill, *refs[9:])
    copies = load(
        [
            (hidden_hbm, tokens.at[0], load_sem.at[0]),
            (gate_hbm, units.at[0], load_sem.at[1]),
            (up_hbm, units.at[1], load_sem.at[2]),
            (grad_hbm, tokens.at[1], load_sem.at[3]),
            (act_hbm, units.at[2], load_sem.at[4]),
            (heads_hbm, heads, load_sem.at[5]),
            (pre_hbm, pre, load_sem.at[6]),
        ]
    )
    greet_cross(cross.seq_count, fsdp_count)
    blocks[line.place * 2 + line.core] = local_ref[...]
    gather.send(line.place)
    grad_key[...] = jnp.zeros_like(grad_key)
    grad_value[...] = jnp.zeros_like(grad_value)
    for copy in copies[:2]:
        copy.wait()
    collect.begin()
    for copy in copies[2:]:
        copy.wait()

    def arrive(step):
        chip = gather.step(step)
        whole = blocks[pl.ds(chip * 2, 2)].reshape(2 * rows, width)
        found = dot_cols(whole, output_ref[...]).astype(jnp.bfloat16)
        gathered[pl.ds(chip * 2 * rows, 2 * rows), :] = found

    arrive(0)
    query_rows = 128
    blocks_of_rows = all_tokens // query_rows
    first_beat = 3 * (chips - 1)

    def attend(block):
        first = pl.multiple_of(block * query_rows, query_rows)
        span = pl.ds(first, query_rows)
        for head in range(0, columns, DH):
            part = pl.ds(head, DH)
            queries, keys, values = heads[0, span, part], heads[1, :, part], heads[2, :, part]
            outer = gathered[span, part]
            probs = attention_weights(
                queries, keys, first, segment_column[span, :], segment_row[...]
            )
            grad_value[:, part] += dot_rows(probs.astype(jnp.bfloat16), outer)
            grad_probs = dot_cols(outer, values)
            delta = jnp.sum(probs * grad_probs, axis=-1, keepdims=True)
            grad_scores = (probs * (grad_probs - delta)).astype(jnp.bfloat16)
            grad_query[span, part] = jnp.dot(
                grad_scores, keys, preferred_element_type=jnp.float32
            )
            grad_key[:, part] += dot_rows(grad_scores, queries)

    def errors(kind, grad):
        scaled = (grad[...] * DH ** (-0.5)).astype(jnp.bfloat16).astype(jnp.float32)
        error = turn_heads(scaled, cosine_ref[...], -sine_ref[...])
        inverse = inverse_ref[:, kind : kind + 1]
        return error, pre[kind] * inverse, inverse

    def send_means():
        total = None
        for kind, grad in enumerate((grad_query, grad_key)):
            error, unit, _ = errors(kind, grad)
            product = error * unit
            gain_out[kind : kind + 1, :] = jnp.sum(product, axis=0, keepdims=True)
            row = lax.dot_general(
                pick_row(kind, (8, columns)),
                product * gains_ref[kind : kind + 1, :],
                (((1,), (1,)), ((), ())),
                precision=EXACT,
                preferred_element_type=jnp.float32,
            )
            total = row if total is None else total + row
        sums.send(total)
        grads_out[2] = grad_value[...].astype(jnp.bfloat16)

        @pl.loop(0, width // tile_of(width))
        def _(tile):
            part = pl.ds(pl.multiple_of(tile * tile_of(width), 128), tile_of(width))
            outer = blocks[:, :, part].reshape(all_tokens, -1)
            output_term[:, part] = dot_rows(heads[3], outer).astype(jnp.bfloat16)

    def finish_grads():
        means = sums.receive() / width
        for kind, grad in enumerate((grad_query, grad_key)):
            error, unit, inverse = errors(kind, grad)
            mean = dot_rows(means, pick_row(kind, (8, 128)), EXACT)[:, :1]
            grads_out[kind] = (
                inverse * (error * gains_ref[kind : kind + 1, :] - unit * mean)
            ).astype(jnp.bfloat16)

    @pl.loop(0, collect.beats)
    def _(turn):
        collect.beat(turn)

        @pl.when((turn % 3 == 2) & (turn // 3 + 1 < chips))
        def _():
            arrive(turn // 3 + 1)

        @pl.when((turn >= first_beat) & (turn < first_beat + blocks_of_rows))
        def _():
            attend(turn - first_beat)

        @pl.when(turn == first_beat + blocks_of_rows)
        def _():
            send_means()

        @pl.when(turn == first_beat + blocks_of_rows + 3)
        def _():
            finish_grads()

    @pl.loop(0, cross.seq_count)
    def _(turn):
        for kind in range(3):

            def put(_, sender, value):
                part = pl.ds(pl.multiple_of(sender * block_units, 128), block_units)
                results[kind][:, part] = value

            collect.receive(kind * cross.seq_count + turn, put)

    collect.finish()
    gather.finish()
    sums.finish()


def gather_back(local, output_rows, gains, inverse, tables, segment_row, far, heads, pre):
    rows, width = local.shape
    slots = lax.axis_size("seq")
    fsdp_count = lax.axis_size("fsdp")
    chips = slots // 2
    own = width // (slots * fsdp_count)
    units = far[2].shape[1]
    _, tokens, columns = heads.shape
    bf16, f32 = jnp.bfloat16, jnp.float32
    found = pl.pallas_call(
        functools.partial(gather_back_kernel, chips, fsdp_count),
        out_shape=(jax.ShapeDtypeStruct((own, units * slots), f32),) * 3
        + (
            jax.ShapeDtypeStruct((columns, width), bf16),
            jax.ShapeDtypeStruct((3, tokens, columns), bf16),
            jax.ShapeDtypeStruct((8, columns), f32),
        ),
        in_specs=[whole_spec()] * 8 + [far_spec()] * 7,
        out_specs=(whole_spec(),) * 6,
        scratch_shapes=[
            pltpu.VMEM((2, tokens, width), bf16),
            pltpu.VMEM((3, tokens, units), bf16),
            pltpu.VMEM((4, tokens, columns), bf16),
            pltpu.VMEM((2, tokens, columns), f32),
            pltpu.VMEM((tokens, columns), bf16),
            pltpu.VMEM((tokens, columns), f32),
            pltpu.VMEM((tokens, columns), f32),
            pltpu.VMEM((tokens, columns), f32),
            pltpu.SemaphoreType.DMA((7,)),
        ]
        + Gather.scratch(chips, rows, width)
        + RowSum.scratch(slots, (8, tokens))
        + Collect.scratch(3, slots, fsdp_count, own, units),
        compiler_params=line_params(6),
        name="gather_back",
    )(
        local,
        output_rows,
        gains,
        inverse,
        *tables,
        segment_row.reshape(tokens, 1),
        segment_row.reshape(1, tokens),
        *far,
        heads,
        pre,
    )
    return found[:3], found[3], found[4], found[5]


def take_out_kernel(
    chips,
    fsdp_count,
    *refs,
):
    grads_ref, rights, tokens_ref = refs[0], refs[1], refs[2]
    output_ref, gains_ref, refs = refs[3], refs[4], refs[5:]
    result, weight_outs, output_out, gains_out, refs = refs[0], refs[1:4], refs[4], refs[5], refs[6:]
    output_in, gain_in, gain_out, gain_rows, refs = refs[0], refs[1], refs[2], refs[3], refs[4:]
    output_send, output_recv, gain_send, gain_recv, gain_row_send, gain_row_recv = refs[:6]
    comm = refs[6:]
    line = Line(chips)
    cross = Cross(2 * chips, fsdp_count)
    seq_count, seq, fsdp = cross.seq_count, cross.seq, cross.fsdp
    scatter = Scatter(line, *comm[:-12])
    columns = rights.shape[-1]
    rows, width = scatter.fresh.shape[1:]

    def fill(kind, owner, slot):
        span = width // seq_count
        part = pl.ds(pl.multiple_of(owner * span, 128), span)
        chosen = tokens_ref[:, part]
        for kind in range(3):
            term = dot_rows(chosen, grads_ref[kind].reshape(-1, columns)).astype(jnp.bfloat16)
            collect.terms[slot, :, :, kind * columns : (kind + 1) * columns] = term.reshape(
                fsdp_count, -1, columns
            )

    collect = Collect(cross, 1, fill, *comm[-12:])

    def output_copy(step):
        peer = cross.fsdp_peer(step)
        return cross.remote(
            output_ref.at[peer],
            output_in.at[step],
            output_send.at[step],
            output_recv.at[step],
            seq,
            peer,
        )

    def gain_copy(step):
        peer = cross.fsdp_peer(step)
        return cross.remote(
            gains_ref.at[peer], gain_in.at[step], gain_send.at[step], gain_recv.at[step], seq, peer
        )

    def gain_row(step):
        peer = cross.seq_peer(step)
        return cross.remote(
            gain_out.at[peer],
            gain_rows.at[step],
            gain_row_send.at[step],
            gain_row_recv.at[step],
            peer,
            fsdp,
        )

    greet_cross(seq_count, fsdp_count)
    for step in range(1, fsdp_count):
        gain_copy(step).start()

    collect.begin()

    @pl.loop(0, chips)
    def _(step):
        product_terms(
            scatter,
            [(grads_ref.at[kind], rights.at[kind], True) for kind in range(3)],
            line.order(chips - 1 - step),
        )

    total = gains_ref[fsdp]
    for step in range(1, fsdp_count):
        gain_copy(step).wait_recv()
        total = total + gain_in[step]
    gain_out[...] = total
    for step in range(1, seq_count):
        gain_row(step).start()

    @pl.loop(0, collect.beats)
    def _(turn):
        collect.beat(turn)

        @pl.when(turn == seq_count - AHEAD)
        def _():
            for step in range(1, fsdp_count):
                output_copy(step).start()

        @pl.when((turn % 2 == 0) & (turn < seq_count))
        def _():
            scatter.hop(turn // 2)

    total = output_ref[fsdp].astype(jnp.float32)
    for step in range(1, fsdp_count):
        output_copy(step).wait_recv()
        total = total + output_in[step].astype(jnp.float32)
    output_out[...] = total
    scatter.settle(result)
    total = gain_out[seq]
    for step in range(1, seq_count):
        gain_row(step).wait_recv()
        total = total + gain_rows[step]
    gains_out[...] = total

    def put(_, sender, value):
        block = pl.ds(pl.multiple_of(sender * columns, 128), columns)
        for kind in range(3):
            weight_outs[kind][:, block] = value[:, kind * columns : (kind + 1) * columns]

    @pl.loop(0, seq_count)
    def _(turn):
        collect.receive(turn, put)

    scatter.finish()
    collect.finish()

    @pl.loop(1, seq_count)
    def _(step):
        gain_row(step).wait_send()

    for step in range(1, fsdp_count):
        output_copy(step).wait_send()
        gain_copy(step).wait_send()


def take_out(grads, weights, tokens, output_term, gain_terms):
    slots = lax.axis_size("seq")
    fsdp_count = lax.axis_size("fsdp")
    chips = slots // 2
    _, width, columns = weights.shape
    rows = tokens.shape[0] // slots
    own = width // (slots * fsdp_count)
    kinds = gain_terms.shape[0]
    bf16, f32, dma = jnp.bfloat16, jnp.float32, pltpu.SemaphoreType.DMA
    gains = gain_terms.reshape(kinds, slots, fsdp_count, own).transpose(2, 1, 0, 3)
    lanes = pl.cdiv(own, 128) * 128
    gains = jnp.pad(gains, ((0, 0), (0, 0), (0, 8 - kinds), (0, lanes - own)))
    result, query, key, value, output, gains = pl.pallas_call(
        functools.partial(take_out_kernel, chips, fsdp_count),
        out_shape=(jax.ShapeDtypeStruct((rows, width), f32),)
        + (jax.ShapeDtypeStruct((own, columns * slots), f32),) * 3
        + (jax.ShapeDtypeStruct((own, width), f32), jax.ShapeDtypeStruct((8, lanes), f32)),
        in_specs=[whole_spec()] * 5,
        out_specs=(whole_spec(),) * 6,
        scratch_shapes=[
            pltpu.VMEM((fsdp_count, own, width), bf16),
            pltpu.VMEM((fsdp_count, slots, 8, lanes), f32),
            pltpu.VMEM((slots, 8, lanes), f32),
            pltpu.VMEM((slots, 8, lanes), f32),
            dma((fsdp_count,)),
            dma((fsdp_count,)),
            dma((fsdp_count,)),
            dma((fsdp_count,)),
            dma((slots,)),
            dma((slots,)),
        ]
        + Scatter.scratch(chips, rows, width)
        + Collect.scratch(1, slots, fsdp_count, own, 3 * columns),
        compiler_params=line_params(4),
        name="take_out",
    )(
        grads.reshape(3, slots, rows, columns),
        weights,
        tokens,
        output_term.reshape(fsdp_count, own, width),
        gains,
    )
    return result, (query, key, value), output, gains[:kinds, :own]


def row_sum_kernel(seq_count, local_ref, result, every, send, recv):
    seq, seq_peer = peers_of("seq", seq_count)
    fsdp = lax.axis_index("fsdp")
    barrier = pltpu.get_barrier_semaphore()
    for step in range(1, seq_count):
        pl.semaphore_signal(
            barrier, inc=1, device_id=(seq_peer(step), fsdp), device_id_type=MESH
        )
    pl.semaphore_wait(barrier, seq_count - 1)
    copies = [
        pltpu.make_async_remote_copy(
            src_ref=local_ref,
            dst_ref=every.at[step],
            send_sem=send.at[step],
            recv_sem=recv.at[step],
            device_id=(seq_peer(step), fsdp),
            device_id_type=MESH,
        )
        for step in range(1, seq_count)
    ]
    for copy in copies:
        copy.start()
    total = local_ref[...]
    for step in range(1, seq_count):
        copies[step - 1].wait_recv()
        total = total + every[step]
    result[...] = total
    for copy in copies:
        copy.wait_send()


def row_sum(collective_id, name, local):
    slots = lax.axis_size("seq")
    flat = local.reshape(-1, 128)
    return pl.pallas_call(
        functools.partial(row_sum_kernel, slots),
        out_shape=jax.ShapeDtypeStruct(flat.shape, jnp.float32),
        in_specs=[whole_spec()],
        out_specs=whole_spec(),
        scratch_shapes=[
            pltpu.VMEM((slots,) + flat.shape, jnp.float32),
            pltpu.SemaphoreType.DMA((slots,)),
            pltpu.SemaphoreType.DMA((slots,)),
        ],
        compiler_params=line_params(collective_id),
        name=name,
    )(flat).reshape(local.shape)


def rope_tables(row_count):
    half_width = DH // 2
    frequency = rope_base ** (-jnp.arange(half_width, dtype=jnp.float32) * 2.0 / DH)
    angles = jnp.arange(row_count, dtype=jnp.int32).astype(jnp.float32)[:, None] * frequency[None, :]
    cosine, sine = jnp.cos(angles), jnp.sin(angles)
    return (
        jnp.concatenate([cosine, cosine], axis=1),
        jnp.concatenate([-sine, sine], axis=1),
    )


def rotate(tensor, tables):
    cosine, sine = tables
    row_count = tensor.shape[0]
    half_width = DH // 2
    grouped = tensor.reshape(row_count, -1, DH)
    swapped = jnp.concatenate([grouped[..., half_width:], grouped[..., :half_width]], axis=-1)
    turned = grouped * cosine[:, None, :] + swapped * sine[:, None, :]
    return turned.reshape(tensor.shape)


def per_device(
    inputs,
    query_weight,
    key_weight,
    value_weight,
    output_weight,
    query_gain,
    key_gain,
    attention_gain,
    gate_weight,
    up_weight,
    down_weight,
    feedforward_gain,
    segments,
    cotangent,
):
    token_count = inputs.shape[1]
    width_all = inputs.shape[2]
    local_in = inputs.reshape(token_count, width_all)
    segment_row = segments[0]
    score_scale = DH ** (-0.5)
    seq_index = lax.axis_index("seq")
    inputs_all, attention_cols, output_rows, gate_cols, gains = bring_in(
        local_in,
        query_weight,
        key_weight,
        value_weight,
        output_weight,
        gate_weight,
        jnp.stack([query_gain, key_gain, attention_gain, feedforward_gain]),
    )
    query_cols, key_cols, value_cols = attention_cols[0], attention_cols[1], attention_cols[2]
    gains = gains.astype(jnp.float32)
    sequence_rows = inputs_all.shape[0]
    head_width = query_cols.shape[1]
    local_heads = head_width // DH
    query_scale = lax.dynamic_slice_in_dim(gains[0], seq_index * head_width, head_width, 0)
    key_scale = lax.dynamic_slice_in_dim(gains[1], seq_index * head_width, head_width, 0)
    attention_scale = gains[2]
    feedforward_scale = gains[3]
    query_pre = jnp.dot(inputs_all, query_cols, preferred_element_type=jnp.float32)
    key_pre = jnp.dot(inputs_all, key_cols, preferred_element_type=jnp.float32)
    values_low = jnp.dot(inputs_all, value_cols, preferred_element_type=jnp.float32).astype(
        jnp.bfloat16
    )
    squares = row_sum(
        7,
        "square_sum",
        jnp.stack([jnp.sum(query_pre * query_pre, axis=-1), jnp.sum(key_pre * key_pre, axis=-1)]),
    )
    inverse = lax.rsqrt(squares / width_all + eps_norm)
    query_unit = query_pre * inverse[0][:, None]
    key_unit = key_pre * inverse[1][:, None]
    tables = rope_tables(sequence_rows)
    queries_low = rotate(query_unit * query_scale, tables).astype(jnp.bfloat16)
    keys_low = rotate(key_unit * key_scale, tables).astype(jnp.bfloat16)
    query_heads = queries_low.reshape(sequence_rows, local_heads, DH)
    key_heads = keys_low.reshape(sequence_rows, local_heads, DH)
    value_heads = values_low.reshape(sequence_rows, local_heads, DH)
    block_rows = min(512, sequence_rows)
    block_count = sequence_rows // block_rows
    block_ids = jnp.arange(block_count, dtype=jnp.int32)

    def attend_block(loop_state, block_index):
        first_row = block_index * block_rows
        query_block = lax.dynamic_slice_in_dim(query_heads, first_row, block_rows, 0)
        scores = masked_scores(query_block, key_heads, first_row, segment_row, score_scale)
        row_max = jnp.max(scores, axis=-1, keepdims=True)
        expanded = jnp.exp(scores - row_max)
        row_total = jnp.sum(expanded, axis=-1, keepdims=True)
        softmax_low = (expanded / row_total).astype(jnp.bfloat16)
        block_out = jnp.einsum(
            "hqk,khd->qhd", softmax_low, value_heads, preferred_element_type=jnp.float32
        )
        return (loop_state, block_out.astype(jnp.bfloat16))

    _, out_blocks = lax.scan(attend_block, jnp.zeros((), jnp.int32), block_ids)
    attended_heads = out_blocks.reshape(sequence_rows, head_width)
    projected, up_cols, down_cols = project(attended_heads, output_rows, up_weight, down_weight)
    hidden = local_in.astype(jnp.float32) + rms_scale(projected, attention_scale)
    hidden_low = hidden.astype(jnp.bfloat16)
    mixed_pre, gate_linear, up_linear, activated, hidden_all = feed_forward(
        hidden_low, gate_cols, up_cols, down_cols
    )
    result = (
        (hidden + rms_scale(mixed_pre, feedforward_scale))
        .astype(jnp.bfloat16)
        .reshape(1, token_count, width_all)
    )
    grad_result = cotangent.reshape(token_count, width_all).astype(jnp.float32)
    _, mixed_pull = jax.vjp(rms_scale, mixed_pre, feedforward_scale)
    grad_mixed, grad_feedforward_gain = mixed_pull(grad_result)
    grad_mixed_low = grad_mixed.astype(jnp.bfloat16)
    hidden_term, grad_gate_low, grad_upward_low, grad_all = feed_forward_back(
        grad_mixed_low, gate_cols, up_cols, down_cols, gate_linear, up_linear
    )
    grad_hidden = grad_result + hidden_term
    _, branch_pull = jax.vjp(rms_scale, projected, attention_scale)
    grad_projected, grad_attention_gain = branch_pull(grad_hidden)
    weight_grads, output_term, attention_grads, gain_rows = gather_back(
        grad_projected.astype(jnp.bfloat16),
        output_rows,
        jnp.stack([query_scale, key_scale]),
        inverse.T,
        tables,
        segment_row,
        [hidden_all, grad_all, grad_gate_low, grad_upward_low, activated],
        jnp.stack([queries_low, keys_low, values_low, attended_heads]),
        jnp.stack([query_pre, key_pre]),
    )
    gate_weight_grad, up_weight_grad, down_weight_grad = weight_grads
    head_gains = lax.dynamic_update_slice_in_dim(
        jnp.zeros((2, width_all), jnp.float32),
        gain_rows[:2],
        seq_index * head_width,
        1,
    )
    gain_terms = jnp.concatenate(
        [head_gains, jnp.stack([grad_attention_gain, grad_feedforward_gain])], axis=0
    )
    input_term, projection_grads, output_weight_grad, gain_grads = take_out(
        attention_grads, attention_cols, inputs_all, output_term, gain_terms
    )
    query_weight_grad, key_weight_grad, value_weight_grad = projection_grads
    grad_input = grad_hidden + input_term
    return (
        result,
        grad_input.reshape(1, token_count, width_all),
        query_weight_grad,
        key_weight_grad,
        value_weight_grad,
        output_weight_grad,
        gain_grads[0],
        gain_grads[1],
        gain_grads[2],
        gate_weight_grad,
        up_weight_grad,
        down_weight_grad,
        gain_grads[3],
    )


def solution(mesh):
    in_specs = (
        P("fsdp", "seq", None),
        P(("seq", "fsdp"), None),
        P(("seq", "fsdp"), None),
        P(("seq", "fsdp"), None),
        P(("seq", "fsdp"), None),
        P(("seq", "fsdp")),
        P(("seq", "fsdp")),
        P(("seq", "fsdp")),
        P(("seq", "fsdp"), None),
        P(("seq", "fsdp"), None),
        P(("seq", "fsdp"), None),
        P(("seq", "fsdp")),
        P("fsdp", None),
        P("fsdp", "seq", None),
    )
    out_specs = (
        P("fsdp", "seq", None),
        P("fsdp", "seq", None),
        P(("seq", "fsdp"), None),
        P(("seq", "fsdp"), None),
        P(("seq", "fsdp"), None),
        P(("seq", "fsdp"), None),
        P(("seq", "fsdp")),
        P(("seq", "fsdp")),
        P(("seq", "fsdp")),
        P(("seq", "fsdp"), None),
        P(("seq", "fsdp"), None),
        P(("seq", "fsdp"), None),
        P(("seq", "fsdp")),
    )
    return jax.shard_map(
        per_device, mesh=mesh, in_specs=in_specs, out_specs=out_specs, check_vma=False
    )
```

```python
import functools

import jax
import jax.numpy as jnp
from jax import lax
from jax.experimental import pallas as pl
from jax.experimental.pallas import tpu as pltpu
from jax.sharding import PartitionSpec as P

DH = 128


eps_norm = 1e-06
rope_base = 500000.0
neg_fill = -1e30


def rms_scale(tensor, gain):
    return tensor * lax.rsqrt(jnp.mean(tensor * tensor, axis=-1, keepdims=True) + eps_norm) * gain


MESH = pl.DeviceIdType.MESH
RS_PARTS = 4


class Line:
    def __init__(self, chips):
        index = lax.axis_index("seq")
        self.chips = chips
        self.fsdp = lax.axis_index("fsdp")
        self.place = index // 2
        self.core = index % 2

    def device(self, place, core):
        return (place * 2 + core, self.fsdp)

    @property
    def partner(self):
        return self.device(self.place, 1 - self.core)

    @property
    def above(self):
        return self.device(jnp.minimum(self.place + 1, self.chips - 1), self.core)

    @property
    def below(self):
        return self.device(jnp.maximum(self.place - 1, 0), self.core)

    @property
    def has_above(self):
        return self.place < self.chips - 1

    @property
    def has_below(self):
        return self.place > 0

    def greet(self):
        barrier = pltpu.get_barrier_semaphore()
        pl.semaphore_signal(barrier, inc=1, device_id=self.partner, device_id_type=MESH)

        @pl.when(self.has_above)
        def _():
            pl.semaphore_signal(barrier, inc=1, device_id=self.above, device_id_type=MESH)

        @pl.when(self.has_below)
        def _():
            pl.semaphore_signal(barrier, inc=1, device_id=self.below, device_id_type=MESH)

        peers = (
            1 + jnp.minimum(self.place, 1) + jnp.minimum(self.chips - 1 - self.place, 1)
        )
        pl.semaphore_wait(barrier, peers)

    def order(self, step):
        place, last = self.place, self.chips - 1
        near = jnp.minimum(place, last - place)
        both = jnp.where(step % 2 == 1, place - (step + 1) // 2, place + step // 2)
        rest = jnp.where(place <= last - place, step, last - step)
        return jnp.where(step <= 2 * near, both, rest)

    def paired(self, step):
        near = jnp.minimum(self.place, self.chips - 1 - self.place)
        return (step % 2 == 1) & (step <= 2 * near)

    def second_of_pair(self, step):
        near = jnp.minimum(self.place, self.chips - 1 - self.place)
        return (step % 2 == 0) & (step > 0) & (step <= 2 * near)


class Gather:
    def __init__(self, line, blocks, arrive, up_sem, down_sem, side_sem):
        self.line, self.blocks, self.arrive = line, blocks, arrive
        self.up_sem, self.down_sem, self.side_sem = up_sem, down_sem, side_sem

    @staticmethod
    def scratch(chips, rows, width):
        return [
            pltpu.VMEM((2 * chips, rows, width), jnp.bfloat16),
            pltpu.SemaphoreType.DMA((2 * chips,)),
            pltpu.SemaphoreType.DMA((chips,)),
            pltpu.SemaphoreType.DMA((chips,)),
            pltpu.SemaphoreType.DMA((chips,)),
        ]

    def copy(self, chip, sem, target):
        slot = chip * 2 + self.line.core
        return pltpu.make_async_remote_copy(
            src_ref=self.blocks.at[slot],
            dst_ref=self.blocks.at[slot],
            send_sem=sem.at[chip],
            recv_sem=self.arrive.at[slot],
            device_id=target,
            device_id_type=MESH,
        )

    def wait_slot(self, slot):
        pltpu.make_async_remote_copy(
            src_ref=self.blocks.at[slot],
            dst_ref=self.blocks.at[slot],
            send_sem=self.side_sem.at[0],
            recv_sem=self.arrive.at[slot],
            device_id=self.line.partner,
            device_id_type=MESH,
        ).wait_recv()

    def send(self, chip):
        line = self.line

        @pl.when((chip <= line.place) & line.has_above)
        def _():
            self.copy(chip, self.up_sem, line.above).start()

        @pl.when((chip >= line.place) & line.has_below)
        def _():
            self.copy(chip, self.down_sem, line.below).start()

        self.copy(chip, self.side_sem, line.partner).start()

    def take(self, chip):
        self.wait_slot(chip * 2 + self.line.core)
        self.send(chip)

    def step(self, step):
        line = self.line
        chip = line.order(step)

        @pl.when((step > 0) & jnp.logical_not(line.second_of_pair(step)))
        def _():
            self.take(chip)

        @pl.when(line.paired(step))
        def _():
            self.take(line.order(step + 1))

        self.wait_slot(chip * 2 + 1 - line.core)
        return chip

    def finish(self):
        line = self.line

        @pl.loop(0, line.chips)
        def _(chip):
            @pl.when((chip <= line.place) & line.has_above)
            def _():
                self.copy(chip, self.up_sem, line.above).wait_send()

            @pl.when((chip >= line.place) & line.has_below)
            def _():
                self.copy(chip, self.down_sem, line.below).wait_send()

            self.copy(chip, self.side_sem, line.partner).wait_send()


class Scatter:
    def __init__(self, line, fresh, terms, side_out, side_in, out, inward, side_send, side_recv, send_sem, recv_sem):
        self.line, self.fresh, self.terms = line, fresh, terms
        self.side_out, self.side_in = side_out, side_in
        self.out, self.inward = out, inward
        self.side_send, self.side_recv = side_send, side_recv
        self.send_sem, self.recv_sem = send_sem, recv_sem
        self.rows = terms.shape[1] // RS_PARTS

    @staticmethod
    def scratch(chips, rows, width):
        return [
            pltpu.VMEM((2, rows, width), jnp.float32),
            pltpu.VMEM((chips, rows, width), jnp.float32),
            pltpu.VMEM((chips, rows, width), jnp.bfloat16),
            pltpu.VMEM((chips, rows, width), jnp.bfloat16),
            pltpu.VMEM((chips, rows, width), jnp.bfloat16),
            pltpu.VMEM((2, chips, rows, width), jnp.bfloat16),
            pltpu.SemaphoreType.DMA((chips,)),
            pltpu.SemaphoreType.DMA((chips,)),
            pltpu.SemaphoreType.DMA((chips, RS_PARTS)),
            pltpu.SemaphoreType.DMA((2, chips, RS_PARTS)),
        ]

    def side(self, chip):
        return pltpu.make_async_remote_copy(
            src_ref=self.side_out.at[chip],
            dst_ref=self.side_in.at[chip],
            send_sem=self.side_send.at[chip],
            recv_sem=self.side_recv.at[chip],
            device_id=self.line.partner,
            device_id_type=MESH,
        )

    def part(self, chip, part, upward, target):
        rows = pl.ds(part * self.rows, self.rows)
        return pltpu.make_async_remote_copy(
            src_ref=self.out.at[chip, rows],
            dst_ref=self.inward.at[upward, chip, rows],
            send_sem=self.send_sem.at[chip, part],
            recv_sem=self.recv_sem.at[upward, chip, part],
            device_id=target,
            device_id_type=MESH,
        )

    def share(self, chip):
        self.side_out[chip] = self.fresh[1 - self.line.core].astype(jnp.bfloat16)
        self.side(chip).start()
        self.terms[chip] = self.fresh[self.line.core]

    def total(self, chip, part, ways):
        rows = pl.ds(part * self.rows, self.rows)
        total = self.terms[chip, rows] + self.side_in[chip, rows].astype(jnp.float32)
        for way in ways:
            total = total + self.inward[way, chip, rows].astype(jnp.float32)
        return rows, total

    def pass_on(self, chip, upward, first):
        target = self.line.above if upward else self.line.below
        self.side(chip).wait_recv()

        @pl.loop(0, RS_PARTS)
        def _(part):
            if not first:
                self.part(chip, part, upward, target).wait_recv()
            rows, total = self.total(chip, part, () if first else (upward,))
            self.out[chip, rows] = total.astype(jnp.bfloat16)
            self.part(chip, part, upward, target).start()

    def after_term(self, chip):
        line = self.line
        self.share(chip)

        @pl.when((chip < line.place) & jnp.logical_not(line.has_above))
        def _():
            self.pass_on(chip, 0, True)

        @pl.when((chip > line.place) & jnp.logical_not(line.has_below))
        def _():
            self.pass_on(chip, 1, True)

    def hop(self, step):
        line = self.line
        lower = line.place * 2 < line.chips
        up_chip, down_chip = step, line.chips - 1 - step
        go_up = (up_chip > line.place) & line.has_below
        go_down = (down_chip < line.place) & line.has_above

        @pl.when(go_up & lower)
        def _():
            self.pass_on(up_chip, 1, False)

        @pl.when(go_down)
        def _():
            self.pass_on(down_chip, 0, False)

        @pl.when(go_up & jnp.logical_not(lower))
        def _():
            self.pass_on(up_chip, 1, False)

    def settle(self, result):
        line = self.line
        place = line.place
        self.side(place).wait_recv()

        @pl.loop(0, RS_PARTS)
        def _(part):
            @pl.when(line.has_above)
            def _():
                self.part(place, part, 0, line.below).wait_recv()

            @pl.when(line.has_below)
            def _():
                self.part(place, part, 1, line.above).wait_recv()

            @pl.when(line.has_above & line.has_below)
            def _():
                rows, total = self.total(place, part, (0, 1))
                result[rows] = total

            @pl.when(line.has_above & jnp.logical_not(line.has_below))
            def _():
                rows, total = self.total(place, part, (0,))
                result[rows] = total

            @pl.when(line.has_below & jnp.logical_not(line.has_above))
            def _():
                rows, total = self.total(place, part, (1,))
                result[rows] = total

    def hops(self):
        @pl.loop(0, self.line.chips)
        def _(step):
            self.hop(step)

    def finish(self):
        line = self.line

        @pl.loop(0, line.chips)
        def _(chip):
            self.side(chip).wait_send()

            @pl.when(chip != line.place)
            def _():
                @pl.loop(0, RS_PARTS)
                def _(part):
                    self.part(chip, part, 0, line.below).wait_send()


def tile_of(extent):
    return min(256, extent)


def dot_cols(left, right):
    return lax.dot_general(
        left, right, (((1,), (1,)), ((), ())), preferred_element_type=jnp.float32
    )


def load(pairs):
    copies = [pltpu.make_async_copy(src, dst, sem) for src, dst, sem in pairs]
    for copy in copies:
        copy.start()
    return copies


def feed_forward_kernel(
    chips,
    hidden_ref,
    gate_hbm,
    up_hbm,
    down_hbm,
    mixed_ref,
    gate_out,
    up_out,
    act_out,
    all_out,
    gate_w,
    up_w,
    down_w,
    gate_keep,
    up_keep,
    act_keep,
    load_sem,
    store_sem,
    *comm,
):
    line = Line(chips)
    gather = Gather(line, *comm[:5])
    scatter = Scatter(line, *comm[5:])
    blocks, fresh = gather.blocks, scatter.fresh
    _, rows, width = blocks.shape
    units = gate_w.shape[1]
    copies = load(
        [
            (gate_hbm, gate_w, load_sem.at[0]),
            (up_hbm, up_w, load_sem.at[1]),
            (down_hbm, down_w, load_sem.at[2]),
        ]
    )
    line.greet()
    blocks[line.place * 2 + line.core] = hidden_ref[...]
    gather.send(line.place)

    def stores(chip):
        pair = pl.ds(chip * 2, 2)
        return [
            pltpu.make_async_copy(gate_keep.at[pair], gate_out.at[pair], store_sem.at[0, chip]),
            pltpu.make_async_copy(up_keep.at[pair], up_out.at[pair], store_sem.at[1, chip]),
            pltpu.make_async_copy(act_keep.at[pair], act_out.at[pair], store_sem.at[2, chip]),
            pltpu.make_async_copy(blocks.at[pair], all_out.at[pair], store_sem.at[3, chip]),
        ]

    for copy in copies:
        copy.wait()

    @pl.loop(0, chips)
    def _(step):
        chip = gather.step(step)
        pair = pl.ds(chip * 2, 2)

        @pl.loop(0, units // tile_of(units))
        def _(tile):
            columns = pl.ds(pl.multiple_of(tile * tile_of(units), 128), tile_of(units))
            tokens = blocks[pair].reshape(2 * rows, width)
            gate = jnp.dot(tokens, gate_w[:, columns], preferred_element_type=jnp.float32)
            up = jnp.dot(tokens, up_w[:, columns], preferred_element_type=jnp.float32)
            gate_keep[pair, :, columns] = gate.reshape(2, rows, -1)
            up_keep[pair, :, columns] = up.reshape(2, rows, -1)
            act_keep[pair, :, columns] = (
                (gate / (1.0 + jnp.exp(-gate)) * up).astype(jnp.bfloat16).reshape(2, rows, -1)
            )

        @pl.loop(0, width // tile_of(width))
        def _(tile):
            columns = pl.ds(pl.multiple_of(tile * tile_of(width), 128), tile_of(width))
            act = act_keep[pair].reshape(2 * rows, units)
            fresh[:, :, columns] = dot_cols(act, down_w[columns, :]).reshape(2, rows, -1)

        for copy in stores(chip):
            copy.start()
        scatter.after_term(chip)

    scatter.hops()
    scatter.settle(mixed_ref)
    scatter.finish()
    gather.finish()

    @pl.loop(0, chips)
    def _(chip):
        for copy in stores(chip):
            copy.wait()


def feed_forward_back_kernel(
    chips,
    grad_ref,
    gate_hbm,
    up_hbm,
    down_hbm,
    gate_lin_hbm,
    up_lin_hbm,
    hidden_grad_ref,
    gate_out,
    up_out,
    all_out,
    gate_w,
    up_w,
    down_w,
    gate_lin,
    up_lin,
    gate_keep,
    up_keep,
    load_sem,
    store_sem,
    *comm,
):
    line = Line(chips)
    gather = Gather(line, *comm[:5])
    scatter = Scatter(line, *comm[5:])
    blocks, fresh = gather.blocks, scatter.fresh
    _, rows, width = blocks.shape
    units = gate_w.shape[1]
    copies = load(
        [
            (down_hbm, down_w, load_sem.at[0]),
            (gate_lin_hbm, gate_lin, load_sem.at[1]),
            (up_lin_hbm, up_lin, load_sem.at[2]),
            (gate_hbm, gate_w, load_sem.at[3]),
            (up_hbm, up_w, load_sem.at[4]),
        ]
    )
    line.greet()
    blocks[line.place * 2 + line.core] = grad_ref[...]
    gather.send(line.place)

    def stores(chip):
        pair = pl.ds(chip * 2, 2)
        return [
            pltpu.make_async_copy(gate_keep.at[pair], gate_out.at[pair], store_sem.at[0, chip]),
            pltpu.make_async_copy(up_keep.at[pair], up_out.at[pair], store_sem.at[1, chip]),
            pltpu.make_async_copy(blocks.at[pair], all_out.at[pair], store_sem.at[2, chip]),
        ]

    for copy in copies:
        copy.wait()

    @pl.loop(0, chips)
    def _(step):
        chip = gather.step(step)
        pair = pl.ds(chip * 2, 2)

        @pl.loop(0, units // tile_of(units))
        def _(tile):
            columns = pl.ds(pl.multiple_of(tile * tile_of(units), 128), tile_of(units))
            tokens = blocks[pair].reshape(2 * rows, width)
            grad = jnp.dot(tokens, down_w[:, columns], preferred_element_type=jnp.float32)
            gate = gate_lin[pair, :, columns].reshape(2 * rows, -1)
            up = up_lin[pair, :, columns].reshape(2 * rows, -1)
            sig = 1.0 / (1.0 + jnp.exp(-gate))
            gate_keep[pair, :, columns] = (
                (grad * up * sig * (1.0 + gate * (1.0 - sig)))
                .astype(jnp.bfloat16)
                .reshape(2, rows, -1)
            )
            up_keep[pair, :, columns] = (
                (grad * (gate * sig)).astype(jnp.bfloat16).reshape(2, rows, -1)
            )

        @pl.loop(0, width // tile_of(width))
        def _(tile):
            columns = pl.ds(pl.multiple_of(tile * tile_of(width), 128), tile_of(width))
            gate = gate_keep[pair].reshape(2 * rows, units)
            up = up_keep[pair].reshape(2 * rows, units)
            fresh[:, :, columns] = (
                dot_cols(gate, gate_w[columns, :]) + dot_cols(up, up_w[columns, :])
            ).reshape(2, rows, -1)

        for copy in stores(chip):
            copy.start()
        scatter.after_term(chip)

    scatter.hops()
    scatter.settle(hidden_grad_ref)
    scatter.finish()
    gather.finish()

    @pl.loop(0, chips)
    def _(chip):
        for copy in stores(chip):
            copy.wait()


def whole_spec():
    return pl.BlockSpec(memory_space=pltpu.VMEM)


def far_spec():
    return pl.BlockSpec(memory_space=pl.ANY)


def line_params(collective_id):
    return pltpu.CompilerParams(
        collective_id=collective_id, has_side_effects=True, vmem_limit_bytes=63 * 2**20
    )


def feed_forward(hidden_low, gate_cols, up_cols, down_cols):
    rows, width = hidden_low.shape
    units = gate_cols.shape[1]
    slots = lax.axis_size("seq")
    chips = slots // 2
    weights = [pltpu.VMEM((width, units), jnp.bfloat16)] * 3
    mixed, gate, up, act, every = pl.pallas_call(
        functools.partial(feed_forward_kernel, chips),
        out_shape=(
            jax.ShapeDtypeStruct((rows, width), jnp.float32),
            jax.ShapeDtypeStruct((slots, rows, units), jnp.float32),
            jax.ShapeDtypeStruct((slots, rows, units), jnp.float32),
            jax.ShapeDtypeStruct((slots, rows, units), jnp.bfloat16),
            jax.ShapeDtypeStruct((slots, rows, width), jnp.bfloat16),
        ),
        in_specs=[whole_spec()] + [far_spec()] * 3,
        out_specs=(whole_spec(),) + (far_spec(),) * 4,
        scratch_shapes=weights
        + [
            pltpu.VMEM((slots, rows, units), jnp.float32),
            pltpu.VMEM((slots, rows, units), jnp.float32),
            pltpu.VMEM((slots, rows, units), jnp.bfloat16),
            pltpu.SemaphoreType.DMA((3,)),
            pltpu.SemaphoreType.DMA((4, chips)),
        ]
        + Gather.scratch(chips, rows, width)
        + Scatter.scratch(chips, rows, width),
        compiler_params=line_params(1),
        name="feed_forward",
    )(hidden_low, gate_cols, up_cols, down_cols)
    return mixed, gate, up, act.reshape(-1, units), every.reshape(-1, width)


def feed_forward_back(grad_low, gate_cols, up_cols, down_cols, gate, up):
    rows, width = grad_low.shape
    units = gate_cols.shape[1]
    slots = lax.axis_size("seq")
    chips = slots // 2
    weights = [pltpu.VMEM((width, units), jnp.bfloat16)] * 3
    hidden_grad, gate_grad, up_grad, every = pl.pallas_call(
        functools.partial(feed_forward_back_kernel, chips),
        out_shape=(
            jax.ShapeDtypeStruct((rows, width), jnp.float32),
            jax.ShapeDtypeStruct((slots, rows, units), jnp.bfloat16),
            jax.ShapeDtypeStruct((slots, rows, units), jnp.bfloat16),
            jax.ShapeDtypeStruct((slots, rows, width), jnp.bfloat16),
        ),
        in_specs=[whole_spec()] + [far_spec()] * 5,
        out_specs=(whole_spec(),) + (far_spec(),) * 3,
        scratch_shapes=weights
        + [
            pltpu.VMEM((slots, rows, units), jnp.float32),
            pltpu.VMEM((slots, rows, units), jnp.float32),
            pltpu.VMEM((slots, rows, units), jnp.bfloat16),
            pltpu.VMEM((slots, rows, units), jnp.bfloat16),
            pltpu.SemaphoreType.DMA((5,)),
            pltpu.SemaphoreType.DMA((3, chips)),
        ]
        + Gather.scratch(chips, rows, width)
        + Scatter.scratch(chips, rows, width),
        compiler_params=line_params(2),
        name="feed_forward_back",
    )(grad_low, gate_cols, up_cols, down_cols, gate, up)
    return (
        hidden_grad,
        gate_grad.reshape(-1, units),
        up_grad.reshape(-1, units),
        every.reshape(-1, width),
    )


def peers_of(axis, size):
    me = lax.axis_index(axis)
    return me, lambda step: (me + step) % size


def greet_cross(seq_count, fsdp_count):
    seq, seq_peer = peers_of("seq", seq_count)
    fsdp, fsdp_peer = peers_of("fsdp", fsdp_count)
    barrier = pltpu.get_barrier_semaphore()
    for step in range(1, seq_count):
        pl.semaphore_signal(
            barrier, inc=1, device_id=(seq_peer(step), fsdp), device_id_type=MESH
        )
    for step in range(1, fsdp_count):
        pl.semaphore_signal(
            barrier, inc=1, device_id=(seq, fsdp_peer(step)), device_id_type=MESH
        )
    pl.semaphore_wait(barrier, seq_count + fsdp_count - 2)


class Cross:
    def __init__(self, seq_count, fsdp_count):
        self.seq_count, self.fsdp_count = seq_count, fsdp_count
        self.seq, self.seq_peer = peers_of("seq", seq_count)
        self.fsdp, self.fsdp_peer = peers_of("fsdp", fsdp_count)
        self.square = fsdp_count == 4
        if self.square:
            row, place = self.fsdp // 2, self.fsdp % 2
            self.sides = (row * 2 + 1 - place, (1 - row) * 2 + place)
            self.corner = (1 - row) * 2 + 1 - place
        else:
            self.sides = tuple(self.fsdp_peer(step) for step in range(1, fsdp_count))

    def remote(self, src, dst, send, recv, seq, fsdp):
        return pltpu.make_async_remote_copy(
            src_ref=src,
            dst_ref=dst,
            send_sem=send,
            recv_sem=recv,
            device_id=(seq, fsdp),
            device_id_type=MESH,
        )


class Spread:
    def __init__(self, cross, group, stack, weights, row_send, row_recv, side_send, side_recv, half_send, half_recv):
        self.cross, self.group, self.stack, self.weights = cross, group, stack, weights
        self.row_send, self.row_recv = row_send, row_recv
        self.side_send, self.side_recv = side_send, side_recv
        self.half_send, self.half_recv = half_send, half_recv
        self.columns, self.rows = weights.shape[-1], weights.shape[-2]
        self.items = weights.shape[0] // group * cross.seq_count

    @staticmethod
    def scratch(kinds, group, seq_count, fsdp_count, rows, columns):
        dma = pltpu.SemaphoreType.DMA
        sides = 2 if fsdp_count == 4 else fsdp_count - 1
        items = kinds // group * seq_count
        return [
            pltpu.VMEM((kinds, rows, seq_count * columns), jnp.bfloat16),
            pltpu.VMEM((kinds, seq_count, fsdp_count, rows, columns), jnp.bfloat16),
            dma((kinds, seq_count)),
            dma((kinds, seq_count)),
            dma((items, sides)),
            dma((items, sides)),
            dma((items, 2)),
            dma((items, 2)),
        ]

    def block(self, owner):
        return pl.ds(pl.multiple_of(owner * self.columns, 128), self.columns)

    def row(self, kind, step):
        cross = self.cross
        peer = cross.seq_peer(step)
        return cross.remote(
            self.stack.at[kind, :, self.block(peer)],
            self.weights.at[kind, cross.seq, cross.fsdp],
            self.row_send.at[kind, step],
            self.row_recv.at[kind, step],
            peer,
            cross.fsdp,
        )

    def place(self, item):
        count = self.cross.seq_count
        step = item % count
        return item // count * self.group, step, (self.cross.seq - step + count) % count

    def side(self, item, side):
        cross = self.cross
        first, _, owner = self.place(item)
        ref = self.weights.at[pl.ds(first, self.group), owner, cross.fsdp]
        return cross.remote(
            ref,
            ref,
            self.side_send.at[item, side],
            self.side_recv.at[item, side],
            cross.seq,
            cross.sides[side],
        )

    def half(self, item, side):
        cross = self.cross
        first, _, owner = self.place(item)
        rows = pl.ds(side * (self.rows // 2), self.rows // 2)
        ref = self.weights.at[pl.ds(first, self.group), owner, cross.sides[side], rows]
        return cross.remote(
            ref,
            ref,
            self.half_send.at[item, side],
            self.half_recv.at[item, side],
            cross.seq,
            cross.sides[1 - side],
        )

    def send_rows(self, item):
        first, step, _ = self.place(item)

        @pl.when(step > 0)
        def _():
            for kind in range(self.group):
                self.row(first + kind, step).start()

    def take(self, item):
        cross = self.cross
        first, step, _ = self.place(item)

        @pl.when(step > 0)
        def _():
            for kind in range(self.group):
                self.row(first + kind, step).wait_recv()

        @pl.when(step == 0)
        def _():
            for kind in range(self.group):
                own = self.stack[first + kind, :, self.block(cross.seq)]
                self.weights[first + kind, cross.seq, cross.fsdp] = own

        for side in range(len(cross.sides)):
            self.side(item, side).start()

    def relay(self, item):
        for side in range(len(self.cross.sides)):
            self.side(item, side).wait_recv()
            if self.cross.square:
                self.half(item, side).start()

    def settle(self, item):
        if self.cross.square:
            for side in range(2):
                self.half(item, side).wait_recv()

    def finish(self):
        cross = self.cross

        @pl.loop(0, self.items)
        def _(item):
            first, step, _ = self.place(item)

            @pl.when(step > 0)
            def _():
                for kind in range(self.group):
                    self.row(first + kind, step).wait_send()

            for side in range(len(cross.sides)):
                self.side(item, side).wait_send()
                if cross.square:
                    self.half(item, side).wait_send()


AHEAD = 2
LAG = 3
RING = 8


class Collect:
    def __init__(self, cross, kinds, fill, terms, side_in, half_out, half_in, row_out, row_in, side_send, side_recv, half_send, half_recv, row_send, row_recv):
        self.cross, self.fill, self.terms = cross, fill, terms
        self.side_in, self.half_out, self.half_in = side_in, half_out, half_in
        self.row_out, self.row_in = row_out, row_in
        self.side_send, self.side_recv = side_send, side_recv
        self.half_send, self.half_recv = half_send, half_recv
        self.row_send, self.row_recv = row_send, row_recv
        self.rows, self.columns = terms.shape[-2:]
        self.items = kinds * cross.seq_count

    @staticmethod
    def scratch(kinds, seq_count, fsdp_count, rows, columns):
        dma = pltpu.SemaphoreType.DMA
        vmem = pltpu.VMEM
        bf16 = jnp.bfloat16
        items = kinds * seq_count
        if fsdp_count == 4:
            arrays = [
                vmem((items, 2, 2, rows // 2, columns), bf16),
                vmem((RING, 2, rows // 2, columns), bf16),
                vmem((items, 2, rows // 2, columns), bf16),
            ]
            sides = (2, 2)
        else:
            arrays = [
                vmem((items, fsdp_count - 1, rows, columns), bf16),
                vmem((1, 1, 16, 128), bf16),
                vmem((1, 1, 16, 128), bf16),
            ]
            sides = (fsdp_count - 1, 1)
        return [vmem((RING, fsdp_count, rows, columns), bf16)] + arrays + [
            vmem((RING, rows, columns), bf16),
            vmem((items, rows, columns), bf16),
            dma((items,) + sides),
            dma((items,) + sides),
            dma((items, 2)),
            dma((items, 2)),
            dma((items,)),
            dma((items,)),
        ]

    def half_rows(self, side):
        return pl.ds(side * (self.rows // 2), self.rows // 2)

    def side(self, turn, side, which):
        cross = self.cross
        if not cross.square:
            return cross.remote(
                self.terms.at[turn % RING, cross.sides[side]],
                self.side_in.at[turn, side],
                self.side_send.at[turn, side, 0],
                self.side_recv.at[turn, side, 0],
                cross.seq,
                cross.sides[side],
            )
        target = cross.sides[side] if which == 0 else cross.corner
        return cross.remote(
            self.terms.at[turn % RING, target, self.half_rows(side)],
            self.side_in.at[turn, side, which],
            self.side_send.at[turn, side, which],
            self.side_recv.at[turn, side, which],
            cross.seq,
            cross.sides[side],
        )

    def half(self, turn, side):
        cross = self.cross
        return cross.remote(
            self.half_out.at[turn % RING, side],
            self.half_in.at[turn, side],
            self.half_send.at[turn, side],
            self.half_recv.at[turn, side],
            cross.seq,
            cross.sides[1 - side],
        )

    def row(self, turn):
        cross = self.cross
        return cross.remote(
            self.row_out.at[turn % RING],
            self.row_in.at[turn],
            self.row_send.at[turn],
            self.row_recv.at[turn],
            self.place(turn)[1],
            cross.fsdp,
        )

    def place(self, turn):
        count = self.cross.seq_count
        return turn // count, self.cross.seq_peer(turn % count + 1)

    def is_own(self, turn):
        return turn % self.cross.seq_count == self.cross.seq_count - 1

    @property
    def ways(self):
        return range(2) if self.cross.square else range(1)

    def sides(self, turn):
        return [
            self.side(turn, side, which)
            for which in reversed(self.ways)
            for side in range(len(self.cross.sides))
        ]

    def send(self, turn, first):
        if not first:

            @pl.when(turn >= RING)
            def _():
                for copy in self.sides(turn - RING):
                    copy.wait_send()

        kind, owner = self.place(turn)
        self.fill(kind, owner, turn % RING)
        for copy in self.sides(turn):
            copy.start()

    def middle(self, turn):
        if not self.cross.square:
            return
        cross = self.cross

        @pl.when(turn >= RING)
        def _():
            for side in range(2):
                self.half(turn - RING, side).wait_send()

        for side in range(2):
            self.side(turn, side, 1).wait_recv()
            mine = self.terms[turn % RING, cross.sides[1 - side], self.half_rows(side)]
            self.half_out[turn % RING, side] = (
                mine.astype(jnp.float32) + self.side_in[turn, side, 1].astype(jnp.float32)
            ).astype(jnp.bfloat16)
            self.half(turn, side).start()

    def totals(self, turn):
        cross = self.cross
        found = []
        if cross.square:
            for side in range(2):
                self.side(turn, side, 0).wait_recv()
                self.half(turn, side).wait_recv()
                rows = self.half_rows(side)
                total = self.terms[turn % RING, cross.fsdp, rows].astype(jnp.float32)
                total = total + self.side_in[turn, side, 0].astype(jnp.float32)
                total = total + self.half_in[turn, side].astype(jnp.float32)
                found.append((rows, total))
        else:
            total = self.terms[turn % RING, cross.fsdp].astype(jnp.float32)
            for side in range(len(cross.sides)):
                self.side(turn, side, 0).wait_recv()
                total = total + self.side_in[turn, side].astype(jnp.float32)
            found.append((pl.ds(0, self.rows), total))
        return found

    def ship(self, turn):
        own = self.is_own(turn)
        self.free_row(turn - RING)

        @pl.when(own)
        def _():
            for rows, total in self.totals(turn):
                self.row_in[turn, rows] = total.astype(jnp.bfloat16)

        @pl.when(jnp.logical_not(own))
        def _():
            for rows, total in self.totals(turn):
                self.row_out[turn % RING, rows] = total.astype(jnp.bfloat16)
            self.row(turn).start()

    def free_row(self, turn):
        @pl.when((turn >= 0) & jnp.logical_not(self.is_own(turn)))
        def _():
            self.row(turn).wait_send()

    def beat(self, turn):
        ahead = turn + AHEAD

        @pl.when(ahead < self.items)
        def _():
            self.send(ahead, False)

        @pl.when(turn < self.items)
        def _():
            self.middle(turn)

        @pl.when(turn >= LAG)
        def _():
            self.ship(turn - LAG)

    def begin(self):
        @pl.loop(0, min(AHEAD, self.items))
        def _(turn):
            self.send(turn, True)

    @property
    def beats(self):
        return self.items + LAG

    def receive(self, turn, put):
        count = self.cross.seq_count

        @pl.when(jnp.logical_not(self.is_own(turn)))
        def _():
            self.row(turn).wait_recv()

        sender = (self.cross.seq - turn % count - 1 + count) % count
        put(turn // count, sender, self.row_in[turn].astype(jnp.float32))

    def finish(self):
        cross = self.cross
        late = max(self.items - RING, 0)

        @pl.loop(late, self.items)
        def _(turn):
            for copy in self.sides(turn):
                copy.wait_send()
            if cross.square:
                for side in range(2):
                    self.half(turn, side).wait_send()
            self.free_row(turn)


def dot_rows(left, right, precision=None):
    return lax.dot_general(
        left,
        right,
        (((0,), (0,)), ((), ())),
        precision=precision,
        preferred_element_type=jnp.float32,
    )


EXACT = lax.Precision.HIGHEST


def turn_heads(tensor, cosine, sine):
    heads = [
        tensor[:, first : first + DH] * cosine
        + pltpu.roll(tensor[:, first : first + DH], DH // 2, 1) * sine
        for first in range(0, tensor.shape[1], DH)
    ]
    return jnp.concatenate(heads, axis=1) if len(heads) > 1 else heads[0]


def attention_weights(queries, keys, first_row, segment_column, segment_row):
    rows, count = queries.shape[0], keys.shape[0]
    scores = dot_cols(queries, keys) * DH ** (-0.5)
    query_place = first_row + lax.broadcasted_iota(jnp.int32, (rows, count), 0)
    key_place = lax.broadcasted_iota(jnp.int32, (rows, count), 1)
    allowed = (key_place <= query_place) & (segment_row == segment_column)
    scores = jnp.where(allowed, scores, neg_fill)
    expanded = jnp.exp(scores - jnp.max(scores, axis=-1, keepdims=True))
    return expanded / jnp.sum(expanded, axis=-1, keepdims=True)


class RowSum:
    def __init__(self, cross, local, every, send_sem, recv_sem):
        self.cross, self.local, self.every = cross, local, every
        self.send_sem, self.recv_sem = send_sem, recv_sem

    @staticmethod
    def scratch(seq_count, shape):
        dma = pltpu.SemaphoreType.DMA
        return [
            pltpu.VMEM(shape, jnp.float32),
            pltpu.VMEM((seq_count,) + shape, jnp.float32),
            dma((seq_count,)),
            dma((seq_count,)),
        ]

    def copy(self, step):
        cross = self.cross
        return cross.remote(
            self.local,
            self.every.at[step],
            self.send_sem.at[step],
            self.recv_sem.at[step],
            cross.seq_peer(step),
            cross.fsdp,
        )

    def send(self, value):
        self.local[...] = value
        for step in range(1, self.cross.seq_count):
            self.copy(step).start()

    def receive(self):
        total = self.local[...]
        for step in range(1, self.cross.seq_count):
            self.copy(step).wait_recv()
            total = total + self.every[step]
        return total

    def finish(self):
        for step in range(1, self.cross.seq_count):
            self.copy(step).wait_send()


def pick_row(row, shape):
    return jnp.where(lax.broadcasted_iota(jnp.int32, shape, 0) == row, 1.0, 0.0)


def product_terms(scatter, pairs, chip):
    _, rows, width = scatter.fresh.shape
    pair = pl.ds(chip * 2, 2)

    @pl.loop(0, width // tile_of(width))
    def _(tile):
        columns = pl.ds(pl.multiple_of(tile * tile_of(width), 128), tile_of(width))
        total = None
        for left, right, across in pairs:
            tokens = left[pair].reshape(2 * rows, -1)
            if across:
                term = dot_cols(tokens, right[columns, :])
            else:
                term = jnp.dot(tokens, right(columns), preferred_element_type=jnp.float32)
            total = term if total is None else total + term
        scatter.fresh[:, :, columns] = total.reshape(2, rows, -1)

    scatter.after_term(chip)


EARLY = 6
LEAD = 2
HOPPING = 4


def bring_in_kernel(chips, fsdp_count, *refs):
    inputs_ref, gains_ref, cosine_ref, sine_ref, segment_column, segment_row = refs[:6]
    sources, output_ref, refs = refs[6:12], refs[12], refs[13:]
    projected, inverse_out, own_gains, gains_out = refs[:4]
    inputs_out, attention_out, output_out, units_out, heads_out, pre_out = refs[4:10]
    outputs, gains, heads, pre, refs = refs[10], refs[11], refs[12], refs[13], refs[14:]
    gain_row_send, gain_row_recv, gain_column_send, gain_column_recv = refs[:4]
    output_send, output_recv, load_sem, store_sem, refs = refs[4], refs[5], refs[6], refs[7], refs[8:]
    line = Line(chips)
    cross = Cross(2 * chips, fsdp_count)
    gather, refs = Gather(line, *refs[:5]), refs[5:]
    sums, refs = RowSum(cross, *refs[:4]), refs[4:]
    attention, refs = Spread(cross, 3, *refs[:8]), refs[8:]
    units, refs = Spread(cross, 1, *refs[:8]), refs[8:]
    scatter = Scatter(line, *refs)
    seq_count, seq, fsdp = cross.seq_count, cross.seq, cross.fsdp
    blocks = gather.blocks
    _, rows, width = blocks.shape
    columns = attention.columns
    tokens = seq_count * rows

    def gain_row(step):
        return cross.remote(
            gains_ref,
            gains.at[seq, fsdp],
            gain_row_send.at[step],
            gain_row_recv.at[step],
            cross.seq_peer(step),
            fsdp,
        )

    def gain_column(owner, step):
        ref = gains.at[owner, fsdp]
        return cross.remote(
            ref,
            ref,
            gain_column_send.at[owner, step],
            gain_column_recv.at[owner, step],
            seq,
            cross.fsdp_peer(step),
        )

    def output_copy(step):
        return cross.remote(
            output_ref,
            outputs.at[fsdp],
            output_send.at[step],
            output_recv.at[step],
            seq,
            cross.fsdp_peer(step),
        )

    stacks = [attention.stack.at[kind] for kind in range(3)]
    stacks += [units.stack.at[kind] for kind in range(3)]
    copies = load(
        [(source, stack, load_sem.at[i]) for i, (source, stack) in enumerate(zip(sources, stacks))]
    )
    greet_cross(seq_count, fsdp_count)
    for copy in copies:
        copy.wait()

    @pl.loop(0, attention.items)
    def _(item):
        attention.send_rows(item)

    for step in range(1, seq_count):
        gain_row(step).start()
    blocks[line.place * 2 + line.core] = inputs_ref[...]
    gather.send(line.place)

    @pl.loop(0, EARLY)
    def _(item):
        units.send_rows(item)

    gains[seq, fsdp] = gains_ref[...]
    outputs[fsdp] = output_ref[...]
    for step in range(1, fsdp_count):
        gain_column(seq, step).start()

    attention.take(0)

    @pl.loop(1, seq_count)
    def _(step):
        attention.take(step)
        gain_row(step).wait_recv()
        owner = (seq - step + seq_count) % seq_count
        for peer in range(1, fsdp_count):
            gain_column(owner, peer).start()
        attention.relay(step - 1)

    def project_inputs(step):
        chip = gather.step(step)
        pair = pl.ds(chip * 2, 2)
        whole = blocks[pair].reshape(2 * rows, width)
        for kind in range(3):
            weight = attention.weights[kind].reshape(width, columns)
            found = jnp.dot(whole, weight, preferred_element_type=jnp.float32)
            if kind < 2:
                pre[kind, pl.ds(chip * 2 * rows, 2 * rows)] = found
            else:
                heads[2, pair] = found.astype(jnp.bfloat16).reshape(2, rows, columns)

    def weights_arrived():
        attention.relay(seq_count - 1)
        for step in range(1, fsdp_count):
            output_copy(step).start()

        @pl.loop(0, seq_count)
        def _(item):
            attention.settle(item)
            for peer in range(1, fsdp_count):
                gain_column(item, peer).wait_recv()

        gains_out[...] = gains[...]
        lanes = gains.shape[-1]
        own = columns // fsdp_count
        lane = lax.broadcasted_iota(jnp.int32, (lanes, columns), 0)
        column = lax.broadcasted_iota(jnp.int32, (lanes, columns), 1)
        total = None
        for peer in range(fsdp_count):
            place = (column == lane + peer * own) & (lane < own)
            term = jnp.dot(
                gains[seq, peer],
                jnp.where(place, 1.0, 0.0).astype(jnp.bfloat16),
                preferred_element_type=jnp.float32,
            )
            total = term if total is None else total + term
        own_gains[...] = total
        project_inputs(0)

    def send_squares():
        total = None
        for kind in range(2):
            row = lax.dot_general(
                pick_row(kind, (8, columns)),
                pre[kind] * pre[kind],
                (((1,), (1,)), ((), ())),
                precision=EXACT,
                preferred_element_type=jnp.float32,
            )
            total = row if total is None else total + row
        sums.send(total)

    def make_heads():
        squares = sums.receive()
        for kind in range(2):
            mean = dot_rows(squares, pick_row(kind, (8, 128)), EXACT) / width
            inverse = lax.rsqrt(mean + eps_norm)
            inverse_out[:, kind : kind + 1] = inverse[:, :1]
            for first in range(0, columns, DH):
                part = pl.ds(first, DH)
                scaled = pre[kind, :, part] * inverse * own_gains[kind : kind + 1, part]
                turned = turn_heads(scaled, cosine_ref[...], sine_ref[...])
                heads[kind, :, :, part] = turned.astype(jnp.bfloat16).reshape(seq_count, rows, DH)

    def attend(step):
        chip = line.order(chips - 1 - step)

        @pl.loop(0, 2)
        def _(core):
            slot = chip * 2 + core
            first = pl.multiple_of(slot * rows, rows)
            for head in range(0, columns, DH):
                part = pl.ds(head, DH)
                probs = attention_weights(
                    heads[0, slot, :, part],
                    heads[1, :, :, part].reshape(tokens, DH),
                    first,
                    segment_column[pl.ds(first, rows), :],
                    segment_row[...],
                )
                heads[3, slot, :, part] = jnp.dot(
                    probs.astype(jnp.bfloat16),
                    heads[2, :, :, part].reshape(tokens, DH),
                    preferred_element_type=jnp.float32,
                ).astype(jnp.bfloat16)

        product_terms(
            scatter,
            [(heads.at[3], lambda part: outputs[:, :, part].reshape(columns, -1), False)],
            chip,
        )

    inputs_store = pltpu.make_async_copy(blocks, inputs_out, store_sem.at[0])
    attention_store = pltpu.make_async_copy(attention.weights, attention_out, store_sem.at[1])
    output_store = pltpu.make_async_copy(outputs, output_out, store_sem.at[2])
    heads_store = pltpu.make_async_copy(heads, heads_out, store_sem.at[3])
    pre_store = pltpu.make_async_copy(pre, pre_out, store_sem.at[4])

    def units_store(kind):
        return pltpu.make_async_copy(units.weights.at[kind], units_out.at[kind], store_sem.at[5 + kind])

    @pl.loop(0, LEAD)
    def _(item):
        units.take(item)

    arrived = 1
    after_gather = 4 * (chips - 1) - 1
    attending = after_gather + 3
    hopping = attending + chips
    beats = max(units.items + 1, hopping + 2 * chips)

    @pl.loop(0, beats)
    def _(beat):
        @pl.when(beat + EARLY < units.items)
        def _():
            units.send_rows(beat + EARLY)

        @pl.when(beat + LEAD < units.items)
        def _():
            units.take(beat + LEAD)

        @pl.when((beat > 0) & (beat <= units.items))
        def _():
            units.relay(beat - 1)

        @pl.when(beat == arrived)
        def _():
            weights_arrived()
            attention_store.start()

        @pl.when((beat % 4 == 2) & (beat // 4 + 1 < chips))
        def _():
            project_inputs(beat // 4 + 1)

        @pl.when(beat == after_gather)
        def _():
            inputs_store.start()
            pre_store.start()
            send_squares()
            for step in range(1, fsdp_count):
                output_copy(step).wait_recv()
            output_store.start()

        @pl.when(beat == after_gather + 2)
        def _():
            make_heads()

        @pl.when((beat >= attending) & (beat < attending + chips))
        def _():
            attend(beat - attending)

        @pl.when((beat >= hopping) & ((beat - hopping) % 2 == 0) & (beat < hopping + 2 * chips))
        def _():
            scatter.hop(chips - 1 - (beat - hopping) // 2)

    heads_store.start()
    scatter.settle(projected)
    for kind in range(3):

        @pl.loop(0, seq_count)
        def _(step):
            units.settle(kind * seq_count + step)

        units_store(kind).start()

    scatter.finish()
    gather.finish()
    sums.finish()
    attention.finish()
    units.finish()

    @pl.loop(1, seq_count)
    def _(step):
        gain_row(step).wait_send()

    @pl.loop(0, seq_count)
    def _(owner):
        for step in range(1, fsdp_count):
            gain_column(owner, step).wait_send()

    for step in range(1, fsdp_count):
        output_copy(step).wait_send()
    for store in (inputs_store, attention_store, output_store, heads_store, pre_store):
        store.wait()
    for kind in range(3):
        units_store(kind).wait()


def bring_in(local_in, attention_rows, unit_rows, output_weight, gains, tables, segment_row):
    rows, width = local_in.shape
    slots = lax.axis_size("seq")
    fsdp_count = lax.axis_size("fsdp")
    chips = slots // 2
    tokens = slots * rows
    own, columns = attention_rows[0].shape[0], attention_rows[0].shape[1] // slots
    units = unit_rows[0].shape[1] // slots
    bf16, f32, dma = jnp.bfloat16, jnp.float32, pltpu.SemaphoreType.DMA
    lanes = pl.cdiv(gains.shape[1], 128) * 128
    padded = jnp.pad(gains, ((0, 16 - gains.shape[0]), (0, lanes - gains.shape[1])))
    found = pl.pallas_call(
        functools.partial(bring_in_kernel, chips, fsdp_count),
        out_shape=(
            jax.ShapeDtypeStruct((rows, width), f32),
            jax.ShapeDtypeStruct((tokens, 8), f32),
            jax.ShapeDtypeStruct((16, columns), f32),
            jax.ShapeDtypeStruct((slots, fsdp_count, 16, lanes), bf16),
            jax.ShapeDtypeStruct((slots, rows, width), bf16),
            jax.ShapeDtypeStruct((3, slots, fsdp_count, own, columns), bf16),
            jax.ShapeDtypeStruct((fsdp_count, own, width), bf16),
            jax.ShapeDtypeStruct((3, slots, fsdp_count, own, units), bf16),
            jax.ShapeDtypeStruct((4, slots, rows, columns), bf16),
            jax.ShapeDtypeStruct((2, tokens, columns), f32),
        ),
        in_specs=[whole_spec()] * 6 + [far_spec()] * 6 + [whole_spec()],
        out_specs=(whole_spec(),) * 4 + (far_spec(),) * 6,
        scratch_shapes=[
            pltpu.VMEM((fsdp_count, own, width), bf16),
            pltpu.VMEM((slots, fsdp_count, 16, lanes), bf16),
            pltpu.VMEM((4, slots, rows, columns), bf16),
            pltpu.VMEM((2, tokens, columns), f32),
            dma((slots,)),
            dma((slots,)),
            dma((slots, fsdp_count)),
            dma((slots, fsdp_count)),
            dma((fsdp_count,)),
            dma((fsdp_count,)),
            dma((6,)),
            dma((8,)),
        ]
        + Gather.scratch(chips, rows, width)
        + RowSum.scratch(slots, (8, tokens))
        + Spread.scratch(3, 3, slots, fsdp_count, own, columns)
        + Spread.scratch(3, 1, slots, fsdp_count, own, units)
        + Scatter.scratch(chips, rows, width),
        compiler_params=line_params(3),
        name="bring_in",
    )(
        local_in,
        padded,
        *tables,
        segment_row.reshape(tokens, 1),
        segment_row.reshape(1, tokens),
        *attention_rows,
        *unit_rows,
        output_weight,
    )
    projected, inverse, own_gains, every_gain = found[:4]
    inputs_all, weights, outputs, unit_columns, heads, pre = found[4:]
    every_gain = every_gain[:, :, : gains.shape[0], : gains.shape[1]]
    return (
        projected,
        inputs_all.reshape(-1, width),
        weights.reshape(3, -1, columns),
        outputs.reshape(-1, width),
        [unit_columns[kind].reshape(-1, units) for kind in range(3)],
        heads.reshape(4, tokens, columns),
        pre,
        inverse,
        own_gains,
        every_gain.transpose(2, 0, 1, 3).reshape(gains.shape[0], -1),
    )


def gather_back_kernel(chips, fsdp_count, *refs):
    local_ref, output_ref, gains_ref, inverse_ref, cosine_ref, sine_ref = refs[:6]
    segment_column, segment_row = refs[6:8]
    hidden_hbm, grad_hbm, gate_hbm, up_hbm, act_hbm = refs[8:13]
    heads_hbm, pre_hbm = refs[13:15]
    refs = refs[15:]
    results, output_term, grads_out, gain_out = refs[:3], refs[3], refs[4], refs[5]
    refs = refs[6:]
    tokens, units, heads, pre, gathered, grad_query, grad_key, grad_value = refs[:8]
    load_sem, refs = refs[8], refs[9:]
    line = Line(chips)
    cross = Cross(2 * chips, fsdp_count)
    gather = Gather(line, *refs[:5])
    sums = RowSum(cross, *refs[5:9])
    all_tokens, width = tokens.shape[1:]
    block_units = units.shape[-1]
    columns = output_ref.shape[0]
    blocks = gather.blocks
    rows = blocks.shape[1]

    def fill(kind, owner, slot):
        span = width // cross.seq_count
        chosen = tokens[kind // 2, :, pl.ds(pl.multiple_of(owner * span, 128), span)]

        @pl.loop(0, block_units // tile_of(block_units))
        def _(tile):
            part = pl.ds(pl.multiple_of(tile * tile_of(block_units), 128), tile_of(block_units))
            term = dot_rows(chosen, units[kind, :, part]).astype(jnp.bfloat16)
            collect.terms[slot, :, :, part] = term.reshape(fsdp_count, -1, term.shape[1])

    collect = Collect(cross, 3, fill, *refs[9:])
    copies = load(
        [
            (hidden_hbm, tokens.at[0], load_sem.at[0]),
            (gate_hbm, units.at[0], load_sem.at[1]),
            (up_hbm, units.at[1], load_sem.at[2]),
            (grad_hbm, tokens.at[1], load_sem.at[3]),
            (act_hbm, units.at[2], load_sem.at[4]),
            (heads_hbm, heads, load_sem.at[5]),
            (pre_hbm, pre, load_sem.at[6]),
        ]
    )
    greet_cross(cross.seq_count, fsdp_count)
    blocks[line.place * 2 + line.core] = local_ref[...]
    gather.send(line.place)
    grad_key[...] = jnp.zeros_like(grad_key)
    grad_value[...] = jnp.zeros_like(grad_value)
    for copy in copies[:2]:
        copy.wait()
    collect.begin()
    for copy in copies[2:]:
        copy.wait()

    def arrive(step):
        chip = gather.step(step)
        whole = blocks[pl.ds(chip * 2, 2)].reshape(2 * rows, width)
        found = dot_cols(whole, output_ref[...]).astype(jnp.bfloat16)
        gathered[pl.ds(chip * 2 * rows, 2 * rows), :] = found

    arrive(0)
    query_rows = 128
    blocks_of_rows = all_tokens // query_rows
    first_beat = 3 * (chips - 1)

    def attend(block):
        first = pl.multiple_of(block * query_rows, query_rows)
        span = pl.ds(first, query_rows)
        for head in range(0, columns, DH):
            part = pl.ds(head, DH)
            queries, keys, values = heads[0, span, part], heads[1, :, part], heads[2, :, part]
            outer = gathered[span, part]
            probs = attention_weights(
                queries, keys, first, segment_column[span, :], segment_row[...]
            )
            grad_value[:, part] += dot_rows(probs.astype(jnp.bfloat16), outer)
            grad_probs = dot_cols(outer, values)
            delta = jnp.sum(probs * grad_probs, axis=-1, keepdims=True)
            grad_scores = (probs * (grad_probs - delta)).astype(jnp.bfloat16)
            grad_query[span, part] = jnp.dot(
                grad_scores, keys, preferred_element_type=jnp.float32
            )
            grad_key[:, part] += dot_rows(grad_scores, queries)

    def errors(kind, grad):
        scaled = (grad[...] * DH ** (-0.5)).astype(jnp.bfloat16).astype(jnp.float32)
        error = turn_heads(scaled, cosine_ref[...], -sine_ref[...])
        inverse = inverse_ref[:, kind : kind + 1]
        return error, pre[kind] * inverse, inverse

    def send_means():
        total = None
        for kind, grad in enumerate((grad_query, grad_key)):
            error, unit, _ = errors(kind, grad)
            product = error * unit
            gain_out[kind : kind + 1, :] = jnp.sum(product, axis=0, keepdims=True)
            row = lax.dot_general(
                pick_row(kind, (8, columns)),
                product * gains_ref[kind : kind + 1, :],
                (((1,), (1,)), ((), ())),
                precision=EXACT,
                preferred_element_type=jnp.float32,
            )
            total = row if total is None else total + row
        sums.send(total)
        grads_out[2] = grad_value[...].astype(jnp.bfloat16)

        @pl.loop(0, width // tile_of(width))
        def _(tile):
            part = pl.ds(pl.multiple_of(tile * tile_of(width), 128), tile_of(width))
            outer = blocks[:, :, part].reshape(all_tokens, -1)
            output_term[:, part] = dot_rows(heads[3], outer).astype(jnp.bfloat16)

    def finish_grads():
        means = sums.receive() / width
        for kind, grad in enumerate((grad_query, grad_key)):
            error, unit, inverse = errors(kind, grad)
            mean = dot_rows(means, pick_row(kind, (8, 128)), EXACT)[:, :1]
            grads_out[kind] = (
                inverse * (error * gains_ref[kind : kind + 1, :] - unit * mean)
            ).astype(jnp.bfloat16)

    @pl.loop(0, collect.beats)
    def _(turn):
        collect.beat(turn)

        @pl.when((turn % 3 == 2) & (turn // 3 + 1 < chips))
        def _():
            arrive(turn // 3 + 1)

        @pl.when((turn >= first_beat) & (turn < first_beat + blocks_of_rows))
        def _():
            attend(turn - first_beat)

        @pl.when(turn == first_beat + blocks_of_rows)
        def _():
            send_means()

        @pl.when(turn == first_beat + blocks_of_rows + 3)
        def _():
            finish_grads()

    @pl.loop(0, cross.seq_count)
    def _(turn):
        for kind in range(3):

            def put(_, sender, value):
                part = pl.ds(pl.multiple_of(sender * block_units, 128), block_units)
                results[kind][:, part] = value

            collect.receive(kind * cross.seq_count + turn, put)

    collect.finish()
    gather.finish()
    sums.finish()


def gather_back(local, output_rows, gains, inverse, tables, segment_row, far, heads, pre):
    rows, width = local.shape
    slots = lax.axis_size("seq")
    fsdp_count = lax.axis_size("fsdp")
    chips = slots // 2
    own = width // (slots * fsdp_count)
    units = far[2].shape[1]
    _, tokens, columns = heads.shape
    bf16, f32 = jnp.bfloat16, jnp.float32
    found = pl.pallas_call(
        functools.partial(gather_back_kernel, chips, fsdp_count),
        out_shape=(jax.ShapeDtypeStruct((own, units * slots), f32),) * 3
        + (
            jax.ShapeDtypeStruct((columns, width), bf16),
            jax.ShapeDtypeStruct((3, tokens, columns), bf16),
            jax.ShapeDtypeStruct((8, columns), f32),
        ),
        in_specs=[whole_spec()] * 8 + [far_spec()] * 7,
        out_specs=(whole_spec(),) * 6,
        scratch_shapes=[
            pltpu.VMEM((2, tokens, width), bf16),
            pltpu.VMEM((3, tokens, units), bf16),
            pltpu.VMEM((4, tokens, columns), bf16),
            pltpu.VMEM((2, tokens, columns), f32),
            pltpu.VMEM((tokens, columns), bf16),
            pltpu.VMEM((tokens, columns), f32),
            pltpu.VMEM((tokens, columns), f32),
            pltpu.VMEM((tokens, columns), f32),
            pltpu.SemaphoreType.DMA((7,)),
        ]
        + Gather.scratch(chips, rows, width)
        + RowSum.scratch(slots, (8, tokens))
        + Collect.scratch(3, slots, fsdp_count, own, units),
        compiler_params=line_params(6),
        name="gather_back",
    )(
        local,
        output_rows,
        gains,
        inverse,
        *tables,
        segment_row.reshape(tokens, 1),
        segment_row.reshape(1, tokens),
        *far,
        heads,
        pre,
    )
    return found[:3], found[3], found[4], found[5]


def take_out_kernel(
    chips,
    fsdp_count,
    *refs,
):
    grads_ref, rights, tokens_ref = refs[0], refs[1], refs[2]
    output_ref, gains_ref, refs = refs[3], refs[4], refs[5:]
    result, weight_outs, output_out, gains_out, refs = refs[0], refs[1:4], refs[4], refs[5], refs[6:]
    output_in, gain_in, gain_out, gain_rows, refs = refs[0], refs[1], refs[2], refs[3], refs[4:]
    output_send, output_recv, gain_send, gain_recv, gain_row_send, gain_row_recv = refs[:6]
    comm = refs[6:]
    line = Line(chips)
    cross = Cross(2 * chips, fsdp_count)
    seq_count, seq, fsdp = cross.seq_count, cross.seq, cross.fsdp
    scatter = Scatter(line, *comm[:-12])
    columns = rights.shape[-1]
    rows, width = scatter.fresh.shape[1:]

    def fill(kind, owner, slot):
        span = width // seq_count
        part = pl.ds(pl.multiple_of(owner * span, 128), span)
        chosen = tokens_ref[:, part]
        for kind in range(3):
            term = dot_rows(chosen, grads_ref[kind].reshape(-1, columns)).astype(jnp.bfloat16)
            collect.terms[slot, :, :, kind * columns : (kind + 1) * columns] = term.reshape(
                fsdp_count, -1, columns
            )

    collect = Collect(cross, 1, fill, *comm[-12:])

    def output_copy(step):
        peer = cross.fsdp_peer(step)
        return cross.remote(
            output_ref.at[peer],
            output_in.at[step],
            output_send.at[step],
            output_recv.at[step],
            seq,
            peer,
        )

    def gain_copy(step):
        peer = cross.fsdp_peer(step)
        return cross.remote(
            gains_ref.at[peer], gain_in.at[step], gain_send.at[step], gain_recv.at[step], seq, peer
        )

    def gain_row(step):
        peer = cross.seq_peer(step)
        return cross.remote(
            gain_out.at[peer],
            gain_rows.at[step],
            gain_row_send.at[step],
            gain_row_recv.at[step],
            peer,
            fsdp,
        )

    greet_cross(seq_count, fsdp_count)
    for step in range(1, fsdp_count):
        gain_copy(step).start()

    collect.begin()

    @pl.loop(0, chips)
    def _(step):
        product_terms(
            scatter,
            [(grads_ref.at[kind], rights.at[kind], True) for kind in range(3)],
            line.order(chips - 1 - step),
        )

    total = gains_ref[fsdp]
    for step in range(1, fsdp_count):
        gain_copy(step).wait_recv()
        total = total + gain_in[step]
    gain_out[...] = total
    for step in range(1, seq_count):
        gain_row(step).start()

    @pl.loop(0, collect.beats)
    def _(turn):
        collect.beat(turn)

        @pl.when(turn == seq_count - AHEAD)
        def _():
            for step in range(1, fsdp_count):
                output_copy(step).start()

        @pl.when((turn >= HOPPING) & (turn < HOPPING + chips))
        def _():
            scatter.hop(chips - 1 - (turn - HOPPING))

    total = output_ref[fsdp].astype(jnp.float32)
    for step in range(1, fsdp_count):
        output_copy(step).wait_recv()
        total = total + output_in[step].astype(jnp.float32)
    output_out[...] = total
    scatter.settle(result)
    total = gain_out[seq]
    for step in range(1, seq_count):
        gain_row(step).wait_recv()
        total = total + gain_rows[step]
    gains_out[...] = total

    def put(_, sender, value):
        block = pl.ds(pl.multiple_of(sender * columns, 128), columns)
        for kind in range(3):
            weight_outs[kind][:, block] = value[:, kind * columns : (kind + 1) * columns]

    @pl.loop(0, seq_count)
    def _(turn):
        collect.receive(turn, put)

    scatter.finish()
    collect.finish()

    @pl.loop(1, seq_count)
    def _(step):
        gain_row(step).wait_send()

    for step in range(1, fsdp_count):
        output_copy(step).wait_send()
        gain_copy(step).wait_send()


def take_out(grads, weights, tokens, output_term, gain_terms):
    slots = lax.axis_size("seq")
    fsdp_count = lax.axis_size("fsdp")
    chips = slots // 2
    _, width, columns = weights.shape
    rows = tokens.shape[0] // slots
    own = width // (slots * fsdp_count)
    kinds = gain_terms.shape[0]
    bf16, f32, dma = jnp.bfloat16, jnp.float32, pltpu.SemaphoreType.DMA
    gains = gain_terms.reshape(kinds, slots, fsdp_count, own).transpose(2, 1, 0, 3)
    lanes = pl.cdiv(own, 128) * 128
    gains = jnp.pad(gains, ((0, 0), (0, 0), (0, 8 - kinds), (0, lanes - own)))
    result, query, key, value, output, gains = pl.pallas_call(
        functools.partial(take_out_kernel, chips, fsdp_count),
        out_shape=(jax.ShapeDtypeStruct((rows, width), f32),)
        + (jax.ShapeDtypeStruct((own, columns * slots), f32),) * 3
        + (jax.ShapeDtypeStruct((own, width), f32), jax.ShapeDtypeStruct((8, lanes), f32)),
        in_specs=[whole_spec()] * 5,
        out_specs=(whole_spec(),) * 6,
        scratch_shapes=[
            pltpu.VMEM((fsdp_count, own, width), bf16),
            pltpu.VMEM((fsdp_count, slots, 8, lanes), f32),
            pltpu.VMEM((slots, 8, lanes), f32),
            pltpu.VMEM((slots, 8, lanes), f32),
            dma((fsdp_count,)),
            dma((fsdp_count,)),
            dma((fsdp_count,)),
            dma((fsdp_count,)),
            dma((slots,)),
            dma((slots,)),
        ]
        + Scatter.scratch(chips, rows, width)
        + Collect.scratch(1, slots, fsdp_count, own, 3 * columns),
        compiler_params=line_params(4),
        name="take_out",
    )(
        grads.reshape(3, slots, rows, columns),
        weights,
        tokens,
        output_term.reshape(fsdp_count, own, width),
        gains,
    )
    return result, (query, key, value), output, gains[:kinds, :own]


def rope_tables(row_count):
    half_width = DH // 2
    frequency = rope_base ** (-jnp.arange(half_width, dtype=jnp.float32) * 2.0 / DH)
    angles = jnp.arange(row_count, dtype=jnp.int32).astype(jnp.float32)[:, None] * frequency[None, :]
    cosine, sine = jnp.cos(angles), jnp.sin(angles)
    return (
        jnp.concatenate([cosine, cosine], axis=1),
        jnp.concatenate([-sine, sine], axis=1),
    )


def per_device(
    inputs,
    query_weight,
    key_weight,
    value_weight,
    output_weight,
    query_gain,
    key_gain,
    attention_gain,
    gate_weight,
    up_weight,
    down_weight,
    feedforward_gain,
    segments,
    cotangent,
):
    token_count = inputs.shape[1]
    width_all = inputs.shape[2]
    local_in = inputs.reshape(token_count, width_all)
    segment_row = segments[0]
    seq_index = lax.axis_index("seq")
    tables = rope_tables(segment_row.shape[0])
    (
        projected,
        inputs_all,
        attention_cols,
        output_rows,
        unit_cols,
        heads,
        pre,
        inverse,
        own_gains,
        gains,
    ) = bring_in(
        local_in,
        [query_weight, key_weight, value_weight],
        [gate_weight, up_weight, down_weight],
        output_weight,
        jnp.stack([query_gain, key_gain, attention_gain, feedforward_gain]),
        tables,
        segment_row,
    )
    gate_cols, up_cols, down_cols = unit_cols
    head_width = heads.shape[2]
    gains = gains.astype(jnp.float32)
    attention_scale = gains[2]
    feedforward_scale = gains[3]
    hidden = local_in.astype(jnp.float32) + rms_scale(projected, attention_scale)
    hidden_low = hidden.astype(jnp.bfloat16)
    mixed_pre, gate_linear, up_linear, activated, hidden_all = feed_forward(
        hidden_low, gate_cols, up_cols, down_cols
    )
    result = (
        (hidden + rms_scale(mixed_pre, feedforward_scale))
        .astype(jnp.bfloat16)
        .reshape(1, token_count, width_all)
    )
    grad_result = cotangent.reshape(token_count, width_all).astype(jnp.float32)
    _, mixed_pull = jax.vjp(rms_scale, mixed_pre, feedforward_scale)
    grad_mixed, grad_feedforward_gain = mixed_pull(grad_result)
    grad_mixed_low = grad_mixed.astype(jnp.bfloat16)
    hidden_term, grad_gate_low, grad_upward_low, grad_all = feed_forward_back(
        grad_mixed_low, gate_cols, up_cols, down_cols, gate_linear, up_linear
    )
    grad_hidden = grad_result + hidden_term
    _, branch_pull = jax.vjp(rms_scale, projected, attention_scale)
    grad_projected, grad_attention_gain = branch_pull(grad_hidden)
    weight_grads, output_term, attention_grads, gain_rows = gather_back(
        grad_projected.astype(jnp.bfloat16),
        output_rows,
        own_gains,
        inverse,
        tables,
        segment_row,
        [hidden_all, grad_all, grad_gate_low, grad_upward_low, activated],
        heads,
        pre,
    )
    gate_weight_grad, up_weight_grad, down_weight_grad = weight_grads
    head_gains = lax.dynamic_update_slice_in_dim(
        jnp.zeros((2, width_all), jnp.float32),
        gain_rows[:2],
        seq_index * head_width,
        1,
    )
    gain_terms = jnp.concatenate(
        [head_gains, jnp.stack([grad_attention_gain, grad_feedforward_gain])], axis=0
    )
    input_term, projection_grads, output_weight_grad, gain_grads = take_out(
        attention_grads, attention_cols, inputs_all, output_term, gain_terms
    )
    query_weight_grad, key_weight_grad, value_weight_grad = projection_grads
    grad_input = grad_hidden + input_term
    return (
        result,
        grad_input.reshape(1, token_count, width_all),
        query_weight_grad,
        key_weight_grad,
        value_weight_grad,
        output_weight_grad,
        gain_grads[0],
        gain_grads[1],
        gain_grads[2],
        gate_weight_grad,
        up_weight_grad,
        down_weight_grad,
        gain_grads[3],
    )


def solution(mesh):
    in_specs = (
        P("fsdp", "seq", None),
        P(("seq", "fsdp"), None),
        P(("seq", "fsdp"), None),
        P(("seq", "fsdp"), None),
        P(("seq", "fsdp"), None),
        P(("seq", "fsdp")),
        P(("seq", "fsdp")),
        P(("seq", "fsdp")),
        P(("seq", "fsdp"), None),
        P(("seq", "fsdp"), None),
        P(("seq", "fsdp"), None),
        P(("seq", "fsdp")),
        P("fsdp", None),
        P("fsdp", "seq", None),
    )
    out_specs = (
        P("fsdp", "seq", None),
        P("fsdp", "seq", None),
        P(("seq", "fsdp"), None),
        P(("seq", "fsdp"), None),
        P(("seq", "fsdp"), None),
        P(("seq", "fsdp"), None),
        P(("seq", "fsdp")),
        P(("seq", "fsdp")),
        P(("seq", "fsdp")),
        P(("seq", "fsdp"), None),
        P(("seq", "fsdp"), None),
        P(("seq", "fsdp"), None),
        P(("seq", "fsdp")),
    )
    return jax.shard_map(
        per_device, mesh=mesh, in_specs=in_specs, out_specs=out_specs, check_vma=False
    )
```

```python
import functools

import jax
import jax.numpy as jnp
from jax import lax
from jax.experimental import pallas as pl
from jax.experimental.pallas import tpu as pltpu
from jax.sharding import PartitionSpec as P

DH = 128


eps_norm = 1e-06
rope_base = 500000.0
neg_fill = -1e30


def rms_scale(tensor, gain):
    return tensor * lax.rsqrt(jnp.mean(tensor * tensor, axis=-1, keepdims=True) + eps_norm) * gain


MESH = pl.DeviceIdType.MESH
RS_PARTS = 4


class Line:
    def __init__(self, chips):
        index = lax.axis_index("seq")
        self.chips = chips
        self.fsdp = lax.axis_index("fsdp")
        self.place = index // 2
        self.core = index % 2

    def device(self, place, core):
        return (place * 2 + core, self.fsdp)

    @property
    def partner(self):
        return self.device(self.place, 1 - self.core)

    @property
    def above(self):
        return self.device(jnp.minimum(self.place + 1, self.chips - 1), self.core)

    @property
    def below(self):
        return self.device(jnp.maximum(self.place - 1, 0), self.core)

    @property
    def has_above(self):
        return self.place < self.chips - 1

    @property
    def has_below(self):
        return self.place > 0

    def greet(self):
        barrier = pltpu.get_barrier_semaphore()
        pl.semaphore_signal(barrier, inc=1, device_id=self.partner, device_id_type=MESH)

        @pl.when(self.has_above)
        def _():
            pl.semaphore_signal(barrier, inc=1, device_id=self.above, device_id_type=MESH)

        @pl.when(self.has_below)
        def _():
            pl.semaphore_signal(barrier, inc=1, device_id=self.below, device_id_type=MESH)

        peers = (
            1 + jnp.minimum(self.place, 1) + jnp.minimum(self.chips - 1 - self.place, 1)
        )
        pl.semaphore_wait(barrier, peers)

    def order(self, step):
        place, last = self.place, self.chips - 1
        near = jnp.minimum(place, last - place)
        both = jnp.where(step % 2 == 1, place - (step + 1) // 2, place + step // 2)
        rest = jnp.where(place <= last - place, step, last - step)
        return jnp.where(step <= 2 * near, both, rest)

    def paired(self, step):
        near = jnp.minimum(self.place, self.chips - 1 - self.place)
        return (step % 2 == 1) & (step <= 2 * near)

    def second_of_pair(self, step):
        near = jnp.minimum(self.place, self.chips - 1 - self.place)
        return (step % 2 == 0) & (step > 0) & (step <= 2 * near)


class Gather:
    def __init__(self, line, blocks, arrive, up_sem, down_sem, side_sem):
        self.line, self.blocks, self.arrive = line, blocks, arrive
        self.up_sem, self.down_sem, self.side_sem = up_sem, down_sem, side_sem

    @staticmethod
    def scratch(chips, rows, width):
        return [
            pltpu.VMEM((2 * chips, rows, width), jnp.bfloat16),
            pltpu.SemaphoreType.DMA((2 * chips,)),
            pltpu.SemaphoreType.DMA((chips,)),
            pltpu.SemaphoreType.DMA((chips,)),
            pltpu.SemaphoreType.DMA((chips,)),
        ]

    def copy(self, chip, sem, target):
        slot = chip * 2 + self.line.core
        return pltpu.make_async_remote_copy(
            src_ref=self.blocks.at[slot],
            dst_ref=self.blocks.at[slot],
            send_sem=sem.at[chip],
            recv_sem=self.arrive.at[slot],
            device_id=target,
            device_id_type=MESH,
        )

    def wait_slot(self, slot):
        pltpu.make_async_remote_copy(
            src_ref=self.blocks.at[slot],
            dst_ref=self.blocks.at[slot],
            send_sem=self.side_sem.at[0],
            recv_sem=self.arrive.at[slot],
            device_id=self.line.partner,
            device_id_type=MESH,
        ).wait_recv()

    def send(self, chip):
        line = self.line

        @pl.when((chip <= line.place) & line.has_above)
        def _():
            self.copy(chip, self.up_sem, line.above).start()

        @pl.when((chip >= line.place) & line.has_below)
        def _():
            self.copy(chip, self.down_sem, line.below).start()

        self.copy(chip, self.side_sem, line.partner).start()

    def take(self, chip):
        self.wait_slot(chip * 2 + self.line.core)
        self.send(chip)

    def step(self, step):
        line = self.line
        chip = line.order(step)

        @pl.when((step > 0) & jnp.logical_not(line.second_of_pair(step)))
        def _():
            self.take(chip)

        @pl.when(line.paired(step))
        def _():
            self.take(line.order(step + 1))

        self.wait_slot(chip * 2 + 1 - line.core)
        return chip

    def finish(self):
        line = self.line

        @pl.loop(0, line.chips)
        def _(chip):
            @pl.when((chip <= line.place) & line.has_above)
            def _():
                self.copy(chip, self.up_sem, line.above).wait_send()

            @pl.when((chip >= line.place) & line.has_below)
            def _():
                self.copy(chip, self.down_sem, line.below).wait_send()

            self.copy(chip, self.side_sem, line.partner).wait_send()


class Scatter:
    def __init__(self, line, fresh, terms, side_out, side_in, out, inward, side_send, side_recv, send_sem, recv_sem):
        self.line, self.fresh, self.terms = line, fresh, terms
        self.side_out, self.side_in = side_out, side_in
        self.out, self.inward = out, inward
        self.side_send, self.side_recv = side_send, side_recv
        self.send_sem, self.recv_sem = send_sem, recv_sem
        self.rows = terms.shape[1] // RS_PARTS

    @staticmethod
    def scratch(chips, rows, width):
        return [
            pltpu.VMEM((2, rows, width), jnp.float32),
            pltpu.VMEM((chips, rows, width), jnp.float32),
            pltpu.VMEM((chips, rows, width), jnp.bfloat16),
            pltpu.VMEM((chips, rows, width), jnp.bfloat16),
            pltpu.VMEM((chips, rows, width), jnp.bfloat16),
            pltpu.VMEM((2, chips, rows, width), jnp.bfloat16),
            pltpu.SemaphoreType.DMA((chips,)),
            pltpu.SemaphoreType.DMA((chips,)),
            pltpu.SemaphoreType.DMA((chips, RS_PARTS)),
            pltpu.SemaphoreType.DMA((2, chips, RS_PARTS)),
        ]

    def side(self, chip):
        return pltpu.make_async_remote_copy(
            src_ref=self.side_out.at[chip],
            dst_ref=self.side_in.at[chip],
            send_sem=self.side_send.at[chip],
            recv_sem=self.side_recv.at[chip],
            device_id=self.line.partner,
            device_id_type=MESH,
        )

    def part(self, chip, part, upward, target):
        rows = pl.ds(part * self.rows, self.rows)
        return pltpu.make_async_remote_copy(
            src_ref=self.out.at[chip, rows],
            dst_ref=self.inward.at[upward, chip, rows],
            send_sem=self.send_sem.at[chip, part],
            recv_sem=self.recv_sem.at[upward, chip, part],
            device_id=target,
            device_id_type=MESH,
        )

    def share(self, chip):
        self.side_out[chip] = self.fresh[1 - self.line.core].astype(jnp.bfloat16)
        self.side(chip).start()
        self.terms[chip] = self.fresh[self.line.core]

    def total(self, chip, part, ways):
        rows = pl.ds(part * self.rows, self.rows)
        total = self.terms[chip, rows] + self.side_in[chip, rows].astype(jnp.float32)
        for way in ways:
            total = total + self.inward[way, chip, rows].astype(jnp.float32)
        return rows, total

    def pass_part(self, chip, part, upward, first):
        target = self.line.above if upward else self.line.below
        if not first:
            self.part(chip, part, upward, target).wait_recv()
        rows, total = self.total(chip, part, () if first else (upward,))
        self.out[chip, rows] = total.astype(jnp.bfloat16)
        self.part(chip, part, upward, target).start()

    def hand_on(self, chip, upward, first):
        self.side(chip).wait_recv()

        @pl.loop(0, RS_PARTS)
        def _(part):
            self.pass_part(chip, part, upward, first)

    def after_term(self, chip):
        line = self.line
        self.share(chip)

        @pl.when((chip < line.place) & jnp.logical_not(line.has_above))
        def _():
            self.hand_on(chip, 0, True)

        @pl.when((chip > line.place) & jnp.logical_not(line.has_below))
        def _():
            self.hand_on(chip, 1, True)

    def hop(self, step):
        line = self.line
        lower = line.place * 2 < line.chips
        up_chip, down_chip = step, line.chips - 1 - step
        go_up = (up_chip > line.place) & line.has_below
        go_down = (down_chip < line.place) & line.has_above

        @pl.when(go_up & lower)
        def _():
            self.hand_on(up_chip, 1, False)

        @pl.when(go_down)
        def _():
            self.hand_on(down_chip, 0, False)

        @pl.when(go_up & jnp.logical_not(lower))
        def _():
            self.hand_on(up_chip, 1, False)

    def settle(self, result):
        line = self.line
        place = line.place
        self.side(place).wait_recv()

        @pl.loop(0, RS_PARTS)
        def _(part):
            @pl.when(line.has_above)
            def _():
                self.part(place, part, 0, line.below).wait_recv()

            @pl.when(line.has_below)
            def _():
                self.part(place, part, 1, line.above).wait_recv()

            @pl.when(line.has_above & line.has_below)
            def _():
                rows, total = self.total(place, part, (0, 1))
                result[rows] = total

            @pl.when(line.has_above & jnp.logical_not(line.has_below))
            def _():
                rows, total = self.total(place, part, (0,))
                result[rows] = total

            @pl.when(line.has_below & jnp.logical_not(line.has_above))
            def _():
                rows, total = self.total(place, part, (1,))
                result[rows] = total

    def hops(self):
        @pl.loop(0, self.line.chips)
        def _(step):
            self.hop(step)

    def finish(self):
        line = self.line

        @pl.loop(0, line.chips)
        def _(chip):
            self.side(chip).wait_send()

            @pl.when(chip != line.place)
            def _():
                @pl.loop(0, RS_PARTS)
                def _(part):
                    self.part(chip, part, 0, line.below).wait_send()


def tile_of(extent):
    return min(256, extent)


def dot_cols(left, right):
    return lax.dot_general(
        left, right, (((1,), (1,)), ((), ())), preferred_element_type=jnp.float32
    )


def load(pairs):
    copies = [pltpu.make_async_copy(src, dst, sem) for src, dst, sem in pairs]
    for copy in copies:
        copy.start()
    return copies


def whole_spec():
    return pl.BlockSpec(memory_space=pltpu.VMEM)


def far_spec():
    return pl.BlockSpec(memory_space=pl.ANY)


def line_params(collective_id):
    return pltpu.CompilerParams(
        collective_id=collective_id, has_side_effects=True, vmem_limit_bytes=67_043_328
    )


def peers_of(axis, size):
    me = lax.axis_index(axis)
    return me, lambda step: (me + step) % size


def greet_cross(seq_count, fsdp_count):
    seq, seq_peer = peers_of("seq", seq_count)
    fsdp, fsdp_peer = peers_of("fsdp", fsdp_count)
    barrier = pltpu.get_barrier_semaphore()
    for step in range(1, seq_count):
        pl.semaphore_signal(
            barrier, inc=1, device_id=(seq_peer(step), fsdp), device_id_type=MESH
        )
    for step in range(1, fsdp_count):
        pl.semaphore_signal(
            barrier, inc=1, device_id=(seq, fsdp_peer(step)), device_id_type=MESH
        )
    pl.semaphore_wait(barrier, seq_count + fsdp_count - 2)


class Cross:
    def __init__(self, seq_count, fsdp_count):
        self.seq_count, self.fsdp_count = seq_count, fsdp_count
        self.seq, self.seq_peer = peers_of("seq", seq_count)
        self.fsdp, self.fsdp_peer = peers_of("fsdp", fsdp_count)
        self.square = fsdp_count == 4
        if self.square:
            row, place = self.fsdp // 2, self.fsdp % 2
            self.sides = (row * 2 + 1 - place, (1 - row) * 2 + place)
            self.corner = (1 - row) * 2 + 1 - place
        else:
            self.sides = tuple(self.fsdp_peer(step) for step in range(1, fsdp_count))

    def remote(self, src, dst, send, recv, seq, fsdp):
        return pltpu.make_async_remote_copy(
            src_ref=src,
            dst_ref=dst,
            send_sem=send,
            recv_sem=recv,
            device_id=(seq, fsdp),
            device_id_type=MESH,
        )


class Spread:
    def __init__(self, cross, group, stack, weights, row_send, row_recv, side_send, side_recv, half_send, half_recv):
        self.cross, self.group, self.stack, self.weights = cross, group, stack, weights
        self.row_send, self.row_recv = row_send, row_recv
        self.side_send, self.side_recv = side_send, side_recv
        self.half_send, self.half_recv = half_send, half_recv
        self.columns, self.rows = weights.shape[-1], weights.shape[-2]
        self.items = weights.shape[0] // group * cross.seq_count

    @staticmethod
    def scratch(kinds, group, seq_count, fsdp_count, rows, columns):
        dma = pltpu.SemaphoreType.DMA
        sides = 2 if fsdp_count == 4 else fsdp_count - 1
        items = kinds // group * seq_count
        return [
            pltpu.VMEM((kinds, rows, seq_count * columns), jnp.bfloat16),
            pltpu.VMEM((kinds, seq_count, fsdp_count, rows, columns), jnp.bfloat16),
            dma((kinds, seq_count)),
            dma((kinds, seq_count)),
            dma((items, sides)),
            dma((items, sides)),
            dma((items, 2)),
            dma((items, 2)),
        ]

    def block(self, owner):
        return pl.ds(pl.multiple_of(owner * self.columns, 128), self.columns)

    def row(self, kind, step):
        cross = self.cross
        peer = cross.seq_peer(step)
        return cross.remote(
            self.stack.at[kind, :, self.block(peer)],
            self.weights.at[kind, cross.seq, cross.fsdp],
            self.row_send.at[kind, step],
            self.row_recv.at[kind, step],
            peer,
            cross.fsdp,
        )

    def place(self, item):
        count = self.cross.seq_count
        step = item % count
        return item // count * self.group, step, (self.cross.seq - step + count) % count

    def side(self, item, side):
        cross = self.cross
        first, _, owner = self.place(item)
        ref = self.weights.at[pl.ds(first, self.group), owner, cross.fsdp]
        return cross.remote(
            ref,
            ref,
            self.side_send.at[item, side],
            self.side_recv.at[item, side],
            cross.seq,
            cross.sides[side],
        )

    def half(self, item, side):
        cross = self.cross
        first, _, owner = self.place(item)
        rows = pl.ds(side * (self.rows // 2), self.rows // 2)
        ref = self.weights.at[pl.ds(first, self.group), owner, cross.sides[side], rows]
        return cross.remote(
            ref,
            ref,
            self.half_send.at[item, side],
            self.half_recv.at[item, side],
            cross.seq,
            cross.sides[1 - side],
        )

    def send_rows(self, item):
        first, step, _ = self.place(item)

        @pl.when(step > 0)
        def _():
            for kind in range(self.group):
                self.row(first + kind, step).start()

    def take(self, item):
        cross = self.cross
        first, step, _ = self.place(item)

        @pl.when(step > 0)
        def _():
            for kind in range(self.group):
                self.row(first + kind, step).wait_recv()

        @pl.when(step == 0)
        def _():
            for kind in range(self.group):
                own = self.stack[first + kind, :, self.block(cross.seq)]
                self.weights[first + kind, cross.seq, cross.fsdp] = own

        self.pass_on(item)

    def pass_on(self, item):
        for side in range(len(self.cross.sides)):
            self.side(item, side).start()

    def relay(self, item):
        for side in range(len(self.cross.sides)):
            self.side(item, side).wait_recv()
            if self.cross.square:
                self.half(item, side).start()

    def settle(self, item):
        if self.cross.square:
            for side in range(2):
                self.half(item, side).wait_recv()

    def finish(self):
        cross = self.cross

        @pl.loop(0, self.items)
        def _(item):
            first, step, _ = self.place(item)

            @pl.when(step > 0)
            def _():
                for kind in range(self.group):
                    self.row(first + kind, step).wait_send()

            self.finish_item(item)

    def finish_item(self, item):
        for side in range(len(self.cross.sides)):
            self.side(item, side).wait_send()
            if self.cross.square:
                self.half(item, side).wait_send()


AHEAD = 2
LAG = 3
RING = 8


class Collect:
    def __init__(self, cross, kinds, fill, terms, side_in, half_out, half_in, row_out, row_in, side_send, side_recv, half_send, half_recv, row_send, row_recv):
        self.cross, self.fill, self.terms = cross, fill, terms
        self.side_in, self.half_out, self.half_in = side_in, half_out, half_in
        self.row_out, self.row_in = row_out, row_in
        self.side_send, self.side_recv = side_send, side_recv
        self.half_send, self.half_recv = half_send, half_recv
        self.row_send, self.row_recv = row_send, row_recv
        self.rows, self.columns = terms.shape[-2:]
        self.items = kinds * cross.seq_count

    @staticmethod
    def scratch(kinds, seq_count, fsdp_count, rows, columns):
        dma = pltpu.SemaphoreType.DMA
        vmem = pltpu.VMEM
        bf16 = jnp.bfloat16
        items = kinds * seq_count
        if fsdp_count == 4:
            arrays = [
                vmem((items, 2, 2, rows // 2, columns), bf16),
                vmem((RING, 2, rows // 2, columns), bf16),
                vmem((items, 2, rows // 2, columns), bf16),
            ]
            sides = (2, 2)
        else:
            arrays = [
                vmem((items, fsdp_count - 1, rows, columns), bf16),
                vmem((1, 1, 16, 128), bf16),
                vmem((1, 1, 16, 128), bf16),
            ]
            sides = (fsdp_count - 1, 1)
        return [vmem((RING, fsdp_count, rows, columns), bf16)] + arrays + [
            vmem((RING, rows, columns), bf16),
            vmem((items, rows, columns), bf16),
            dma((items,) + sides),
            dma((items,) + sides),
            dma((items, 2)),
            dma((items, 2)),
            dma((items,)),
            dma((items,)),
        ]

    def half_rows(self, side):
        return pl.ds(side * (self.rows // 2), self.rows // 2)

    def side(self, turn, side, which):
        cross = self.cross
        if not cross.square:
            return cross.remote(
                self.terms.at[turn % RING, cross.sides[side]],
                self.side_in.at[turn, side],
                self.side_send.at[turn, side, 0],
                self.side_recv.at[turn, side, 0],
                cross.seq,
                cross.sides[side],
            )
        target = cross.sides[side] if which == 0 else cross.corner
        return cross.remote(
            self.terms.at[turn % RING, target, self.half_rows(side)],
            self.side_in.at[turn, side, which],
            self.side_send.at[turn, side, which],
            self.side_recv.at[turn, side, which],
            cross.seq,
            cross.sides[side],
        )

    def half(self, turn, side):
        cross = self.cross
        return cross.remote(
            self.half_out.at[turn % RING, side],
            self.half_in.at[turn, side],
            self.half_send.at[turn, side],
            self.half_recv.at[turn, side],
            cross.seq,
            cross.sides[1 - side],
        )

    def row(self, turn):
        cross = self.cross
        return cross.remote(
            self.row_out.at[turn % RING],
            self.row_in.at[turn],
            self.row_send.at[turn],
            self.row_recv.at[turn],
            self.place(turn)[1],
            cross.fsdp,
        )

    def place(self, turn):
        count = self.cross.seq_count
        return turn // count, self.cross.seq_peer(turn % count + 1)

    def is_own(self, turn):
        return turn % self.cross.seq_count == self.cross.seq_count - 1

    @property
    def ways(self):
        return range(2) if self.cross.square else range(1)

    def sides(self, turn):
        return [
            self.side(turn, side, which)
            for which in reversed(self.ways)
            for side in range(len(self.cross.sides))
        ]

    def send(self, turn, first):
        if not first:

            @pl.when(turn >= RING)
            def _():
                for copy in self.sides(turn - RING):
                    copy.wait_send()

        kind, owner = self.place(turn)
        self.fill(kind, owner, turn % RING)
        for copy in self.sides(turn):
            copy.start()

    def middle(self, turn):
        if not self.cross.square:
            return
        cross = self.cross

        @pl.when(turn >= RING)
        def _():
            for side in range(2):
                self.half(turn - RING, side).wait_send()

        for side in range(2):
            self.side(turn, side, 1).wait_recv()
            mine = self.terms[turn % RING, cross.sides[1 - side], self.half_rows(side)]
            self.half_out[turn % RING, side] = (
                mine.astype(jnp.float32) + self.side_in[turn, side, 1].astype(jnp.float32)
            ).astype(jnp.bfloat16)
            self.half(turn, side).start()

    def totals(self, turn):
        cross = self.cross
        found = []
        if cross.square:
            for side in range(2):
                self.side(turn, side, 0).wait_recv()
                self.half(turn, side).wait_recv()
                rows = self.half_rows(side)
                total = self.terms[turn % RING, cross.fsdp, rows].astype(jnp.float32)
                total = total + self.side_in[turn, side, 0].astype(jnp.float32)
                total = total + self.half_in[turn, side].astype(jnp.float32)
                found.append((rows, total))
        else:
            total = self.terms[turn % RING, cross.fsdp].astype(jnp.float32)
            for side in range(len(cross.sides)):
                self.side(turn, side, 0).wait_recv()
                total = total + self.side_in[turn, side].astype(jnp.float32)
            found.append((pl.ds(0, self.rows), total))
        return found

    def ship(self, turn):
        own = self.is_own(turn)
        self.free_row(turn - RING)

        @pl.when(own)
        def _():
            for rows, total in self.totals(turn):
                self.row_in[turn, rows] = total.astype(jnp.bfloat16)

        @pl.when(jnp.logical_not(own))
        def _():
            for rows, total in self.totals(turn):
                self.row_out[turn % RING, rows] = total.astype(jnp.bfloat16)
            self.row(turn).start()

    def free_row(self, turn):
        @pl.when((turn >= 0) & jnp.logical_not(self.is_own(turn)))
        def _():
            self.row(turn).wait_send()

    def beat(self, turn):
        ahead = turn + AHEAD

        @pl.when(ahead < self.items)
        def _():
            self.send(ahead, False)

        @pl.when(turn < self.items)
        def _():
            self.middle(turn)

        @pl.when((turn >= LAG) & (turn < self.beats))
        def _():
            self.ship(turn - LAG)

    def begin(self):
        @pl.loop(0, min(AHEAD, self.items))
        def _(turn):
            self.send(turn, True)

    @property
    def beats(self):
        return self.items + LAG

    def receive(self, turn, put):
        count = self.cross.seq_count

        @pl.when(jnp.logical_not(self.is_own(turn)))
        def _():
            self.row(turn).wait_recv()

        sender = (self.cross.seq - turn % count - 1 + count) % count
        put(turn // count, sender, self.row_in[turn])

    def finish(self):
        cross = self.cross
        late = max(self.items - RING, 0)

        @pl.loop(late, self.items)
        def _(turn):
            for copy in self.sides(turn):
                copy.wait_send()
            if cross.square:
                for side in range(2):
                    self.half(turn, side).wait_send()
            self.free_row(turn)


def dot_rows(left, right, precision=None):
    return lax.dot_general(
        left,
        right,
        (((0,), (0,)), ((), ())),
        precision=precision,
        preferred_element_type=jnp.float32,
    )


EXACT = lax.Precision.HIGHEST


def turn_heads(tensor, cosine, sine):
    heads = [
        tensor[:, first : first + DH] * cosine
        + pltpu.roll(tensor[:, first : first + DH], DH // 2, 1) * sine
        for first in range(0, tensor.shape[1], DH)
    ]
    return jnp.concatenate(heads, axis=1) if len(heads) > 1 else heads[0]


def attention_weights(queries, keys, first_row, segment_column, segment_row):
    rows, count = queries.shape[0], keys.shape[0]
    scores = dot_cols(queries, keys) * DH ** (-0.5)
    query_place = first_row + lax.broadcasted_iota(jnp.int32, (rows, count), 0)
    key_place = lax.broadcasted_iota(jnp.int32, (rows, count), 1)
    allowed = (key_place <= query_place) & (segment_row == segment_column)
    scores = jnp.where(allowed, scores, neg_fill)
    expanded = jnp.exp(scores - jnp.max(scores, axis=-1, keepdims=True))
    return expanded / jnp.sum(expanded, axis=-1, keepdims=True)


class RowSum:
    def __init__(self, cross, local, every, send_sem, recv_sem):
        self.cross, self.local, self.every = cross, local, every
        self.send_sem, self.recv_sem = send_sem, recv_sem

    @staticmethod
    def scratch(seq_count, shape):
        dma = pltpu.SemaphoreType.DMA
        return [
            pltpu.VMEM(shape, jnp.float32),
            pltpu.VMEM((seq_count,) + shape, jnp.float32),
            dma((seq_count,)),
            dma((seq_count,)),
        ]

    def copy(self, step):
        cross = self.cross
        return cross.remote(
            self.local,
            self.every.at[step],
            self.send_sem.at[step],
            self.recv_sem.at[step],
            cross.seq_peer(step),
            cross.fsdp,
        )

    def send(self, value):
        self.local[...] = value
        for step in range(1, self.cross.seq_count):
            self.copy(step).start()

    def receive(self):
        total = self.local[...]
        for step in range(1, self.cross.seq_count):
            self.copy(step).wait_recv()
            total = total + self.every[step]
        return total

    def finish(self):
        for step in range(1, self.cross.seq_count):
            self.copy(step).wait_send()


def pick_row(row, shape):
    return jnp.where(lax.broadcasted_iota(jnp.int32, shape, 0) == row, 1.0, 0.0)


def product_terms(scatter, pairs, chip):
    _, rows, width = scatter.fresh.shape
    pair = pl.ds(chip * 2, 2)

    @pl.loop(0, width // tile_of(width))
    def _(tile):
        columns = pl.ds(pl.multiple_of(tile * tile_of(width), 128), tile_of(width))
        total = None
        for left, right, across in pairs:
            tokens = left[pair].reshape(2 * rows, -1)
            if across:
                term = dot_cols(tokens, right[columns, :])
            else:
                term = jnp.dot(tokens, right(columns), preferred_element_type=jnp.float32)
            total = term if total is None else total + term
        scatter.fresh[:, :, columns] = total.reshape(2, rows, -1)

    scatter.after_term(chip)


EARLY = 6
LEAD = 2
HOPPING = 4


def bring_in_kernel(chips, fsdp_count, *refs):
    inputs_ref, gains_ref, cosine_ref, sine_ref, segment_column, segment_row = refs[:6]
    sources, output_ref, refs = refs[6:12], refs[12], refs[13:]
    projected, inverse_out, own_gains, gains_out = refs[:4]
    inputs_out, attention_out, output_out, heads_out, pre_out = refs[4:9]
    units_out, outputs, gains, heads, pre, refs = refs[9:12], refs[12], refs[13], refs[14], refs[15], refs[16:]
    gain_row_send, gain_row_recv, gain_column_send, gain_column_recv = refs[:4]
    output_send, output_recv, load_sem, store_sem, refs = refs[4], refs[5], refs[6], refs[7], refs[8:]
    line = Line(chips)
    cross = Cross(2 * chips, fsdp_count)
    gather, refs = Gather(line, *refs[:5]), refs[5:]
    sums, refs = RowSum(cross, *refs[:4]), refs[4:]
    attention, refs = Spread(cross, 3, *refs[:8]), refs[8:]
    units, refs = Spread(cross, 1, *refs[:8]), refs[8:]
    scatter = Scatter(line, *refs)
    seq_count, seq, fsdp = cross.seq_count, cross.seq, cross.fsdp
    blocks = gather.blocks
    _, rows, width = blocks.shape
    columns = attention.columns
    tokens = seq_count * rows

    def gain_row(step):
        return cross.remote(
            gains_ref,
            gains.at[seq, fsdp],
            gain_row_send.at[step],
            gain_row_recv.at[step],
            cross.seq_peer(step),
            fsdp,
        )

    def gain_column(owner, step):
        ref = gains.at[owner, fsdp]
        return cross.remote(
            ref,
            ref,
            gain_column_send.at[owner, step],
            gain_column_recv.at[owner, step],
            seq,
            cross.fsdp_peer(step),
        )

    def output_copy(step):
        return cross.remote(
            output_ref,
            outputs.at[fsdp],
            output_send.at[step],
            output_recv.at[step],
            seq,
            cross.fsdp_peer(step),
        )

    stacks = [attention.stack.at[kind] for kind in range(3)]
    stacks += [units.stack.at[kind] for kind in range(3)]
    copies = load(
        [(source, stack, load_sem.at[i]) for i, (source, stack) in enumerate(zip(sources, stacks))]
    )
    greet_cross(seq_count, fsdp_count)
    for copy in copies:
        copy.wait()

    @pl.loop(0, attention.items)
    def _(item):
        attention.send_rows(item)

    for step in range(1, seq_count):
        gain_row(step).start()
    blocks[line.place * 2 + line.core] = inputs_ref[...]
    gather.send(line.place)

    @pl.loop(0, EARLY)
    def _(item):
        units.send_rows(item)

    gains[seq, fsdp] = gains_ref[...]
    outputs[fsdp] = output_ref[...]
    for step in range(1, fsdp_count):
        gain_column(seq, step).start()

    attention.take(0)

    @pl.loop(1, seq_count)
    def _(step):
        attention.take(step)
        gain_row(step).wait_recv()
        owner = (seq - step + seq_count) % seq_count
        for peer in range(1, fsdp_count):
            gain_column(owner, peer).start()
        attention.relay(step - 1)

    def project_inputs(step):
        chip = gather.step(step)
        pair = pl.ds(chip * 2, 2)
        whole = blocks[pair].reshape(2 * rows, width)
        for kind in range(3):
            weight = attention.weights[kind].reshape(width, columns)
            found = jnp.dot(whole, weight, preferred_element_type=jnp.float32)
            if kind < 2:
                pre[kind, pl.ds(chip * 2 * rows, 2 * rows)] = found
            else:
                heads[2, pair] = found.astype(jnp.bfloat16).reshape(2, rows, columns)

    def weights_arrived():
        attention.relay(seq_count - 1)
        for step in range(1, fsdp_count):
            output_copy(step).start()

        @pl.loop(0, seq_count)
        def _(item):
            attention.settle(item)
            for peer in range(1, fsdp_count):
                gain_column(item, peer).wait_recv()

        gains_out[...] = gains[...]
        lanes = gains.shape[-1]
        own = columns // fsdp_count
        lane = lax.broadcasted_iota(jnp.int32, (lanes, columns), 0)
        column = lax.broadcasted_iota(jnp.int32, (lanes, columns), 1)
        total = None
        for peer in range(fsdp_count):
            place = (column == lane + peer * own) & (lane < own)
            term = jnp.dot(
                gains[seq, peer],
                jnp.where(place, 1.0, 0.0).astype(jnp.bfloat16),
                preferred_element_type=jnp.float32,
            )
            total = term if total is None else total + term
        own_gains[...] = total
        project_inputs(0)

    def send_squares():
        total = None
        for kind in range(2):
            row = lax.dot_general(
                pick_row(kind, (8, columns)),
                pre[kind] * pre[kind],
                (((1,), (1,)), ((), ())),
                precision=EXACT,
                preferred_element_type=jnp.float32,
            )
            total = row if total is None else total + row
        sums.send(total)

    def make_heads():
        squares = sums.receive()
        for kind in range(2):
            mean = dot_rows(squares, pick_row(kind, (8, 128)), EXACT) / width
            inverse = lax.rsqrt(mean + eps_norm)
            inverse_out[:, kind : kind + 1] = inverse[:, :1]
            for first in range(0, columns, DH):
                part = pl.ds(first, DH)
                scaled = pre[kind, :, part] * inverse * own_gains[kind : kind + 1, part]
                turned = turn_heads(scaled, cosine_ref[...], sine_ref[...])
                heads[kind, :, :, part] = turned.astype(jnp.bfloat16).reshape(seq_count, rows, DH)

    def attend(step):
        chip = line.order(chips - 1 - step)

        @pl.loop(0, 2)
        def _(core):
            slot = chip * 2 + core
            first = pl.multiple_of(slot * rows, rows)
            for head in range(0, columns, DH):
                part = pl.ds(head, DH)
                probs = attention_weights(
                    heads[0, slot, :, part],
                    heads[1, :, :, part].reshape(tokens, DH),
                    first,
                    segment_column[pl.ds(first, rows), :],
                    segment_row[...],
                )
                heads[3, slot, :, part] = jnp.dot(
                    probs.astype(jnp.bfloat16),
                    heads[2, :, :, part].reshape(tokens, DH),
                    preferred_element_type=jnp.float32,
                ).astype(jnp.bfloat16)

        product_terms(
            scatter,
            [(heads.at[3], lambda part: outputs[:, :, part].reshape(columns, -1), False)],
            chip,
        )

    inputs_store = pltpu.make_async_copy(blocks, inputs_out, store_sem.at[0])
    attention_store = pltpu.make_async_copy(attention.weights, attention_out, store_sem.at[1])
    output_store = pltpu.make_async_copy(outputs, output_out, store_sem.at[2])
    heads_store = pltpu.make_async_copy(heads, heads_out, store_sem.at[3])
    pre_store = pltpu.make_async_copy(pre, pre_out, store_sem.at[4])

    def units_store(kind):
        return pltpu.make_async_copy(units.weights.at[kind], units_out[kind], store_sem.at[5 + kind])

    @pl.loop(0, LEAD)
    def _(item):
        units.take(item)

    arrived = 1
    after_gather = 4 * (chips - 1) - 1
    attending = after_gather + 3
    hopping = attending + chips
    beats = max(units.items + 1, hopping + 2 * chips)

    @pl.loop(0, beats)
    def _(beat):
        @pl.when(beat + EARLY < units.items)
        def _():
            units.send_rows(beat + EARLY)

        @pl.when(beat + LEAD < units.items)
        def _():
            units.take(beat + LEAD)

        @pl.when((beat > 0) & (beat <= units.items))
        def _():
            units.relay(beat - 1)

        @pl.when(beat == arrived)
        def _():
            weights_arrived()
            attention_store.start()

        @pl.when((beat % 4 == 2) & (beat // 4 + 1 < chips))
        def _():
            project_inputs(beat // 4 + 1)

        @pl.when(beat == after_gather)
        def _():
            inputs_store.start()
            pre_store.start()
            send_squares()
            for step in range(1, fsdp_count):
                output_copy(step).wait_recv()
            output_store.start()

        @pl.when(beat == after_gather + 2)
        def _():
            make_heads()

        @pl.when((beat >= attending) & (beat < attending + chips))
        def _():
            attend(beat - attending)

        @pl.when((beat >= hopping) & ((beat - hopping) % 2 == 0) & (beat < hopping + 2 * chips))
        def _():
            scatter.hop(chips - 1 - (beat - hopping) // 2)

    heads_store.start()
    scatter.settle(projected)
    for kind in range(3):

        @pl.loop(0, seq_count)
        def _(step):
            units.settle(kind * seq_count + step)

        units_store(kind).start()

    scatter.finish()
    gather.finish()
    sums.finish()
    attention.finish()
    units.finish()

    @pl.loop(1, seq_count)
    def _(step):
        gain_row(step).wait_send()

    @pl.loop(0, seq_count)
    def _(owner):
        for step in range(1, fsdp_count):
            gain_column(owner, step).wait_send()

    for step in range(1, fsdp_count):
        output_copy(step).wait_send()
    for store in (inputs_store, attention_store, output_store, heads_store, pre_store):
        store.wait()
    for kind in range(3):
        units_store(kind).wait()


def bring_in(local_in, attention_rows, unit_rows, output_weight, gains, tables, segment_row):
    rows, width = local_in.shape
    slots = lax.axis_size("seq")
    fsdp_count = lax.axis_size("fsdp")
    chips = slots // 2
    tokens = slots * rows
    own, columns = attention_rows[0].shape[0], attention_rows[0].shape[1] // slots
    units = unit_rows[0].shape[1] // slots
    bf16, f32, dma = jnp.bfloat16, jnp.float32, pltpu.SemaphoreType.DMA
    lanes = pl.cdiv(gains.shape[1], 128) * 128
    padded = jnp.pad(gains, ((0, 16 - gains.shape[0]), (0, lanes - gains.shape[1])))
    found = pl.pallas_call(
        functools.partial(bring_in_kernel, chips, fsdp_count),
        out_shape=(
            jax.ShapeDtypeStruct((rows, width), f32),
            jax.ShapeDtypeStruct((tokens, 8), f32),
            jax.ShapeDtypeStruct((16, columns), f32),
            jax.ShapeDtypeStruct((slots, fsdp_count, 16, lanes), bf16),
            jax.ShapeDtypeStruct((slots, rows, width), bf16),
            jax.ShapeDtypeStruct((3, slots, fsdp_count, own, columns), bf16),
            jax.ShapeDtypeStruct((fsdp_count, own, width), bf16),
            jax.ShapeDtypeStruct((4, slots, rows, columns), bf16),
            jax.ShapeDtypeStruct((2, tokens, columns), f32),
        )
        + (jax.ShapeDtypeStruct((slots, fsdp_count, own, units), bf16),) * 3,
        in_specs=[whole_spec()] * 6 + [far_spec()] * 6 + [whole_spec()],
        out_specs=(whole_spec(),) * 4 + (far_spec(),) * 8,
        scratch_shapes=[
            pltpu.VMEM((fsdp_count, own, width), bf16),
            pltpu.VMEM((slots, fsdp_count, 16, lanes), bf16),
            pltpu.VMEM((4, slots, rows, columns), bf16),
            pltpu.VMEM((2, tokens, columns), f32),
            dma((slots,)),
            dma((slots,)),
            dma((slots, fsdp_count)),
            dma((slots, fsdp_count)),
            dma((fsdp_count,)),
            dma((fsdp_count,)),
            dma((6,)),
            dma((8,)),
        ]
        + Gather.scratch(chips, rows, width)
        + RowSum.scratch(slots, (8, tokens))
        + Spread.scratch(3, 3, slots, fsdp_count, own, columns)
        + Spread.scratch(3, 1, slots, fsdp_count, own, units)
        + Scatter.scratch(chips, rows, width),
        compiler_params=line_params(3),
        name="bring_in",
    )(
        local_in,
        padded,
        *tables,
        segment_row.reshape(tokens, 1),
        segment_row.reshape(1, tokens),
        *attention_rows,
        *unit_rows,
        output_weight,
    )
    projected, inverse, own_gains, every_gain = found[:4]
    inputs_all, weights, outputs, heads, pre = found[4:9]
    every_gain = every_gain[:, :, : gains.shape[0], : gains.shape[1]]
    return (
        projected,
        inputs_all.reshape(-1, width),
        weights.reshape(3, -1, columns),
        outputs.reshape(-1, width),
        [columns_of.reshape(-1, units) for columns_of in found[9:]],
        heads.reshape(4, tokens, columns),
        pre,
        inverse,
        own_gains,
        every_gain.transpose(2, 0, 1, 3).reshape(gains.shape[0], -1),
    )


def gather_back_kernel(chips, fsdp_count, *refs):
    local_ref, output_ref, gains_ref, inverse_ref, cosine_ref, sine_ref = refs[:6]
    segment_column, segment_row = refs[6:8]
    hidden_hbm, gate_hbm, up_hbm, heads_hbm, pre_hbm = refs[8:13]
    refs = refs[13:]
    results, output_term, grads_out, gain_out = refs[:2], refs[2], refs[3], refs[4]
    refs = refs[5:]
    tokens, units, heads, pre, gathered, grad_query, grad_key, grad_value = refs[:8]
    load_sem, refs = refs[8], refs[9:]
    line = Line(chips)
    cross = Cross(2 * chips, fsdp_count)
    gather = Gather(line, *refs[:5])
    sums = RowSum(cross, *refs[5:9])
    all_tokens, width = tokens.shape
    block_units = units.shape[-1]
    columns = output_ref.shape[0]
    blocks = gather.blocks
    rows = blocks.shape[1]

    def fill(kind, owner, slot):
        span = width // cross.seq_count
        chosen = tokens[:, pl.ds(pl.multiple_of(owner * span, 128), span)]

        @pl.loop(0, block_units // tile_of(block_units))
        def _(tile):
            part = pl.ds(pl.multiple_of(tile * tile_of(block_units), 128), tile_of(block_units))
            term = dot_rows(chosen, units[kind, :, part]).astype(jnp.bfloat16)
            collect.terms[slot, :, :, part] = term.reshape(fsdp_count, -1, term.shape[1])

    collect = Collect(cross, 2, fill, *refs[9:])
    copies = load(
        [
            (hidden_hbm, tokens, load_sem.at[0]),
            (gate_hbm, units.at[0], load_sem.at[1]),
            (up_hbm, units.at[1], load_sem.at[2]),
            (heads_hbm, heads, load_sem.at[3]),
            (pre_hbm, pre, load_sem.at[4]),
        ]
    )
    greet_cross(cross.seq_count, fsdp_count)
    blocks[line.place * 2 + line.core] = local_ref[...]
    gather.send(line.place)
    grad_key[...] = jnp.zeros_like(grad_key)
    grad_value[...] = jnp.zeros_like(grad_value)
    for copy in copies[:2]:
        copy.wait()
    collect.begin()
    for copy in copies[2:]:
        copy.wait()

    def arrive(step):
        chip = gather.step(step)
        whole = blocks[pl.ds(chip * 2, 2)].reshape(2 * rows, width)
        found = dot_cols(whole, output_ref[...]).astype(jnp.bfloat16)
        gathered[pl.ds(chip * 2 * rows, 2 * rows), :] = found

    arrive(0)
    def attend(slot):
        first = pl.multiple_of(slot * rows, rows)
        span = pl.ds(first, rows)
        for head in range(0, columns, DH):
            part = pl.ds(head, DH)
            queries, keys, values = heads[0, span, part], heads[1, :, part], heads[2, :, part]
            outer = gathered[span, part]
            probs = attention_weights(
                queries, keys, first, segment_column[span, :], segment_row[...]
            )
            grad_value[:, part] += dot_rows(probs.astype(jnp.bfloat16), outer)
            grad_probs = dot_cols(outer, values)
            delta = jnp.sum(probs * grad_probs, axis=-1, keepdims=True)
            grad_scores = (probs * (grad_probs - delta)).astype(jnp.bfloat16)
            grad_query[span, part] = jnp.dot(
                grad_scores, keys, preferred_element_type=jnp.float32
            )
            grad_key[:, part] += dot_rows(grad_scores, queries)

    def errors(kind, grad):
        scaled = (grad[...] * DH ** (-0.5)).astype(jnp.bfloat16).astype(jnp.float32)
        error = turn_heads(scaled, cosine_ref[...], -sine_ref[...])
        inverse = inverse_ref[:, kind : kind + 1]
        return error, pre[kind] * inverse, inverse

    def send_means():
        total = None
        for kind, grad in enumerate((grad_query, grad_key)):
            error, unit, _ = errors(kind, grad)
            product = error * unit
            gain_out[kind : kind + 1, :] = jnp.sum(product, axis=0, keepdims=True)
            row = lax.dot_general(
                pick_row(kind, (8, columns)),
                product * gains_ref[kind : kind + 1, :],
                (((1,), (1,)), ((), ())),
                precision=EXACT,
                preferred_element_type=jnp.float32,
            )
            total = row if total is None else total + row
        sums.send(total)
        grads_out[2] = grad_value[...].astype(jnp.bfloat16)

        @pl.loop(0, width // tile_of(width))
        def _(tile):
            part = pl.ds(pl.multiple_of(tile * tile_of(width), 128), tile_of(width))
            outer = blocks[:, :, part].reshape(all_tokens, -1)
            output_term[:, part] = dot_rows(heads[3], outer).astype(jnp.bfloat16)

    def finish_grads():
        means = sums.receive() / width
        for kind, grad in enumerate((grad_query, grad_key)):
            error, unit, inverse = errors(kind, grad)
            mean = dot_rows(means, pick_row(kind, (8, 128)), EXACT)[:, :1]
            grads_out[kind] = (
                inverse * (error * gains_ref[kind : kind + 1, :] - unit * mean)
            ).astype(jnp.bfloat16)

    attended = 3 * chips - 1

    @pl.loop(0, max(collect.beats, attended + 4))
    def _(turn):
        collect.beat(turn)

        @pl.when((turn % 3 < 2) & (turn // 3 < chips))
        def _():
            attend(line.order(turn // 3) * 2 + turn % 3)

        @pl.when((turn % 3 == 2) & (turn // 3 + 1 < chips))
        def _():
            arrive(turn // 3 + 1)

        @pl.when(turn == attended)
        def _():
            send_means()

        @pl.when(turn == attended + 3)
        def _():
            finish_grads()

    @pl.loop(0, cross.seq_count)
    def _(turn):
        for kind in range(2):

            def put(_, sender, value):
                part = pl.ds(pl.multiple_of(sender * block_units, 128), block_units)
                results[kind][:, part] = value

            collect.receive(kind * cross.seq_count + turn, put)

    collect.finish()
    gather.finish()
    sums.finish()


def gather_back(local, output_rows, gains, inverse, tables, segment_row, far, heads, pre):
    rows, width = local.shape
    slots = lax.axis_size("seq")
    fsdp_count = lax.axis_size("fsdp")
    chips = slots // 2
    own = width // (slots * fsdp_count)
    units = far[1].shape[1]
    _, tokens, columns = heads.shape
    bf16, f32 = jnp.bfloat16, jnp.float32
    found = pl.pallas_call(
        functools.partial(gather_back_kernel, chips, fsdp_count),
        out_shape=(jax.ShapeDtypeStruct((own, units * slots), bf16),) * 2
        + (
            jax.ShapeDtypeStruct((columns, width), bf16),
            jax.ShapeDtypeStruct((3, tokens, columns), bf16),
            jax.ShapeDtypeStruct((8, columns), f32),
        ),
        in_specs=[whole_spec()] * 8 + [far_spec()] * 5,
        out_specs=(whole_spec(),) * 5,
        scratch_shapes=[
            pltpu.VMEM((tokens, width), bf16),
            pltpu.VMEM((2, tokens, units), bf16),
            pltpu.VMEM((4, tokens, columns), bf16),
            pltpu.VMEM((2, tokens, columns), f32),
            pltpu.VMEM((tokens, columns), bf16),
            pltpu.VMEM((tokens, columns), f32),
            pltpu.VMEM((tokens, columns), f32),
            pltpu.VMEM((tokens, columns), f32),
            pltpu.SemaphoreType.DMA((5,)),
        ]
        + Gather.scratch(chips, rows, width)
        + RowSum.scratch(slots, (8, tokens))
        + Collect.scratch(2, slots, fsdp_count, own, units),
        compiler_params=line_params(6),
        name="gather_back",
    )(
        local,
        output_rows,
        gains,
        inverse,
        *tables,
        segment_row.reshape(tokens, 1),
        segment_row.reshape(1, tokens),
        *far,
        heads,
        pre,
    )
    return found[:2], found[2], found[3], found[4]


def take_out_kernel(
    chips,
    fsdp_count,
    *refs,
):
    grads_ref, rights, tokens_ref = refs[0], refs[1], refs[2]
    output_ref, gains_ref, refs = refs[3], refs[4], refs[5:]
    result, weight_outs, output_out, gains_out, refs = refs[0], refs[1:4], refs[4], refs[5], refs[6:]
    output_in, gain_in, gain_out, gain_rows, refs = refs[0], refs[1], refs[2], refs[3], refs[4:]
    output_send, output_recv, gain_send, gain_recv, gain_row_send, gain_row_recv = refs[:6]
    comm = refs[6:]
    line = Line(chips)
    cross = Cross(2 * chips, fsdp_count)
    seq_count, seq, fsdp = cross.seq_count, cross.seq, cross.fsdp
    scatter = Scatter(line, *comm[:-12])
    columns = rights.shape[-1]
    rows, width = scatter.fresh.shape[1:]

    def fill(kind, owner, slot):
        span = width // seq_count
        part = pl.ds(pl.multiple_of(owner * span, 128), span)
        chosen = tokens_ref[:, part]
        for kind in range(3):
            term = dot_rows(chosen, grads_ref[kind].reshape(-1, columns)).astype(jnp.bfloat16)
            collect.terms[slot, :, :, kind * columns : (kind + 1) * columns] = term.reshape(
                fsdp_count, -1, columns
            )

    collect = Collect(cross, 1, fill, *comm[-12:])

    def output_copy(step):
        peer = cross.fsdp_peer(step)
        return cross.remote(
            output_ref.at[peer],
            output_in.at[step],
            output_send.at[step],
            output_recv.at[step],
            seq,
            peer,
        )

    def gain_copy(step):
        peer = cross.fsdp_peer(step)
        return cross.remote(
            gains_ref.at[peer], gain_in.at[step], gain_send.at[step], gain_recv.at[step], seq, peer
        )

    def gain_row(step):
        peer = cross.seq_peer(step)
        return cross.remote(
            gain_out.at[peer],
            gain_rows.at[step],
            gain_row_send.at[step],
            gain_row_recv.at[step],
            peer,
            fsdp,
        )

    greet_cross(seq_count, fsdp_count)
    for step in range(1, fsdp_count):
        gain_copy(step).start()

    collect.begin()

    @pl.loop(0, chips)
    def _(step):
        product_terms(
            scatter,
            [(grads_ref.at[kind], rights.at[kind], True) for kind in range(3)],
            line.order(chips - 1 - step),
        )

    total = gains_ref[fsdp]
    for step in range(1, fsdp_count):
        gain_copy(step).wait_recv()
        total = total + gain_in[step]
    gain_out[...] = total
    for step in range(1, seq_count):
        gain_row(step).start()

    @pl.loop(0, collect.beats)
    def _(turn):
        collect.beat(turn)

        @pl.when(turn == seq_count - AHEAD)
        def _():
            for step in range(1, fsdp_count):
                output_copy(step).start()

        @pl.when((turn >= HOPPING) & (turn < HOPPING + chips))
        def _():
            scatter.hop(chips - 1 - (turn - HOPPING))

    total = output_ref[fsdp].astype(jnp.float32)
    for step in range(1, fsdp_count):
        output_copy(step).wait_recv()
        total = total + output_in[step].astype(jnp.float32)
    output_out[...] = total
    scatter.settle(result)
    total = gain_out[seq]
    for step in range(1, seq_count):
        gain_row(step).wait_recv()
        total = total + gain_rows[step]
    gains_out[...] = total

    def put(_, sender, value):
        block = pl.ds(pl.multiple_of(sender * columns, 128), columns)
        for kind in range(3):
            weight_outs[kind][:, block] = value[:, kind * columns : (kind + 1) * columns]

    @pl.loop(0, seq_count)
    def _(turn):
        collect.receive(turn, put)

    scatter.finish()
    collect.finish()

    @pl.loop(1, seq_count)
    def _(step):
        gain_row(step).wait_send()

    for step in range(1, fsdp_count):
        output_copy(step).wait_send()
        gain_copy(step).wait_send()


def take_out(grads, weights, tokens, output_term, gain_terms):
    slots = lax.axis_size("seq")
    fsdp_count = lax.axis_size("fsdp")
    chips = slots // 2
    _, width, columns = weights.shape
    rows = tokens.shape[0] // slots
    own = width // (slots * fsdp_count)
    kinds = gain_terms.shape[0]
    bf16, f32, dma = jnp.bfloat16, jnp.float32, pltpu.SemaphoreType.DMA
    gains = gain_terms.reshape(kinds, slots, fsdp_count, own).transpose(2, 1, 0, 3)
    lanes = pl.cdiv(own, 128) * 128
    gains = jnp.pad(gains, ((0, 0), (0, 0), (0, 8 - kinds), (0, lanes - own)))
    result, query, key, value, output, gains = pl.pallas_call(
        functools.partial(take_out_kernel, chips, fsdp_count),
        out_shape=(jax.ShapeDtypeStruct((rows, width), f32),)
        + (jax.ShapeDtypeStruct((own, columns * slots), bf16),) * 3
        + (jax.ShapeDtypeStruct((own, width), f32), jax.ShapeDtypeStruct((8, lanes), f32)),
        in_specs=[whole_spec()] * 5,
        out_specs=(whole_spec(),) * 6,
        scratch_shapes=[
            pltpu.VMEM((fsdp_count, own, width), bf16),
            pltpu.VMEM((fsdp_count, slots, 8, lanes), f32),
            pltpu.VMEM((slots, 8, lanes), f32),
            pltpu.VMEM((slots, 8, lanes), f32),
            dma((fsdp_count,)),
            dma((fsdp_count,)),
            dma((fsdp_count,)),
            dma((fsdp_count,)),
            dma((slots,)),
            dma((slots,)),
        ]
        + Scatter.scratch(chips, rows, width)
        + Collect.scratch(1, slots, fsdp_count, own, 3 * columns),
        compiler_params=line_params(4),
        name="take_out",
    )(
        grads.reshape(3, slots, rows, columns),
        weights,
        tokens,
        output_term.reshape(fsdp_count, own, width),
        gains,
    )
    return result, (query, key, value), output, gains[:kinds, :own]


def feed_forward_kernel(
    chips,
    hidden_ref,
    gate_hbm,
    up_hbm,
    down_hbm,
    stream_ref,
    cotangent_ref,
    gain_ref,
    result_ref,
    grad_ref,
    gain_grad_ref,
    gate_out,
    up_out,
    act_out,
    all_out,
    gate_w,
    up_w,
    down_w,
    gate_keep,
    up_keep,
    act_keep,
    load_sem,
    store_sem,
    mixed_ref,
    *comm,
):
    line = Line(chips)
    gather = Gather(line, *comm[:5])
    scatter = Scatter(line, *comm[5:])
    blocks, fresh = gather.blocks, scatter.fresh
    _, rows, width = blocks.shape
    units = gate_w.shape[1]
    copies = load(
        [
            (gate_hbm, gate_w, load_sem.at[0]),
            (up_hbm, up_w, load_sem.at[1]),
            (down_hbm, down_w, load_sem.at[2]),
        ]
    )
    line.greet()
    blocks[line.place * 2 + line.core] = hidden_ref[...]
    gather.send(line.place)

    def stores(chip):
        pair = pl.ds(chip * 2, 2)
        return [
            pltpu.make_async_copy(gate_keep.at[pair], gate_out.at[pair], store_sem.at[0, chip]),
            pltpu.make_async_copy(up_keep.at[pair], up_out.at[pair], store_sem.at[1, chip]),
            pltpu.make_async_copy(act_keep.at[pair], act_out.at[pair], store_sem.at[2, chip]),
            pltpu.make_async_copy(blocks.at[pair], all_out.at[pair], store_sem.at[3, chip]),
        ]

    for copy in copies:
        copy.wait()

    @pl.loop(0, chips)
    def _(step):
        chip = gather.step(step)
        pair = pl.ds(chip * 2, 2)

        @pl.loop(0, units // tile_of(units))
        def _(tile):
            columns = pl.ds(pl.multiple_of(tile * tile_of(units), 128), tile_of(units))
            tokens = blocks[pair].reshape(2 * rows, width)
            gate = jnp.dot(tokens, gate_w[:, columns], preferred_element_type=jnp.float32)
            up = jnp.dot(tokens, up_w[:, columns], preferred_element_type=jnp.float32)
            gate_keep[pair, :, columns] = gate.reshape(2, rows, -1)
            up_keep[pair, :, columns] = up.reshape(2, rows, -1)
            act_keep[pair, :, columns] = (
                (gate / (1.0 + jnp.exp(-gate)) * up).astype(jnp.bfloat16).reshape(2, rows, -1)
            )

        @pl.loop(0, width // tile_of(width))
        def _(tile):
            columns = pl.ds(pl.multiple_of(tile * tile_of(width), 128), tile_of(width))
            act = act_keep[pair].reshape(2 * rows, units)
            fresh[:, :, columns] = dot_cols(act, down_w[columns, :]).reshape(2, rows, -1)

        for copy in stores(chip):
            copy.start()
        scatter.after_term(chip)

    scatter.hops()
    scatter.settle(mixed_ref)
    gain_grad_ref[...] = jnp.zeros_like(gain_grad_ref)
    part_rows = min(32, rows)

    @pl.loop(0, rows // part_rows)
    def _(part):
        span = pl.ds(pl.multiple_of(part * part_rows, part_rows), part_rows)
        mixed, outer, gain = mixed_ref[span], cotangent_ref[span].astype(jnp.float32), gain_ref[0:1]
        inverse = lax.rsqrt(jnp.mean(mixed * mixed, axis=-1, keepdims=True) + eps_norm)
        unit = mixed * inverse
        result_ref[span] = (stream_ref[span] + unit * gain).astype(jnp.bfloat16)
        gain_grad_ref[0:1] += jnp.sum(outer * unit, axis=0, keepdims=True)
        outer = outer * gain
        mean = jnp.mean(outer * unit, axis=-1, keepdims=True)
        grad_ref[span] = (inverse * (outer - unit * mean)).astype(jnp.bfloat16)

    scatter.finish()
    gather.finish()

    @pl.loop(0, chips)
    def _(chip):
        for copy in stores(chip):
            copy.wait()


def feed_forward(hidden_low, gate_cols, up_cols, down_cols, stream, cotangent, gain):
    rows, width = hidden_low.shape
    units = gate_cols.shape[1]
    slots = lax.axis_size("seq")
    chips = slots // 2
    weights = [pltpu.VMEM((width, units), jnp.bfloat16)] * 3
    result, grad, gain_grad, gate, up, act, every = pl.pallas_call(
        functools.partial(feed_forward_kernel, chips),
        out_shape=(
            jax.ShapeDtypeStruct((rows, width), jnp.bfloat16),
            jax.ShapeDtypeStruct((rows, width), jnp.bfloat16),
            jax.ShapeDtypeStruct((8, width), jnp.float32),
            jax.ShapeDtypeStruct((slots, rows, units), jnp.float32),
            jax.ShapeDtypeStruct((slots, rows, units), jnp.float32),
            jax.ShapeDtypeStruct((slots, rows, units), jnp.bfloat16),
            jax.ShapeDtypeStruct((slots, rows, width), jnp.bfloat16),
        ),
        in_specs=[whole_spec()] + [far_spec()] * 3 + [whole_spec()] * 3,
        out_specs=(whole_spec(),) * 3 + (far_spec(),) * 4,
        scratch_shapes=weights
        + [
            pltpu.VMEM((slots, rows, units), jnp.float32),
            pltpu.VMEM((slots, rows, units), jnp.float32),
            pltpu.VMEM((slots, rows, units), jnp.bfloat16),
            pltpu.SemaphoreType.DMA((3,)),
            pltpu.SemaphoreType.DMA((4, chips)),
            pltpu.VMEM((rows, width), jnp.float32),
        ]
        + Gather.scratch(chips, rows, width)
        + Scatter.scratch(chips, rows, width),
        compiler_params=line_params(1),
        name="feed_forward",
    )(hidden_low, gate_cols, up_cols, down_cols, stream, cotangent, gain.reshape(1, width))
    return (
        result,
        grad,
        gain_grad[0],
        gate,
        up,
        act.reshape(-1, units),
        every.reshape(-1, width),
    )


def feed_forward_back_kernel(chips, fsdp_count, *refs):
    grad_ref, gate_hbm, up_hbm, down_hbm, gate_lin_hbm, up_lin_hbm, act_hbm = refs[:7]
    hidden_grad_ref, gate_out, up_out, down_grad, refs = *refs[7:11], refs[11:]
    gate_w, up_w, down_w, gate_lin, up_lin, gate_keep, up_keep, act, refs = *refs[:8], refs[8:]
    load_sem, store_sem, refs = refs[0], refs[1], refs[2:]
    line = Line(chips)
    cross = Cross(2 * chips, fsdp_count)
    gather = Gather(line, *refs[:5])
    scatter = Scatter(line, *refs[5:15])
    blocks, fresh = gather.blocks, scatter.fresh
    _, rows, width = blocks.shape
    units = gate_w.shape[1]
    all_tokens = cross.seq_count * rows

    def fill(kind, owner, slot):
        span = width // cross.seq_count
        part = pl.ds(pl.multiple_of(owner * span, 128), span)
        chosen = blocks[:, :, part].reshape(all_tokens, span)

        @pl.loop(0, units // tile_of(units))
        def _(tile):
            columns = pl.ds(pl.multiple_of(tile * tile_of(units), 128), tile_of(units))
            term = dot_rows(chosen, act[:, columns]).astype(jnp.bfloat16)
            collect.terms[slot, :, :, columns] = term.reshape(fsdp_count, -1, term.shape[1])

    collect = Collect(cross, 1, fill, *refs[15:])
    copies = load(
        [
            (down_hbm, down_w, load_sem.at[0]),
            (gate_lin_hbm, gate_lin, load_sem.at[1]),
            (up_lin_hbm, up_lin, load_sem.at[2]),
            (gate_hbm, gate_w, load_sem.at[3]),
            (up_hbm, up_w, load_sem.at[4]),
            (act_hbm, act, load_sem.at[5]),
        ]
    )
    greet_cross(cross.seq_count, fsdp_count)
    blocks[line.place * 2 + line.core] = grad_ref[...]
    gather.send(line.place)

    def stores(chip):
        pair = pl.ds(chip * 2, 2)
        return [
            pltpu.make_async_copy(gate_keep.at[pair], gate_out.at[pair], store_sem.at[0, chip]),
            pltpu.make_async_copy(up_keep.at[pair], up_out.at[pair], store_sem.at[1, chip]),
        ]

    for copy in copies:
        copy.wait()

    @pl.loop(0, chips)
    def _(step):
        chip = gather.step(step)
        pair = pl.ds(chip * 2, 2)

        @pl.loop(0, units // tile_of(units))
        def _(tile):
            columns = pl.ds(pl.multiple_of(tile * tile_of(units), 128), tile_of(units))
            tokens = blocks[pair].reshape(2 * rows, width)
            grad = jnp.dot(tokens, down_w[:, columns], preferred_element_type=jnp.float32)
            gate = gate_lin[pair, :, columns].reshape(2 * rows, -1)
            up = up_lin[pair, :, columns].reshape(2 * rows, -1)
            sig = 1.0 / (1.0 + jnp.exp(-gate))
            gate_keep[pair, :, columns] = (
                (grad * up * sig * (1.0 + gate * (1.0 - sig)))
                .astype(jnp.bfloat16)
                .reshape(2, rows, -1)
            )
            up_keep[pair, :, columns] = (
                (grad * (gate * sig)).astype(jnp.bfloat16).reshape(2, rows, -1)
            )

        @pl.loop(0, width // tile_of(width))
        def _(tile):
            columns = pl.ds(pl.multiple_of(tile * tile_of(width), 128), tile_of(width))
            gate = gate_keep[pair].reshape(2 * rows, units)
            up = up_keep[pair].reshape(2 * rows, units)
            fresh[:, :, columns] = (
                dot_cols(gate, gate_w[columns, :]) + dot_cols(up, up_w[columns, :])
            ).reshape(2, rows, -1)

        for copy in stores(chip):
            copy.start()
        scatter.after_term(chip)

    collect.begin()

    @pl.loop(0, collect.beats)
    def _(turn):
        collect.beat(turn)

        @pl.when(turn < chips)
        def _():
            scatter.hop(turn)

    scatter.settle(hidden_grad_ref)

    def put(_, sender, value):
        columns = pl.ds(pl.multiple_of(sender * units, 128), units)
        down_grad[:, columns] = value

    @pl.loop(0, cross.seq_count)
    def _(turn):
        collect.receive(turn, put)

    scatter.finish()
    gather.finish()
    collect.finish()

    @pl.loop(0, chips)
    def _(chip):
        for copy in stores(chip):
            copy.wait()


def feed_forward_back(grad_low, gate_cols, up_cols, down_cols, gate, up, act):
    rows, width = grad_low.shape
    units = gate_cols.shape[1]
    slots = lax.axis_size("seq")
    fsdp_count = lax.axis_size("fsdp")
    chips = slots // 2
    own = width // (slots * fsdp_count)
    bf16, f32 = jnp.bfloat16, jnp.float32
    hidden_grad, gate_grad, up_grad, down_grad = pl.pallas_call(
        functools.partial(feed_forward_back_kernel, chips, fsdp_count),
        out_shape=(
            jax.ShapeDtypeStruct((rows, width), f32),
            jax.ShapeDtypeStruct((slots, rows, units), bf16),
            jax.ShapeDtypeStruct((slots, rows, units), bf16),
            jax.ShapeDtypeStruct((own, units * slots), bf16),
        ),
        in_specs=[whole_spec()] + [far_spec()] * 6,
        out_specs=(whole_spec(), far_spec(), far_spec(), whole_spec()),
        scratch_shapes=[pltpu.VMEM((width, units), bf16)] * 3
        + [
            pltpu.VMEM((slots, rows, units), f32),
            pltpu.VMEM((slots, rows, units), f32),
            pltpu.VMEM((slots, rows, units), bf16),
            pltpu.VMEM((slots, rows, units), bf16),
            pltpu.VMEM((slots * rows, units), bf16),
            pltpu.SemaphoreType.DMA((6,)),
            pltpu.SemaphoreType.DMA((2, chips)),
        ]
        + Gather.scratch(chips, rows, width)
        + Scatter.scratch(chips, rows, width)
        + Collect.scratch(1, slots, fsdp_count, own, units),
        compiler_params=line_params(2),
        name="feed_forward_back",
    )(grad_low, gate_cols, up_cols, down_cols, gate, up, act)
    return hidden_grad, gate_grad.reshape(-1, units), up_grad.reshape(-1, units), down_grad


def rope_tables(row_count):
    half_width = DH // 2
    frequency = rope_base ** (-jnp.arange(half_width, dtype=jnp.float32) * 2.0 / DH)
    angles = jnp.arange(row_count, dtype=jnp.int32).astype(jnp.float32)[:, None] * frequency[None, :]
    cosine, sine = jnp.cos(angles), jnp.sin(angles)
    return (
        jnp.concatenate([cosine, cosine], axis=1),
        jnp.concatenate([-sine, sine], axis=1),
    )


def per_device(
    inputs,
    query_weight,
    key_weight,
    value_weight,
    output_weight,
    query_gain,
    key_gain,
    attention_gain,
    gate_weight,
    up_weight,
    down_weight,
    feedforward_gain,
    segments,
    cotangent,
):
    token_count = inputs.shape[1]
    width_all = inputs.shape[2]
    local_in = inputs.reshape(token_count, width_all)
    segment_row = segments[0]
    seq_index = lax.axis_index("seq")
    tables = rope_tables(segment_row.shape[0])
    (
        projected,
        inputs_all,
        attention_cols,
        output_rows,
        unit_cols,
        heads,
        pre,
        inverse,
        own_gains,
        gains,
    ) = bring_in(
        local_in,
        [query_weight, key_weight, value_weight],
        [gate_weight, up_weight, down_weight],
        output_weight,
        jnp.stack([query_gain, key_gain, attention_gain, feedforward_gain]),
        tables,
        segment_row,
    )
    gate_cols, up_cols, down_cols = unit_cols
    head_width = heads.shape[2]
    gains = gains.astype(jnp.float32)
    attention_scale = gains[2]
    feedforward_scale = gains[3]
    hidden = local_in.astype(jnp.float32) + rms_scale(projected, attention_scale)
    hidden_low = hidden.astype(jnp.bfloat16)
    grad_result = cotangent.reshape(token_count, width_all)
    result, grad_mixed_low, grad_feedforward_gain, gate_linear, up_linear, activated, hidden_all = (
        feed_forward(
            hidden_low, gate_cols, up_cols, down_cols, hidden, grad_result, feedforward_scale
        )
    )
    result = result.reshape(1, token_count, width_all)
    hidden_term, grad_gate_low, grad_upward_low, down_weight_grad = feed_forward_back(
        grad_mixed_low, gate_cols, up_cols, down_cols, gate_linear, up_linear, activated
    )
    grad_hidden = grad_result.astype(jnp.float32) + hidden_term
    _, branch_pull = jax.vjp(rms_scale, projected, attention_scale)
    grad_projected, grad_attention_gain = branch_pull(grad_hidden)
    weight_grads, output_term, attention_grads, gain_rows = gather_back(
        grad_projected.astype(jnp.bfloat16),
        output_rows,
        own_gains,
        inverse,
        tables,
        segment_row,
        [hidden_all, grad_gate_low, grad_upward_low],
        heads,
        pre,
    )
    gate_weight_grad, up_weight_grad = weight_grads
    head_gains = lax.dynamic_update_slice_in_dim(
        jnp.zeros((2, width_all), jnp.float32),
        gain_rows[:2],
        seq_index * head_width,
        1,
    )
    gain_terms = jnp.concatenate(
        [head_gains, jnp.stack([grad_attention_gain, grad_feedforward_gain])], axis=0
    )
    input_term, projection_grads, output_weight_grad, gain_grads = take_out(
        attention_grads, attention_cols, inputs_all, output_term, gain_terms
    )
    query_weight_grad, key_weight_grad, value_weight_grad = projection_grads
    grad_input = grad_hidden + input_term
    return (
        result,
        grad_input.reshape(1, token_count, width_all),
        query_weight_grad.astype(jnp.float32),
        key_weight_grad.astype(jnp.float32),
        value_weight_grad.astype(jnp.float32),
        output_weight_grad,
        gain_grads[0],
        gain_grads[1],
        gain_grads[2],
        gate_weight_grad.astype(jnp.float32),
        up_weight_grad.astype(jnp.float32),
        down_weight_grad.astype(jnp.float32),
        gain_grads[3],
    )


def solution(mesh):
    in_specs = (
        P("fsdp", "seq", None),
        P(("seq", "fsdp"), None),
        P(("seq", "fsdp"), None),
        P(("seq", "fsdp"), None),
        P(("seq", "fsdp"), None),
        P(("seq", "fsdp")),
        P(("seq", "fsdp")),
        P(("seq", "fsdp")),
        P(("seq", "fsdp"), None),
        P(("seq", "fsdp"), None),
        P(("seq", "fsdp"), None),
        P(("seq", "fsdp")),
        P("fsdp", None),
        P("fsdp", "seq", None),
    )
    out_specs = (
        P("fsdp", "seq", None),
        P("fsdp", "seq", None),
        P(("seq", "fsdp"), None),
        P(("seq", "fsdp"), None),
        P(("seq", "fsdp"), None),
        P(("seq", "fsdp"), None),
        P(("seq", "fsdp")),
        P(("seq", "fsdp")),
        P(("seq", "fsdp")),
        P(("seq", "fsdp"), None),
        P(("seq", "fsdp"), None),
        P(("seq", "fsdp"), None),
        P(("seq", "fsdp")),
    )
    return jax.shard_map(
        per_device, mesh=mesh, in_specs=in_specs, out_specs=out_specs, check_vma=False
    )
```

```python
import functools

import jax
import jax.numpy as jnp
from jax import lax
from jax.experimental import pallas as pl
from jax.experimental.pallas import tpu as pltpu
from jax.sharding import PartitionSpec as P

DH = 128


eps_norm = 1e-06
rope_base = 500000.0
neg_fill = -1e30


def rms_scale(tensor, gain):
    return tensor * lax.rsqrt(jnp.mean(tensor * tensor, axis=-1, keepdims=True) + eps_norm) * gain


MESH = pl.DeviceIdType.MESH
RS_PARTS = 4


class Line:
    def __init__(self, chips):
        index = lax.axis_index("seq")
        self.chips = chips
        self.fsdp = lax.axis_index("fsdp")
        self.place = index // 2
        self.core = index % 2

    def device(self, place, core):
        return (place * 2 + core, self.fsdp)

    @property
    def partner(self):
        return self.device(self.place, 1 - self.core)

    @property
    def above(self):
        return self.device(jnp.minimum(self.place + 1, self.chips - 1), self.core)

    @property
    def below(self):
        return self.device(jnp.maximum(self.place - 1, 0), self.core)

    @property
    def has_above(self):
        return self.place < self.chips - 1

    @property
    def has_below(self):
        return self.place > 0

    def greet(self):
        barrier = pltpu.get_barrier_semaphore()
        pl.semaphore_signal(barrier, inc=1, device_id=self.partner, device_id_type=MESH)

        @pl.when(self.has_above)
        def _():
            pl.semaphore_signal(barrier, inc=1, device_id=self.above, device_id_type=MESH)

        @pl.when(self.has_below)
        def _():
            pl.semaphore_signal(barrier, inc=1, device_id=self.below, device_id_type=MESH)

        peers = (
            1 + jnp.minimum(self.place, 1) + jnp.minimum(self.chips - 1 - self.place, 1)
        )
        pl.semaphore_wait(barrier, peers)

    def order(self, step):
        place, last = self.place, self.chips - 1
        near = jnp.minimum(place, last - place)
        both = jnp.where(step % 2 == 1, place - (step + 1) // 2, place + step // 2)
        rest = jnp.where(place <= last - place, step, last - step)
        return jnp.where(step <= 2 * near, both, rest)

    def paired(self, step):
        near = jnp.minimum(self.place, self.chips - 1 - self.place)
        return (step % 2 == 1) & (step <= 2 * near)

    def second_of_pair(self, step):
        near = jnp.minimum(self.place, self.chips - 1 - self.place)
        return (step % 2 == 0) & (step > 0) & (step <= 2 * near)


class Gather:
    def __init__(self, line, blocks, arrive, up_sem, down_sem, side_sem):
        self.line, self.blocks, self.arrive = line, blocks, arrive
        self.up_sem, self.down_sem, self.side_sem = up_sem, down_sem, side_sem

    @staticmethod
    def scratch(chips, rows, width):
        return [
            pltpu.VMEM((2 * chips, rows, width), jnp.bfloat16),
            pltpu.SemaphoreType.DMA((2 * chips,)),
            pltpu.SemaphoreType.DMA((chips,)),
            pltpu.SemaphoreType.DMA((chips,)),
            pltpu.SemaphoreType.DMA((chips,)),
        ]

    def copy(self, chip, sem, target):
        slot = chip * 2 + self.line.core
        return pltpu.make_async_remote_copy(
            src_ref=self.blocks.at[slot],
            dst_ref=self.blocks.at[slot],
            send_sem=sem.at[chip],
            recv_sem=self.arrive.at[slot],
            device_id=target,
            device_id_type=MESH,
        )

    def wait_slot(self, slot):
        pltpu.make_async_remote_copy(
            src_ref=self.blocks.at[slot],
            dst_ref=self.blocks.at[slot],
            send_sem=self.side_sem.at[0],
            recv_sem=self.arrive.at[slot],
            device_id=self.line.partner,
            device_id_type=MESH,
        ).wait_recv()

    def send(self, chip):
        line = self.line

        @pl.when((chip <= line.place) & line.has_above)
        def _():
            self.copy(chip, self.up_sem, line.above).start()

        @pl.when((chip >= line.place) & line.has_below)
        def _():
            self.copy(chip, self.down_sem, line.below).start()

        self.copy(chip, self.side_sem, line.partner).start()

    def take(self, chip):
        self.wait_slot(chip * 2 + self.line.core)
        self.send(chip)

    def step(self, step):
        line = self.line
        chip = line.order(step)

        @pl.when((step > 0) & jnp.logical_not(line.second_of_pair(step)))
        def _():
            self.take(chip)

        @pl.when(line.paired(step))
        def _():
            self.take(line.order(step + 1))

        self.wait_slot(chip * 2 + 1 - line.core)
        return chip

    def finish(self):
        line = self.line

        @pl.loop(0, line.chips)
        def _(chip):
            @pl.when((chip <= line.place) & line.has_above)
            def _():
                self.copy(chip, self.up_sem, line.above).wait_send()

            @pl.when((chip >= line.place) & line.has_below)
            def _():
                self.copy(chip, self.down_sem, line.below).wait_send()

            self.copy(chip, self.side_sem, line.partner).wait_send()


class Scatter:
    def __init__(self, line, fresh, terms, side_out, side_in, out, inward, side_send, side_recv, send_sem, recv_sem):
        self.line, self.fresh, self.terms = line, fresh, terms
        self.side_out, self.side_in = side_out, side_in
        self.out, self.inward = out, inward
        self.side_send, self.side_recv = side_send, side_recv
        self.send_sem, self.recv_sem = send_sem, recv_sem
        self.rows = terms.shape[1] // RS_PARTS

    @staticmethod
    def scratch(chips, rows, width):
        return [
            pltpu.VMEM((2, rows, width), jnp.float32),
            pltpu.VMEM((chips, rows, width), jnp.float32),
            pltpu.VMEM((chips, rows, width), jnp.bfloat16),
            pltpu.VMEM((chips, rows, width), jnp.bfloat16),
            pltpu.VMEM((chips, rows, width), jnp.bfloat16),
            pltpu.VMEM((2, chips, rows, width), jnp.bfloat16),
            pltpu.SemaphoreType.DMA((chips,)),
            pltpu.SemaphoreType.DMA((chips,)),
            pltpu.SemaphoreType.DMA((chips, RS_PARTS)),
            pltpu.SemaphoreType.DMA((2, chips, RS_PARTS)),
        ]

    def side(self, chip):
        return pltpu.make_async_remote_copy(
            src_ref=self.side_out.at[chip],
            dst_ref=self.side_in.at[chip],
            send_sem=self.side_send.at[chip],
            recv_sem=self.side_recv.at[chip],
            device_id=self.line.partner,
            device_id_type=MESH,
        )

    def part(self, chip, part, upward, target):
        rows = pl.ds(part * self.rows, self.rows)
        return pltpu.make_async_remote_copy(
            src_ref=self.out.at[chip, rows],
            dst_ref=self.inward.at[upward, chip, rows],
            send_sem=self.send_sem.at[chip, part],
            recv_sem=self.recv_sem.at[upward, chip, part],
            device_id=target,
            device_id_type=MESH,
        )

    def share(self, chip):
        self.side_out[chip] = self.fresh[1 - self.line.core].astype(jnp.bfloat16)
        self.side(chip).start()
        self.terms[chip] = self.fresh[self.line.core]

    def total(self, chip, part, ways):
        rows = pl.ds(part * self.rows, self.rows)
        total = self.terms[chip, rows] + self.side_in[chip, rows].astype(jnp.float32)
        for way in ways:
            total = total + self.inward[way, chip, rows].astype(jnp.float32)
        return rows, total

    def pass_part(self, chip, part, upward, first):
        target = self.line.above if upward else self.line.below
        if not first:
            self.part(chip, part, upward, target).wait_recv()
        rows, total = self.total(chip, part, () if first else (upward,))
        self.out[chip, rows] = total.astype(jnp.bfloat16)
        self.part(chip, part, upward, target).start()

    def hand_on(self, chip, upward, first):
        self.side(chip).wait_recv()

        @pl.loop(0, RS_PARTS)
        def _(part):
            self.pass_part(chip, part, upward, first)

    def after_term(self, chip):
        line = self.line
        self.share(chip)

        @pl.when((chip < line.place) & jnp.logical_not(line.has_above))
        def _():
            self.hand_on(chip, 0, True)

        @pl.when((chip > line.place) & jnp.logical_not(line.has_below))
        def _():
            self.hand_on(chip, 1, True)

    def hop(self, step):
        line = self.line
        lower = line.place * 2 < line.chips
        up_chip, down_chip = step, line.chips - 1 - step
        go_up = (up_chip > line.place) & line.has_below
        go_down = (down_chip < line.place) & line.has_above

        @pl.when(go_up & lower)
        def _():
            self.hand_on(up_chip, 1, False)

        @pl.when(go_down)
        def _():
            self.hand_on(down_chip, 0, False)

        @pl.when(go_up & jnp.logical_not(lower))
        def _():
            self.hand_on(up_chip, 1, False)

    def settle(self, result):
        line = self.line
        place = line.place
        self.side(place).wait_recv()

        @pl.loop(0, RS_PARTS)
        def _(part):
            @pl.when(line.has_above)
            def _():
                self.part(place, part, 0, line.below).wait_recv()

            @pl.when(line.has_below)
            def _():
                self.part(place, part, 1, line.above).wait_recv()

            @pl.when(line.has_above & line.has_below)
            def _():
                rows, total = self.total(place, part, (0, 1))
                result[rows] = total

            @pl.when(line.has_above & jnp.logical_not(line.has_below))
            def _():
                rows, total = self.total(place, part, (0,))
                result[rows] = total

            @pl.when(line.has_below & jnp.logical_not(line.has_above))
            def _():
                rows, total = self.total(place, part, (1,))
                result[rows] = total

    def hops(self):
        @pl.loop(0, self.line.chips)
        def _(step):
            self.hop(step)

    def finish(self):
        line = self.line

        @pl.loop(0, line.chips)
        def _(chip):
            self.side(chip).wait_send()

            @pl.when(chip != line.place)
            def _():
                @pl.loop(0, RS_PARTS)
                def _(part):
                    self.part(chip, part, 0, line.below).wait_send()


def tile_of(extent):
    return min(256, extent)


def dot_cols(left, right):
    return lax.dot_general(
        left, right, (((1,), (1,)), ((), ())), preferred_element_type=jnp.float32
    )


def load(pairs):
    copies = [pltpu.make_async_copy(src, dst, sem) for src, dst, sem in pairs]
    for copy in copies:
        copy.start()
    return copies


def whole_spec():
    return pl.BlockSpec(memory_space=pltpu.VMEM)


def far_spec():
    return pl.BlockSpec(memory_space=pl.ANY)


def line_params(collective_id):
    return pltpu.CompilerParams(
        collective_id=collective_id, has_side_effects=True, vmem_limit_bytes=67_043_328
    )


def peers_of(axis, size):
    me = lax.axis_index(axis)
    return me, lambda step: (me + step) % size


def greet_cross(seq_count, fsdp_count):
    seq, seq_peer = peers_of("seq", seq_count)
    fsdp, fsdp_peer = peers_of("fsdp", fsdp_count)
    barrier = pltpu.get_barrier_semaphore()
    for step in range(1, seq_count):
        pl.semaphore_signal(
            barrier, inc=1, device_id=(seq_peer(step), fsdp), device_id_type=MESH
        )
    for step in range(1, fsdp_count):
        pl.semaphore_signal(
            barrier, inc=1, device_id=(seq, fsdp_peer(step)), device_id_type=MESH
        )
    pl.semaphore_wait(barrier, seq_count + fsdp_count - 2)


class Cross:
    def __init__(self, seq_count, fsdp_count):
        self.seq_count, self.fsdp_count = seq_count, fsdp_count
        self.seq, self.seq_peer = peers_of("seq", seq_count)
        self.fsdp, self.fsdp_peer = peers_of("fsdp", fsdp_count)
        self.square = fsdp_count == 4
        if self.square:
            row, place = self.fsdp // 2, self.fsdp % 2
            self.sides = (row * 2 + 1 - place, (1 - row) * 2 + place)
            self.corner = (1 - row) * 2 + 1 - place
        else:
            self.sides = tuple(self.fsdp_peer(step) for step in range(1, fsdp_count))

    def remote(self, src, dst, send, recv, seq, fsdp):
        return pltpu.make_async_remote_copy(
            src_ref=src,
            dst_ref=dst,
            send_sem=send,
            recv_sem=recv,
            device_id=(seq, fsdp),
            device_id_type=MESH,
        )


class Spread:
    def __init__(self, cross, group, stack, weights, row_send, row_recv, side_send, side_recv, half_send, half_recv):
        self.cross, self.group, self.stack, self.weights = cross, group, stack, weights
        self.row_send, self.row_recv = row_send, row_recv
        self.side_send, self.side_recv = side_send, side_recv
        self.half_send, self.half_recv = half_send, half_recv
        self.columns, self.rows = weights.shape[-1], weights.shape[-2]
        self.items = weights.shape[0] // group * cross.seq_count

    @staticmethod
    def scratch(kinds, group, seq_count, fsdp_count, rows, columns):
        dma = pltpu.SemaphoreType.DMA
        sides = 2 if fsdp_count == 4 else fsdp_count - 1
        items = kinds // group * seq_count
        return [
            pltpu.VMEM((kinds, rows, seq_count * columns), jnp.bfloat16),
            pltpu.VMEM((kinds, seq_count, fsdp_count, rows, columns), jnp.bfloat16),
            dma((kinds, seq_count)),
            dma((kinds, seq_count)),
            dma((items, sides)),
            dma((items, sides)),
            dma((items, 2)),
            dma((items, 2)),
        ]

    def block(self, owner):
        return pl.ds(pl.multiple_of(owner * self.columns, 128), self.columns)

    def row(self, kind, step):
        cross = self.cross
        peer = cross.seq_peer(step)
        return cross.remote(
            self.stack.at[kind, :, self.block(peer)],
            self.weights.at[kind, cross.seq, cross.fsdp],
            self.row_send.at[kind, step],
            self.row_recv.at[kind, step],
            peer,
            cross.fsdp,
        )

    def place(self, item):
        count = self.cross.seq_count
        step = item % count
        return item // count * self.group, step, (self.cross.seq - step + count) % count

    def side(self, item, side):
        cross = self.cross
        first, _, owner = self.place(item)
        ref = self.weights.at[pl.ds(first, self.group), owner, cross.fsdp]
        return cross.remote(
            ref,
            ref,
            self.side_send.at[item, side],
            self.side_recv.at[item, side],
            cross.seq,
            cross.sides[side],
        )

    def half(self, item, side):
        cross = self.cross
        first, _, owner = self.place(item)
        rows = pl.ds(side * (self.rows // 2), self.rows // 2)
        ref = self.weights.at[pl.ds(first, self.group), owner, cross.sides[side], rows]
        return cross.remote(
            ref,
            ref,
            self.half_send.at[item, side],
            self.half_recv.at[item, side],
            cross.seq,
            cross.sides[1 - side],
        )

    def send_rows(self, item):
        first, step, _ = self.place(item)

        @pl.when(step > 0)
        def _():
            for kind in range(self.group):
                self.row(first + kind, step).start()

    def take(self, item):
        cross = self.cross
        first, step, _ = self.place(item)

        @pl.when(step > 0)
        def _():
            for kind in range(self.group):
                self.row(first + kind, step).wait_recv()

        @pl.when(step == 0)
        def _():
            for kind in range(self.group):
                own = self.stack[first + kind, :, self.block(cross.seq)]
                self.weights[first + kind, cross.seq, cross.fsdp] = own

        self.pass_on(item)

    def pass_on(self, item):
        for side in range(len(self.cross.sides)):
            self.side(item, side).start()

    def relay(self, item):
        for side in range(len(self.cross.sides)):
            self.side(item, side).wait_recv()
            if self.cross.square:
                self.half(item, side).start()

    def settle(self, item):
        if self.cross.square:
            for side in range(2):
                self.half(item, side).wait_recv()

    def finish(self):
        cross = self.cross

        @pl.loop(0, self.items)
        def _(item):
            first, step, _ = self.place(item)

            @pl.when(step > 0)
            def _():
                for kind in range(self.group):
                    self.row(first + kind, step).wait_send()

            self.finish_item(item)

    def finish_item(self, item):
        for side in range(len(self.cross.sides)):
            self.side(item, side).wait_send()
            if self.cross.square:
                self.half(item, side).wait_send()


AHEAD = 2
LAG = 3
RING = 8


class Collect:
    def __init__(self, cross, kinds, fill, terms, side_in, half_out, half_in, row_out, row_in, side_send, side_recv, half_send, half_recv, row_send, row_recv):
        self.cross, self.fill, self.terms = cross, fill, terms
        self.side_in, self.half_out, self.half_in = side_in, half_out, half_in
        self.row_out, self.row_in = row_out, row_in
        self.side_send, self.side_recv = side_send, side_recv
        self.half_send, self.half_recv = half_send, half_recv
        self.row_send, self.row_recv = row_send, row_recv
        self.rows, self.columns = terms.shape[-2:]
        self.items = kinds * cross.seq_count

    @staticmethod
    def scratch(kinds, seq_count, fsdp_count, rows, columns):
        dma = pltpu.SemaphoreType.DMA
        vmem = pltpu.VMEM
        bf16 = jnp.bfloat16
        items = kinds * seq_count
        if fsdp_count == 4:
            arrays = [
                vmem((items, 2, 2, rows // 2, columns), bf16),
                vmem((RING, 2, rows // 2, columns), bf16),
                vmem((items, 2, rows // 2, columns), bf16),
            ]
            sides = (2, 2)
        else:
            arrays = [
                vmem((items, fsdp_count - 1, rows, columns), bf16),
                vmem((1, 1, 16, 128), bf16),
                vmem((1, 1, 16, 128), bf16),
            ]
            sides = (fsdp_count - 1, 1)
        return [vmem((RING, fsdp_count, rows, columns), bf16)] + arrays + [
            vmem((RING, rows, columns), bf16),
            vmem((items, rows, columns), bf16),
            dma((items,) + sides),
            dma((items,) + sides),
            dma((items, 2)),
            dma((items, 2)),
            dma((items,)),
            dma((items,)),
        ]

    def half_rows(self, side):
        return pl.ds(side * (self.rows // 2), self.rows // 2)

    def side(self, turn, side, which):
        cross = self.cross
        if not cross.square:
            return cross.remote(
                self.terms.at[turn % RING, cross.sides[side]],
                self.side_in.at[turn, side],
                self.side_send.at[turn, side, 0],
                self.side_recv.at[turn, side, 0],
                cross.seq,
                cross.sides[side],
            )
        target = cross.sides[side] if which == 0 else cross.corner
        return cross.remote(
            self.terms.at[turn % RING, target, self.half_rows(side)],
            self.side_in.at[turn, side, which],
            self.side_send.at[turn, side, which],
            self.side_recv.at[turn, side, which],
            cross.seq,
            cross.sides[side],
        )

    def half(self, turn, side):
        cross = self.cross
        return cross.remote(
            self.half_out.at[turn % RING, side],
            self.half_in.at[turn, side],
            self.half_send.at[turn, side],
            self.half_recv.at[turn, side],
            cross.seq,
            cross.sides[1 - side],
        )

    def row(self, turn):
        cross = self.cross
        return cross.remote(
            self.row_out.at[turn % RING],
            self.row_in.at[turn],
            self.row_send.at[turn],
            self.row_recv.at[turn],
            self.place(turn)[1],
            cross.fsdp,
        )

    def place(self, turn):
        count = self.cross.seq_count
        return turn // count, self.cross.seq_peer(turn % count + 1)

    def is_own(self, turn):
        return turn % self.cross.seq_count == self.cross.seq_count - 1

    @property
    def ways(self):
        return range(2) if self.cross.square else range(1)

    def sides(self, turn):
        return [
            self.side(turn, side, which)
            for which in reversed(self.ways)
            for side in range(len(self.cross.sides))
        ]

    def send(self, turn, first):
        if not first:

            @pl.when(turn >= RING)
            def _():
                for copy in self.sides(turn - RING):
                    copy.wait_send()

        kind, owner = self.place(turn)
        self.fill(kind, owner, turn % RING)
        for copy in self.sides(turn):
            copy.start()

    def middle(self, turn):
        if not self.cross.square:
            return
        cross = self.cross

        @pl.when(turn >= RING)
        def _():
            for side in range(2):
                self.half(turn - RING, side).wait_send()

        for side in range(2):
            self.side(turn, side, 1).wait_recv()
            mine = self.terms[turn % RING, cross.sides[1 - side], self.half_rows(side)]
            self.half_out[turn % RING, side] = (
                mine.astype(jnp.float32) + self.side_in[turn, side, 1].astype(jnp.float32)
            ).astype(jnp.bfloat16)
            self.half(turn, side).start()

    def totals(self, turn):
        cross = self.cross
        found = []
        if cross.square:
            for side in range(2):
                self.side(turn, side, 0).wait_recv()
                self.half(turn, side).wait_recv()
                rows = self.half_rows(side)
                total = self.terms[turn % RING, cross.fsdp, rows].astype(jnp.float32)
                total = total + self.side_in[turn, side, 0].astype(jnp.float32)
                total = total + self.half_in[turn, side].astype(jnp.float32)
                found.append((rows, total))
        else:
            total = self.terms[turn % RING, cross.fsdp].astype(jnp.float32)
            for side in range(len(cross.sides)):
                self.side(turn, side, 0).wait_recv()
                total = total + self.side_in[turn, side].astype(jnp.float32)
            found.append((pl.ds(0, self.rows), total))
        return found

    def ship(self, turn):
        own = self.is_own(turn)
        self.free_row(turn - RING)

        @pl.when(own)
        def _():
            for rows, total in self.totals(turn):
                self.row_in[turn, rows] = total.astype(jnp.bfloat16)

        @pl.when(jnp.logical_not(own))
        def _():
            for rows, total in self.totals(turn):
                self.row_out[turn % RING, rows] = total.astype(jnp.bfloat16)
            self.row(turn).start()

    def free_row(self, turn):
        @pl.when((turn >= 0) & jnp.logical_not(self.is_own(turn)))
        def _():
            self.row(turn).wait_send()

    def beat(self, turn):
        ahead = turn + AHEAD

        @pl.when(ahead < self.items)
        def _():
            self.send(ahead, False)

        @pl.when(turn < self.items)
        def _():
            self.middle(turn)

        @pl.when((turn >= LAG) & (turn < self.beats))
        def _():
            self.ship(turn - LAG)

    def begin(self):
        @pl.loop(0, min(AHEAD, self.items))
        def _(turn):
            self.send(turn, True)

    @property
    def beats(self):
        return self.items + LAG

    def receive(self, turn, put):
        count = self.cross.seq_count

        @pl.when(jnp.logical_not(self.is_own(turn)))
        def _():
            self.row(turn).wait_recv()

        sender = (self.cross.seq - turn % count - 1 + count) % count
        put(turn // count, sender, self.row_in[turn])

    def finish(self):
        cross = self.cross
        late = max(self.items - RING, 0)

        @pl.loop(late, self.items)
        def _(turn):
            for copy in self.sides(turn):
                copy.wait_send()
            if cross.square:
                for side in range(2):
                    self.half(turn, side).wait_send()
            self.free_row(turn)


def dot_rows(left, right, precision=None):
    return lax.dot_general(
        left,
        right,
        (((0,), (0,)), ((), ())),
        precision=precision,
        preferred_element_type=jnp.float32,
    )


EXACT = lax.Precision.HIGHEST


def turn_heads(tensor, cosine, sine):
    heads = [
        tensor[:, first : first + DH] * cosine
        + pltpu.roll(tensor[:, first : first + DH], DH // 2, 1) * sine
        for first in range(0, tensor.shape[1], DH)
    ]
    return jnp.concatenate(heads, axis=1) if len(heads) > 1 else heads[0]


def attention_weights(queries, keys, first_row, segment_column, segment_row):
    rows, count = queries.shape[0], keys.shape[0]
    scores = dot_cols(queries, keys) * DH ** (-0.5)
    query_place = first_row + lax.broadcasted_iota(jnp.int32, (rows, count), 0)
    key_place = lax.broadcasted_iota(jnp.int32, (rows, count), 1)
    allowed = (key_place <= query_place) & (segment_row == segment_column)
    scores = jnp.where(allowed, scores, neg_fill)
    expanded = jnp.exp(scores - jnp.max(scores, axis=-1, keepdims=True))
    return expanded / jnp.sum(expanded, axis=-1, keepdims=True)


class RowSum:
    def __init__(self, cross, local, every, send_sem, recv_sem):
        self.cross, self.local, self.every = cross, local, every
        self.send_sem, self.recv_sem = send_sem, recv_sem

    @staticmethod
    def scratch(seq_count, shape):
        dma = pltpu.SemaphoreType.DMA
        return [
            pltpu.VMEM(shape, jnp.float32),
            pltpu.VMEM((seq_count,) + shape, jnp.float32),
            dma((seq_count,)),
            dma((seq_count,)),
        ]

    def copy(self, step):
        cross = self.cross
        return cross.remote(
            self.local,
            self.every.at[step],
            self.send_sem.at[step],
            self.recv_sem.at[step],
            cross.seq_peer(step),
            cross.fsdp,
        )

    def send(self, value):
        self.local[...] = value
        for step in range(1, self.cross.seq_count):
            self.copy(step).start()

    def receive(self):
        total = self.local[...]
        for step in range(1, self.cross.seq_count):
            self.copy(step).wait_recv()
            total = total + self.every[step]
        return total

    def finish(self):
        for step in range(1, self.cross.seq_count):
            self.copy(step).wait_send()


def pick_row(row, shape):
    return jnp.where(lax.broadcasted_iota(jnp.int32, shape, 0) == row, 1.0, 0.0)


def product_terms(scatter, pairs, chip):
    _, rows, width = scatter.fresh.shape
    pair = pl.ds(chip * 2, 2)

    @pl.loop(0, width // tile_of(width))
    def _(tile):
        columns = pl.ds(pl.multiple_of(tile * tile_of(width), 128), tile_of(width))
        total = None
        for left, right, across in pairs:
            tokens = left[pair].reshape(2 * rows, -1)
            if across:
                term = dot_cols(tokens, right[columns, :])
            else:
                term = jnp.dot(tokens, right(columns), preferred_element_type=jnp.float32)
            total = term if total is None else total + term
        scatter.fresh[:, :, columns] = total.reshape(2, rows, -1)

    scatter.after_term(chip)


EARLY = 6
LEAD = 2
HOPPING = 1


def bring_in_kernel(chips, fsdp_count, *refs):
    inputs_ref, gains_ref, cosine_ref, sine_ref, segment_column, segment_row = refs[:6]
    sources, output_ref, refs = refs[6:12], refs[12], refs[13:]
    projected, inverse_out, own_gains, gains_out = refs[:4]
    inputs_out, attention_out, output_out, heads_out, pre_out = refs[4:9]
    units_out, outputs, gains, heads, pre, refs = refs[9:12], refs[12], refs[13], refs[14], refs[15], refs[16:]
    gain_row_send, gain_row_recv, gain_column_send, gain_column_recv = refs[:4]
    output_send, output_recv, load_sem, store_sem, refs = refs[4], refs[5], refs[6], refs[7], refs[8:]
    line = Line(chips)
    cross = Cross(2 * chips, fsdp_count)
    gather, refs = Gather(line, *refs[:5]), refs[5:]
    sums, refs = RowSum(cross, *refs[:4]), refs[4:]
    attention, refs = Spread(cross, 3, *refs[:8]), refs[8:]
    units, refs = Spread(cross, 1, *refs[:8]), refs[8:]
    scatter = Scatter(line, *refs)
    seq_count, seq, fsdp = cross.seq_count, cross.seq, cross.fsdp
    blocks = gather.blocks
    _, rows, width = blocks.shape
    columns = attention.columns
    tokens = seq_count * rows

    def gain_row(step):
        return cross.remote(
            gains_ref,
            gains.at[seq, fsdp],
            gain_row_send.at[step],
            gain_row_recv.at[step],
            cross.seq_peer(step),
            fsdp,
        )

    def gain_column(owner, step):
        ref = gains.at[owner, fsdp]
        return cross.remote(
            ref,
            ref,
            gain_column_send.at[owner, step],
            gain_column_recv.at[owner, step],
            seq,
            cross.fsdp_peer(step),
        )

    def output_copy(step):
        return cross.remote(
            output_ref,
            outputs.at[fsdp],
            output_send.at[step],
            output_recv.at[step],
            seq,
            cross.fsdp_peer(step),
        )

    stacks = [attention.stack.at[kind] for kind in range(3)]
    stacks += [units.stack.at[kind] for kind in range(3)]
    copies = load(
        [(source, stack, load_sem.at[i]) for i, (source, stack) in enumerate(zip(sources, stacks))]
    )
    greet_cross(seq_count, fsdp_count)
    for copy in copies:
        copy.wait()

    @pl.loop(0, attention.items)
    def _(item):
        attention.send_rows(item)

    for step in range(1, seq_count):
        gain_row(step).start()
    blocks[line.place * 2 + line.core] = inputs_ref[...]
    gather.send(line.place)

    @pl.loop(0, EARLY)
    def _(item):
        units.send_rows(item)

    gains[seq, fsdp] = gains_ref[...]
    outputs[fsdp] = output_ref[...]
    for step in range(1, fsdp_count):
        gain_column(seq, step).start()

    attention.take(0)

    @pl.loop(1, seq_count)
    def _(step):
        attention.take(step)
        gain_row(step).wait_recv()
        owner = (seq - step + seq_count) % seq_count
        for peer in range(1, fsdp_count):
            gain_column(owner, peer).start()
        attention.relay(step - 1)

    def project_inputs(step):
        chip = gather.step(step)
        pair = pl.ds(chip * 2, 2)
        whole = blocks[pair].reshape(2 * rows, width)
        for kind in range(3):
            weight = attention.weights[kind].reshape(width, columns)
            found = jnp.dot(whole, weight, preferred_element_type=jnp.float32)
            if kind < 2:
                pre[kind, pl.ds(chip * 2 * rows, 2 * rows)] = found
            else:
                heads[2, pair] = found.astype(jnp.bfloat16).reshape(2, rows, columns)

    def weights_arrived():
        attention.relay(seq_count - 1)
        for step in range(1, fsdp_count):
            output_copy(step).start()

        @pl.loop(0, seq_count)
        def _(item):
            attention.settle(item)
            for peer in range(1, fsdp_count):
                gain_column(item, peer).wait_recv()

        gains_out[...] = gains[...]
        lanes = gains.shape[-1]
        own = columns // fsdp_count
        lane = lax.broadcasted_iota(jnp.int32, (lanes, columns), 0)
        column = lax.broadcasted_iota(jnp.int32, (lanes, columns), 1)
        total = None
        for peer in range(fsdp_count):
            place = (column == lane + peer * own) & (lane < own)
            term = jnp.dot(
                gains[seq, peer],
                jnp.where(place, 1.0, 0.0).astype(jnp.bfloat16),
                preferred_element_type=jnp.float32,
            )
            total = term if total is None else total + term
        own_gains[...] = total
        project_inputs(0)

    def send_squares():
        total = None
        for kind in range(2):
            row = lax.dot_general(
                pick_row(kind, (8, columns)),
                pre[kind] * pre[kind],
                (((1,), (1,)), ((), ())),
                precision=EXACT,
                preferred_element_type=jnp.float32,
            )
            total = row if total is None else total + row
        sums.send(total)

    def make_heads():
        squares = sums.receive()
        for kind in range(2):
            mean = dot_rows(squares, pick_row(kind, (8, 128)), EXACT) / width
            inverse = lax.rsqrt(mean + eps_norm)
            inverse_out[:, kind : kind + 1] = inverse[:, :1]
            for first in range(0, columns, DH):
                part = pl.ds(first, DH)
                scaled = pre[kind, :, part] * inverse * own_gains[kind : kind + 1, part]
                turned = turn_heads(scaled, cosine_ref[...], sine_ref[...])
                heads[kind, :, :, part] = turned.astype(jnp.bfloat16).reshape(seq_count, rows, DH)

    def attend(step):
        chip = line.order(chips - 1 - step)

        @pl.loop(0, 2)
        def _(core):
            slot = chip * 2 + core
            first = pl.multiple_of(slot * rows, rows)
            for head in range(0, columns, DH):
                part = pl.ds(head, DH)
                probs = attention_weights(
                    heads[0, slot, :, part],
                    heads[1, :, :, part].reshape(tokens, DH),
                    first,
                    segment_column[pl.ds(first, rows), :],
                    segment_row[...],
                )
                heads[3, slot, :, part] = jnp.dot(
                    probs.astype(jnp.bfloat16),
                    heads[2, :, :, part].reshape(tokens, DH),
                    preferred_element_type=jnp.float32,
                ).astype(jnp.bfloat16)

        product_terms(
            scatter,
            [(heads.at[3], lambda part: outputs[:, :, part].reshape(columns, -1), False)],
            chip,
        )

    inputs_store = pltpu.make_async_copy(blocks, inputs_out, store_sem.at[0])
    attention_store = pltpu.make_async_copy(attention.weights, attention_out, store_sem.at[1])
    output_store = pltpu.make_async_copy(outputs, output_out, store_sem.at[2])
    heads_store = pltpu.make_async_copy(heads, heads_out, store_sem.at[3])
    pre_store = pltpu.make_async_copy(pre, pre_out, store_sem.at[4])

    def units_store(kind):
        return pltpu.make_async_copy(units.weights.at[kind], units_out[kind], store_sem.at[5 + kind])

    def settle_units(kind):
        @pl.loop(0, seq_count)
        def _(step):
            units.settle(kind * seq_count + step)

        units_store(kind).start()

    @pl.loop(0, LEAD)
    def _(item):
        units.take(item)

    arrived = 1
    after_gather = 4 * (chips - 1) - 1
    attending = after_gather + 3
    hopping = attending + chips
    beats = max(units.items + 1, hopping + 2 * chips)

    @pl.loop(0, beats)
    def _(beat):
        @pl.when(beat + EARLY < units.items)
        def _():
            units.send_rows(beat + EARLY)

        @pl.when(beat + LEAD < units.items)
        def _():
            units.take(beat + LEAD)

        @pl.when((beat > 0) & (beat <= units.items))
        def _():
            units.relay(beat - 1)

        @pl.when(beat == arrived)
        def _():
            weights_arrived()
            attention_store.start()

        @pl.when((beat % 4 == 2) & (beat // 4 + 1 < chips))
        def _():
            project_inputs(beat // 4 + 1)

        @pl.when(beat == after_gather)
        def _():
            inputs_store.start()
            pre_store.start()
            send_squares()
            for step in range(1, fsdp_count):
                output_copy(step).wait_recv()
            output_store.start()

        @pl.when(beat == after_gather + 2)
        def _():
            make_heads()

        @pl.when((beat >= attending) & (beat < attending + chips))
        def _():
            attend(beat - attending)

        for kind in range(2):

            @pl.when(beat == (kind + 1) * seq_count + 3)
            def _():
                settle_units(kind)

        @pl.when((beat >= hopping) & (beat < hopping + chips))
        def _():
            scatter.hop(chips - 1 - (beat - hopping))

    heads_store.start()
    scatter.settle(projected)
    settle_units(2)
    scatter.finish()
    gather.finish()
    sums.finish()
    attention.finish()
    units.finish()

    @pl.loop(1, seq_count)
    def _(step):
        gain_row(step).wait_send()

    @pl.loop(0, seq_count)
    def _(owner):
        for step in range(1, fsdp_count):
            gain_column(owner, step).wait_send()

    for step in range(1, fsdp_count):
        output_copy(step).wait_send()
    for store in (inputs_store, attention_store, output_store, heads_store, pre_store):
        store.wait()
    for kind in range(3):
        units_store(kind).wait()


def bring_in(local_in, attention_rows, unit_rows, output_weight, gains, tables, segment_row):
    rows, width = local_in.shape
    slots = lax.axis_size("seq")
    fsdp_count = lax.axis_size("fsdp")
    chips = slots // 2
    tokens = slots * rows
    own, columns = attention_rows[0].shape[0], attention_rows[0].shape[1] // slots
    units = unit_rows[0].shape[1] // slots
    bf16, f32, dma = jnp.bfloat16, jnp.float32, pltpu.SemaphoreType.DMA
    lanes = pl.cdiv(gains.shape[1], 128) * 128
    padded = jnp.pad(gains, ((0, 16 - gains.shape[0]), (0, lanes - gains.shape[1])))
    found = pl.pallas_call(
        functools.partial(bring_in_kernel, chips, fsdp_count),
        out_shape=(
            jax.ShapeDtypeStruct((rows, width), f32),
            jax.ShapeDtypeStruct((tokens, 8), f32),
            jax.ShapeDtypeStruct((16, columns), f32),
            jax.ShapeDtypeStruct((slots, fsdp_count, 16, lanes), bf16),
            jax.ShapeDtypeStruct((slots, rows, width), bf16),
            jax.ShapeDtypeStruct((3, slots, fsdp_count, own, columns), bf16),
            jax.ShapeDtypeStruct((fsdp_count, own, width), bf16),
            jax.ShapeDtypeStruct((4, slots, rows, columns), bf16),
            jax.ShapeDtypeStruct((2, tokens, columns), f32),
        )
        + (jax.ShapeDtypeStruct((slots, fsdp_count, own, units), bf16),) * 3,
        in_specs=[whole_spec()] * 6 + [far_spec()] * 6 + [whole_spec()],
        out_specs=(whole_spec(),) * 4 + (far_spec(),) * 8,
        scratch_shapes=[
            pltpu.VMEM((fsdp_count, own, width), bf16),
            pltpu.VMEM((slots, fsdp_count, 16, lanes), bf16),
            pltpu.VMEM((4, slots, rows, columns), bf16),
            pltpu.VMEM((2, tokens, columns), f32),
            dma((slots,)),
            dma((slots,)),
            dma((slots, fsdp_count)),
            dma((slots, fsdp_count)),
            dma((fsdp_count,)),
            dma((fsdp_count,)),
            dma((6,)),
            dma((8,)),
        ]
        + Gather.scratch(chips, rows, width)
        + RowSum.scratch(slots, (8, tokens))
        + Spread.scratch(3, 3, slots, fsdp_count, own, columns)
        + Spread.scratch(3, 1, slots, fsdp_count, own, units)
        + Scatter.scratch(chips, rows, width),
        compiler_params=line_params(3),
        name="bring_in",
    )(
        local_in,
        padded,
        *tables,
        segment_row.reshape(tokens, 1),
        segment_row.reshape(1, tokens),
        *attention_rows,
        *unit_rows,
        output_weight,
    )
    projected, inverse, own_gains, every_gain = found[:4]
    inputs_all, weights, outputs, heads, pre = found[4:9]
    every_gain = every_gain[:, :, : gains.shape[0], : gains.shape[1]]
    return (
        projected,
        inputs_all.reshape(-1, width),
        weights.reshape(3, -1, columns),
        outputs.reshape(-1, width),
        [columns_of.reshape(-1, units) for columns_of in found[9:]],
        heads.reshape(4, tokens, columns),
        pre,
        inverse,
        own_gains,
        every_gain.transpose(2, 0, 1, 3).reshape(gains.shape[0], -1),
    )


def gather_back_kernel(chips, fsdp_count, *refs):
    local_ref, output_ref, gains_ref, inverse_ref, cosine_ref, sine_ref = refs[:6]
    segment_column, segment_row = refs[6:8]
    hidden_hbm, gate_hbm, up_hbm, heads_hbm, pre_hbm = refs[8:13]
    refs = refs[13:]
    results, output_term, grads_out, gain_out = refs[:2], refs[2], refs[3], refs[4]
    refs = refs[5:]
    tokens, units, heads, pre, gathered, grad_query, grad_key, grad_value = refs[:8]
    load_sem, refs = refs[8], refs[9:]
    line = Line(chips)
    cross = Cross(2 * chips, fsdp_count)
    gather = Gather(line, *refs[:5])
    sums = RowSum(cross, *refs[5:9])
    all_tokens, width = tokens.shape
    block_units = units.shape[-1]
    columns = output_ref.shape[0]
    blocks = gather.blocks
    rows = blocks.shape[1]

    def fill(kind, owner, slot):
        span = width // cross.seq_count
        chosen = tokens[:, pl.ds(pl.multiple_of(owner * span, 128), span)]

        @pl.loop(0, block_units // tile_of(block_units))
        def _(tile):
            part = pl.ds(pl.multiple_of(tile * tile_of(block_units), 128), tile_of(block_units))
            term = dot_rows(chosen, units[kind, :, part]).astype(jnp.bfloat16)
            collect.terms[slot, :, :, part] = term.reshape(fsdp_count, -1, term.shape[1])

    collect = Collect(cross, 2, fill, *refs[9:])
    copies = load(
        [
            (hidden_hbm, tokens, load_sem.at[0]),
            (gate_hbm, units.at[0], load_sem.at[1]),
            (up_hbm, units.at[1], load_sem.at[2]),
            (heads_hbm, heads, load_sem.at[3]),
            (pre_hbm, pre, load_sem.at[4]),
        ]
    )
    greet_cross(cross.seq_count, fsdp_count)
    blocks[line.place * 2 + line.core] = local_ref[...]
    gather.send(line.place)
    grad_key[...] = jnp.zeros_like(grad_key)
    grad_value[...] = jnp.zeros_like(grad_value)
    for copy in copies[:2]:
        copy.wait()
    collect.begin()
    for copy in copies[2:]:
        copy.wait()

    def arrive(step):
        chip = gather.step(step)
        whole = blocks[pl.ds(chip * 2, 2)].reshape(2 * rows, width)
        found = dot_cols(whole, output_ref[...]).astype(jnp.bfloat16)
        gathered[pl.ds(chip * 2 * rows, 2 * rows), :] = found

    arrive(0)
    def attend(slot):
        first = pl.multiple_of(slot * rows, rows)
        span = pl.ds(first, rows)
        for head in range(0, columns, DH):
            part = pl.ds(head, DH)
            queries, keys, values = heads[0, span, part], heads[1, :, part], heads[2, :, part]
            outer = gathered[span, part]
            probs = attention_weights(
                queries, keys, first, segment_column[span, :], segment_row[...]
            )
            grad_value[:, part] += dot_rows(probs.astype(jnp.bfloat16), outer)
            grad_probs = dot_cols(outer, values)
            delta = jnp.sum(probs * grad_probs, axis=-1, keepdims=True)
            grad_scores = (probs * (grad_probs - delta)).astype(jnp.bfloat16)
            grad_query[span, part] = jnp.dot(
                grad_scores, keys, preferred_element_type=jnp.float32
            )
            grad_key[:, part] += dot_rows(grad_scores, queries)

    def errors(kind, grad):
        scaled = (grad[...] * DH ** (-0.5)).astype(jnp.bfloat16).astype(jnp.float32)
        error = turn_heads(scaled, cosine_ref[...], -sine_ref[...])
        inverse = inverse_ref[:, kind : kind + 1]
        return error, pre[kind] * inverse, inverse

    def send_means():
        total = None
        for kind, grad in enumerate((grad_query, grad_key)):
            error, unit, _ = errors(kind, grad)
            product = error * unit
            gain_out[kind : kind + 1, :] = jnp.sum(product, axis=0, keepdims=True)
            row = lax.dot_general(
                pick_row(kind, (8, columns)),
                product * gains_ref[kind : kind + 1, :],
                (((1,), (1,)), ((), ())),
                precision=EXACT,
                preferred_element_type=jnp.float32,
            )
            total = row if total is None else total + row
        sums.send(total)
        grads_out[2] = grad_value[...].astype(jnp.bfloat16)

        @pl.loop(0, width // tile_of(width))
        def _(tile):
            part = pl.ds(pl.multiple_of(tile * tile_of(width), 128), tile_of(width))
            outer = blocks[:, :, part].reshape(all_tokens, -1)
            output_term[:, part] = dot_rows(heads[3], outer).astype(jnp.bfloat16)

    def finish_grads():
        means = sums.receive() / width
        for kind, grad in enumerate((grad_query, grad_key)):
            error, unit, inverse = errors(kind, grad)
            mean = dot_rows(means, pick_row(kind, (8, 128)), EXACT)[:, :1]
            grads_out[kind] = (
                inverse * (error * gains_ref[kind : kind + 1, :] - unit * mean)
            ).astype(jnp.bfloat16)

    attended = 3 * chips - 1

    @pl.loop(0, max(collect.beats, attended + 4))
    def _(turn):
        collect.beat(turn)

        @pl.when((turn % 3 < 2) & (turn // 3 < chips))
        def _():
            attend(line.order(turn // 3) * 2 + turn % 3)

        @pl.when((turn % 3 == 2) & (turn // 3 + 1 < chips))
        def _():
            arrive(turn // 3 + 1)

        @pl.when(turn == attended)
        def _():
            send_means()

        @pl.when(turn == attended + 3)
        def _():
            finish_grads()

    @pl.loop(0, cross.seq_count)
    def _(turn):
        for kind in range(2):

            def put(_, sender, value):
                part = pl.ds(pl.multiple_of(sender * block_units, 128), block_units)
                results[kind][:, part] = value

            collect.receive(kind * cross.seq_count + turn, put)

    collect.finish()
    gather.finish()
    sums.finish()


def gather_back(local, output_rows, gains, inverse, tables, segment_row, far, heads, pre):
    rows, width = local.shape
    slots = lax.axis_size("seq")
    fsdp_count = lax.axis_size("fsdp")
    chips = slots // 2
    own = width // (slots * fsdp_count)
    units = far[1].shape[1]
    _, tokens, columns = heads.shape
    bf16, f32 = jnp.bfloat16, jnp.float32
    found = pl.pallas_call(
        functools.partial(gather_back_kernel, chips, fsdp_count),
        out_shape=(jax.ShapeDtypeStruct((own, units * slots), bf16),) * 2
        + (
            jax.ShapeDtypeStruct((columns, width), bf16),
            jax.ShapeDtypeStruct((3, tokens, columns), bf16),
            jax.ShapeDtypeStruct((8, columns), f32),
        ),
        in_specs=[whole_spec()] * 8 + [far_spec()] * 5,
        out_specs=(whole_spec(),) * 5,
        scratch_shapes=[
            pltpu.VMEM((tokens, width), bf16),
            pltpu.VMEM((2, tokens, units), bf16),
            pltpu.VMEM((4, tokens, columns), bf16),
            pltpu.VMEM((2, tokens, columns), f32),
            pltpu.VMEM((tokens, columns), bf16),
            pltpu.VMEM((tokens, columns), f32),
            pltpu.VMEM((tokens, columns), f32),
            pltpu.VMEM((tokens, columns), f32),
            pltpu.SemaphoreType.DMA((5,)),
        ]
        + Gather.scratch(chips, rows, width)
        + RowSum.scratch(slots, (8, tokens))
        + Collect.scratch(2, slots, fsdp_count, own, units),
        compiler_params=line_params(6),
        name="gather_back",
    )(
        local,
        output_rows,
        gains,
        inverse,
        *tables,
        segment_row.reshape(tokens, 1),
        segment_row.reshape(1, tokens),
        *far,
        heads,
        pre,
    )
    return found[:2], found[2], found[3], found[4]


def take_out_kernel(
    chips,
    fsdp_count,
    *refs,
):
    grads_ref, rights, tokens_ref = refs[0], refs[1], refs[2]
    output_ref, gains_ref, refs = refs[3], refs[4], refs[5:]
    result, weight_outs, output_out, gains_out, refs = refs[0], refs[1:4], refs[4], refs[5], refs[6:]
    output_in, gain_in, gain_out, gain_rows, refs = refs[0], refs[1], refs[2], refs[3], refs[4:]
    output_send, output_recv, gain_send, gain_recv, gain_row_send, gain_row_recv = refs[:6]
    comm = refs[6:]
    line = Line(chips)
    cross = Cross(2 * chips, fsdp_count)
    seq_count, seq, fsdp = cross.seq_count, cross.seq, cross.fsdp
    scatter = Scatter(line, *comm[:-12])
    columns = rights.shape[-1]
    rows, width = scatter.fresh.shape[1:]

    def fill(kind, owner, slot):
        span = width // seq_count
        part = pl.ds(pl.multiple_of(owner * span, 128), span)
        chosen = tokens_ref[:, part]
        for kind in range(3):
            term = dot_rows(chosen, grads_ref[kind].reshape(-1, columns)).astype(jnp.bfloat16)
            collect.terms[slot, :, :, kind * columns : (kind + 1) * columns] = term.reshape(
                fsdp_count, -1, columns
            )

    collect = Collect(cross, 1, fill, *comm[-12:])

    def output_copy(step):
        peer = cross.fsdp_peer(step)
        return cross.remote(
            output_ref.at[peer],
            output_in.at[step],
            output_send.at[step],
            output_recv.at[step],
            seq,
            peer,
        )

    def gain_copy(step):
        peer = cross.fsdp_peer(step)
        return cross.remote(
            gains_ref.at[peer], gain_in.at[step], gain_send.at[step], gain_recv.at[step], seq, peer
        )

    def gain_row(step):
        peer = cross.seq_peer(step)
        return cross.remote(
            gain_out.at[peer],
            gain_rows.at[step],
            gain_row_send.at[step],
            gain_row_recv.at[step],
            peer,
            fsdp,
        )

    greet_cross(seq_count, fsdp_count)
    for step in range(1, fsdp_count):
        gain_copy(step).start()

    collect.begin()

    @pl.loop(0, chips)
    def _(step):
        product_terms(
            scatter,
            [(grads_ref.at[kind], rights.at[kind], True) for kind in range(3)],
            line.order(chips - 1 - step),
        )

    total = gains_ref[fsdp]
    for step in range(1, fsdp_count):
        gain_copy(step).wait_recv()
        total = total + gain_in[step]
    gain_out[...] = total
    for step in range(1, seq_count):
        gain_row(step).start()

    @pl.loop(0, collect.beats)
    def _(turn):
        collect.beat(turn)

        @pl.when(turn == seq_count - AHEAD)
        def _():
            for step in range(1, fsdp_count):
                output_copy(step).start()

        @pl.when((turn >= HOPPING) & (turn < HOPPING + chips))
        def _():
            scatter.hop(chips - 1 - (turn - HOPPING))

    total = output_ref[fsdp].astype(jnp.float32)
    for step in range(1, fsdp_count):
        output_copy(step).wait_recv()
        total = total + output_in[step].astype(jnp.float32)
    output_out[...] = total
    scatter.settle(result)
    total = gain_out[seq]
    for step in range(1, seq_count):
        gain_row(step).wait_recv()
        total = total + gain_rows[step]
    gains_out[...] = total

    def put(_, sender, value):
        block = pl.ds(pl.multiple_of(sender * columns, 128), columns)
        for kind in range(3):
            weight_outs[kind][:, block] = value[:, kind * columns : (kind + 1) * columns]

    @pl.loop(0, seq_count)
    def _(turn):
        collect.receive(turn, put)

    scatter.finish()
    collect.finish()

    @pl.loop(1, seq_count)
    def _(step):
        gain_row(step).wait_send()

    for step in range(1, fsdp_count):
        output_copy(step).wait_send()
        gain_copy(step).wait_send()


def take_out(grads, weights, tokens, output_term, gain_terms):
    slots = lax.axis_size("seq")
    fsdp_count = lax.axis_size("fsdp")
    chips = slots // 2
    _, width, columns = weights.shape
    rows = tokens.shape[0] // slots
    own = width // (slots * fsdp_count)
    kinds = gain_terms.shape[0]
    bf16, f32, dma = jnp.bfloat16, jnp.float32, pltpu.SemaphoreType.DMA
    gains = gain_terms.reshape(kinds, slots, fsdp_count, own).transpose(2, 1, 0, 3)
    lanes = pl.cdiv(own, 128) * 128
    gains = jnp.pad(gains, ((0, 0), (0, 0), (0, 8 - kinds), (0, lanes - own)))
    result, query, key, value, output, gains = pl.pallas_call(
        functools.partial(take_out_kernel, chips, fsdp_count),
        out_shape=(jax.ShapeDtypeStruct((rows, width), f32),)
        + (jax.ShapeDtypeStruct((own, columns * slots), bf16),) * 3
        + (jax.ShapeDtypeStruct((own, width), f32), jax.ShapeDtypeStruct((8, lanes), f32)),
        in_specs=[whole_spec()] * 5,
        out_specs=(whole_spec(),) * 6,
        scratch_shapes=[
            pltpu.VMEM((fsdp_count, own, width), bf16),
            pltpu.VMEM((fsdp_count, slots, 8, lanes), f32),
            pltpu.VMEM((slots, 8, lanes), f32),
            pltpu.VMEM((slots, 8, lanes), f32),
            dma((fsdp_count,)),
            dma((fsdp_count,)),
            dma((fsdp_count,)),
            dma((fsdp_count,)),
            dma((slots,)),
            dma((slots,)),
        ]
        + Scatter.scratch(chips, rows, width)
        + Collect.scratch(1, slots, fsdp_count, own, 3 * columns),
        compiler_params=line_params(4),
        name="take_out",
    )(
        grads.reshape(3, slots, rows, columns),
        weights,
        tokens,
        output_term.reshape(fsdp_count, own, width),
        gains,
    )
    return result, (query, key, value), output, gains[:kinds, :own]


def feed_forward_kernel(
    chips,
    hidden_ref,
    gate_hbm,
    up_hbm,
    down_hbm,
    stream_ref,
    cotangent_ref,
    gain_ref,
    result_ref,
    grad_ref,
    gain_grad_ref,
    gate_out,
    up_out,
    act_out,
    all_out,
    gate_w,
    up_w,
    down_w,
    gate_keep,
    up_keep,
    act_keep,
    load_sem,
    store_sem,
    mixed_ref,
    *comm,
):
    line = Line(chips)
    gather = Gather(line, *comm[:5])
    scatter = Scatter(line, *comm[5:])
    blocks, fresh = gather.blocks, scatter.fresh
    _, rows, width = blocks.shape
    units = gate_w.shape[1]
    copies = load(
        [
            (gate_hbm, gate_w, load_sem.at[0]),
            (up_hbm, up_w, load_sem.at[1]),
            (down_hbm, down_w, load_sem.at[2]),
        ]
    )
    line.greet()
    blocks[line.place * 2 + line.core] = hidden_ref[...]
    gather.send(line.place)

    def stores(chip):
        pair = pl.ds(chip * 2, 2)
        return [
            pltpu.make_async_copy(gate_keep.at[pair], gate_out.at[pair], store_sem.at[0, chip]),
            pltpu.make_async_copy(up_keep.at[pair], up_out.at[pair], store_sem.at[1, chip]),
            pltpu.make_async_copy(act_keep.at[pair], act_out.at[pair], store_sem.at[2, chip]),
            pltpu.make_async_copy(blocks.at[pair], all_out.at[pair], store_sem.at[3, chip]),
        ]

    for copy in copies:
        copy.wait()

    @pl.loop(0, chips)
    def _(step):
        chip = gather.step(step)
        pair = pl.ds(chip * 2, 2)

        @pl.loop(0, units // tile_of(units))
        def _(tile):
            columns = pl.ds(pl.multiple_of(tile * tile_of(units), 128), tile_of(units))
            tokens = blocks[pair].reshape(2 * rows, width)
            gate = jnp.dot(tokens, gate_w[:, columns], preferred_element_type=jnp.float32)
            up = jnp.dot(tokens, up_w[:, columns], preferred_element_type=jnp.float32)
            gate_keep[pair, :, columns] = gate.reshape(2, rows, -1)
            up_keep[pair, :, columns] = up.reshape(2, rows, -1)
            act_keep[pair, :, columns] = (
                (gate / (1.0 + jnp.exp(-gate)) * up).astype(jnp.bfloat16).reshape(2, rows, -1)
            )

        @pl.loop(0, width // tile_of(width))
        def _(tile):
            columns = pl.ds(pl.multiple_of(tile * tile_of(width), 128), tile_of(width))
            act = act_keep[pair].reshape(2 * rows, units)
            fresh[:, :, columns] = dot_cols(act, down_w[columns, :]).reshape(2, rows, -1)

        for copy in stores(chip):
            copy.start()
        scatter.after_term(chip)

    scatter.hops()
    scatter.settle(mixed_ref)
    gain_grad_ref[...] = jnp.zeros_like(gain_grad_ref)
    part_rows = min(32, rows)

    @pl.loop(0, rows // part_rows)
    def _(part):
        span = pl.ds(pl.multiple_of(part * part_rows, part_rows), part_rows)
        mixed, outer, gain = mixed_ref[span], cotangent_ref[span].astype(jnp.float32), gain_ref[0:1]
        inverse = lax.rsqrt(jnp.mean(mixed * mixed, axis=-1, keepdims=True) + eps_norm)
        unit = mixed * inverse
        result_ref[span] = (stream_ref[span] + unit * gain).astype(jnp.bfloat16)
        gain_grad_ref[0:1] += jnp.sum(outer * unit, axis=0, keepdims=True)
        outer = outer * gain
        mean = jnp.mean(outer * unit, axis=-1, keepdims=True)
        grad_ref[span] = (inverse * (outer - unit * mean)).astype(jnp.bfloat16)

    scatter.finish()
    gather.finish()

    @pl.loop(0, chips)
    def _(chip):
        for copy in stores(chip):
            copy.wait()


def feed_forward(hidden_low, gate_cols, up_cols, down_cols, stream, cotangent, gain):
    rows, width = hidden_low.shape
    units = gate_cols.shape[1]
    slots = lax.axis_size("seq")
    chips = slots // 2
    weights = [pltpu.VMEM((width, units), jnp.bfloat16)] * 3
    result, grad, gain_grad, gate, up, act, every = pl.pallas_call(
        functools.partial(feed_forward_kernel, chips),
        out_shape=(
            jax.ShapeDtypeStruct((rows, width), jnp.bfloat16),
            jax.ShapeDtypeStruct((rows, width), jnp.bfloat16),
            jax.ShapeDtypeStruct((8, width), jnp.float32),
            jax.ShapeDtypeStruct((slots, rows, units), jnp.float32),
            jax.ShapeDtypeStruct((slots, rows, units), jnp.float32),
            jax.ShapeDtypeStruct((slots, rows, units), jnp.bfloat16),
            jax.ShapeDtypeStruct((slots, rows, width), jnp.bfloat16),
        ),
        in_specs=[whole_spec()] + [far_spec()] * 3 + [whole_spec()] * 3,
        out_specs=(whole_spec(),) * 3 + (far_spec(),) * 4,
        scratch_shapes=weights
        + [
            pltpu.VMEM((slots, rows, units), jnp.float32),
            pltpu.VMEM((slots, rows, units), jnp.float32),
            pltpu.VMEM((slots, rows, units), jnp.bfloat16),
            pltpu.SemaphoreType.DMA((3,)),
            pltpu.SemaphoreType.DMA((4, chips)),
            pltpu.VMEM((rows, width), jnp.float32),
        ]
        + Gather.scratch(chips, rows, width)
        + Scatter.scratch(chips, rows, width),
        compiler_params=line_params(1),
        name="feed_forward",
    )(hidden_low, gate_cols, up_cols, down_cols, stream, cotangent, gain.reshape(1, width))
    return (
        result,
        grad,
        gain_grad[0],
        gate,
        up,
        act.reshape(-1, units),
        every.reshape(-1, width),
    )


def feed_forward_back_kernel(chips, fsdp_count, *refs):
    grad_ref, gate_hbm, up_hbm, down_hbm, gate_lin_hbm, up_lin_hbm, act_hbm = refs[:7]
    hidden_grad_ref, gate_out, up_out, down_grad, refs = *refs[7:11], refs[11:]
    gate_w, up_w, down_w, gate_lin, up_lin, gate_keep, up_keep, act, refs = *refs[:8], refs[8:]
    load_sem, store_sem, refs = refs[0], refs[1], refs[2:]
    line = Line(chips)
    cross = Cross(2 * chips, fsdp_count)
    gather = Gather(line, *refs[:5])
    scatter = Scatter(line, *refs[5:15])
    blocks, fresh = gather.blocks, scatter.fresh
    _, rows, width = blocks.shape
    units = gate_w.shape[1]
    all_tokens = cross.seq_count * rows

    def fill(kind, owner, slot):
        span = width // cross.seq_count
        part = pl.ds(pl.multiple_of(owner * span, 128), span)
        chosen = blocks[:, :, part].reshape(all_tokens, span)

        @pl.loop(0, units // tile_of(units))
        def _(tile):
            columns = pl.ds(pl.multiple_of(tile * tile_of(units), 128), tile_of(units))
            term = dot_rows(chosen, act[:, columns]).astype(jnp.bfloat16)
            collect.terms[slot, :, :, columns] = term.reshape(fsdp_count, -1, term.shape[1])

    collect = Collect(cross, 1, fill, *refs[15:])
    copies = load(
        [
            (down_hbm, down_w, load_sem.at[0]),
            (gate_lin_hbm, gate_lin, load_sem.at[1]),
            (up_lin_hbm, up_lin, load_sem.at[2]),
            (gate_hbm, gate_w, load_sem.at[3]),
            (up_hbm, up_w, load_sem.at[4]),
            (act_hbm, act, load_sem.at[5]),
        ]
    )
    greet_cross(cross.seq_count, fsdp_count)
    blocks[line.place * 2 + line.core] = grad_ref[...]
    gather.send(line.place)

    def stores(chip):
        pair = pl.ds(chip * 2, 2)
        return [
            pltpu.make_async_copy(gate_keep.at[pair], gate_out.at[pair], store_sem.at[0, chip]),
            pltpu.make_async_copy(up_keep.at[pair], up_out.at[pair], store_sem.at[1, chip]),
        ]

    for copy in copies:
        copy.wait()

    @pl.loop(0, chips)
    def _(step):
        chip = gather.step(step)
        pair = pl.ds(chip * 2, 2)

        @pl.loop(0, units // tile_of(units))
        def _(tile):
            columns = pl.ds(pl.multiple_of(tile * tile_of(units), 128), tile_of(units))
            tokens = blocks[pair].reshape(2 * rows, width)
            grad = jnp.dot(tokens, down_w[:, columns], preferred_element_type=jnp.float32)
            gate = gate_lin[pair, :, columns].reshape(2 * rows, -1)
            up = up_lin[pair, :, columns].reshape(2 * rows, -1)
            sig = 1.0 / (1.0 + jnp.exp(-gate))
            gate_keep[pair, :, columns] = (
                (grad * up * sig * (1.0 + gate * (1.0 - sig)))
                .astype(jnp.bfloat16)
                .reshape(2, rows, -1)
            )
            up_keep[pair, :, columns] = (
                (grad * (gate * sig)).astype(jnp.bfloat16).reshape(2, rows, -1)
            )

        @pl.loop(0, width // tile_of(width))
        def _(tile):
            columns = pl.ds(pl.multiple_of(tile * tile_of(width), 128), tile_of(width))
            gate = gate_keep[pair].reshape(2 * rows, units)
            up = up_keep[pair].reshape(2 * rows, units)
            fresh[:, :, columns] = (
                dot_cols(gate, gate_w[columns, :]) + dot_cols(up, up_w[columns, :])
            ).reshape(2, rows, -1)

        for copy in stores(chip):
            copy.start()
        scatter.after_term(chip)

    collect.begin()

    @pl.loop(0, collect.beats)
    def _(turn):
        collect.beat(turn)

        @pl.when(turn < chips)
        def _():
            scatter.hop(turn)

    scatter.settle(hidden_grad_ref)

    def put(_, sender, value):
        columns = pl.ds(pl.multiple_of(sender * units, 128), units)
        down_grad[:, columns] = value

    @pl.loop(0, cross.seq_count)
    def _(turn):
        collect.receive(turn, put)

    scatter.finish()
    gather.finish()
    collect.finish()

    @pl.loop(0, chips)
    def _(chip):
        for copy in stores(chip):
            copy.wait()


def feed_forward_back(grad_low, gate_cols, up_cols, down_cols, gate, up, act):
    rows, width = grad_low.shape
    units = gate_cols.shape[1]
    slots = lax.axis_size("seq")
    fsdp_count = lax.axis_size("fsdp")
    chips = slots // 2
    own = width // (slots * fsdp_count)
    bf16, f32 = jnp.bfloat16, jnp.float32
    hidden_grad, gate_grad, up_grad, down_grad = pl.pallas_call(
        functools.partial(feed_forward_back_kernel, chips, fsdp_count),
        out_shape=(
            jax.ShapeDtypeStruct((rows, width), f32),
            jax.ShapeDtypeStruct((slots, rows, units), bf16),
            jax.ShapeDtypeStruct((slots, rows, units), bf16),
            jax.ShapeDtypeStruct((own, units * slots), bf16),
        ),
        in_specs=[whole_spec()] + [far_spec()] * 6,
        out_specs=(whole_spec(), far_spec(), far_spec(), whole_spec()),
        scratch_shapes=[pltpu.VMEM((width, units), bf16)] * 3
        + [
            pltpu.VMEM((slots, rows, units), f32),
            pltpu.VMEM((slots, rows, units), f32),
            pltpu.VMEM((slots, rows, units), bf16),
            pltpu.VMEM((slots, rows, units), bf16),
            pltpu.VMEM((slots * rows, units), bf16),
            pltpu.SemaphoreType.DMA((6,)),
            pltpu.SemaphoreType.DMA((2, chips)),
        ]
        + Gather.scratch(chips, rows, width)
        + Scatter.scratch(chips, rows, width)
        + Collect.scratch(1, slots, fsdp_count, own, units),
        compiler_params=line_params(2),
        name="feed_forward_back",
    )(grad_low, gate_cols, up_cols, down_cols, gate, up, act)
    return hidden_grad, gate_grad.reshape(-1, units), up_grad.reshape(-1, units), down_grad


def rope_tables(row_count):
    half_width = DH // 2
    frequency = rope_base ** (-jnp.arange(half_width, dtype=jnp.float32) * 2.0 / DH)
    angles = jnp.arange(row_count, dtype=jnp.int32).astype(jnp.float32)[:, None] * frequency[None, :]
    cosine, sine = jnp.cos(angles), jnp.sin(angles)
    return (
        jnp.concatenate([cosine, cosine], axis=1),
        jnp.concatenate([-sine, sine], axis=1),
    )


def per_device(
    inputs,
    query_weight,
    key_weight,
    value_weight,
    output_weight,
    query_gain,
    key_gain,
    attention_gain,
    gate_weight,
    up_weight,
    down_weight,
    feedforward_gain,
    segments,
    cotangent,
):
    token_count = inputs.shape[1]
    width_all = inputs.shape[2]
    local_in = inputs.reshape(token_count, width_all)
    segment_row = segments[0]
    seq_index = lax.axis_index("seq")
    tables = rope_tables(segment_row.shape[0])
    (
        projected,
        inputs_all,
        attention_cols,
        output_rows,
        unit_cols,
        heads,
        pre,
        inverse,
        own_gains,
        gains,
    ) = bring_in(
        local_in,
        [query_weight, key_weight, value_weight],
        [gate_weight, up_weight, down_weight],
        output_weight,
        jnp.stack([query_gain, key_gain, attention_gain, feedforward_gain]),
        tables,
        segment_row,
    )
    gate_cols, up_cols, down_cols = unit_cols
    head_width = heads.shape[2]
    gains = gains.astype(jnp.float32)
    attention_scale = gains[2]
    feedforward_scale = gains[3]
    hidden = local_in.astype(jnp.float32) + rms_scale(projected, attention_scale)
    hidden_low = hidden.astype(jnp.bfloat16)
    grad_result = cotangent.reshape(token_count, width_all)
    result, grad_mixed_low, grad_feedforward_gain, gate_linear, up_linear, activated, hidden_all = (
        feed_forward(
            hidden_low, gate_cols, up_cols, down_cols, hidden, grad_result, feedforward_scale
        )
    )
    result = result.reshape(1, token_count, width_all)
    hidden_term, grad_gate_low, grad_upward_low, down_weight_grad = feed_forward_back(
        grad_mixed_low, gate_cols, up_cols, down_cols, gate_linear, up_linear, activated
    )
    grad_hidden = grad_result.astype(jnp.float32) + hidden_term
    _, branch_pull = jax.vjp(rms_scale, projected, attention_scale)
    grad_projected, grad_attention_gain = branch_pull(grad_hidden)
    weight_grads, output_term, attention_grads, gain_rows = gather_back(
        grad_projected.astype(jnp.bfloat16),
        output_rows,
        own_gains,
        inverse,
        tables,
        segment_row,
        [hidden_all, grad_gate_low, grad_upward_low],
        heads,
        pre,
    )
    gate_weight_grad, up_weight_grad = weight_grads
    head_gains = lax.dynamic_update_slice_in_dim(
        jnp.zeros((2, width_all), jnp.float32),
        gain_rows[:2],
        seq_index * head_width,
        1,
    )
    gain_terms = jnp.concatenate(
        [head_gains, jnp.stack([grad_attention_gain, grad_feedforward_gain])], axis=0
    )
    input_term, projection_grads, output_weight_grad, gain_grads = take_out(
        attention_grads, attention_cols, inputs_all, output_term, gain_terms
    )
    query_weight_grad, key_weight_grad, value_weight_grad = projection_grads
    grad_input = grad_hidden + input_term
    return (
        result,
        grad_input.reshape(1, token_count, width_all),
        query_weight_grad.astype(jnp.float32),
        key_weight_grad.astype(jnp.float32),
        value_weight_grad.astype(jnp.float32),
        output_weight_grad,
        gain_grads[0],
        gain_grads[1],
        gain_grads[2],
        gate_weight_grad.astype(jnp.float32),
        up_weight_grad.astype(jnp.float32),
        down_weight_grad.astype(jnp.float32),
        gain_grads[3],
    )


def solution(mesh):
    in_specs = (
        P("fsdp", "seq", None),
        P(("seq", "fsdp"), None),
        P(("seq", "fsdp"), None),
        P(("seq", "fsdp"), None),
        P(("seq", "fsdp"), None),
        P(("seq", "fsdp")),
        P(("seq", "fsdp")),
        P(("seq", "fsdp")),
        P(("seq", "fsdp"), None),
        P(("seq", "fsdp"), None),
        P(("seq", "fsdp"), None),
        P(("seq", "fsdp")),
        P("fsdp", None),
        P("fsdp", "seq", None),
    )
    out_specs = (
        P("fsdp", "seq", None),
        P("fsdp", "seq", None),
        P(("seq", "fsdp"), None),
        P(("seq", "fsdp"), None),
        P(("seq", "fsdp"), None),
        P(("seq", "fsdp"), None),
        P(("seq", "fsdp")),
        P(("seq", "fsdp")),
        P(("seq", "fsdp")),
        P(("seq", "fsdp"), None),
        P(("seq", "fsdp"), None),
        P(("seq", "fsdp"), None),
        P(("seq", "fsdp")),
    )
    return jax.shard_map(
        per_device, mesh=mesh, in_specs=in_specs, out_specs=out_specs, check_vma=False
    )
```

```python
import functools

import jax
import jax.numpy as jnp
from jax import lax
from jax.experimental import pallas as pl
from jax.experimental.pallas import tpu as pltpu
from jax.sharding import PartitionSpec as P

DH = 128


eps_norm = 1e-06
rope_base = 500000.0
neg_fill = -1e30


def rms_scale(tensor, gain):
    return tensor * lax.rsqrt(jnp.mean(tensor * tensor, axis=-1, keepdims=True) + eps_norm) * gain


MESH = pl.DeviceIdType.MESH
RS_PARTS = 4


class Line:
    def __init__(self, chips):
        index = lax.axis_index("seq")
        self.chips = chips
        self.fsdp = lax.axis_index("fsdp")
        self.place = index // 2
        self.core = index % 2

    def device(self, place, core):
        return (place * 2 + core, self.fsdp)

    @property
    def partner(self):
        return self.device(self.place, 1 - self.core)

    @property
    def above(self):
        return self.device(jnp.minimum(self.place + 1, self.chips - 1), self.core)

    @property
    def below(self):
        return self.device(jnp.maximum(self.place - 1, 0), self.core)

    @property
    def has_above(self):
        return self.place < self.chips - 1

    @property
    def has_below(self):
        return self.place > 0

    def greet(self):
        barrier = pltpu.get_barrier_semaphore()
        pl.semaphore_signal(barrier, inc=1, device_id=self.partner, device_id_type=MESH)

        @pl.when(self.has_above)
        def _():
            pl.semaphore_signal(barrier, inc=1, device_id=self.above, device_id_type=MESH)

        @pl.when(self.has_below)
        def _():
            pl.semaphore_signal(barrier, inc=1, device_id=self.below, device_id_type=MESH)

        peers = (
            1 + jnp.minimum(self.place, 1) + jnp.minimum(self.chips - 1 - self.place, 1)
        )
        pl.semaphore_wait(barrier, peers)

    def order(self, step):
        place, last = self.place, self.chips - 1
        near = jnp.minimum(place, last - place)
        both = jnp.where(step % 2 == 1, place - (step + 1) // 2, place + step // 2)
        rest = jnp.where(place <= last - place, step, last - step)
        return jnp.where(step <= 2 * near, both, rest)

    def paired(self, step):
        near = jnp.minimum(self.place, self.chips - 1 - self.place)
        return (step % 2 == 1) & (step <= 2 * near)

    def second_of_pair(self, step):
        near = jnp.minimum(self.place, self.chips - 1 - self.place)
        return (step % 2 == 0) & (step > 0) & (step <= 2 * near)


class Gather:
    def __init__(self, line, blocks, arrive, up_sem, down_sem, side_sem):
        self.line, self.blocks, self.arrive = line, blocks, arrive
        self.up_sem, self.down_sem, self.side_sem = up_sem, down_sem, side_sem

    @staticmethod
    def scratch(chips, rows, width):
        return [
            pltpu.VMEM((2 * chips, rows, width), jnp.bfloat16),
            pltpu.SemaphoreType.DMA((2 * chips,)),
            pltpu.SemaphoreType.DMA((chips,)),
            pltpu.SemaphoreType.DMA((chips,)),
            pltpu.SemaphoreType.DMA((chips,)),
        ]

    def copy(self, chip, sem, target):
        slot = chip * 2 + self.line.core
        return pltpu.make_async_remote_copy(
            src_ref=self.blocks.at[slot],
            dst_ref=self.blocks.at[slot],
            send_sem=sem.at[chip],
            recv_sem=self.arrive.at[slot],
            device_id=target,
            device_id_type=MESH,
        )

    def wait_slot(self, slot):
        pltpu.make_async_remote_copy(
            src_ref=self.blocks.at[slot],
            dst_ref=self.blocks.at[slot],
            send_sem=self.side_sem.at[0],
            recv_sem=self.arrive.at[slot],
            device_id=self.line.partner,
            device_id_type=MESH,
        ).wait_recv()

    def send(self, chip):
        line = self.line

        @pl.when((chip <= line.place) & line.has_above)
        def _():
            self.copy(chip, self.up_sem, line.above).start()

        @pl.when((chip >= line.place) & line.has_below)
        def _():
            self.copy(chip, self.down_sem, line.below).start()

        self.copy(chip, self.side_sem, line.partner).start()

    def take(self, chip):
        self.wait_slot(chip * 2 + self.line.core)
        self.send(chip)

    def step(self, step):
        line = self.line
        chip = line.order(step)

        @pl.when((step > 0) & jnp.logical_not(line.second_of_pair(step)))
        def _():
            self.take(chip)

        @pl.when(line.paired(step))
        def _():
            self.take(line.order(step + 1))

        self.wait_slot(chip * 2 + 1 - line.core)
        return chip

    def finish(self):
        line = self.line

        @pl.loop(0, line.chips)
        def _(chip):
            @pl.when((chip <= line.place) & line.has_above)
            def _():
                self.copy(chip, self.up_sem, line.above).wait_send()

            @pl.when((chip >= line.place) & line.has_below)
            def _():
                self.copy(chip, self.down_sem, line.below).wait_send()

            self.copy(chip, self.side_sem, line.partner).wait_send()


class Scatter:
    def __init__(self, line, fresh, terms, side_out, side_in, out, inward, side_send, side_recv, send_sem, recv_sem):
        self.line, self.fresh, self.terms = line, fresh, terms
        self.side_out, self.side_in = side_out, side_in
        self.out, self.inward = out, inward
        self.side_send, self.side_recv = side_send, side_recv
        self.send_sem, self.recv_sem = send_sem, recv_sem
        self.rows = terms.shape[1] // RS_PARTS

    @staticmethod
    def scratch(chips, rows, width):
        return [
            pltpu.VMEM((2, rows, width), jnp.float32),
            pltpu.VMEM((chips, rows, width), jnp.float32),
            pltpu.VMEM((chips, rows, width), jnp.bfloat16),
            pltpu.VMEM((chips, rows, width), jnp.bfloat16),
            pltpu.VMEM((chips, rows, width), jnp.bfloat16),
            pltpu.VMEM((2, chips, rows, width), jnp.bfloat16),
            pltpu.SemaphoreType.DMA((chips,)),
            pltpu.SemaphoreType.DMA((chips,)),
            pltpu.SemaphoreType.DMA((chips, RS_PARTS)),
            pltpu.SemaphoreType.DMA((2, chips, RS_PARTS)),
        ]

    def side(self, chip):
        return pltpu.make_async_remote_copy(
            src_ref=self.side_out.at[chip],
            dst_ref=self.side_in.at[chip],
            send_sem=self.side_send.at[chip],
            recv_sem=self.side_recv.at[chip],
            device_id=self.line.partner,
            device_id_type=MESH,
        )

    def part(self, chip, part, upward, target):
        rows = pl.ds(part * self.rows, self.rows)
        return pltpu.make_async_remote_copy(
            src_ref=self.out.at[chip, rows],
            dst_ref=self.inward.at[upward, chip, rows],
            send_sem=self.send_sem.at[chip, part],
            recv_sem=self.recv_sem.at[upward, chip, part],
            device_id=target,
            device_id_type=MESH,
        )

    def share(self, chip):
        self.side_out[chip] = self.fresh[1 - self.line.core].astype(jnp.bfloat16)
        self.side(chip).start()
        self.terms[chip] = self.fresh[self.line.core]

    def total(self, chip, part, ways):
        rows = pl.ds(part * self.rows, self.rows)
        total = self.terms[chip, rows] + self.side_in[chip, rows].astype(jnp.float32)
        for way in ways:
            total = total + self.inward[way, chip, rows].astype(jnp.float32)
        return rows, total

    def pass_part(self, chip, part, upward, first):
        target = self.line.above if upward else self.line.below
        if not first:
            self.part(chip, part, upward, target).wait_recv()
        rows, total = self.total(chip, part, () if first else (upward,))
        self.out[chip, rows] = total.astype(jnp.bfloat16)
        self.part(chip, part, upward, target).start()

    def hand_on(self, chip, upward, first):
        self.side(chip).wait_recv()

        @pl.loop(0, RS_PARTS)
        def _(part):
            self.pass_part(chip, part, upward, first)

    def after_term(self, chip):
        line = self.line
        self.share(chip)

        @pl.when((chip < line.place) & jnp.logical_not(line.has_above))
        def _():
            self.hand_on(chip, 0, True)

        @pl.when((chip > line.place) & jnp.logical_not(line.has_below))
        def _():
            self.hand_on(chip, 1, True)

    def hop(self, step):
        line = self.line
        lower = line.place * 2 < line.chips
        up_chip, down_chip = step, line.chips - 1 - step
        go_up = (up_chip > line.place) & line.has_below
        go_down = (down_chip < line.place) & line.has_above

        @pl.when(go_up & lower)
        def _():
            self.hand_on(up_chip, 1, False)

        @pl.when(go_down)
        def _():
            self.hand_on(down_chip, 0, False)

        @pl.when(go_up & jnp.logical_not(lower))
        def _():
            self.hand_on(up_chip, 1, False)

    def settle(self, result):
        line = self.line
        place = line.place
        self.side(place).wait_recv()

        @pl.loop(0, RS_PARTS)
        def _(part):
            @pl.when(line.has_above)
            def _():
                self.part(place, part, 0, line.below).wait_recv()

            @pl.when(line.has_below)
            def _():
                self.part(place, part, 1, line.above).wait_recv()

            @pl.when(line.has_above & line.has_below)
            def _():
                rows, total = self.total(place, part, (0, 1))
                result[rows] = total

            @pl.when(line.has_above & jnp.logical_not(line.has_below))
            def _():
                rows, total = self.total(place, part, (0,))
                result[rows] = total

            @pl.when(line.has_below & jnp.logical_not(line.has_above))
            def _():
                rows, total = self.total(place, part, (1,))
                result[rows] = total

    def hops(self):
        @pl.loop(0, self.line.chips)
        def _(step):
            self.hop(step)

    def finish(self):
        line = self.line

        @pl.loop(0, line.chips)
        def _(chip):
            self.side(chip).wait_send()

            @pl.when(chip != line.place)
            def _():
                @pl.loop(0, RS_PARTS)
                def _(part):
                    self.part(chip, part, 0, line.below).wait_send()


def tile_of(extent):
    return min(256, extent)


def dot_cols(left, right):
    return lax.dot_general(
        left, right, (((1,), (1,)), ((), ())), preferred_element_type=jnp.float32
    )


def load(pairs):
    copies = [pltpu.make_async_copy(src, dst, sem) for src, dst, sem in pairs]
    for copy in copies:
        copy.start()
    return copies


def whole_spec():
    return pl.BlockSpec(memory_space=pltpu.VMEM)


def far_spec():
    return pl.BlockSpec(memory_space=pl.ANY)


def line_params(collective_id):
    return pltpu.CompilerParams(
        collective_id=collective_id, has_side_effects=True, vmem_limit_bytes=67_043_328
    )


def peers_of(axis, size):
    me = lax.axis_index(axis)
    return me, lambda step: (me + step) % size


def greet_cross(seq_count, fsdp_count):
    seq, seq_peer = peers_of("seq", seq_count)
    fsdp, fsdp_peer = peers_of("fsdp", fsdp_count)
    barrier = pltpu.get_barrier_semaphore()
    for step in range(1, seq_count):
        pl.semaphore_signal(
            barrier, inc=1, device_id=(seq_peer(step), fsdp), device_id_type=MESH
        )
    for step in range(1, fsdp_count):
        pl.semaphore_signal(
            barrier, inc=1, device_id=(seq, fsdp_peer(step)), device_id_type=MESH
        )
    pl.semaphore_wait(barrier, seq_count + fsdp_count - 2)


class Cross:
    def __init__(self, seq_count, fsdp_count):
        self.seq_count, self.fsdp_count = seq_count, fsdp_count
        self.seq, self.seq_peer = peers_of("seq", seq_count)
        self.fsdp, self.fsdp_peer = peers_of("fsdp", fsdp_count)
        self.square = fsdp_count == 4
        if self.square:
            row, place = self.fsdp // 2, self.fsdp % 2
            self.sides = (row * 2 + 1 - place, (1 - row) * 2 + place)
            self.corner = (1 - row) * 2 + 1 - place
        else:
            self.sides = tuple(self.fsdp_peer(step) for step in range(1, fsdp_count))

    def remote(self, src, dst, send, recv, seq, fsdp):
        return pltpu.make_async_remote_copy(
            src_ref=src,
            dst_ref=dst,
            send_sem=send,
            recv_sem=recv,
            device_id=(seq, fsdp),
            device_id_type=MESH,
        )


class Spread:
    def __init__(self, cross, group, stack, weights, row_send, row_recv, side_send, side_recv, half_send, half_recv):
        self.cross, self.group, self.stack, self.weights = cross, group, stack, weights
        self.row_send, self.row_recv = row_send, row_recv
        self.side_send, self.side_recv = side_send, side_recv
        self.half_send, self.half_recv = half_send, half_recv
        self.columns, self.rows = weights.shape[-1], weights.shape[-2]
        self.items = weights.shape[0] // group * cross.seq_count

    @staticmethod
    def scratch(kinds, group, seq_count, fsdp_count, rows, columns):
        dma = pltpu.SemaphoreType.DMA
        sides = 2 if fsdp_count == 4 else fsdp_count - 1
        items = kinds // group * seq_count
        return [
            pltpu.VMEM((kinds, rows, seq_count * columns), jnp.bfloat16),
            pltpu.VMEM((kinds, seq_count, fsdp_count, rows, columns), jnp.bfloat16),
            dma((kinds, seq_count)),
            dma((kinds, seq_count)),
            dma((items, sides)),
            dma((items, sides)),
            dma((items, 2)),
            dma((items, 2)),
        ]

    def block(self, owner):
        return pl.ds(pl.multiple_of(owner * self.columns, 128), self.columns)

    def row(self, kind, step):
        cross = self.cross
        peer = cross.seq_peer(step)
        return cross.remote(
            self.stack.at[kind, :, self.block(peer)],
            self.weights.at[kind, cross.seq, cross.fsdp],
            self.row_send.at[kind, step],
            self.row_recv.at[kind, step],
            peer,
            cross.fsdp,
        )

    def place(self, item):
        count = self.cross.seq_count
        step = item % count
        return item // count * self.group, step, (self.cross.seq - step + count) % count

    def side(self, item, side):
        cross = self.cross
        first, _, owner = self.place(item)
        ref = self.weights.at[pl.ds(first, self.group), owner, cross.fsdp]
        return cross.remote(
            ref,
            ref,
            self.side_send.at[item, side],
            self.side_recv.at[item, side],
            cross.seq,
            cross.sides[side],
        )

    def half(self, item, side):
        cross = self.cross
        first, _, owner = self.place(item)
        rows = pl.ds(side * (self.rows // 2), self.rows // 2)
        ref = self.weights.at[pl.ds(first, self.group), owner, cross.sides[side], rows]
        return cross.remote(
            ref,
            ref,
            self.half_send.at[item, side],
            self.half_recv.at[item, side],
            cross.seq,
            cross.sides[1 - side],
        )

    def send_rows(self, item):
        first, step, _ = self.place(item)

        @pl.when(step > 0)
        def _():
            for kind in range(self.group):
                self.row(first + kind, step).start()

    def take(self, item):
        cross = self.cross
        first, step, _ = self.place(item)

        @pl.when(step > 0)
        def _():
            for kind in range(self.group):
                self.row(first + kind, step).wait_recv()

        @pl.when(step == 0)
        def _():
            for kind in range(self.group):
                own = self.stack[first + kind, :, self.block(cross.seq)]
                self.weights[first + kind, cross.seq, cross.fsdp] = own

        self.pass_on(item)

    def pass_on(self, item):
        for side in range(len(self.cross.sides)):
            self.side(item, side).start()

    def relay(self, item):
        for side in range(len(self.cross.sides)):
            self.side(item, side).wait_recv()
            if self.cross.square:
                self.half(item, side).start()

    def settle(self, item):
        if self.cross.square:
            for side in range(2):
                self.half(item, side).wait_recv()

    def finish(self):
        cross = self.cross

        @pl.loop(0, self.items)
        def _(item):
            first, step, _ = self.place(item)

            @pl.when(step > 0)
            def _():
                for kind in range(self.group):
                    self.row(first + kind, step).wait_send()

            self.finish_item(item)

    def finish_item(self, item):
        for side in range(len(self.cross.sides)):
            self.side(item, side).wait_send()
            if self.cross.square:
                self.half(item, side).wait_send()


AHEAD = 2
LAG = 3
RING = 8


class Collect:
    def __init__(self, cross, kinds, fill, terms, side_in, half_out, half_in, row_out, row_in, side_send, side_recv, half_send, half_recv, row_send, row_recv):
        self.cross, self.fill, self.terms = cross, fill, terms
        self.side_in, self.half_out, self.half_in = side_in, half_out, half_in
        self.row_out, self.row_in = row_out, row_in
        self.side_send, self.side_recv = side_send, side_recv
        self.half_send, self.half_recv = half_send, half_recv
        self.row_send, self.row_recv = row_send, row_recv
        self.rows, self.columns = terms.shape[-2:]
        self.items = kinds * cross.seq_count

    @staticmethod
    def scratch(kinds, seq_count, fsdp_count, rows, columns):
        dma = pltpu.SemaphoreType.DMA
        vmem = pltpu.VMEM
        bf16 = jnp.bfloat16
        items = kinds * seq_count
        if fsdp_count == 4:
            arrays = [
                vmem((items, 2, 2, rows // 2, columns), bf16),
                vmem((RING, 2, rows // 2, columns), bf16),
                vmem((items, 2, rows // 2, columns), bf16),
            ]
            sides = (2, 2)
        else:
            arrays = [
                vmem((items, fsdp_count - 1, rows, columns), bf16),
                vmem((1, 1, 16, 128), bf16),
                vmem((1, 1, 16, 128), bf16),
            ]
            sides = (fsdp_count - 1, 1)
        return [vmem((RING, fsdp_count, rows, columns), bf16)] + arrays + [
            vmem((RING, rows, columns), bf16),
            vmem((items, rows, columns), bf16),
            dma((items,) + sides),
            dma((items,) + sides),
            dma((items, 2)),
            dma((items, 2)),
            dma((items,)),
            dma((items,)),
        ]

    def half_rows(self, side):
        return pl.ds(side * (self.rows // 2), self.rows // 2)

    def side(self, turn, side, which):
        cross = self.cross
        if not cross.square:
            return cross.remote(
                self.terms.at[turn % RING, cross.sides[side]],
                self.side_in.at[turn, side],
                self.side_send.at[turn, side, 0],
                self.side_recv.at[turn, side, 0],
                cross.seq,
                cross.sides[side],
            )
        target = cross.sides[side] if which == 0 else cross.corner
        return cross.remote(
            self.terms.at[turn % RING, target, self.half_rows(side)],
            self.side_in.at[turn, side, which],
            self.side_send.at[turn, side, which],
            self.side_recv.at[turn, side, which],
            cross.seq,
            cross.sides[side],
        )

    def half(self, turn, side):
        cross = self.cross
        return cross.remote(
            self.half_out.at[turn % RING, side],
            self.half_in.at[turn, side],
            self.half_send.at[turn, side],
            self.half_recv.at[turn, side],
            cross.seq,
            cross.sides[1 - side],
        )

    def row(self, turn):
        cross = self.cross
        return cross.remote(
            self.row_out.at[turn % RING],
            self.row_in.at[turn],
            self.row_send.at[turn],
            self.row_recv.at[turn],
            self.place(turn)[1],
            cross.fsdp,
        )

    def place(self, turn):
        count = self.cross.seq_count
        return turn // count, self.cross.seq_peer(turn % count + 1)

    def is_own(self, turn):
        return turn % self.cross.seq_count == self.cross.seq_count - 1

    @property
    def ways(self):
        return range(2) if self.cross.square else range(1)

    def sides(self, turn):
        return [
            self.side(turn, side, which)
            for which in reversed(self.ways)
            for side in range(len(self.cross.sides))
        ]

    def send(self, turn, first):
        if not first:

            @pl.when(turn >= RING)
            def _():
                for copy in self.sides(turn - RING):
                    copy.wait_send()

        kind, owner = self.place(turn)
        self.fill(kind, owner, turn % RING)
        for copy in self.sides(turn):
            copy.start()

    def middle(self, turn):
        if not self.cross.square:
            return
        cross = self.cross

        @pl.when(turn >= RING)
        def _():
            for side in range(2):
                self.half(turn - RING, side).wait_send()

        for side in range(2):
            self.side(turn, side, 1).wait_recv()
            mine = self.terms[turn % RING, cross.sides[1 - side], self.half_rows(side)]
            self.half_out[turn % RING, side] = (
                mine.astype(jnp.float32) + self.side_in[turn, side, 1].astype(jnp.float32)
            ).astype(jnp.bfloat16)
            self.half(turn, side).start()

    def totals(self, turn):
        cross = self.cross
        found = []
        if cross.square:
            for side in range(2):
                self.side(turn, side, 0).wait_recv()
                self.half(turn, side).wait_recv()
                rows = self.half_rows(side)
                total = self.terms[turn % RING, cross.fsdp, rows].astype(jnp.float32)
                total = total + self.side_in[turn, side, 0].astype(jnp.float32)
                total = total + self.half_in[turn, side].astype(jnp.float32)
                found.append((rows, total))
        else:
            total = self.terms[turn % RING, cross.fsdp].astype(jnp.float32)
            for side in range(len(cross.sides)):
                self.side(turn, side, 0).wait_recv()
                total = total + self.side_in[turn, side].astype(jnp.float32)
            found.append((pl.ds(0, self.rows), total))
        return found

    def ship(self, turn):
        own = self.is_own(turn)
        self.free_row(turn - RING)

        @pl.when(own)
        def _():
            for rows, total in self.totals(turn):
                self.row_in[turn, rows] = total.astype(jnp.bfloat16)

        @pl.when(jnp.logical_not(own))
        def _():
            for rows, total in self.totals(turn):
                self.row_out[turn % RING, rows] = total.astype(jnp.bfloat16)
            self.row(turn).start()

    def free_row(self, turn):
        @pl.when((turn >= 0) & jnp.logical_not(self.is_own(turn)))
        def _():
            self.row(turn).wait_send()

    def beat(self, turn):
        ahead = turn + AHEAD

        @pl.when(ahead < self.items)
        def _():
            self.send(ahead, False)

        @pl.when(turn < self.items)
        def _():
            self.middle(turn)

        @pl.when((turn >= LAG) & (turn < self.beats))
        def _():
            self.ship(turn - LAG)

    def begin(self):
        @pl.loop(0, min(AHEAD, self.items))
        def _(turn):
            self.send(turn, True)

    @property
    def beats(self):
        return self.items + LAG

    def receive(self, turn, put):
        count = self.cross.seq_count

        @pl.when(jnp.logical_not(self.is_own(turn)))
        def _():
            self.row(turn).wait_recv()

        sender = (self.cross.seq - turn % count - 1 + count) % count
        put(turn // count, sender, self.row_in[turn])

    def finish(self):
        cross = self.cross
        late = max(self.items - RING, 0)

        @pl.loop(late, self.items)
        def _(turn):
            for copy in self.sides(turn):
                copy.wait_send()
            if cross.square:
                for side in range(2):
                    self.half(turn, side).wait_send()
            self.free_row(turn)


def dot_rows(left, right, precision=None):
    return lax.dot_general(
        left,
        right,
        (((0,), (0,)), ((), ())),
        precision=precision,
        preferred_element_type=jnp.float32,
    )


EXACT = lax.Precision.HIGHEST


def turn_heads(tensor, cosine, sine):
    heads = [
        tensor[:, first : first + DH] * cosine
        + pltpu.roll(tensor[:, first : first + DH], DH // 2, 1) * sine
        for first in range(0, tensor.shape[1], DH)
    ]
    return jnp.concatenate(heads, axis=1) if len(heads) > 1 else heads[0]


def attention_weights(queries, keys, first_row, segment_column, segment_row):
    rows, count = queries.shape[0], keys.shape[0]
    scores = dot_cols(queries, keys) * DH ** (-0.5)
    query_place = first_row + lax.broadcasted_iota(jnp.int32, (rows, count), 0)
    key_place = lax.broadcasted_iota(jnp.int32, (rows, count), 1)
    allowed = (key_place <= query_place) & (segment_row == segment_column)
    scores = jnp.where(allowed, scores, neg_fill)
    expanded = jnp.exp(scores - jnp.max(scores, axis=-1, keepdims=True))
    return expanded / jnp.sum(expanded, axis=-1, keepdims=True)


class RowSum:
    def __init__(self, cross, local, every, send_sem, recv_sem):
        self.cross, self.local, self.every = cross, local, every
        self.send_sem, self.recv_sem = send_sem, recv_sem

    @staticmethod
    def scratch(seq_count, shape):
        dma = pltpu.SemaphoreType.DMA
        return [
            pltpu.VMEM(shape, jnp.float32),
            pltpu.VMEM((seq_count,) + shape, jnp.float32),
            dma((seq_count,)),
            dma((seq_count,)),
        ]

    def copy(self, step):
        cross = self.cross
        return cross.remote(
            self.local,
            self.every.at[step],
            self.send_sem.at[step],
            self.recv_sem.at[step],
            cross.seq_peer(step),
            cross.fsdp,
        )

    def send(self, value):
        self.local[...] = value
        for step in range(1, self.cross.seq_count):
            self.copy(step).start()

    def receive(self):
        total = self.local[...]
        for step in range(1, self.cross.seq_count):
            self.copy(step).wait_recv()
            total = total + self.every[step]
        return total

    def finish(self):
        for step in range(1, self.cross.seq_count):
            self.copy(step).wait_send()


def pick_row(row, shape):
    return jnp.where(lax.broadcasted_iota(jnp.int32, shape, 0) == row, 1.0, 0.0)


def product_terms(scatter, pairs, chip):
    _, rows, width = scatter.fresh.shape
    pair = pl.ds(chip * 2, 2)

    @pl.loop(0, width // tile_of(width))
    def _(tile):
        columns = pl.ds(pl.multiple_of(tile * tile_of(width), 128), tile_of(width))
        total = None
        for left, right, across in pairs:
            tokens = left[pair].reshape(2 * rows, -1)
            if across:
                term = dot_cols(tokens, right[columns, :])
            else:
                term = jnp.dot(tokens, right(columns), preferred_element_type=jnp.float32)
            total = term if total is None else total + term
        scatter.fresh[:, :, columns] = total.reshape(2, rows, -1)

    scatter.after_term(chip)


EARLY = 6
LEAD = 2
HOPPING = 1


def bring_in_kernel(chips, fsdp_count, *refs):
    inputs_ref, gains_ref, cosine_ref, sine_ref, segment_column, segment_row = refs[:6]
    sources, output_ref, refs = refs[6:12], refs[12], refs[13:]
    projected, inverse_out, own_gains, gains_out = refs[:4]
    inputs_out, attention_out, output_out, heads_out, pre_out = refs[4:9]
    units_out, outputs, gains, heads, pre, refs = refs[9:12], refs[12], refs[13], refs[14], refs[15], refs[16:]
    gain_row_send, gain_row_recv, gain_column_send, gain_column_recv = refs[:4]
    output_send, output_recv, load_sem, store_sem, refs = refs[4], refs[5], refs[6], refs[7], refs[8:]
    line = Line(chips)
    cross = Cross(2 * chips, fsdp_count)
    gather, refs = Gather(line, *refs[:5]), refs[5:]
    sums, refs = RowSum(cross, *refs[:4]), refs[4:]
    attention, refs = Spread(cross, 3, *refs[:8]), refs[8:]
    units, refs = Spread(cross, 1, *refs[:8]), refs[8:]
    scatter = Scatter(line, *refs)
    seq_count, seq, fsdp = cross.seq_count, cross.seq, cross.fsdp
    blocks = gather.blocks
    _, rows, width = blocks.shape
    columns = attention.columns
    tokens = seq_count * rows

    def gain_row(step):
        return cross.remote(
            gains_ref,
            gains.at[seq, fsdp],
            gain_row_send.at[step],
            gain_row_recv.at[step],
            cross.seq_peer(step),
            fsdp,
        )

    def gain_column(owner, step):
        ref = gains.at[owner, fsdp]
        return cross.remote(
            ref,
            ref,
            gain_column_send.at[owner, step],
            gain_column_recv.at[owner, step],
            seq,
            cross.fsdp_peer(step),
        )

    def output_copy(step):
        return cross.remote(
            output_ref,
            outputs.at[fsdp],
            output_send.at[step],
            output_recv.at[step],
            seq,
            cross.fsdp_peer(step),
        )

    stacks = [attention.stack.at[kind] for kind in range(3)]
    stacks += [units.stack.at[kind] for kind in range(3)]
    copies = load(
        [(source, stack, load_sem.at[i]) for i, (source, stack) in enumerate(zip(sources, stacks))]
    )
    greet_cross(seq_count, fsdp_count)
    for copy in copies:
        copy.wait()

    @pl.loop(0, attention.items)
    def _(item):
        attention.send_rows(item)

    for step in range(1, seq_count):
        gain_row(step).start()
    blocks[line.place * 2 + line.core] = inputs_ref[...]
    gather.send(line.place)

    @pl.loop(0, EARLY)
    def _(item):
        units.send_rows(item)

    gains[seq, fsdp] = gains_ref[...]
    outputs[fsdp] = output_ref[...]
    for step in range(1, fsdp_count):
        gain_column(seq, step).start()

    attention.take(0)

    @pl.loop(1, seq_count)
    def _(step):
        attention.take(step)
        gain_row(step).wait_recv()
        owner = (seq - step + seq_count) % seq_count
        for peer in range(1, fsdp_count):
            gain_column(owner, peer).start()
        attention.relay(step - 1)

    def project_inputs(step):
        chip = gather.step(step)
        pair = pl.ds(chip * 2, 2)
        whole = blocks[pair].reshape(2 * rows, width)
        for kind in range(3):
            weight = attention.weights[kind].reshape(width, columns)
            found = jnp.dot(whole, weight, preferred_element_type=jnp.float32)
            if kind < 2:
                pre[kind, pl.ds(chip * 2 * rows, 2 * rows)] = found
            else:
                heads[2, pair] = found.astype(jnp.bfloat16).reshape(2, rows, columns)

    def weights_arrived():
        attention.relay(seq_count - 1)
        for step in range(1, fsdp_count):
            output_copy(step).start()

        @pl.loop(0, seq_count)
        def _(item):
            attention.settle(item)
            for peer in range(1, fsdp_count):
                gain_column(item, peer).wait_recv()

        gains_out[...] = gains[...]
        lanes = gains.shape[-1]
        own = columns // fsdp_count
        lane = lax.broadcasted_iota(jnp.int32, (lanes, columns), 0)
        column = lax.broadcasted_iota(jnp.int32, (lanes, columns), 1)
        total = None
        for peer in range(fsdp_count):
            place = (column == lane + peer * own) & (lane < own)
            term = jnp.dot(
                gains[seq, peer],
                jnp.where(place, 1.0, 0.0).astype(jnp.bfloat16),
                preferred_element_type=jnp.float32,
            )
            total = term if total is None else total + term
        own_gains[...] = total
        project_inputs(0)

    def send_squares():
        total = None
        for kind in range(2):
            row = lax.dot_general(
                pick_row(kind, (8, columns)),
                pre[kind] * pre[kind],
                (((1,), (1,)), ((), ())),
                precision=EXACT,
                preferred_element_type=jnp.float32,
            )
            total = row if total is None else total + row
        sums.send(total)

    def make_heads():
        squares = sums.receive()
        for kind in range(2):
            mean = dot_rows(squares, pick_row(kind, (8, 128)), EXACT) / width
            inverse = lax.rsqrt(mean + eps_norm)
            inverse_out[:, kind : kind + 1] = inverse[:, :1]
            for first in range(0, columns, DH):
                part = pl.ds(first, DH)
                scaled = pre[kind, :, part] * inverse * own_gains[kind : kind + 1, part]
                turned = turn_heads(scaled, cosine_ref[...], sine_ref[...])
                heads[kind, :, :, part] = turned.astype(jnp.bfloat16).reshape(seq_count, rows, DH)

    def attend(step):
        chip = line.order(chips - 1 - step)

        @pl.loop(0, 2)
        def _(core):
            slot = chip * 2 + core
            first = pl.multiple_of(slot * rows, rows)
            for head in range(0, columns, DH):
                part = pl.ds(head, DH)
                probs = attention_weights(
                    heads[0, slot, :, part],
                    heads[1, :, :, part].reshape(tokens, DH),
                    first,
                    segment_column[pl.ds(first, rows), :],
                    segment_row[...],
                )
                heads[3, slot, :, part] = jnp.dot(
                    probs.astype(jnp.bfloat16),
                    heads[2, :, :, part].reshape(tokens, DH),
                    preferred_element_type=jnp.float32,
                ).astype(jnp.bfloat16)

        product_terms(
            scatter,
            [(heads.at[3], lambda part: outputs[:, :, part].reshape(columns, -1), False)],
            chip,
        )

    inputs_store = pltpu.make_async_copy(blocks, inputs_out, store_sem.at[0])
    attention_store = pltpu.make_async_copy(attention.weights, attention_out, store_sem.at[1])
    output_store = pltpu.make_async_copy(outputs, output_out, store_sem.at[2])
    heads_store = pltpu.make_async_copy(heads, heads_out, store_sem.at[3])
    pre_store = pltpu.make_async_copy(pre, pre_out, store_sem.at[4])

    def units_store(kind):
        return pltpu.make_async_copy(units.weights.at[kind], units_out[kind], store_sem.at[5 + kind])

    def settle_units(kind):
        @pl.loop(0, seq_count)
        def _(step):
            units.settle(kind * seq_count + step)

        units_store(kind).start()

    @pl.loop(0, LEAD)
    def _(item):
        units.take(item)

    arrived = 1
    after_gather = 4 * (chips - 1) - 1
    attending = after_gather + 3
    hopping = attending + chips
    beats = max(units.items + 1, hopping + 2 * chips)

    @pl.loop(0, beats)
    def _(beat):
        @pl.when(beat + EARLY < units.items)
        def _():
            units.send_rows(beat + EARLY)

        @pl.when(beat + LEAD < units.items)
        def _():
            units.take(beat + LEAD)

        @pl.when((beat > 0) & (beat <= units.items))
        def _():
            units.relay(beat - 1)

        @pl.when(beat == arrived)
        def _():
            weights_arrived()
            attention_store.start()

        @pl.when((beat % 4 == 2) & (beat // 4 + 1 < chips))
        def _():
            project_inputs(beat // 4 + 1)

        @pl.when(beat == after_gather)
        def _():
            inputs_store.start()
            pre_store.start()
            send_squares()
            for step in range(1, fsdp_count):
                output_copy(step).wait_recv()
            output_store.start()

        @pl.when(beat == after_gather + 2)
        def _():
            make_heads()

        @pl.when((beat >= attending) & (beat < attending + chips))
        def _():
            attend(beat - attending)

        for kind in range(2):

            @pl.when(beat == (kind + 1) * seq_count + 3)
            def _():
                settle_units(kind)

        @pl.when((beat >= hopping) & (beat < hopping + chips))
        def _():
            scatter.hop(chips - 1 - (beat - hopping))

    heads_store.start()
    scatter.settle(projected)
    settle_units(2)
    scatter.finish()
    gather.finish()
    sums.finish()
    attention.finish()
    units.finish()

    @pl.loop(1, seq_count)
    def _(step):
        gain_row(step).wait_send()

    @pl.loop(0, seq_count)
    def _(owner):
        for step in range(1, fsdp_count):
            gain_column(owner, step).wait_send()

    for step in range(1, fsdp_count):
        output_copy(step).wait_send()
    for store in (inputs_store, attention_store, output_store, heads_store, pre_store):
        store.wait()
    for kind in range(3):
        units_store(kind).wait()


def bring_in(local_in, attention_rows, unit_rows, output_weight, gains, tables, segment_row):
    rows, width = local_in.shape
    slots = lax.axis_size("seq")
    fsdp_count = lax.axis_size("fsdp")
    chips = slots // 2
    tokens = slots * rows
    own, columns = attention_rows[0].shape[0], attention_rows[0].shape[1] // slots
    units = unit_rows[0].shape[1] // slots
    bf16, f32, dma = jnp.bfloat16, jnp.float32, pltpu.SemaphoreType.DMA
    lanes = pl.cdiv(gains.shape[1], 128) * 128
    padded = jnp.pad(gains, ((0, 16 - gains.shape[0]), (0, lanes - gains.shape[1])))
    found = pl.pallas_call(
        functools.partial(bring_in_kernel, chips, fsdp_count),
        out_shape=(
            jax.ShapeDtypeStruct((rows, width), f32),
            jax.ShapeDtypeStruct((tokens, 8), f32),
            jax.ShapeDtypeStruct((16, columns), f32),
            jax.ShapeDtypeStruct((slots, fsdp_count, 16, lanes), bf16),
            jax.ShapeDtypeStruct((slots, rows, width), bf16),
            jax.ShapeDtypeStruct((3, slots, fsdp_count, own, columns), bf16),
            jax.ShapeDtypeStruct((fsdp_count, own, width), bf16),
            jax.ShapeDtypeStruct((4, slots, rows, columns), bf16),
            jax.ShapeDtypeStruct((2, tokens, columns), f32),
        )
        + (jax.ShapeDtypeStruct((slots, fsdp_count, own, units), bf16),) * 3,
        in_specs=[whole_spec()] * 6 + [far_spec()] * 6 + [whole_spec()],
        out_specs=(whole_spec(),) * 4 + (far_spec(),) * 8,
        scratch_shapes=[
            pltpu.VMEM((fsdp_count, own, width), bf16),
            pltpu.VMEM((slots, fsdp_count, 16, lanes), bf16),
            pltpu.VMEM((4, slots, rows, columns), bf16),
            pltpu.VMEM((2, tokens, columns), f32),
            dma((slots,)),
            dma((slots,)),
            dma((slots, fsdp_count)),
            dma((slots, fsdp_count)),
            dma((fsdp_count,)),
            dma((fsdp_count,)),
            dma((6,)),
            dma((8,)),
        ]
        + Gather.scratch(chips, rows, width)
        + RowSum.scratch(slots, (8, tokens))
        + Spread.scratch(3, 3, slots, fsdp_count, own, columns)
        + Spread.scratch(3, 1, slots, fsdp_count, own, units)
        + Scatter.scratch(chips, rows, width),
        compiler_params=line_params(3),
        name="bring_in",
    )(
        local_in,
        padded,
        *tables,
        segment_row.reshape(tokens, 1),
        segment_row.reshape(1, tokens),
        *attention_rows,
        *unit_rows,
        output_weight,
    )
    projected, inverse, own_gains, every_gain = found[:4]
    inputs_all, weights, outputs, heads, pre = found[4:9]
    every_gain = every_gain[:, :, : gains.shape[0], : gains.shape[1]]
    return (
        projected,
        inputs_all.reshape(-1, width),
        weights.reshape(3, -1, columns),
        outputs.reshape(-1, width),
        [columns_of.reshape(-1, units) for columns_of in found[9:]],
        heads.reshape(4, tokens, columns),
        pre,
        inverse,
        own_gains,
        every_gain.transpose(2, 0, 1, 3).reshape(gains.shape[0], -1),
    )


def gather_back_kernel(chips, fsdp_count, *refs):
    local_ref, output_ref, gains_ref, inverse_ref, cosine_ref, sine_ref = refs[:6]
    segment_column, segment_row = refs[6:8]
    hidden_hbm, gate_hbm, up_hbm, heads_hbm, pre_hbm = refs[8:13]
    refs = refs[13:]
    results, output_term, grads_out, gain_out = refs[:2], refs[2], refs[3], refs[4]
    refs = refs[5:]
    tokens, units, heads, pre, gathered, grad_query, grad_key, grad_value = refs[:8]
    load_sem, refs = refs[8], refs[9:]
    line = Line(chips)
    cross = Cross(2 * chips, fsdp_count)
    gather = Gather(line, *refs[:5])
    sums = RowSum(cross, *refs[5:9])
    all_tokens, width = tokens.shape
    block_units = units.shape[-1]
    columns = output_ref.shape[0]
    blocks = gather.blocks
    rows = blocks.shape[1]

    def fill(kind, owner, slot):
        span = width // cross.seq_count
        chosen = tokens[:, pl.ds(pl.multiple_of(owner * span, 128), span)]

        @pl.loop(0, block_units // tile_of(block_units))
        def _(tile):
            part = pl.ds(pl.multiple_of(tile * tile_of(block_units), 128), tile_of(block_units))
            term = dot_rows(chosen, units[kind, :, part]).astype(jnp.bfloat16)
            collect.terms[slot, :, :, part] = term.reshape(fsdp_count, -1, term.shape[1])

    collect = Collect(cross, 2, fill, *refs[9:])
    copies = load(
        [
            (hidden_hbm, tokens, load_sem.at[0]),
            (gate_hbm, units.at[0], load_sem.at[1]),
            (up_hbm, units.at[1], load_sem.at[2]),
            (heads_hbm, heads, load_sem.at[3]),
            (pre_hbm, pre, load_sem.at[4]),
        ]
    )
    greet_cross(cross.seq_count, fsdp_count)
    blocks[line.place * 2 + line.core] = local_ref[...]
    gather.send(line.place)
    grad_key[...] = jnp.zeros_like(grad_key)
    grad_value[...] = jnp.zeros_like(grad_value)
    for copy in copies[:2]:
        copy.wait()
    collect.begin()
    for copy in copies[2:]:
        copy.wait()

    def arrive(step):
        chip = gather.step(step)
        whole = blocks[pl.ds(chip * 2, 2)].reshape(2 * rows, width)
        found = dot_cols(whole, output_ref[...]).astype(jnp.bfloat16)
        gathered[pl.ds(chip * 2 * rows, 2 * rows), :] = found

    arrive(0)
    def attend(slot):
        first = pl.multiple_of(slot * rows, rows)
        span = pl.ds(first, rows)
        for head in range(0, columns, DH):
            part = pl.ds(head, DH)
            queries, keys, values = heads[0, span, part], heads[1, :, part], heads[2, :, part]
            outer = gathered[span, part]
            probs = attention_weights(
                queries, keys, first, segment_column[span, :], segment_row[...]
            )
            grad_value[:, part] += dot_rows(probs.astype(jnp.bfloat16), outer)
            grad_probs = dot_cols(outer, values)
            delta = jnp.sum(probs * grad_probs, axis=-1, keepdims=True)
            grad_scores = (probs * (grad_probs - delta)).astype(jnp.bfloat16)
            grad_query[span, part] = jnp.dot(
                grad_scores, keys, preferred_element_type=jnp.float32
            )
            grad_key[:, part] += dot_rows(grad_scores, queries)

    def errors(kind, grad):
        scaled = (grad[...] * DH ** (-0.5)).astype(jnp.bfloat16).astype(jnp.float32)
        error = turn_heads(scaled, cosine_ref[...], -sine_ref[...])
        inverse = inverse_ref[:, kind : kind + 1]
        return error, pre[kind] * inverse, inverse

    def send_means():
        total = None
        for kind, grad in enumerate((grad_query, grad_key)):
            error, unit, _ = errors(kind, grad)
            product = error * unit
            gain_out[kind : kind + 1, :] = jnp.sum(product, axis=0, keepdims=True)
            row = lax.dot_general(
                pick_row(kind, (8, columns)),
                product * gains_ref[kind : kind + 1, :],
                (((1,), (1,)), ((), ())),
                precision=EXACT,
                preferred_element_type=jnp.float32,
            )
            total = row if total is None else total + row
        sums.send(total)
        grads_out[2] = grad_value[...].astype(jnp.bfloat16)

        @pl.loop(0, width // tile_of(width))
        def _(tile):
            part = pl.ds(pl.multiple_of(tile * tile_of(width), 128), tile_of(width))
            outer = blocks[:, :, part].reshape(all_tokens, -1)
            output_term[:, part] = dot_rows(heads[3], outer).astype(jnp.bfloat16)

    def finish_grads():
        means = sums.receive() / width
        for kind, grad in enumerate((grad_query, grad_key)):
            error, unit, inverse = errors(kind, grad)
            mean = dot_rows(means, pick_row(kind, (8, 128)), EXACT)[:, :1]
            grads_out[kind] = (
                inverse * (error * gains_ref[kind : kind + 1, :] - unit * mean)
            ).astype(jnp.bfloat16)

    attended = 3 * chips - 1

    @pl.loop(0, max(collect.beats, attended + 4))
    def _(turn):
        collect.beat(turn)

        @pl.when((turn % 3 < 2) & (turn // 3 < chips))
        def _():
            attend(line.order(turn // 3) * 2 + turn % 3)

        @pl.when((turn % 3 == 2) & (turn // 3 + 1 < chips))
        def _():
            arrive(turn // 3 + 1)

        @pl.when(turn == attended)
        def _():
            send_means()

        @pl.when(turn == attended + 3)
        def _():
            finish_grads()

    @pl.loop(0, cross.seq_count)
    def _(turn):
        for kind in range(2):

            def put(_, sender, value):
                part = pl.ds(pl.multiple_of(sender * block_units, 128), block_units)
                results[kind][:, part] = value

            collect.receive(kind * cross.seq_count + turn, put)

    collect.finish()
    gather.finish()
    sums.finish()


def gather_back(local, output_rows, gains, inverse, tables, segment_row, far, heads, pre):
    rows, width = local.shape
    slots = lax.axis_size("seq")
    fsdp_count = lax.axis_size("fsdp")
    chips = slots // 2
    own = width // (slots * fsdp_count)
    units = far[1].shape[1]
    _, tokens, columns = heads.shape
    bf16, f32 = jnp.bfloat16, jnp.float32
    found = pl.pallas_call(
        functools.partial(gather_back_kernel, chips, fsdp_count),
        out_shape=(jax.ShapeDtypeStruct((own, units * slots), bf16),) * 2
        + (
            jax.ShapeDtypeStruct((columns, width), bf16),
            jax.ShapeDtypeStruct((3, tokens, columns), bf16),
            jax.ShapeDtypeStruct((8, columns), f32),
        ),
        in_specs=[whole_spec()] * 8 + [far_spec()] * 5,
        out_specs=(whole_spec(),) * 5,
        scratch_shapes=[
            pltpu.VMEM((tokens, width), bf16),
            pltpu.VMEM((2, tokens, units), bf16),
            pltpu.VMEM((4, tokens, columns), bf16),
            pltpu.VMEM((2, tokens, columns), f32),
            pltpu.VMEM((tokens, columns), bf16),
            pltpu.VMEM((tokens, columns), f32),
            pltpu.VMEM((tokens, columns), f32),
            pltpu.VMEM((tokens, columns), f32),
            pltpu.SemaphoreType.DMA((5,)),
        ]
        + Gather.scratch(chips, rows, width)
        + RowSum.scratch(slots, (8, tokens))
        + Collect.scratch(2, slots, fsdp_count, own, units),
        compiler_params=line_params(6),
        name="gather_back",
    )(
        local,
        output_rows,
        gains,
        inverse,
        *tables,
        segment_row.reshape(tokens, 1),
        segment_row.reshape(1, tokens),
        *far,
        heads,
        pre,
    )
    return found[:2], found[2], found[3], found[4]


def take_out_kernel(
    chips,
    fsdp_count,
    *refs,
):
    sources, output_ref, gains_ref, refs = refs[:3], refs[3], refs[4], refs[5:]
    result, weight_outs, output_out, gains_out, refs = refs[0], refs[1:4], refs[4], refs[5], refs[6:]
    output_in, gain_in, gain_out, gain_rows, refs = refs[0], refs[1], refs[2], refs[3], refs[4:]
    output_send, output_recv, gain_send, gain_recv, gain_row_send, gain_row_recv = refs[:6]
    grads_ref, rights, tokens_ref, load_sem, comm = *refs[6:10], refs[10:]
    line = Line(chips)
    cross = Cross(2 * chips, fsdp_count)
    seq_count, seq, fsdp = cross.seq_count, cross.seq, cross.fsdp
    scatter = Scatter(line, *comm[:-12])
    columns = rights.shape[-1]
    rows, width = scatter.fresh.shape[1:]

    def fill(kind, owner, slot):
        span = width // seq_count
        part = pl.ds(pl.multiple_of(owner * span, 128), span)
        chosen = tokens_ref[:, part]
        for kind in range(3):
            term = dot_rows(chosen, grads_ref[kind].reshape(-1, columns)).astype(jnp.bfloat16)
            collect.terms[slot, :, :, kind * columns : (kind + 1) * columns] = term.reshape(
                fsdp_count, -1, columns
            )

    collect = Collect(cross, 1, fill, *comm[-12:])

    def output_copy(step):
        peer = cross.fsdp_peer(step)
        return cross.remote(
            output_ref.at[peer],
            output_in.at[step],
            output_send.at[step],
            output_recv.at[step],
            seq,
            peer,
        )

    def gain_copy(step):
        peer = cross.fsdp_peer(step)
        return cross.remote(
            gains_ref.at[peer], gain_in.at[step], gain_send.at[step], gain_recv.at[step], seq, peer
        )

    def gain_row(step):
        peer = cross.seq_peer(step)
        return cross.remote(
            gain_out.at[peer],
            gain_rows.at[step],
            gain_row_send.at[step],
            gain_row_recv.at[step],
            peer,
            fsdp,
        )

    copies = load(
        [
            (source, target, load_sem.at[i])
            for i, (source, target) in enumerate(zip(sources, (grads_ref, rights, tokens_ref)))
        ]
    )
    greet_cross(seq_count, fsdp_count)
    for step in range(1, fsdp_count):
        gain_copy(step).start()

    for copy in copies:
        copy.wait()
    collect.begin()

    @pl.loop(0, chips)
    def _(step):
        product_terms(
            scatter,
            [(grads_ref.at[kind], rights.at[kind], True) for kind in range(3)],
            line.order(chips - 1 - step),
        )

    total = gains_ref[fsdp]
    for step in range(1, fsdp_count):
        gain_copy(step).wait_recv()
        total = total + gain_in[step]
    gain_out[...] = total
    for step in range(1, seq_count):
        gain_row(step).start()

    @pl.loop(0, collect.beats)
    def _(turn):
        collect.beat(turn)

        @pl.when(turn == seq_count - AHEAD)
        def _():
            for step in range(1, fsdp_count):
                output_copy(step).start()

        @pl.when((turn >= HOPPING) & (turn < HOPPING + chips))
        def _():
            scatter.hop(chips - 1 - (turn - HOPPING))

    total = output_ref[fsdp].astype(jnp.float32)
    for step in range(1, fsdp_count):
        output_copy(step).wait_recv()
        total = total + output_in[step].astype(jnp.float32)
    output_out[...] = total
    scatter.settle(result)
    total = gain_out[seq]
    for step in range(1, seq_count):
        gain_row(step).wait_recv()
        total = total + gain_rows[step]
    gains_out[...] = total

    def put(_, sender, value):
        block = pl.ds(pl.multiple_of(sender * columns, 128), columns)
        for kind in range(3):
            weight_outs[kind][:, block] = value[:, kind * columns : (kind + 1) * columns]

    @pl.loop(0, seq_count)
    def _(turn):
        collect.receive(turn, put)

    scatter.finish()
    collect.finish()

    @pl.loop(1, seq_count)
    def _(step):
        gain_row(step).wait_send()

    for step in range(1, fsdp_count):
        output_copy(step).wait_send()
        gain_copy(step).wait_send()


def take_out(grads, weights, tokens, output_term, gain_terms):
    slots = lax.axis_size("seq")
    fsdp_count = lax.axis_size("fsdp")
    chips = slots // 2
    _, width, columns = weights.shape
    rows = tokens.shape[0] // slots
    own = width // (slots * fsdp_count)
    kinds = gain_terms.shape[0]
    bf16, f32, dma = jnp.bfloat16, jnp.float32, pltpu.SemaphoreType.DMA
    gains = gain_terms.reshape(kinds, slots, fsdp_count, own).transpose(2, 1, 0, 3)
    lanes = pl.cdiv(own, 128) * 128
    gains = jnp.pad(gains, ((0, 0), (0, 0), (0, 8 - kinds), (0, lanes - own)))
    result, query, key, value, output, gains = pl.pallas_call(
        functools.partial(take_out_kernel, chips, fsdp_count),
        out_shape=(jax.ShapeDtypeStruct((rows, width), f32),)
        + (jax.ShapeDtypeStruct((own, columns * slots), bf16),) * 3
        + (jax.ShapeDtypeStruct((own, width), f32), jax.ShapeDtypeStruct((8, lanes), f32)),
        in_specs=[far_spec()] * 3 + [whole_spec()] * 2,
        out_specs=(whole_spec(),) * 6,
        scratch_shapes=[
            pltpu.VMEM((fsdp_count, own, width), bf16),
            pltpu.VMEM((fsdp_count, slots, 8, lanes), f32),
            pltpu.VMEM((slots, 8, lanes), f32),
            pltpu.VMEM((slots, 8, lanes), f32),
            dma((fsdp_count,)),
            dma((fsdp_count,)),
            dma((fsdp_count,)),
            dma((fsdp_count,)),
            dma((slots,)),
            dma((slots,)),
            pltpu.VMEM((3, slots, rows, columns), bf16),
            pltpu.VMEM((3, width, columns), bf16),
            pltpu.VMEM((slots * rows, width), bf16),
            dma((3,)),
        ]
        + Scatter.scratch(chips, rows, width)
        + Collect.scratch(1, slots, fsdp_count, own, 3 * columns),
        compiler_params=line_params(4),
        name="take_out",
    )(
        grads.reshape(3, slots, rows, columns),
        weights,
        tokens,
        output_term.reshape(fsdp_count, own, width),
        gains,
    )
    return result, (query, key, value), output, gains[:kinds, :own]


def feed_forward_kernel(
    chips,
    projected_ref,
    inputs_ref,
    gate_hbm,
    up_hbm,
    down_hbm,
    cotangent_ref,
    gains_ref,
    result_ref,
    grad_ref,
    gain_grad_ref,
    gate_out,
    up_out,
    act_out,
    all_out,
    gate_w,
    up_w,
    down_w,
    gate_keep,
    up_keep,
    act_keep,
    load_sem,
    store_sem,
    mixed_ref,
    stream_ref,
    *comm,
):
    line = Line(chips)
    gather = Gather(line, *comm[:5])
    scatter = Scatter(line, *comm[5:])
    blocks, fresh = gather.blocks, scatter.fresh
    _, rows, width = blocks.shape
    units = gate_w.shape[1]
    copies = load(
        [
            (gate_hbm, gate_w, load_sem.at[0]),
            (up_hbm, up_w, load_sem.at[1]),
            (down_hbm, down_w, load_sem.at[2]),
        ]
    )
    part_rows = min(32, rows)
    own_slot = line.place * 2 + line.core

    @pl.loop(0, rows // part_rows)
    def _(part):
        span = pl.ds(pl.multiple_of(part * part_rows, part_rows), part_rows)
        value = projected_ref[span]
        inverse = lax.rsqrt(jnp.mean(value * value, axis=-1, keepdims=True) + eps_norm)
        stream = inputs_ref[span].astype(jnp.float32) + value * inverse * gains_ref[0:1]
        stream_ref[span] = stream
        blocks[own_slot, span] = stream.astype(jnp.bfloat16)

    line.greet()
    gather.send(line.place)

    def stores(chip):
        pair = pl.ds(chip * 2, 2)
        return [
            pltpu.make_async_copy(gate_keep.at[pair], gate_out.at[pair], store_sem.at[0, chip]),
            pltpu.make_async_copy(up_keep.at[pair], up_out.at[pair], store_sem.at[1, chip]),
            pltpu.make_async_copy(act_keep.at[pair], act_out.at[pair], store_sem.at[2, chip]),
            pltpu.make_async_copy(blocks.at[pair], all_out.at[pair], store_sem.at[3, chip]),
        ]

    for copy in copies:
        copy.wait()

    @pl.loop(0, chips)
    def _(step):
        chip = gather.step(step)
        pair = pl.ds(chip * 2, 2)

        @pl.loop(0, units // tile_of(units))
        def _(tile):
            columns = pl.ds(pl.multiple_of(tile * tile_of(units), 128), tile_of(units))
            tokens = blocks[pair].reshape(2 * rows, width)
            gate = jnp.dot(tokens, gate_w[:, columns], preferred_element_type=jnp.float32)
            up = jnp.dot(tokens, up_w[:, columns], preferred_element_type=jnp.float32)
            gate_keep[pair, :, columns] = gate.reshape(2, rows, -1)
            up_keep[pair, :, columns] = up.reshape(2, rows, -1)
            act_keep[pair, :, columns] = (
                (gate / (1.0 + jnp.exp(-gate)) * up).astype(jnp.bfloat16).reshape(2, rows, -1)
            )

        @pl.loop(0, width // tile_of(width))
        def _(tile):
            columns = pl.ds(pl.multiple_of(tile * tile_of(width), 128), tile_of(width))
            act = act_keep[pair].reshape(2 * rows, units)
            fresh[:, :, columns] = dot_cols(act, down_w[columns, :]).reshape(2, rows, -1)

        for copy in stores(chip):
            copy.start()
        scatter.after_term(chip)

    scatter.hops()
    scatter.settle(mixed_ref)
    gain_grad_ref[...] = jnp.zeros_like(gain_grad_ref)

    @pl.loop(0, rows // part_rows)
    def _(part):
        span = pl.ds(pl.multiple_of(part * part_rows, part_rows), part_rows)
        mixed, outer, gain = mixed_ref[span], cotangent_ref[span].astype(jnp.float32), gains_ref[1:2]
        inverse = lax.rsqrt(jnp.mean(mixed * mixed, axis=-1, keepdims=True) + eps_norm)
        unit = mixed * inverse
        result_ref[span] = (stream_ref[span] + unit * gain).astype(jnp.bfloat16)
        gain_grad_ref[0:1] += jnp.sum(outer * unit, axis=0, keepdims=True)
        outer = outer * gain
        mean = jnp.mean(outer * unit, axis=-1, keepdims=True)
        grad_ref[span] = (inverse * (outer - unit * mean)).astype(jnp.bfloat16)

    scatter.finish()
    gather.finish()

    @pl.loop(0, chips)
    def _(chip):
        for copy in stores(chip):
            copy.wait()


def feed_forward(projected, inputs, gate_cols, up_cols, down_cols, cotangent, gains):
    rows, width = projected.shape
    units = gate_cols.shape[1]
    slots = lax.axis_size("seq")
    chips = slots // 2
    weights = [pltpu.VMEM((width, units), jnp.bfloat16)] * 3
    result, grad, gain_grad, gate, up, act, every = pl.pallas_call(
        functools.partial(feed_forward_kernel, chips),
        out_shape=(
            jax.ShapeDtypeStruct((rows, width), jnp.bfloat16),
            jax.ShapeDtypeStruct((rows, width), jnp.bfloat16),
            jax.ShapeDtypeStruct((8, width), jnp.float32),
            jax.ShapeDtypeStruct((slots, rows, units), jnp.float32),
            jax.ShapeDtypeStruct((slots, rows, units), jnp.float32),
            jax.ShapeDtypeStruct((slots, rows, units), jnp.bfloat16),
            jax.ShapeDtypeStruct((slots, rows, width), jnp.bfloat16),
        ),
        in_specs=[whole_spec()] * 2 + [far_spec()] * 3 + [whole_spec()] * 2,
        out_specs=(whole_spec(),) * 3 + (far_spec(),) * 4,
        scratch_shapes=weights
        + [
            pltpu.VMEM((slots, rows, units), jnp.float32),
            pltpu.VMEM((slots, rows, units), jnp.float32),
            pltpu.VMEM((slots, rows, units), jnp.bfloat16),
            pltpu.SemaphoreType.DMA((3,)),
            pltpu.SemaphoreType.DMA((4, chips)),
            pltpu.VMEM((rows, width), jnp.float32),
            pltpu.VMEM((rows, width), jnp.float32),
        ]
        + Gather.scratch(chips, rows, width)
        + Scatter.scratch(chips, rows, width),
        compiler_params=line_params(1),
        name="feed_forward",
    )(projected, inputs, gate_cols, up_cols, down_cols, cotangent, gains)
    return (
        result,
        grad,
        gain_grad[0],
        gate,
        up,
        act.reshape(-1, units),
        every.reshape(-1, width),
    )


def feed_forward_back_kernel(chips, fsdp_count, *refs):
    grad_ref, gate_hbm, up_hbm, down_hbm, gate_lin_hbm, up_lin_hbm, act_hbm = refs[:7]
    hidden_grad_ref, gate_out, up_out, down_grad, refs = *refs[7:11], refs[11:]
    gate_w, up_w, down_w, gate_lin, up_lin, gate_keep, up_keep, act, refs = *refs[:8], refs[8:]
    load_sem, store_sem, refs = refs[0], refs[1], refs[2:]
    line = Line(chips)
    cross = Cross(2 * chips, fsdp_count)
    gather = Gather(line, *refs[:5])
    scatter = Scatter(line, *refs[5:15])
    blocks, fresh = gather.blocks, scatter.fresh
    _, rows, width = blocks.shape
    units = gate_w.shape[1]
    all_tokens = cross.seq_count * rows

    def fill(kind, owner, slot):
        span = width // cross.seq_count
        part = pl.ds(pl.multiple_of(owner * span, 128), span)
        chosen = blocks[:, :, part].reshape(all_tokens, span)

        @pl.loop(0, units // tile_of(units))
        def _(tile):
            columns = pl.ds(pl.multiple_of(tile * tile_of(units), 128), tile_of(units))
            term = dot_rows(chosen, act[:, columns]).astype(jnp.bfloat16)
            collect.terms[slot, :, :, columns] = term.reshape(fsdp_count, -1, term.shape[1])

    collect = Collect(cross, 1, fill, *refs[15:])
    copies = load(
        [
            (down_hbm, down_w, load_sem.at[0]),
            (gate_lin_hbm, gate_lin, load_sem.at[1]),
            (up_lin_hbm, up_lin, load_sem.at[2]),
            (gate_hbm, gate_w, load_sem.at[3]),
            (up_hbm, up_w, load_sem.at[4]),
            (act_hbm, act, load_sem.at[5]),
        ]
    )
    greet_cross(cross.seq_count, fsdp_count)
    blocks[line.place * 2 + line.core] = grad_ref[...]
    gather.send(line.place)

    def stores(chip):
        pair = pl.ds(chip * 2, 2)
        return [
            pltpu.make_async_copy(gate_keep.at[pair], gate_out.at[pair], store_sem.at[0, chip]),
            pltpu.make_async_copy(up_keep.at[pair], up_out.at[pair], store_sem.at[1, chip]),
        ]

    for copy in copies:
        copy.wait()

    @pl.loop(0, chips)
    def _(step):
        chip = gather.step(step)
        pair = pl.ds(chip * 2, 2)

        @pl.loop(0, units // tile_of(units))
        def _(tile):
            columns = pl.ds(pl.multiple_of(tile * tile_of(units), 128), tile_of(units))
            tokens = blocks[pair].reshape(2 * rows, width)
            grad = jnp.dot(tokens, down_w[:, columns], preferred_element_type=jnp.float32)
            gate = gate_lin[pair, :, columns].reshape(2 * rows, -1)
            up = up_lin[pair, :, columns].reshape(2 * rows, -1)
            sig = 1.0 / (1.0 + jnp.exp(-gate))
            gate_keep[pair, :, columns] = (
                (grad * up * sig * (1.0 + gate * (1.0 - sig)))
                .astype(jnp.bfloat16)
                .reshape(2, rows, -1)
            )
            up_keep[pair, :, columns] = (
                (grad * (gate * sig)).astype(jnp.bfloat16).reshape(2, rows, -1)
            )

        @pl.loop(0, width // tile_of(width))
        def _(tile):
            columns = pl.ds(pl.multiple_of(tile * tile_of(width), 128), tile_of(width))
            gate = gate_keep[pair].reshape(2 * rows, units)
            up = up_keep[pair].reshape(2 * rows, units)
            fresh[:, :, columns] = (
                dot_cols(gate, gate_w[columns, :]) + dot_cols(up, up_w[columns, :])
            ).reshape(2, rows, -1)

        for copy in stores(chip):
            copy.start()
        scatter.after_term(chip)

    collect.begin()

    @pl.loop(0, collect.beats)
    def _(turn):
        collect.beat(turn)

        @pl.when(turn < chips)
        def _():
            scatter.hop(turn)

    scatter.settle(hidden_grad_ref)

    def put(_, sender, value):
        columns = pl.ds(pl.multiple_of(sender * units, 128), units)
        down_grad[:, columns] = value

    @pl.loop(0, cross.seq_count)
    def _(turn):
        collect.receive(turn, put)

    scatter.finish()
    gather.finish()
    collect.finish()

    @pl.loop(0, chips)
    def _(chip):
        for copy in stores(chip):
            copy.wait()


def feed_forward_back(grad_low, gate_cols, up_cols, down_cols, gate, up, act):
    rows, width = grad_low.shape
    units = gate_cols.shape[1]
    slots = lax.axis_size("seq")
    fsdp_count = lax.axis_size("fsdp")
    chips = slots // 2
    own = width // (slots * fsdp_count)
    bf16, f32 = jnp.bfloat16, jnp.float32
    hidden_grad, gate_grad, up_grad, down_grad = pl.pallas_call(
        functools.partial(feed_forward_back_kernel, chips, fsdp_count),
        out_shape=(
            jax.ShapeDtypeStruct((rows, width), f32),
            jax.ShapeDtypeStruct((slots, rows, units), bf16),
            jax.ShapeDtypeStruct((slots, rows, units), bf16),
            jax.ShapeDtypeStruct((own, units * slots), bf16),
        ),
        in_specs=[whole_spec()] + [far_spec()] * 6,
        out_specs=(whole_spec(), far_spec(), far_spec(), whole_spec()),
        scratch_shapes=[pltpu.VMEM((width, units), bf16)] * 3
        + [
            pltpu.VMEM((slots, rows, units), f32),
            pltpu.VMEM((slots, rows, units), f32),
            pltpu.VMEM((slots, rows, units), bf16),
            pltpu.VMEM((slots, rows, units), bf16),
            pltpu.VMEM((slots * rows, units), bf16),
            pltpu.SemaphoreType.DMA((6,)),
            pltpu.SemaphoreType.DMA((2, chips)),
        ]
        + Gather.scratch(chips, rows, width)
        + Scatter.scratch(chips, rows, width)
        + Collect.scratch(1, slots, fsdp_count, own, units),
        compiler_params=line_params(2),
        name="feed_forward_back",
    )(grad_low, gate_cols, up_cols, down_cols, gate, up, act)
    return hidden_grad, gate_grad.reshape(-1, units), up_grad.reshape(-1, units), down_grad


def rope_tables(row_count):
    half_width = DH // 2
    frequency = rope_base ** (-jnp.arange(half_width, dtype=jnp.float32) * 2.0 / DH)
    angles = jnp.arange(row_count, dtype=jnp.int32).astype(jnp.float32)[:, None] * frequency[None, :]
    cosine, sine = jnp.cos(angles), jnp.sin(angles)
    return (
        jnp.concatenate([cosine, cosine], axis=1),
        jnp.concatenate([-sine, sine], axis=1),
    )


def per_device(
    inputs,
    query_weight,
    key_weight,
    value_weight,
    output_weight,
    query_gain,
    key_gain,
    attention_gain,
    gate_weight,
    up_weight,
    down_weight,
    feedforward_gain,
    segments,
    cotangent,
):
    token_count = inputs.shape[1]
    width_all = inputs.shape[2]
    local_in = inputs.reshape(token_count, width_all)
    segment_row = segments[0]
    seq_index = lax.axis_index("seq")
    tables = rope_tables(segment_row.shape[0])
    (
        projected,
        inputs_all,
        attention_cols,
        output_rows,
        unit_cols,
        heads,
        pre,
        inverse,
        own_gains,
        gains,
    ) = bring_in(
        local_in,
        [query_weight, key_weight, value_weight],
        [gate_weight, up_weight, down_weight],
        output_weight,
        jnp.stack([query_gain, key_gain, attention_gain, feedforward_gain]),
        tables,
        segment_row,
    )
    gate_cols, up_cols, down_cols = unit_cols
    head_width = heads.shape[2]
    gains = gains.astype(jnp.float32)
    attention_scale = gains[2]
    grad_result = cotangent.reshape(token_count, width_all)
    result, grad_mixed_low, grad_feedforward_gain, gate_linear, up_linear, activated, hidden_all = (
        feed_forward(
            projected, local_in, gate_cols, up_cols, down_cols, grad_result, gains[2:4]
        )
    )
    result = result.reshape(1, token_count, width_all)
    hidden_term, grad_gate_low, grad_upward_low, down_weight_grad = feed_forward_back(
        grad_mixed_low, gate_cols, up_cols, down_cols, gate_linear, up_linear, activated
    )
    grad_hidden = grad_result.astype(jnp.float32) + hidden_term
    _, branch_pull = jax.vjp(rms_scale, projected, attention_scale)
    grad_projected, grad_attention_gain = branch_pull(grad_hidden)
    weight_grads, output_term, attention_grads, gain_rows = gather_back(
        grad_projected.astype(jnp.bfloat16),
        output_rows,
        own_gains,
        inverse,
        tables,
        segment_row,
        [hidden_all, grad_gate_low, grad_upward_low],
        heads,
        pre,
    )
    gate_weight_grad, up_weight_grad = weight_grads
    head_gains = lax.dynamic_update_slice_in_dim(
        jnp.zeros((2, width_all), jnp.float32),
        gain_rows[:2],
        seq_index * head_width,
        1,
    )
    gain_terms = jnp.concatenate(
        [head_gains, jnp.stack([grad_attention_gain, grad_feedforward_gain])], axis=0
    )
    input_term, projection_grads, output_weight_grad, gain_grads = take_out(
        attention_grads, attention_cols, inputs_all, output_term, gain_terms
    )
    query_weight_grad, key_weight_grad, value_weight_grad = projection_grads
    grad_input = grad_hidden + input_term
    return (
        result,
        grad_input.reshape(1, token_count, width_all),
        query_weight_grad.astype(jnp.float32),
        key_weight_grad.astype(jnp.float32),
        value_weight_grad.astype(jnp.float32),
        output_weight_grad,
        gain_grads[0],
        gain_grads[1],
        gain_grads[2],
        gate_weight_grad.astype(jnp.float32),
        up_weight_grad.astype(jnp.float32),
        down_weight_grad.astype(jnp.float32),
        gain_grads[3],
    )


def solution(mesh):
    in_specs = (
        P("fsdp", "seq", None),
        P(("seq", "fsdp"), None),
        P(("seq", "fsdp"), None),
        P(("seq", "fsdp"), None),
        P(("seq", "fsdp"), None),
        P(("seq", "fsdp")),
        P(("seq", "fsdp")),
        P(("seq", "fsdp")),
        P(("seq", "fsdp"), None),
        P(("seq", "fsdp"), None),
        P(("seq", "fsdp"), None),
        P(("seq", "fsdp")),
        P("fsdp", None),
        P("fsdp", "seq", None),
    )
    out_specs = (
        P("fsdp", "seq", None),
        P("fsdp", "seq", None),
        P(("seq", "fsdp"), None),
        P(("seq", "fsdp"), None),
        P(("seq", "fsdp"), None),
        P(("seq", "fsdp"), None),
        P(("seq", "fsdp")),
        P(("seq", "fsdp")),
        P(("seq", "fsdp")),
        P(("seq", "fsdp"), None),
        P(("seq", "fsdp"), None),
        P(("seq", "fsdp"), None),
        P(("seq", "fsdp")),
    )
    return jax.shard_map(
        per_device, mesh=mesh, in_specs=in_specs, out_specs=out_specs, check_vma=False
    )
```
